64 devices in a mesh: rep: 8 (over x, y, core), dp: 8 (over z).
Axes of the slice: x: 2, y: 2, z: 8, core: 2. Of those that a mesh axis runs over, the one named last changes fastest.
The devices are a block of a 4x4x8 slice.
Arguments:
- x: bfloat16 [64, 2048, 512], P(('rep', 'dp')), parts along dimension 0
- dy: bfloat16 [64, 2048, 512], P(('rep', 'dp')), parts along dimension 0
- w_gate: bfloat16 [2, 512, 3072], replicated
- w_up: bfloat16 [2, 512, 3072], replicated
- w_down: bfloat16 [2, 3072, 512], replicated
- m_w_gate: float32 [2, 512, 3072], P(None, 'dp')
- m_w_up: float32 [2, 512, 3072], P(None, 'dp')
- m_w_down: float32 [2, 3072, 512], P(None, 'dp')
- v_w_gate: float32 [2, 512, 3072], P(None, 'dp')
- v_w_up: float32 [2, 512, 3072], P(None, 'dp')
- v_w_down: float32 [2, 3072, 512], P(None, 'dp')
Outputs:
- output 1: bfloat16 [16, 512, 3072], P('rep'), parts along dimension 0
- output 2: bfloat16 [16, 512, 3072], P('rep'), parts along dimension 0
- output 3: bfloat16 [16, 3072, 512], P('rep'), parts along dimension 0
- output 4: float32 [16, 512, 3072], P('rep', 'dp'), parts along dimension 0
- output 5: float32 [16, 512, 3072], P('rep', 'dp'), parts along dimension 0
- output 6: float32 [16, 3072, 512], P('rep', 'dp'), parts along dimension 0
- output 7: float32 [16, 512, 3072], P('rep', 'dp'), parts along dimension 0
- output 8: float32 [16, 512, 3072], P('rep', 'dp'), parts along dimension 0
- output 9: float32 [16, 3072, 512], P('rep', 'dp'), parts along dimension 0
There are 8 independent parts. The reference program is written for one: setup_inputs(seed, part) draws one part's arguments, and reference() takes and returns one part's arrays. A program takes and returns all parts, laid end to end along the dimension named above; an argument that names none is the same for every part.
All inputs are finite; a program needn't handle non-finite values.
Results may differ from the reference program's by a relative error of at most 0.022.
Values are sent between devices in bfloat16 or wider.
A program may use at most 768 MiB of HBM per device.

```python
import jax
import jax.numpy as jnp
from jax import lax

SEQUENCES = 8
TOKENS = 2048
D = 512
FF = 3072
LAYERS = 2
NAMES = ("w_gate", "w_up", "w_down")
SHAPES = {"w_gate": (LAYERS, D, FF), "w_up": (LAYERS, D, FF), "w_down": (LAYERS, FF, D)}


def bump(key, n, height):
    away = (jnp.arange(n, dtype=jnp.int32) - jax.random.randint(key, (), 0, n, jnp.int32)) % n
    return jnp.where(away < n // 8, height, 1.0)


def together(key, own, strength):
    shared = jax.random.normal(key, own.shape[1:], jnp.float32)
    return (own + strength * shared) * lax.rsqrt(1 + strength * strength)


def setup_inputs(seed: int = 0, part: int = 0) -> dict:
    kx, kdy, ka, kb, kz, kf, kh, kl, *keys = jax.random.split(jax.random.key(seed), 8 + 3 * len(NAMES))
    kx, kdy, ka, kb = (jax.random.fold_in(k, part) for k in (kx, kdy, ka, kb))
    kw, km, kv = (keys[i::3] for i in range(3))
    shape = (SEQUENCES, TOKENS, D)
    much_x, much_dy = jax.random.uniform(kz, (2,), jnp.float32, 0.0, 1.0)
    loud = 2.0 ** jax.random.uniform(jax.random.fold_in(kz, 1), (), jnp.float32, -1.0, 2.0)
    layers = 2.0 ** jax.random.uniform(kl, (LAYERS, 1, 1), jnp.float32, -1.0, 1.0)
    x = together(ka, jax.random.normal(kx, shape, jnp.float32), much_x) * bump(kf, D, 4.0)
    dy = together(kb, jax.random.normal(kdy, shape, jnp.float32), much_dy)
    drawn = {"x": x.astype(jnp.bfloat16), "dy": (loud * dy * (SEQUENCES * TOKENS) ** -0.5).astype(jnp.bfloat16)}
    for key, name in zip(kw, NAMES, strict=True):
        w = jax.random.normal(key, SHAPES[name], jnp.float32) * SHAPES[name][1] ** -0.5
        drawn[name] = (w * {"w_gate": 1.0, "w_up": bump(kh, FF, 4.0), "w_down": layers}[name]).astype(jnp.bfloat16)
    for key, name in zip(km, NAMES, strict=True):
        drawn[f"m_{name}"] = 0.1 * jax.random.normal(key, SHAPES[name], jnp.float32)
    for key, name in zip(kv, NAMES, strict=True):
        drawn[f"v_{name}"] = jax.random.uniform(key, SHAPES[name], jnp.float32, 0.005, 0.015)
    return drawn


def matmul(a, w):
    return jnp.dot(a, w, preferred_element_type=jnp.float32).astype(jnp.bfloat16)


def normed(h):
    wide = h.astype(jnp.float32)
    scale = lax.rsqrt(jnp.mean(wide**2, -1, keepdims=True) + 1e-6)
    return (wide * scale).astype(jnp.bfloat16)


def layer(h, w):
    a = normed(h)
    gate = jnp.dot(a, w["w_gate"], preferred_element_type=jnp.float32)
    up = jnp.dot(a, w["w_up"], preferred_element_type=jnp.float32)
    return h + matmul((jax.nn.silu(gate) * up).astype(jnp.bfloat16), w["w_down"])


def adamw(w, m, v, g):
    m = 0.9 * m + 0.1 * g
    v = 0.95 * v + 0.05 * g * g
    step = m * lax.rsqrt(v + 1e-8) + 0.1 * w
    return (w - 0.02 * step).astype(jnp.bfloat16), m, v


def clipped(gradients, sum_of_squares, count):
    factor = jnp.minimum(1.0, 0.5 * lax.rsqrt(sum_of_squares / count + 1e-30))
    return [g * factor for g in gradients]


def stack(weights, h):
    return lax.scan(lambda h, w: (layer(h, w), None), h, weights)[0]


def reference(x, dy, w_gate, w_up, w_down, m_w_gate, m_w_up, m_w_down, v_w_gate, v_w_up, v_w_down):
    weights = dict(zip(NAMES, (w_gate, w_up, w_down), strict=True))

    def take(so_far, sequence):
        h, by_y = sequence
        _, back = jax.vjp(lambda w: stack(w, h), weights)
        return jax.tree.map(lambda total, term: total + term.astype(jnp.float32), so_far, back(by_y)[0]), None

    none_yet = {name: jnp.zeros(w.shape, jnp.float32) for name, w in weights.items()}
    by_weights, _ = lax.scan(take, none_yet, (x, dy))
    gradients = [by_weights[name].astype(jnp.bfloat16).astype(jnp.float32) for name in NAMES]
    gradients = clipped(gradients, sum(jnp.sum(g * g) for g in gradients), sum(g.size for g in gradients))
    new = [
        adamw(w.astype(jnp.float32), m, v, g)
        for w, m, v, g in zip((w_gate, w_up, w_down), (m_w_gate, m_w_up, m_w_down), (v_w_gate, v_w_up, v_w_down), gradients, strict=True)
    ]
    return tuple(one[which] for which in range(3) for one in new)
```

```python
import functools

import jax
import jax.numpy as jnp
from jax import lax
from jax.experimental import pallas as pl
from jax.experimental.pallas import tpu as pltpu
from jax.sharding import PartitionSpec as P

F32 = jnp.float32
BF16 = jnp.bfloat16
MESH = pl.DeviceIdType.MESH
LANES = 128
VMEM_LIMIT = 67043328


def dot(a, b):
    return jnp.dot(a, b, preferred_element_type=F32)


def dot_t(a, b):
    return lax.dot_general(a, b, (((1,), (1,)), ((), ())), preferred_element_type=F32)


def scale_of(wide):
    return lax.rsqrt(jnp.mean(wide * wide, -1, keepdims=True) + 1e-6)


def loop(count, body):
    lax.fori_loop(0, count, lambda i, c: (body(i), c)[1], 0)


def at(i, size):
    return pl.ds(pl.multiple_of(i * size, size), size)


def grad_kernel(n, layers, shapes, *refs):
    (x_hbm, dy_hbm, wg_hbm, wu_hbm, wd_hbm) = refs[:5]
    (og_hbm, ou_hbm, od_hbm, sq_hbm) = refs[5:9]
    (A, AT, D, DT, H, ACT, DG, DU, DA, WG, WU, WD, G, RU, RD, OG, OU, OD, SQ, x_sem, dy_sem, w_sem, out_sem, send_sem, recv_sem) = refs[9:]
    tokens, dim, ff, blocks = shapes
    share = ff // n
    tiles = share // LANES
    tile = n * LANES
    tb = tokens // blocks
    half = n // 2
    hr = LANES // 2
    cols = tile // 2
    strip = tile // 4
    me = lax.axis_index("dp")
    up, down = lax.rem(me + 1, n), lax.rem(me + n - 1, n)
    ring = lambda d: lax.rem(me + d + n, n)

    def tok(i):
        return at(i, tb)

    def fetch(k):
        slot = lax.rem(k, 2)
        layer = lax.rem(k // tiles, 2)
        t = lax.rem(k, tiles)

        def one(b):
            place = pl.ds(pl.multiple_of(b * share + t * LANES, LANES), LANES)
            here = at(b, LANES)
            pltpu.make_async_copy(wg_hbm.at[layer, :, place], WG.at[slot, :, here], w_sem.at[slot, 0]).start()
            pltpu.make_async_copy(wu_hbm.at[layer, :, place], WU.at[slot, :, here], w_sem.at[slot, 1]).start()
            pltpu.make_async_copy(wd_hbm.at[layer, place, :], WD.at[slot, here, :], w_sem.at[slot, 2]).start()

        loop(n, one)

    def fetched(k):
        slot = lax.rem(k, 2)
        pltpu.make_async_copy(WG.at[slot], WG.at[slot], w_sem.at[slot, 0]).wait()
        pltpu.make_async_copy(WU.at[slot], WU.at[slot], w_sem.at[slot, 1]).wait()
        pltpu.make_async_copy(WD.at[slot], WD.at[slot], w_sem.at[slot, 2]).wait()

    def x_copy(i):
        return pltpu.make_async_copy(x_hbm.at[0, tok(i), :], H.at[tok(i), :], x_sem.at[i])

    def x_again(i):
        return pltpu.make_async_copy(x_hbm.at[0, tok(i), :], ACT.at[tok(i), pl.ds(0, dim)], x_sem.at[i])

    def dy_copy(i):
        return pltpu.make_async_copy(dy_hbm.at[0, tok(i), :], D.at[tok(i), :], dy_sem.at[i])

    barrier = pltpu.get_barrier_semaphore()
    for peer in (up, down):
        pl.semaphore_signal(barrier, inc=1, device_id={"dp": peer}, device_id_type=MESH)

    loop(blocks, lambda i: x_copy(i).start())
    fetch(0)
    loop(blocks, lambda i: dy_copy(i).start())

    def first_norm(i):
        x_copy(i).wait()
        wide = H[tok(i), :].astype(F32)
        A[tok(i), :] = (wide * scale_of(wide)).astype(BF16)
        DA[tok(i), :] = jnp.zeros((tb, dim), F32)

    loop(blocks, first_norm)

    def forward_tile(k):
        slot = lax.rem(k, 2)
        fetched(k)
        fetch(k + 1)

        def some(i):
            for j in range(2):
                here = pl.ds(j * cols, cols)
                g = dot(A[tok(i), :], WG[slot, :, here])
                u = dot(A[tok(i), :], WU[slot, :, here])
                s = 0.5 * jnp.tanh(0.5 * g) + 0.5
                ACT[tok(i), here] = (g * s * u).astype(BF16)
            DA[tok(i), :] += dot(ACT[tok(i), :], WD[slot])

        loop(blocks, some)

    loop(tiles, forward_tile)

    def second_norm(i):
        h = (H[tok(i), :].astype(F32) + DA[tok(i), :].astype(BF16).astype(F32)).astype(BF16)
        H[tok(i), :] = h
        wide = h.astype(F32)
        a = (wide * scale_of(wide)).astype(BF16)
        A[tok(i), :] = a
        AT[:, tok(i)] = a.T
        DA[tok(i), :] = jnp.zeros((tb, dim), F32)
        dy_copy(i).wait()
        DT[:, tok(i)] = D[tok(i), :].T

    loop(blocks, second_norm)

    pl.semaphore_wait(barrier, 2)

    def remote(src, dst, slot, u, way, step):
        return pltpu.make_async_remote_copy(
            src_ref=src,
            dst_ref=dst,
            send_sem=send_sem.at[slot, way, step],
            recv_sem=recv_sem.at[u, way, step],
            device_id={"dp": (up, down)[way]},
            device_id_type=MESH,
        )

    low, high, whole = pl.ds(0, hr), pl.ds(hr, hr), pl.ds(0, 2 * hr)
    lands = (RU, RD)

    def rows(step):
        return pl.ds(pl.multiple_of(hr + (step - 1) * 2 * hr, hr), 2 * hr)

    def begin(u, slot):
        far = ring(half)
        remote(G.at[slot, far, low], RU.at[u, low], slot, u, 0, 0).start()
        remote(G.at[slot, far, high], RD.at[u, low], slot, u, 1, 0).start()
        remote(G.at[slot, ring(half - 1), high], RU.at[u, pl.ds(2 * hr, hr)], slot, u, 0, 1).start()
        remote(G.at[slot, ring(1 - half), low], RD.at[u, pl.ds(hr, hr)], slot, u, 1, 1).start()

    def received(u, way, step):
        dst = lands[way].at[u, low] if isinstance(step, int) and step == 0 else lands[way].at[u, rows(step)]
        pltpu.make_async_copy(dst, dst, recv_sem.at[u, way, step]).wait()

    def add(land, place, mine):
        land[place] = (land[place].astype(F32) + mine.astype(F32)).astype(BF16)

    def second(u, slot):
        received(u, 0, 0)
        received(u, 1, 0)
        add(RU, (u, low), G[slot, ring(half - 1), low])
        add(RD, (u, low), G[slot, ring(1 - half), high])
        remote(RU.at[u, low], RU.at[u, pl.ds(hr, hr)], slot, u, 0, 1).start()
        remote(RD.at[u, low], RD.at[u, pl.ds(2 * hr, hr)], slot, u, 1, 1).start()

    def later(u, slot, step):
        received(u, 0, step - 1)
        received(u, 1, step - 1)
        add(RU, (u, rows(step - 1)), G[slot, ring(half - step)])
        add(RD, (u, rows(step - 1)), G[slot, ring(step - half)])
        remote(RU.at[u, rows(step - 1)], RU.at[u, rows(step)], slot, u, 0, step).start()
        remote(RD.at[u, rows(step - 1)], RD.at[u, rows(step)], slot, u, 1, step).start()

    def finish(u, slot, which, layer, t):
        received(u, 0, half - 1)
        received(u, 1, half - 1)
        total = G[slot, me].astype(F32) + RU[u, rows(half - 1)].astype(F32) + RD[u, rows(half - 1)].astype(F32)
        total = total.astype(BF16)
        wide = total.astype(F32)
        SQ[...] += jnp.sum((wide * wide).reshape(-1, 8, dim), axis=0)
        if which == 0:
            OD[layer, at(t, LANES), :] = total
        else:
            out = (OG, OU)[which - 1]
            for b in range(n):
                piece = total[hr * (b // (n // 2)) : hr * (b // (n // 2)) + hr, LANES * (b % (n // 2)) : LANES * (b % (n // 2)) + LANES]
                out[layer, :, pl.ds(pl.multiple_of(b * share + t * LANES, LANES), LANES)] = piece
        for way in range(2):
            for step in range(half):
                src = G.at[slot, 0, whole] if step > 0 else G.at[slot, 0, low]
                pltpu.make_async_copy(src, src, send_sem.at[slot, way, step]).wait()

    SQ[...] = jnp.zeros_like(SQ)

    def tile_step(k):
        wk = k + tiles
        slot = lax.rem(wk, 2)
        base = lax.rem(k, 2) * 3
        prev = 3 - base
        u0 = 3 * k
        p0 = u0 - 3
        last_layer = k < tiles
        going = k >= 1
        pt = lax.rem(k - 1 + tiles, tiles)
        pl_layer = jnp.where(k - 1 < tiles, 1, 0)
        fetched(wk)

        @pl.when(k < 2 * tiles - 1)
        def _():
            fetch(wk + 1)

        def hidden(i):
            b, j = i // 2, lax.rem(i, 2)
            here = at(j, cols)
            g = dot(A[tok(b), :], WG[slot, :, here])
            u = dot(A[tok(b), :], WU[slot, :, here])
            back = dot_t(D[tok(b), :], WD[slot, here, :]).astype(BF16).astype(F32)
            s = 0.5 * jnp.tanh(0.5 * g) + 0.5
            silu = g * s
            ACT[tok(b), here] = (silu * u).astype(BF16)
            DU[tok(b), here] = (back * silu).astype(BF16)
            DG[tok(b), here] = (back * u * (s + silu * (1.0 - s))).astype(BF16)

            @pl.when(going & (i == 0))
            def _():
                second(p0 + 2, prev + 2)

            @pl.when(going & (lax.rem(i, 2) == 1))
            def _():
                e = i // 2
                j3 = lax.rem(e, 3)
                later(p0 + j3, prev + j3, 2 + e // 3)

        loop(2 * blocks, hidden)

        def down_part(i):
            part = dot(DT[...], ACT[:, at(i, strip)])
            flipped = part.T.astype(BF16)
            for b in range(strip // LANES):
                G[base, i * (strip // LANES) + b] = flipped[b * LANES : (b + 1) * LANES]

            @pl.when(going & (lax.rem(i, 2) == 1))
            def _():
                j3 = 1 + i // 2
                later(p0 + j3, prev + j3, 3)

        loop(4, down_part)
        begin(u0, base)

        def wide_part(src, unit, i):
            part = dot(AT[...], src[:, at(i, strip)]).astype(BF16)
            G[base + unit, :, at(i // 2, hr), at(lax.rem(i, 2), strip)] = part.reshape(n, dim // n, strip)

        def gate_part(i):
            wide_part(DG, 1, i)

            @pl.when(going & (i == 0))
            def _():
                finish(p0, prev, 0, pl_layer, pt)

            @pl.when(going & (i == 2))
            def _():
                finish(p0 + 1, prev + 1, 1, pl_layer, pt)

        loop(4, gate_part)
        begin(u0 + 1, base + 1)
        second(u0, base)

        def up_part(i):
            wide_part(DU, 2, i)

            @pl.when(going & (i == 1))
            def _():
                finish(p0 + 2, prev + 2, 2, pl_layer, pt)

        loop(4, up_part)
        begin(u0 + 2, base + 2)

        @pl.when(k == tiles - 1)
        def _():
            loop(blocks, lambda i: x_again(i).start())

        @pl.when(last_layer)
        def _():
            def input_part(i):
                DA[tok(i), :] += dot_t(DG[tok(i), :], WG[slot]) + dot_t(DU[tok(i), :], WU[slot])

            loop(blocks, input_part)

        second(u0 + 1, base + 1)

        @pl.when(k == tiles - 1)
        def _():
            def between(i):
                h = H[tok(i), :].astype(F32)
                da = DA[tok(i), :].astype(BF16).astype(F32)
                r = scale_of(h)
                dh = (r * da - h * (r * r * r * jnp.mean(h * da, -1, keepdims=True))).astype(BF16)
                d = (D[tok(i), :].astype(F32) + dh.astype(F32)).astype(BF16)
                D[tok(i), :] = d
                DT[:, tok(i)] = d.T
                x_again(i).wait()
                wide = ACT[tok(i), pl.ds(0, dim)].astype(F32)
                a = (wide * scale_of(wide)).astype(BF16)
                A[tok(i), :] = a
                AT[:, tok(i)] = a.T

            loop(blocks, between)

    loop(2 * tiles, tile_step)

    end = 2 * tiles - 1
    u0, base = 3 * end, (end % 2) * 3
    second(u0 + 2, base + 2)
    for step in range(2, half):
        loop(3, lambda j, step=step: later(u0 + j, base + j, step))
    for j in range(3):
        finish(u0 + j, base + j, j, 0, tiles - 1)

    outs = (
        pltpu.make_async_copy(OG, og_hbm, out_sem.at[0]),
        pltpu.make_async_copy(OU, ou_hbm, out_sem.at[1]),
        pltpu.make_async_copy(OD, od_hbm, out_sem.at[2]),
        pltpu.make_async_copy(SQ, sq_hbm, out_sem.at[3]),
    )
    for copy in outs:
        copy.start()
    for copy in outs:
        copy.wait()


def gradients(n, x, dy, w_gate, w_up, w_down):
    layers, dim, ff = w_gate.shape
    tokens = x.shape[1]
    blocks = 4
    share = ff // n
    tiles = share // LANES
    tile = n * LANES
    units = 3 * layers * tiles
    half = n // 2
    land = LANES // 2 + LANES * (half - 1)
    any_space = pl.BlockSpec(memory_space=pl.ANY)
    return pl.pallas_call(
        functools.partial(grad_kernel, n, layers, (tokens, dim, ff, blocks)),
        out_shape=(
            jax.ShapeDtypeStruct((layers, dim // n, ff), BF16),
            jax.ShapeDtypeStruct((layers, dim // n, ff), BF16),
            jax.ShapeDtypeStruct((layers, share, dim), BF16),
            jax.ShapeDtypeStruct((8, dim), F32),
        ),
        in_specs=[any_space] * 5,
        out_specs=(any_space,) * 4,
        scratch_shapes=[
            pltpu.VMEM((tokens, dim), BF16),
            pltpu.VMEM((dim, tokens), BF16),
            pltpu.VMEM((tokens, dim), BF16),
            pltpu.VMEM((dim, tokens), BF16),
            pltpu.VMEM((tokens, dim), BF16),
            pltpu.VMEM((tokens, tile), BF16),
            pltpu.VMEM((tokens, tile), BF16),
            pltpu.VMEM((tokens, tile), BF16),
            pltpu.VMEM((tokens, dim), F32),
            pltpu.VMEM((2, dim, tile), BF16),
            pltpu.VMEM((2, dim, tile), BF16),
            pltpu.VMEM((2, tile, dim), BF16),
            pltpu.VMEM((6, n, LANES, dim), BF16),
            pltpu.VMEM((units, land, dim), BF16),
            pltpu.VMEM((units, land, dim), BF16),
            pltpu.VMEM((layers, dim // n, ff), BF16),
            pltpu.VMEM((layers, dim // n, ff), BF16),
            pltpu.VMEM((layers, share, dim), BF16),
            pltpu.VMEM((8, dim), F32),
            pltpu.SemaphoreType.DMA((blocks,)),
            pltpu.SemaphoreType.DMA((blocks,)),
            pltpu.SemaphoreType.DMA((2, 3)),
            pltpu.SemaphoreType.DMA((4,)),
            pltpu.SemaphoreType.DMA((6, 2, half)),
            pltpu.SemaphoreType.DMA((units, 2, half)),
        ],
        compiler_params=pltpu.CompilerParams(collective_id=0, has_side_effects=True, vmem_limit_bytes=VMEM_LIMIT),
        name="grads",
    )(x, dy, w_gate, w_up, w_down)


def update_kernel(n, count, parts, *refs):
    g_hbm, w_hbm, m_hbm, v_hbm = (refs[i : i + 3] for i in (0, 3, 6, 9))
    sq_hbm = refs[12]
    nw_hbm, nm_hbm, nv_hbm = (refs[i : i + 3] for i in (13, 16, 19))
    G, W, M, V, N = (refs[i : i + 3] for i in (22, 25, 28, 31, 34))
    SQ, in_sem, sq_sem, sq_send, sq_recv, mv_sem, nw_sem, send_sem, recv_sem = refs[37:]
    me = lax.axis_index("dp")
    half = n // 2
    up, down = lax.rem(me + 1, n), lax.rem(me + n - 1, n)
    ring = lambda d: lax.rem(me + d + n, n)
    layers = G[0].shape[0]

    barrier = pltpu.get_barrier_semaphore()
    for d in range(1, n):
        pl.semaphore_signal(barrier, inc=1, device_id={"dp": ring(d)}, device_id_type=MESH)

    mine = pltpu.make_async_copy(sq_hbm, SQ.at[me], sq_sem)
    mine.start()
    loads = []
    for a in range(3):
        rows = G[a].shape[1]
        own = pl.ds(pl.multiple_of(me * rows, rows), rows)
        for l in range(layers):
            loads.append(
                (
                    pltpu.make_async_copy(g_hbm[a].at[l], G[a].at[l], in_sem.at[0, a, l]),
                    pltpu.make_async_copy(w_hbm[a].at[l, own, :], W[a].at[l], in_sem.at[1, a, l]),
                    pltpu.make_async_copy(m_hbm[a].at[l], M[a].at[l], in_sem.at[2, a, l]),
                    pltpu.make_async_copy(v_hbm[a].at[l], V[a].at[l], in_sem.at[3, a, l]),
                )
            )
            for copy in loads[-1]:
                copy.start()
    mine.wait()
    pl.semaphore_wait(barrier, n - 1)

    def tell(d):
        return pltpu.make_async_remote_copy(
            src_ref=SQ.at[me],
            dst_ref=SQ.at[me],
            send_sem=sq_send.at[d],
            recv_sem=sq_recv.at[d],
            device_id={"dp": ring(d)},
            device_id_type=MESH,
        )

    for d in range(1, n):
        tell(d).start()
    for d in range(1, n):
        tell(d).wait_recv()
    total = jnp.sum(jnp.sum(SQ[...], axis=0), axis=(0, 1), keepdims=True)
    factor = jnp.minimum(1.0, 0.5 * lax.rsqrt(total / count + 1e-30))

    def shape(a):
        rows, cols = G[a].shape[1:]
        return (rows, cols // parts, 0) if a < 2 else (rows // parts, cols, 1)

    def place(a, l, p, owner, part):
        rows = G[a].shape[1]
        r, c, split = shape(a)
        hr = r // 2
        start = owner * rows + (p * r if split else 0)
        start, size = (start, r) if part == 2 else (start + part * hr, hr)
        return (l, pl.ds(pl.multiple_of(start, hr), size), pl.ds(0 if split else p * c, c))

    def send(i, a, l, p, way, step):
        owner = ring(-step) if way == 0 else ring(step)
        ref = N[a].at[place(a, l, p, owner, 2 if step < half - 1 else way)]
        return pltpu.make_async_remote_copy(
            src_ref=ref,
            dst_ref=ref,
            send_sem=send_sem.at[i, way, step],
            recv_sem=recv_sem.at[i, way, step],
            device_id={"dp": (up, down)[way]},
            device_id_type=MESH,
        )

    def came(i, a, l, p, way, step):
        owner = ring(-step - 1) if way == 0 else ring(step + 1)
        where = place(a, l, p, owner, 2 if step < half - 1 else way)
        ref = N[a].at[where]
        pltpu.make_async_copy(ref, ref, recv_sem.at[i, way, step]).wait()
        pltpu.make_async_copy(ref, nw_hbm[a].at[where], nw_sem.at[a]).start()

    def adam(a, l, p):
        r, c, split = shape(a)
        rows = G[a].shape[1]
        step = 16
        lane = pl.ds(0 if split else p * c, c)

        def some(i):
            row = pl.ds(pl.multiple_of((p * r if split else 0) + i * step, step), step)
            g = G[a][l, row, lane].astype(F32) * factor
            m = 0.9 * M[a][l, row, lane] + 0.1 * g
            v = 0.95 * V[a][l, row, lane] + 0.05 * g * g
            M[a][l, row, lane] = m
            V[a][l, row, lane] = v
            w = W[a][l, row, lane].astype(F32)
            new = (w - 0.02 * (m * lax.rsqrt(v + 1e-8) + 0.1 * w)).astype(BF16)
            there = pl.ds(pl.multiple_of(me * rows + (p * r if split else 0) + i * step, step), step)
            N[a][l, there, lane] = new

        loop(r // step, some)

    chunks = []
    for l in reversed(range(layers)):
        for a in (2, 0, 1):
            for p in range(parts):
                chunks.append((len(chunks), a, l, p))
    for i, a, l, p in chunks:
        if p == 0:
            for copy in loads[a * layers + l]:
                copy.wait()
        adam(a, l, p)
        send(i, a, l, p, 0, 0).start()
        send(i, a, l, p, 1, 0).start()
        where = place(a, l, p, me, 2)
        pltpu.make_async_copy(N[a].at[where], nw_hbm[a].at[where], nw_sem.at[a]).start()
        if p == parts - 1:
            pltpu.make_async_copy(M[a].at[l], nm_hbm[a].at[l], mv_sem.at[0, a, l]).start()
            pltpu.make_async_copy(V[a].at[l], nv_hbm[a].at[l], mv_sem.at[1, a, l]).start()
    for step in range(half):
        for i, a, l, p in chunks:
            for way in range(2):
                came(i, a, l, p, way, step)
                if step < half - 1:
                    send(i, a, l, p, way, step + 1).start()
    for i, a, l, p in chunks:
        for way in range(2):
            for step in range(half):
                send(i, a, l, p, way, step).wait_send()
    for d in range(1, n):
        tell(d).wait_send()
    for a in range(3):
        for l in range(layers):
            pltpu.make_async_copy(M[a].at[l], nm_hbm[a].at[l], mv_sem.at[0, a, l]).wait()
            pltpu.make_async_copy(V[a].at[l], nv_hbm[a].at[l], mv_sem.at[1, a, l]).wait()
        pltpu.make_async_copy(N[a], nw_hbm[a], nw_sem.at[a]).wait()


def update(n, g, w, m, v, squares):
    layers = w[0].shape[0]
    parts = 2
    chunks = layers * 3 * parts
    count = sum(t.size for t in w)
    shard = [t.shape for t in m]
    any_space = pl.BlockSpec(memory_space=pl.ANY)
    half = n // 2
    return pl.pallas_call(
        functools.partial(update_kernel, n, float(count), parts),
        out_shape=tuple(jax.ShapeDtypeStruct(t.shape, BF16) for t in w) + tuple(jax.ShapeDtypeStruct(t.shape, F32) for t in m + v),
        in_specs=[any_space] * 13,
        out_specs=(any_space,) * 9,
        scratch_shapes=[pltpu.VMEM(s, d) for d in (BF16, BF16, F32, F32) for s in shard]
        + [pltpu.VMEM(t.shape, BF16) for t in w]
        + [
            pltpu.VMEM((n,) + squares.shape, F32),
            pltpu.SemaphoreType.DMA((4, 3, layers)),
            pltpu.SemaphoreType.DMA,
            pltpu.SemaphoreType.DMA((n,)),
            pltpu.SemaphoreType.DMA((n,)),
            pltpu.SemaphoreType.DMA((2, 3, layers)),
            pltpu.SemaphoreType.DMA((3,)),
            pltpu.SemaphoreType.DMA((chunks, 2, half)),
            pltpu.SemaphoreType.DMA((chunks, 2, half)),
        ],
        compiler_params=pltpu.CompilerParams(collective_id=1, has_side_effects=True, vmem_limit_bytes=VMEM_LIMIT),
        name="update",
    )(*g, *w, *m, *v, squares)


def solution(mesh):
    n = mesh.shape["dp"]

    def step(x, dy, *arrays):
        w, m, v = (arrays[i : i + 3] for i in (0, 3, 6))
        *g, squares = gradients(n, x, dy, *w)
        return update(n, g, w, m, v, squares)

    shard = P(None, "dp", None)
    return jax.shard_map(
        step,
        mesh=mesh,
        in_specs=(P(("rep", "dp"), None, None),) * 2 + (P(),) * 3 + (shard,) * 6,
        out_specs=(P("rep", None, None),) * 3 + (P("rep", "dp", None),) * 6,
        check_vma=False,
    )
```

```python
import functools

import jax
import jax.numpy as jnp
from jax import lax
from jax.experimental import pallas as pl
from jax.experimental.pallas import tpu as pltpu
from jax.sharding import PartitionSpec as P

F32 = jnp.float32
BF16 = jnp.bfloat16
MESH = pl.DeviceIdType.MESH
LANES = 128
VMEM_LIMIT = 67043328


def dot(a, b):
    return jnp.dot(a, b, preferred_element_type=F32)


def dot_t(a, b):
    return lax.dot_general(a, b, (((1,), (1,)), ((), ())), preferred_element_type=F32)


def scale_of(wide):
    return lax.rsqrt(jnp.mean(wide * wide, -1, keepdims=True) + 1e-6)


def pinned(t, space):
    return pltpu.with_memory_space_constraint(t, space)


def kept(t, dtype):
    return pltpu.VMEM(t.shape, dtype)


def loop(count, body):
    lax.fori_loop(0, count, lambda i, c: (body(i), c)[1], 0)


def at(i, size):
    return pl.ds(pl.multiple_of(i * size, size), size)


def grad_kernel(n, layers, shapes, *refs):
    (x_hbm, dy_hbm, wg_hbm, wu_hbm, wd_hbm) = refs[:5]
    (og_hbm, ou_hbm, od_hbm, sq_hbm) = refs[5:9]
    (A, AT, D, DT, H, ACT, DG, DU, DA, WG, WU, WD, G, RU, RD, OG, OU, OD, SQ, ALL, *sems) = refs[9:]
    x_sem, dy_sem, w_sem, out_sem, send_sem, recv_sem, sq_send, sq_recv = sems
    tokens, dim, ff, blocks = shapes
    share = ff // n
    tiles = share // LANES
    tile = n * LANES
    tb = tokens // blocks
    half = n // 2
    hr = LANES // 2
    cols = tile // 2
    me = lax.axis_index("dp")
    up, down = lax.rem(me + 1, n), lax.rem(me + n - 1, n)
    ring = lambda d: lax.rem(me + d + n, n)

    def tok(i):
        return at(i, tb)

    def fetch(k):
        slot = lax.rem(k, 2)
        layer = lax.rem(k // tiles, 2)
        t = lax.rem(k, tiles)

        def one(b):
            place = pl.ds(pl.multiple_of(b * share + t * LANES, LANES), LANES)
            here = at(b, LANES)
            pltpu.make_async_copy(wg_hbm.at[layer, :, place], WG.at[slot, :, here], w_sem.at[slot, 0]).start()
            pltpu.make_async_copy(wu_hbm.at[layer, :, place], WU.at[slot, :, here], w_sem.at[slot, 1]).start()
            pltpu.make_async_copy(wd_hbm.at[layer, place, :], WD.at[slot, here, :], w_sem.at[slot, 2]).start()

        loop(n, one)

    def fetched(k):
        slot = lax.rem(k, 2)
        pltpu.make_async_copy(WG.at[slot], WG.at[slot], w_sem.at[slot, 0]).wait()
        pltpu.make_async_copy(WU.at[slot], WU.at[slot], w_sem.at[slot, 1]).wait()
        pltpu.make_async_copy(WD.at[slot], WD.at[slot], w_sem.at[slot, 2]).wait()

    def x_copy(i):
        return pltpu.make_async_copy(x_hbm.at[0, tok(i), :], H.at[tok(i), :], x_sem.at[i])

    def x_again(i):
        return pltpu.make_async_copy(x_hbm.at[0, tok(i), :], ACT.at[tok(i), pl.ds(0, dim)], x_sem.at[i])

    def dy_copy(i):
        return pltpu.make_async_copy(dy_hbm.at[0, tok(i), :], D.at[tok(i), :], dy_sem.at[i])

    barrier = pltpu.get_barrier_semaphore()
    for d in range(1, n):
        pl.semaphore_signal(barrier, inc=1, device_id={"dp": ring(d)}, device_id_type=MESH)

    loop(blocks, lambda i: x_copy(i).start())
    fetch(0)
    loop(blocks, lambda i: dy_copy(i).start())

    def first_norm(i):
        x_copy(i).wait()
        wide = H[tok(i), :].astype(F32)
        A[tok(i), :] = (wide * scale_of(wide)).astype(BF16)
        DA[tok(i), :] = jnp.zeros((tb, dim), F32)

    loop(blocks, first_norm)

    def forward_tile(k):
        slot = lax.rem(k, 2)
        fetched(k)
        fetch(k + 1)

        def some(i):
            for j in range(2):
                here = pl.ds(j * cols, cols)
                g = dot(A[tok(i), :], WG[slot, :, here])
                u = dot(A[tok(i), :], WU[slot, :, here])
                s = 0.5 * jnp.tanh(0.5 * g) + 0.5
                ACT[tok(i), here] = (g * s * u).astype(BF16)
            DA[tok(i), :] += dot(ACT[tok(i), :], WD[slot])

        loop(blocks, some)

    loop(tiles, forward_tile)

    def second_norm(i):
        h = (H[tok(i), :].astype(F32) + DA[tok(i), :].astype(BF16).astype(F32)).astype(BF16)
        H[tok(i), :] = h
        wide = h.astype(F32)
        a = (wide * scale_of(wide)).astype(BF16)
        A[tok(i), :] = a
        AT[:, tok(i)] = a.T
        DA[tok(i), :] = jnp.zeros((tb, dim), F32)
        dy_copy(i).wait()
        DT[:, tok(i)] = D[tok(i), :].T

    loop(blocks, second_norm)

    pl.semaphore_wait(barrier, n - 1)

    def remote(src, dst, slot, u, way, step):
        return pltpu.make_async_remote_copy(
            src_ref=src,
            dst_ref=dst,
            send_sem=send_sem.at[slot, way, step],
            recv_sem=recv_sem.at[u, way, step],
            device_id={"dp": (up, down)[way]},
            device_id_type=MESH,
        )

    low, high, whole = pl.ds(0, hr), pl.ds(hr, hr), pl.ds(0, 2 * hr)
    lands = (RU, RD)

    def rows(step):
        return pl.ds(pl.multiple_of(hr + (step - 1) * 2 * hr, hr), 2 * hr)

    def begin_low(u, slot):
        remote(G.at[slot, ring(half), low], RU.at[u, low], slot, u, 0, 0).start()
        remote(G.at[slot, ring(1 - half), low], RD.at[u, pl.ds(hr, hr)], slot, u, 1, 1).start()

    def begin_high(u, slot):
        remote(G.at[slot, ring(half), high], RD.at[u, low], slot, u, 1, 0).start()
        remote(G.at[slot, ring(half - 1), high], RU.at[u, pl.ds(2 * hr, hr)], slot, u, 0, 1).start()

    def received(u, way, step):
        dst = lands[way].at[u, low] if isinstance(step, int) and step == 0 else lands[way].at[u, rows(step)]
        pltpu.make_async_copy(dst, dst, recv_sem.at[u, way, step]).wait()

    def add(land, place, mine):
        land[place] = (land[place].astype(F32) + mine.astype(F32)).astype(BF16)

    def second_low(u, slot):
        received(u, 0, 0)
        add(RU, (u, low), G[slot, ring(half - 1), low])
        remote(RU.at[u, low], RU.at[u, pl.ds(hr, hr)], slot, u, 0, 1).start()

    def second_high(u, slot):
        received(u, 1, 0)
        add(RD, (u, low), G[slot, ring(1 - half), high])
        remote(RD.at[u, low], RD.at[u, pl.ds(2 * hr, hr)], slot, u, 1, 1).start()

    def later(u, slot, step):
        received(u, 0, step - 1)
        received(u, 1, step - 1)
        add(RU, (u, rows(step - 1)), G[slot, ring(half - step)])
        add(RD, (u, rows(step - 1)), G[slot, ring(step - half)])
        remote(RU.at[u, rows(step - 1)], RU.at[u, rows(step)], slot, u, 0, step).start()
        remote(RD.at[u, rows(step - 1)], RD.at[u, rows(step)], slot, u, 1, step).start()

    def finish(u, slot, which, layer, t):
        received(u, 0, half - 1)
        received(u, 1, half - 1)
        total = G[slot, me].astype(F32) + RU[u, rows(half - 1)].astype(F32) + RD[u, rows(half - 1)].astype(F32)
        total = total.astype(BF16)
        wide = total.astype(F32)
        SQ[...] += jnp.sum((wide * wide).reshape(-1, 8, dim), axis=0)
        if which == 0:
            OD[layer, at(t, LANES), :] = total
        else:
            out = (OG, OU)[which - 1]
            for b in range(n):
                piece = total[hr * (b // (n // 2)) : hr * (b // (n // 2)) + hr, LANES * (b % (n // 2)) : LANES * (b % (n // 2)) + LANES]
                out[layer, :, pl.ds(pl.multiple_of(b * share + t * LANES, LANES), LANES)] = piece
        for way in range(2):
            for step in range(half):
                src = G.at[slot, 0, whole] if step > 0 else G.at[slot, 0, low]
                pltpu.make_async_copy(src, src, send_sem.at[slot, way, step]).wait()

    SQ[...] = jnp.zeros_like(SQ)

    def tile_step(k):
        wk = k + tiles
        slot = lax.rem(wk, 2)
        base = lax.rem(k, 2) * 3
        prev = 3 - base
        u0 = 3 * k
        p0 = u0 - 3
        going = k >= 1
        old_t = lax.rem(k - 1 + tiles, tiles)
        old_layer = jnp.where(k - 1 < tiles, 1, 0)
        fetched(wk)

        @pl.when(k < 2 * tiles - 1)
        def _():
            fetch(wk + 1)

        def when(cond):
            return pl.when(going & cond)

        def hidden(j, i):
            here = at(j, cols)
            for b in range(2):
                place = tok(2 * i + b)
                g = dot(A[place, :], WG[slot, :, here])
                u = dot(A[place, :], WU[slot, :, here])
                back = dot_t(D[place, :], WD[slot, here, :]).astype(BF16).astype(F32)
                s = 0.5 * jnp.tanh(0.5 * g) + 0.5
                silu = g * s
                ACT[place, here] = (silu * u).astype(BF16)
                DU[place, here] = (back * silu).astype(BF16)
                DG[place, here] = (back * u * (s + silu * (1.0 - s))).astype(BF16)

        def wide_part(src, unit, j):
            part = dot(AT[...], src[:, at(j, cols)]).astype(BF16)
            G[base + unit, :, at(j, hr), :] = part.reshape(n, dim // n, cols)

        def halves(j):
            def some(i):
                hidden(j, i)

                @when((j == 0) & (i == 0))
                def _():
                    later(p0 + 1, prev + 1, 3)

            loop(blocks // 2, some)

            @when(j == 1)
            def _():
                finish(p0 + 1, prev + 1, 1, old_layer, old_t)

            wide_part(DG, 1, j)

            @pl.when(j == 0)
            def _():
                begin_low(u0 + 1, base + 1)

            @when(j == 0)
            def _():
                later(p0, prev, 2)

            @pl.when(j == 1)
            def _():
                begin_high(u0 + 1, base + 1)

            @when(j == 1)
            def _():
                later(p0, prev, 3)

            @pl.when(j == 1)
            def _():
                second_low(u0 + 1, base + 1)

            wide_part(DU, 2, j)

            @pl.when(j == 0)
            def _():
                begin_low(u0 + 2, base + 2)

            @when(j == 0)
            def _():
                later(p0 + 2, prev + 2, 3)

            @pl.when(j == 1)
            def _():
                begin_high(u0 + 2, base + 2)
                second_low(u0 + 2, base + 2)

        loop(2, halves)

        def down_part(j):
            part = dot(DT[...], ACT[:, at(j, cols)])
            flipped = part.T.astype(BF16)
            for b in range(cols // LANES):
                G[base, j * (cols // LANES) + b] = flipped[b * LANES : (b + 1) * LANES]

            @pl.when(j == 0)
            def _():
                second_high(u0 + 1, base + 1)

            @when(j == 0)
            def _():
                finish(p0 + 2, prev + 2, 2, old_layer, old_t)

        loop(2, down_part)
        begin_low(u0, base)
        begin_high(u0, base)

        @pl.when(k == tiles - 1)
        def _():
            loop(blocks, lambda i: x_again(i).start())

        def ring_part(i):
            @pl.when(i == 1)
            def _():
                second_high(u0 + 2, base + 2)

            @when(i == 1)
            def _():
                finish(p0, prev, 0, old_layer, old_t)

            @pl.when(i == 2)
            def _():
                later(u0 + 1, base + 1, 2)

        @pl.when(k < tiles)
        def _():
            def input_part(i):
                DA[tok(i), :] += dot_t(DG[tok(i), :], WG[slot]) + dot_t(DU[tok(i), :], WU[slot])
                ring_part(i)

            loop(blocks, input_part)

        @pl.when(k >= tiles)
        def _():
            loop(blocks, ring_part)

        @pl.when(k == tiles - 1)
        def _():
            def between(i):
                h = H[tok(i), :].astype(F32)
                da = DA[tok(i), :].astype(BF16).astype(F32)
                r = scale_of(h)
                dh = (r * da - h * (r * r * r * jnp.mean(h * da, -1, keepdims=True))).astype(BF16)
                d = (D[tok(i), :].astype(F32) + dh.astype(F32)).astype(BF16)
                D[tok(i), :] = d
                DT[:, tok(i)] = d.T
                x_again(i).wait()
                wide = ACT[tok(i), pl.ds(0, dim)].astype(F32)
                a = (wide * scale_of(wide)).astype(BF16)
                A[tok(i), :] = a
                AT[:, tok(i)] = a.T

            loop(blocks, between)

        second_low(u0, base)
        second_high(u0, base)
        later(u0 + 2, base + 2, 2)

    loop(2 * tiles, tile_step)

    end = 2 * tiles - 1
    u0, base = 3 * end, (end % 2) * 3
    later(u0 + 1, base + 1, 3)
    later(u0, base, 2)
    later(u0 + 2, base + 2, 3)
    later(u0, base, 3)
    for j in (1, 2, 0):
        finish(u0 + j, base + j, j, 0, tiles - 1)

    squares = SQ[:, :LANES]
    for j in range(1, dim // LANES):
        squares += SQ[:, j * LANES : (j + 1) * LANES]
    ALL[me] = squares

    outs = (
        pltpu.make_async_copy(OG, og_hbm, out_sem.at[0]),
        pltpu.make_async_copy(OU, ou_hbm, out_sem.at[1]),
        pltpu.make_async_copy(OD, od_hbm, out_sem.at[2]),
    )
    for copy in outs:
        copy.start()

    def tell(d):
        return pltpu.make_async_remote_copy(
            src_ref=ALL.at[me],
            dst_ref=ALL.at[me],
            send_sem=sq_send.at[d],
            recv_sem=sq_recv.at[d],
            device_id={"dp": ring(d)},
            device_id_type=MESH,
        )

    for d in range(1, n):
        tell(d).start()
    for d in range(1, n):
        tell(d).wait()
    last = pltpu.make_async_copy(ALL, sq_hbm, out_sem.at[3])
    last.start()
    for copy in outs + (last,):
        copy.wait()


def gradients(n, x, dy, w_gate, w_up, w_down):
    layers, dim, ff = w_gate.shape
    tokens = x.shape[1]
    blocks = 4
    share = ff // n
    tiles = share // LANES
    tile = n * LANES
    units = 3 * layers * tiles
    half = n // 2
    land = LANES // 2 + LANES * (half - 1)
    any_space = pl.BlockSpec(memory_space=pl.ANY)
    return pl.pallas_call(
        functools.partial(grad_kernel, n, layers, (tokens, dim, ff, blocks)),
        out_shape=(
            jax.ShapeDtypeStruct((layers, dim // n, ff), BF16),
            jax.ShapeDtypeStruct((layers, dim // n, ff), BF16),
            jax.ShapeDtypeStruct((layers, share, dim), BF16),
            jax.ShapeDtypeStruct((n, 8, LANES), F32),
        ),
        in_specs=[any_space] * 5,
        out_specs=(any_space,) * 4,
        scratch_shapes=[
            pltpu.VMEM((tokens, dim), BF16),
            pltpu.VMEM((dim, tokens), BF16),
            pltpu.VMEM((tokens, dim), BF16),
            pltpu.VMEM((dim, tokens), BF16),
            pltpu.VMEM((tokens, dim), BF16),
            pltpu.VMEM((tokens, tile), BF16),
            pltpu.VMEM((tokens, tile), BF16),
            pltpu.VMEM((tokens, tile), BF16),
            pltpu.VMEM((tokens, dim), F32),
            pltpu.VMEM((2, dim, tile), BF16),
            pltpu.VMEM((2, dim, tile), BF16),
            pltpu.VMEM((2, tile, dim), BF16),
            pltpu.VMEM((6, n, LANES, dim), BF16),
            pltpu.VMEM((units, land, dim), BF16),
            pltpu.VMEM((units, land, dim), BF16),
            pltpu.VMEM((layers, dim // n, ff), BF16),
            pltpu.VMEM((layers, dim // n, ff), BF16),
            pltpu.VMEM((layers, share, dim), BF16),
            pltpu.VMEM((8, dim), F32),
            pltpu.VMEM((n, 8, LANES), F32),
            pltpu.SemaphoreType.DMA((blocks,)),
            pltpu.SemaphoreType.DMA((blocks,)),
            pltpu.SemaphoreType.DMA((2, 3)),
            pltpu.SemaphoreType.DMA((4,)),
            pltpu.SemaphoreType.DMA((6, 2, half)),
            pltpu.SemaphoreType.DMA((units, 2, half)),
            pltpu.SemaphoreType.DMA((n,)),
            pltpu.SemaphoreType.DMA((n,)),
        ],
        compiler_params=pltpu.CompilerParams(collective_id=0, has_side_effects=True, vmem_limit_bytes=VMEM_LIMIT),
        name="grads",
    )(x, dy, w_gate, w_up, w_down)


def update_kernel(n, count, parts, *refs):
    g_hbm, w_hbm, m_hbm, v_hbm = (refs[i : i + 3] for i in (0, 3, 6, 9))
    sq_hbm = refs[12]
    N, M, V = (refs[i : i + 3] for i in (13, 16, 19))
    G, W = (refs[i : i + 3] for i in (22, 25))
    SQ, in_sem, sq_sem, send_sem, recv_sem = refs[28:]
    me = lax.axis_index("dp")
    half = n // 2
    up, down = lax.rem(me + 1, n), lax.rem(me + n - 1, n)
    ring = lambda d: lax.rem(me + d + n, n)
    layers = G[0].shape[0]

    barrier = pltpu.get_barrier_semaphore()
    for peer in (up, down):
        pl.semaphore_signal(barrier, inc=1, device_id={"dp": peer}, device_id_type=MESH)

    squares = pltpu.make_async_copy(sq_hbm, SQ, sq_sem)
    squares.start()
    loads = {}
    for l in reversed(range(layers)):
        for a in (2, 0, 1):
            rows = G[a].shape[1]
            own = pl.ds(pl.multiple_of(me * rows, rows), rows)
            loads[a, l] = (
                pltpu.make_async_copy(g_hbm[a].at[l], G[a].at[l], in_sem.at[0, a, l]),
                pltpu.make_async_copy(w_hbm[a].at[l, own, :], W[a].at[l], in_sem.at[1, a, l]),
                pltpu.make_async_copy(m_hbm[a].at[l], M[a].at[l], in_sem.at[2, a, l]),
                pltpu.make_async_copy(v_hbm[a].at[l], V[a].at[l], in_sem.at[3, a, l]),
            )
            for copy in loads[a, l]:
                copy.start()
    squares.wait()
    total = jnp.sum(jnp.sum(SQ[...], axis=0), axis=(0, 1), keepdims=True)
    factor = jnp.minimum(1.0, 0.5 * lax.rsqrt(total / count + 1e-30))

    def shape(a):
        rows, cols = G[a].shape[1:]
        return (rows, cols // parts, 0) if a < 2 else (rows // parts, cols, 1)

    def place(a, l, p, owner, part):
        rows = G[a].shape[1]
        r, c, split = shape(a)
        hr = r // 2
        start = owner * rows + (p * r if split else 0)
        start, size = (start, r) if part == 2 else (start + part * hr, hr)
        return (l, pl.ds(pl.multiple_of(start, hr), size), pl.ds(0 if split else p * c, c))

    def send(i, a, l, p, way, step):
        owner = ring(-step) if way == 0 else ring(step)
        ref = N[a].at[place(a, l, p, owner, 2 if step < half - 1 else way)]
        return pltpu.make_async_remote_copy(
            src_ref=ref,
            dst_ref=ref,
            send_sem=send_sem.at[i, way, step],
            recv_sem=recv_sem.at[i, way, step],
            device_id={"dp": (up, down)[way]},
            device_id_type=MESH,
        )

    def came(i, a, l, p, way, step):
        owner = ring(-step - 1) if way == 0 else ring(step + 1)
        where = place(a, l, p, owner, 2 if step < half - 1 else way)
        ref = N[a].at[where]
        pltpu.make_async_copy(ref, ref, recv_sem.at[i, way, step]).wait()

    def adam(a, l, p):
        r, c, split = shape(a)
        rows = G[a].shape[1]
        step = 16
        lane = pl.ds(0 if split else p * c, c)

        def some(i):
            row = pl.ds(pl.multiple_of((p * r if split else 0) + i * step, step), step)
            g = G[a][l, row, lane].astype(F32) * factor
            m = 0.9 * M[a][l, row, lane] + 0.1 * g
            v = 0.95 * V[a][l, row, lane] + 0.05 * g * g
            M[a][l, row, lane] = m
            V[a][l, row, lane] = v
            w = W[a][l, row, lane].astype(F32)
            new = (w - 0.02 * (m * lax.rsqrt(v + 1e-8) + 0.1 * w)).astype(BF16)
            there = pl.ds(pl.multiple_of(me * rows + (p * r if split else 0) + i * step, step), step)
            N[a][l, there, lane] = new

        loop(r // step, some)

    chunks = []
    for l in reversed(range(layers)):
        for a in (2, 0, 1):
            for p in range(parts):
                chunks.append((len(chunks), a, l, p))
    for i, a, l, p in chunks:
        if p == 0:
            for copy in loads[a, l]:
                copy.wait()
        adam(a, l, p)
        if i == 0:
            pl.semaphore_wait(barrier, 2)
        send(i, a, l, p, 0, 0).start()
        send(i, a, l, p, 1, 0).start()
    for step in range(half):
        for i, a, l, p in chunks:
            for way in range(2):
                came(i, a, l, p, way, step)
                if step < half - 1:
                    send(i, a, l, p, way, step + 1).start()
    for i, a, l, p in chunks:
        for way in range(2):
            for step in range(half):
                send(i, a, l, p, way, step).wait_send()


def store_kernel(count, *refs):
    src, dst, sem = refs[:count], refs[count : 2 * count], refs[-1]
    copies = [pltpu.make_async_copy(a, b, sem.at[i]) for i, (a, b) in enumerate(zip(src, dst, strict=True))]
    for copy in copies:
        copy.start()
    for copy in copies:
        copy.wait()


def store(arrays):
    count = len(arrays)
    return pl.pallas_call(
        functools.partial(store_kernel, count),
        out_shape=tuple(jax.ShapeDtypeStruct(t.shape, t.dtype) for t in arrays),
        in_specs=[pl.BlockSpec(memory_space=pltpu.VMEM)] * count,
        out_specs=(pl.BlockSpec(memory_space=pl.ANY),) * count,
        scratch_shapes=[pltpu.SemaphoreType.DMA((count,))],
        compiler_params=pltpu.CompilerParams(vmem_limit_bytes=2**20),
        name="store",
    )(*(pinned(t, pltpu.VMEM) for t in arrays))


def update(n, g, w, m, v, squares):
    layers = w[0].shape[0]
    parts = 2
    chunks = layers * 3 * parts
    count = sum(t.size for t in w)
    shard = [t.shape for t in m]
    any_space = pl.BlockSpec(memory_space=pl.ANY)
    half = n // 2
    return pl.pallas_call(
        functools.partial(update_kernel, n, float(count), parts),
        out_shape=tuple(kept(t, BF16) for t in w) + tuple(kept(t, F32) for t in m + v),
        in_specs=[any_space] * 13,
        out_specs=(pl.BlockSpec(memory_space=pltpu.VMEM),) * 9,
        scratch_shapes=[pltpu.VMEM(s, BF16) for _ in range(2) for s in shard]
        + [
            pltpu.VMEM(squares.shape, F32),
            pltpu.SemaphoreType.DMA((4, 3, layers)),
            pltpu.SemaphoreType.DMA,
            pltpu.SemaphoreType.DMA((chunks, 2, half)),
            pltpu.SemaphoreType.DMA((chunks, 2, half)),
        ],
        compiler_params=pltpu.CompilerParams(collective_id=1, has_side_effects=True, vmem_limit_bytes=12 * 2**20),
        name="update",
    )(*(pinned(t, pltpu.HBM) for t in (*g, *w, *m, *v, squares)))


def solution(mesh):
    n = mesh.shape["dp"]

    def step(x, dy, *arrays):
        w, m, v = (arrays[i : i + 3] for i in (0, 3, 6))
        *g, squares = gradients(n, x, dy, *w)
        return store(update(n, g, w, m, v, squares))

    shard = P(None, "dp", None)
    return jax.shard_map(
        step,
        mesh=mesh,
        in_specs=(P(("rep", "dp"), None, None),) * 2 + (P(),) * 3 + (shard,) * 6,
        out_specs=(P("rep", None, None),) * 3 + (P("rep", "dp", None),) * 6,
        check_vma=False,
    )
```

```python
import functools

import jax
import jax.numpy as jnp
from jax import lax
from jax.experimental import pallas as pl
from jax.experimental.pallas import tpu as pltpu
from jax.sharding import PartitionSpec as P

F32 = jnp.float32
BF16 = jnp.bfloat16
MESH = pl.DeviceIdType.MESH
LANES = 128
VMEM_LIMIT = 67043328


def dot(a, b):
    return jnp.dot(a, b, preferred_element_type=F32)


def dot_t(a, b):
    return lax.dot_general(a, b, (((1,), (1,)), ((), ())), preferred_element_type=F32)


def scale_of(wide):
    return lax.rsqrt(jnp.mean(wide * wide, -1, keepdims=True) + 1e-6)


def pinned(t, space):
    return pltpu.with_memory_space_constraint(t, space)


def kept(shape, dtype):
    return pltpu.VMEM(shape, dtype)


def loop(count, body):
    lax.fori_loop(0, count, lambda i, c: (body(i), c)[1], 0)


def at(i, size):
    return pl.ds(pl.multiple_of(i * size, size), size)


def grad_kernel(n, layers, shapes, *refs):
    (x_hbm, dy_hbm, wg_hbm, wu_hbm, wd_hbm, md_hbm, vd_hbm) = refs[:7]
    (OG, OU, OD, ALL, PW, PM, PV) = refs[7:14]
    (A, AT, D, DT, H, ACT, DG, DU, DA, WG, WU, WD, G, RU, RD, SQ, *sems) = refs[14:]
    x_sem, dy_sem, w_sem, ahead_sem, send_sem, recv_sem, sq_send, sq_recv = sems
    tokens, dim, ff, blocks = shapes
    share = ff // n
    tiles = share // LANES
    tile = n * LANES
    tb = tokens // blocks
    half = n // 2
    hr = LANES // 2
    cols = tile // 2
    me = lax.axis_index("dp")
    up, down = lax.rem(me + 1, n), lax.rem(me + n - 1, n)
    ring = lambda d: lax.rem(me + d + n, n)

    def tok(i):
        return at(i, tb)

    def fetch(k):
        slot = lax.rem(k, 2)
        layer = lax.rem(k // tiles, 2)
        t = lax.rem(k, tiles)

        def one(b):
            place = pl.ds(pl.multiple_of(b * share + t * LANES, LANES), LANES)
            here = at(b, LANES)
            pltpu.make_async_copy(wg_hbm.at[layer, :, place], WG.at[slot, :, here], w_sem.at[slot, 0]).start()
            pltpu.make_async_copy(wu_hbm.at[layer, :, place], WU.at[slot, :, here], w_sem.at[slot, 1]).start()
            pltpu.make_async_copy(wd_hbm.at[layer, place, :], WD.at[slot, here, :], w_sem.at[slot, 2]).start()

        loop(n, one)

    def fetched(k):
        slot = lax.rem(k, 2)
        pltpu.make_async_copy(WG.at[slot], WG.at[slot], w_sem.at[slot, 0]).wait()
        pltpu.make_async_copy(WU.at[slot], WU.at[slot], w_sem.at[slot, 1]).wait()
        pltpu.make_async_copy(WD.at[slot], WD.at[slot], w_sem.at[slot, 2]).wait()

    def x_copy(i):
        return pltpu.make_async_copy(x_hbm.at[0, tok(i), :], H.at[tok(i), :], x_sem.at[i])

    def x_again(i):
        return pltpu.make_async_copy(x_hbm.at[0, tok(i), :], ACT.at[tok(i), pl.ds(0, dim)], x_sem.at[i])

    def dy_copy(i):
        return pltpu.make_async_copy(dy_hbm.at[0, tok(i), :], D.at[tok(i), :], dy_sem.at[i])

    barrier = pltpu.get_barrier_semaphore()
    for d in range(1, n):
        pl.semaphore_signal(barrier, inc=1, device_id={"dp": ring(d)}, device_id_type=MESH)

    loop(blocks, lambda i: x_copy(i).start())
    fetch(0)
    loop(blocks, lambda i: dy_copy(i).start())

    def first_norm(i):
        wide = H[tok(i), :].astype(F32)
        A[tok(i), :] = (wide * scale_of(wide)).astype(BF16)
        DA[tok(i), :] = jnp.zeros((tb, dim), F32)

    def forward(k, i):
        slot = lax.rem(k, 2)
        for j in range(2):
            here = pl.ds(j * cols, cols)
            g = dot(A[tok(i), :], WG[slot, :, here])
            u = dot(A[tok(i), :], WU[slot, :, here])
            s = 0.5 * jnp.tanh(0.5 * g) + 0.5
            ACT[tok(i), here] = (g * s * u).astype(BF16)
        DA[tok(i), :] += dot(ACT[tok(i), :], WD[slot])

    def second_norm(i):
        h = (H[tok(i), :].astype(F32) + DA[tok(i), :].astype(BF16).astype(F32)).astype(BF16)
        H[tok(i), :] = h
        wide = h.astype(F32)
        a = (wide * scale_of(wide)).astype(BF16)
        A[tok(i), :] = a
        AT[:, tok(i)] = a.T
        DA[tok(i), :] = jnp.zeros((tb, dim), F32)

    x_copy(0).wait()
    first_norm(0)
    fetched(0)
    fetch(1)

    def opening(i):
        x_copy(i + 1).wait()
        forward(0, i)
        first_norm(i + 1)

    loop(blocks - 1, opening)

    def middle(j):
        q = blocks - 1 + j
        k, i = q // blocks, lax.rem(q, blocks)

        @pl.when(i == 0)
        def _():
            fetched(k)
            fetch(k + 1)

        @pl.when(j < blocks)
        def _():
            dy_copy(j).wait()

        forward(k, i)
        seen = jnp.minimum(j, blocks - 1)
        DT[:, tok(seen)] = D[tok(seen), :].T

    loop((tiles - 2) * blocks + 2, middle)

    def closing(i):
        forward(tiles - 1, i + 1)
        second_norm(i)

    loop(blocks - 1, closing)
    second_norm(blocks - 1)

    pl.semaphore_wait(barrier, n - 1)

    def remote(src, dst, slot, u, way, step):
        return pltpu.make_async_remote_copy(
            src_ref=src,
            dst_ref=dst,
            send_sem=send_sem.at[slot, way, step],
            recv_sem=recv_sem.at[u, way, step],
            device_id={"dp": (up, down)[way]},
            device_id_type=MESH,
        )

    low, high, whole = pl.ds(0, hr), pl.ds(hr, hr), pl.ds(0, 2 * hr)
    lands = (RU, RD)

    def rows(step):
        return pl.ds(pl.multiple_of(hr + (step - 1) * 2 * hr, hr), 2 * hr)

    def begin_low(u, slot):
        remote(G.at[slot, ring(half), low], RU.at[u, low], slot, u, 0, 0).start()
        remote(G.at[slot, ring(1 - half), low], RD.at[u, pl.ds(hr, hr)], slot, u, 1, 1).start()

    def begin_high(u, slot):
        remote(G.at[slot, ring(half), high], RD.at[u, low], slot, u, 1, 0).start()
        remote(G.at[slot, ring(half - 1), high], RU.at[u, pl.ds(2 * hr, hr)], slot, u, 0, 1).start()

    def received(u, way, step):
        dst = lands[way].at[u, low] if isinstance(step, int) and step == 0 else lands[way].at[u, rows(step)]
        pltpu.make_async_copy(dst, dst, recv_sem.at[u, way, step]).wait()

    def add(land, place, mine):
        land[place] = (land[place].astype(F32) + mine.astype(F32)).astype(BF16)

    def second_low(u, slot):
        received(u, 0, 0)
        add(RU, (u, low), G[slot, ring(half - 1), low])
        remote(RU.at[u, low], RU.at[u, pl.ds(hr, hr)], slot, u, 0, 1).start()

    def second_high(u, slot):
        received(u, 1, 0)
        add(RD, (u, low), G[slot, ring(1 - half), high])
        remote(RD.at[u, low], RD.at[u, pl.ds(2 * hr, hr)], slot, u, 1, 1).start()

    def later(u, slot, step):
        received(u, 0, step - 1)
        received(u, 1, step - 1)
        add(RU, (u, rows(step - 1)), G[slot, ring(half - step)])
        add(RD, (u, rows(step - 1)), G[slot, ring(step - half)])
        remote(RU.at[u, rows(step - 1)], RU.at[u, rows(step)], slot, u, 0, step).start()
        remote(RD.at[u, rows(step - 1)], RD.at[u, rows(step)], slot, u, 1, step).start()

    def finish(u, slot, which, layer, t):
        received(u, 0, half - 1)
        received(u, 1, half - 1)
        total = G[slot, me].astype(F32) + RU[u, rows(half - 1)].astype(F32) + RD[u, rows(half - 1)].astype(F32)
        total = total.astype(BF16)
        wide = total.astype(F32)
        SQ[...] += jnp.sum((wide * wide).reshape(-1, 8, dim), axis=0)
        if which == 0:
            OD[layer, at(t, LANES), :] = total
        else:
            out = (OG, OU)[which - 1]
            for b in range(n):
                piece = total[hr * (b // (n // 2)) : hr * (b // (n // 2)) + hr, LANES * (b % (n // 2)) : LANES * (b % (n // 2)) + LANES]
                out[layer, :, pl.ds(pl.multiple_of(b * share + t * LANES, LANES), LANES)] = piece
        for way in range(2):
            for step in range(half):
                src = G.at[slot, 0, whole] if step > 0 else G.at[slot, 0, low]
                pltpu.make_async_copy(src, src, send_sem.at[slot, way, step]).wait()

    SQ[...] = jnp.zeros_like(SQ)

    def tile_step(k):
        wk = k + tiles
        slot = lax.rem(wk, 2)
        base = lax.rem(k, 2) * 3
        prev = 3 - base
        u0 = 3 * k
        p0 = u0 - 3
        going = k >= 1
        old_t = lax.rem(k - 1 + tiles, tiles)
        old_layer = jnp.where(k - 1 < tiles, 1, 0)
        fetched(wk)

        @pl.when(k < 2 * tiles - 1)
        def _():
            fetch(wk + 1)

        def when(cond):
            return pl.when(going & cond)

        def hidden(j, i):
            here = at(j, cols)
            for b in range(2):
                place = tok(2 * i + b)
                g = dot(A[place, :], WG[slot, :, here])
                u = dot(A[place, :], WU[slot, :, here])
                back = dot_t(D[place, :], WD[slot, here, :]).astype(BF16).astype(F32)
                s = 0.5 * jnp.tanh(0.5 * g) + 0.5
                silu = g * s
                ACT[place, here] = (silu * u).astype(BF16)
                DU[place, here] = (back * silu).astype(BF16)
                DG[place, here] = (back * u * (s + silu * (1.0 - s))).astype(BF16)

        def wide_part(src, unit, j):
            part = dot(AT[...], src[:, at(j, cols)]).astype(BF16)
            G[base + unit, :, at(j, hr), :] = part.reshape(n, dim // n, cols)

        def halves(j):
            def some(i):
                hidden(j, i)

                @when((j == 0) & (i == 0))
                def _():
                    later(p0 + 1, prev + 1, 3)

            loop(blocks // 2, some)

            @when(j == 1)
            def _():
                finish(p0 + 1, prev + 1, 1, old_layer, old_t)

            wide_part(DG, 1, j)

            @pl.when(j == 0)
            def _():
                begin_low(u0 + 1, base + 1)

            @when(j == 0)
            def _():
                later(p0, prev, 2)

            @pl.when(j == 1)
            def _():
                begin_high(u0 + 1, base + 1)

            @when(j == 1)
            def _():
                later(p0, prev, 3)

            @pl.when(j == 1)
            def _():
                second_low(u0 + 1, base + 1)

            wide_part(DU, 2, j)

            @pl.when(j == 0)
            def _():
                begin_low(u0 + 2, base + 2)

            @when(j == 0)
            def _():
                later(p0 + 2, prev + 2, 3)

            @pl.when(j == 1)
            def _():
                begin_high(u0 + 2, base + 2)
                second_low(u0 + 2, base + 2)

        loop(2, halves)

        def down_part(j):
            part = dot(DT[...], ACT[:, at(j, cols)])
            flipped = part.T.astype(BF16)
            for b in range(cols // LANES):
                G[base, j * (cols // LANES) + b] = flipped[b * LANES : (b + 1) * LANES]

            @pl.when(j == 0)
            def _():
                second_high(u0 + 1, base + 1)

            @when(j == 0)
            def _():
                finish(p0 + 2, prev + 2, 2, old_layer, old_t)

        loop(2, down_part)
        begin_low(u0, base)
        begin_high(u0, base)

        @pl.when(k == tiles - 1)
        def _():
            loop(blocks, lambda i: x_again(i).start())

        def ring_part(i):
            @pl.when(i == 1)
            def _():
                second_high(u0 + 2, base + 2)

            @when(i == 1)
            def _():
                finish(p0, prev, 0, old_layer, old_t)

            @pl.when(i == 2)
            def _():
                later(u0 + 1, base + 1, 2)

        @pl.when(k < tiles)
        def _():
            def input_part(i):
                DA[tok(i), :] += dot_t(DG[tok(i), :], WG[slot]) + dot_t(DU[tok(i), :], WU[slot])
                ring_part(i)

            loop(blocks, input_part)

        @pl.when(k >= tiles)
        def _():
            loop(blocks, ring_part)

        @pl.when(k == tiles - 1)
        def _():
            def between(i):
                h = H[tok(i), :].astype(F32)
                da = DA[tok(i), :].astype(BF16).astype(F32)
                r = scale_of(h)
                dh = (r * da - h * (r * r * r * jnp.mean(h * da, -1, keepdims=True))).astype(BF16)
                d = (D[tok(i), :].astype(F32) + dh.astype(F32)).astype(BF16)
                D[tok(i), :] = d
                DT[:, tok(i)] = d.T
                x_again(i).wait()
                wide = ACT[tok(i), pl.ds(0, dim)].astype(F32)
                a = (wide * scale_of(wide)).astype(BF16)
                A[tok(i), :] = a
                AT[:, tok(i)] = a.T

            loop(blocks, between)

        second_low(u0, base)
        second_high(u0, base)
        later(u0 + 2, base + 2, 2)

    loop(2 * tiles, tile_step)

    ahead = (
        pltpu.make_async_copy(wd_hbm.at[layers - 1, at(me, share), :], PW, ahead_sem.at[0]),
        pltpu.make_async_copy(md_hbm.at[layers - 1], PM, ahead_sem.at[1]),
        pltpu.make_async_copy(vd_hbm.at[layers - 1], PV, ahead_sem.at[2]),
    )
    for copy in ahead:
        copy.start()

    end = 2 * tiles - 1
    u0, base = 3 * end, (end % 2) * 3
    later(u0 + 1, base + 1, 3)
    later(u0, base, 2)
    later(u0 + 2, base + 2, 3)
    later(u0, base, 3)
    for j in (1, 2, 0):
        finish(u0 + j, base + j, j, 0, tiles - 1)

    squares = SQ[:, :LANES]
    for j in range(1, dim // LANES):
        squares += SQ[:, j * LANES : (j + 1) * LANES]
    ALL[me] = squares

    def tell(d):
        return pltpu.make_async_remote_copy(
            src_ref=ALL.at[me],
            dst_ref=ALL.at[me],
            send_sem=sq_send.at[d],
            recv_sem=sq_recv.at[d],
            device_id={"dp": ring(d)},
            device_id_type=MESH,
        )

    for d in range(1, n):
        tell(d).start()
    for d in range(1, n):
        tell(d).wait()
    for copy in ahead:
        copy.wait()


def gradients(n, x, dy, w_gate, w_up, w_down, m_down, v_down):
    layers, dim, ff = w_gate.shape
    tokens = x.shape[1]
    blocks = 4
    share = ff // n
    tiles = share // LANES
    tile = n * LANES
    units = 3 * layers * tiles
    half = n // 2
    land = LANES // 2 + LANES * (half - 1)
    any_space = pl.BlockSpec(memory_space=pl.ANY)
    return pl.pallas_call(
        functools.partial(grad_kernel, n, layers, (tokens, dim, ff, blocks)),
        out_shape=tuple(
            kept(shape, dtype)
            for shape, dtype in (
                ((layers, dim // n, ff), BF16),
                ((layers, dim // n, ff), BF16),
                ((layers, share, dim), BF16),
                ((n, 8, LANES), F32),
                ((share, dim), BF16),
                ((share, dim), F32),
                ((share, dim), F32),
            )
        ),
        in_specs=[any_space] * 7,
        out_specs=(pl.BlockSpec(memory_space=pltpu.VMEM),) * 7,
        scratch_shapes=[
            pltpu.VMEM((tokens, dim), BF16),
            pltpu.VMEM((dim, tokens), BF16),
            pltpu.VMEM((tokens, dim), BF16),
            pltpu.VMEM((dim, tokens), BF16),
            pltpu.VMEM((tokens, dim), BF16),
            pltpu.VMEM((tokens, tile), BF16),
            pltpu.VMEM((tokens, tile), BF16),
            pltpu.VMEM((tokens, tile), BF16),
            pltpu.VMEM((tokens, dim), F32),
            pltpu.VMEM((2, dim, tile), BF16),
            pltpu.VMEM((2, dim, tile), BF16),
            pltpu.VMEM((2, tile, dim), BF16),
            pltpu.VMEM((6, n, LANES, dim), BF16),
            pltpu.VMEM((units, land, dim), BF16),
            pltpu.VMEM((units, land, dim), BF16),
            pltpu.VMEM((8, dim), F32),
            pltpu.SemaphoreType.DMA((blocks,)),
            pltpu.SemaphoreType.DMA((blocks,)),
            pltpu.SemaphoreType.DMA((2, 3)),
            pltpu.SemaphoreType.DMA((3,)),
            pltpu.SemaphoreType.DMA((6, 2, half)),
            pltpu.SemaphoreType.DMA((units, 2, half)),
            pltpu.SemaphoreType.DMA((n,)),
            pltpu.SemaphoreType.DMA((n,)),
        ],
        compiler_params=pltpu.CompilerParams(collective_id=0, has_side_effects=True, vmem_limit_bytes=59 * 2**20),
        name="grads",
    )(*(pinned(t, pltpu.HBM) for t in (x, dy, w_gate, w_up, w_down, m_down, v_down)))


def update_kernel(n, count, parts, *refs):
    G, w_hbm, m_hbm, v_hbm = (refs[i : i + 3] for i in (0, 4, 10, 13))
    SQ, PW, PM, PV = refs[3], *refs[7:10]
    N, M, V = (refs[i : i + 3] for i in (16, 19, 22))
    W = refs[25:28]
    in_sem, send_sem, recv_sem = refs[28:]
    me = lax.axis_index("dp")
    half = n // 2
    up, down = lax.rem(me + 1, n), lax.rem(me + n - 1, n)
    ring = lambda d: lax.rem(me + d + n, n)
    layers = G[0].shape[0]

    barrier = pltpu.get_barrier_semaphore()
    for peer in (up, down):
        pl.semaphore_signal(barrier, inc=1, device_id={"dp": peer}, device_id_type=MESH)

    order = [(a, l) for l in reversed(range(layers)) for a in (2, 0, 1)]
    loads = {}
    for a, l in order[1:]:
        rows = G[a].shape[1]
        own = pl.ds(pl.multiple_of(me * rows, rows), rows)
        loads[a, l] = (
            pltpu.make_async_copy(w_hbm[a].at[l, own, :], W[a].at[l], in_sem.at[0, a, l]),
            pltpu.make_async_copy(m_hbm[a].at[l], M[a].at[l], in_sem.at[1, a, l]),
            pltpu.make_async_copy(v_hbm[a].at[l], V[a].at[l], in_sem.at[2, a, l]),
        )
        for copy in loads[a, l]:
            copy.start()
    total = jnp.sum(jnp.sum(SQ[...], axis=0), axis=(0, 1), keepdims=True)
    factor = jnp.minimum(1.0, 0.5 * lax.rsqrt(total / count + 1e-30))

    def shape(a):
        rows, cols = G[a].shape[1:]
        return (rows, cols // parts, 0) if a < 2 else (rows // parts, cols, 1)

    def place(a, l, p, owner, part):
        rows = G[a].shape[1]
        r, c, split = shape(a)
        hr = r // 2
        start = owner * rows + (p * r if split else 0)
        start, size = (start, r) if part == 2 else (start + part * hr, hr)
        return (l, pl.ds(pl.multiple_of(start, hr), size), pl.ds(0 if split else p * c, c))

    def send(i, a, l, p, way, step):
        owner = ring(-step) if way == 0 else ring(step)
        ref = N[a].at[place(a, l, p, owner, 2 if step < half - 1 else way)]
        return pltpu.make_async_remote_copy(
            src_ref=ref,
            dst_ref=ref,
            send_sem=send_sem.at[i, way, step],
            recv_sem=recv_sem.at[i, way, step],
            device_id={"dp": (up, down)[way]},
            device_id_type=MESH,
        )

    def came(i, a, l, p, way, step):
        owner = ring(-step - 1) if way == 0 else ring(step + 1)
        where = place(a, l, p, owner, 2 if step < half - 1 else way)
        ref = N[a].at[where]
        pltpu.make_async_copy(ref, ref, recv_sem.at[i, way, step]).wait()

    def adam(a, l, p):
        r, c, split = shape(a)
        rows = G[a].shape[1]
        step = 16
        lane = pl.ds(0 if split else p * c, c)

        def some(i):
            row = pl.ds(pl.multiple_of((p * r if split else 0) + i * step, step), step)
            old = (PW[row, lane], PM[row, lane], PV[row, lane]) if (a, l) == order[0] else (W[a][l, row, lane], M[a][l, row, lane], V[a][l, row, lane])
            g = G[a][l, row, lane].astype(F32) * factor
            m = 0.9 * old[1] + 0.1 * g
            v = 0.95 * old[2] + 0.05 * g * g
            M[a][l, row, lane] = m
            V[a][l, row, lane] = v
            w = old[0].astype(F32)
            new = (w - 0.02 * (m * lax.rsqrt(v + 1e-8) + 0.1 * w)).astype(BF16)
            there = pl.ds(pl.multiple_of(me * rows + (p * r if split else 0) + i * step, step), step)
            N[a][l, there, lane] = new

        loop(r // step, some)

    chunks = []
    for a, l in order:
        for p in range(parts):
            chunks.append((len(chunks), a, l, p))
    for i, a, l, p in chunks:
        if p == 0:
            for copy in loads.get((a, l), ()):
                copy.wait()
        adam(a, l, p)
        if i == 0:
            pl.semaphore_wait(barrier, 2)
        send(i, a, l, p, 0, 0).start()
        send(i, a, l, p, 1, 0).start()
    for step in range(half):
        for i, a, l, p in chunks:
            for way in range(2):
                came(i, a, l, p, way, step)
                if step < half - 1:
                    send(i, a, l, p, way, step + 1).start()
    for i, a, l, p in chunks:
        for way in range(2):
            for step in range(half):
                send(i, a, l, p, way, step).wait_send()


def store_kernel(count, *refs):
    src, dst, sem = refs[:count], refs[count : 2 * count], refs[-1]
    copies = [pltpu.make_async_copy(a, b, sem.at[i]) for i, (a, b) in enumerate(zip(src, dst, strict=True))]
    for copy in copies:
        copy.start()
    for copy in copies:
        copy.wait()


def store(arrays):
    count = len(arrays)
    return pl.pallas_call(
        functools.partial(store_kernel, count),
        out_shape=tuple(jax.ShapeDtypeStruct(t.shape, t.dtype) for t in arrays),
        in_specs=[pl.BlockSpec(memory_space=pltpu.VMEM)] * count,
        out_specs=(pl.BlockSpec(memory_space=pl.ANY),) * count,
        scratch_shapes=[pltpu.SemaphoreType.DMA((count,))],
        compiler_params=pltpu.CompilerParams(vmem_limit_bytes=2**20),
        name="store",
    )(*(pinned(t, pltpu.VMEM) for t in arrays))


def update(n, made, w, m, v):
    layers = w[0].shape[0]
    parts = 2
    chunks = layers * 3 * parts
    count = sum(t.size for t in w)
    any_space = pl.BlockSpec(memory_space=pl.ANY)
    in_vmem = pl.BlockSpec(memory_space=pltpu.VMEM)
    half = n // 2
    g, squares, ahead = made[:3], made[3], made[4:]
    return pl.pallas_call(
        functools.partial(update_kernel, n, float(count), parts),
        out_shape=tuple(kept(t.shape, BF16) for t in w) + tuple(kept(t.shape, F32) for t in m + v),
        in_specs=[in_vmem] * 4 + [any_space] * 3 + [in_vmem] * 3 + [any_space] * 6,
        out_specs=(in_vmem,) * 9,
        scratch_shapes=[pltpu.VMEM(t.shape, BF16) for t in m]
        + [
            pltpu.SemaphoreType.DMA((3, 3, layers)),
            pltpu.SemaphoreType.DMA((chunks, 2, half)),
            pltpu.SemaphoreType.DMA((chunks, 2, half)),
        ],
        compiler_params=pltpu.CompilerParams(collective_id=1, has_side_effects=True, vmem_limit_bytes=12 * 2**20),
        name="update",
    )(
        *(pinned(t, pltpu.VMEM) for t in (*g, squares)),
        *(pinned(t, pltpu.HBM) for t in w),
        *(pinned(t, pltpu.VMEM) for t in ahead),
        *(pinned(t, pltpu.HBM) for t in (*m, *v)),
    )


def solution(mesh):
    n = mesh.shape["dp"]

    def step(x, dy, *arrays):
        w, m, v = (arrays[i : i + 3] for i in (0, 3, 6))
        return store(update(n, gradients(n, x, dy, *w, m[2], v[2]), w, m, v))

    shard = P(None, "dp", None)
    return jax.shard_map(
        step,
        mesh=mesh,
        in_specs=(P(("rep", "dp"), None, None),) * 2 + (P(),) * 3 + (shard,) * 6,
        out_specs=(P("rep", None, None),) * 3 + (P("rep", "dp", None),) * 6,
        check_vma=False,
    )
```

```python
import functools

import jax
import jax.numpy as jnp
from jax import lax
from jax.experimental import pallas as pl
from jax.experimental.pallas import tpu as pltpu
from jax.sharding import PartitionSpec as P

F32 = jnp.float32
BF16 = jnp.bfloat16
MESH = pl.DeviceIdType.MESH
LANES = 128
VMEM_LIMIT = 67043328


def dot(a, b):
    return jnp.dot(a, b, preferred_element_type=F32)


def dot_t(a, b):
    return lax.dot_general(a, b, (((1,), (1,)), ((), ())), preferred_element_type=F32)


def scale_of(wide):
    return lax.rsqrt(jnp.mean(wide * wide, -1, keepdims=True) + 1e-6)


def pinned(t, space):
    return pltpu.with_memory_space_constraint(t, space)


def kept(shape, dtype):
    return pltpu.VMEM(shape, dtype)


def loop(count, body):
    lax.fori_loop(0, count, lambda i, c: (body(i), c)[1], 0)


def at(i, size):
    return pl.ds(pl.multiple_of(i * size, size), size)


def grad_kernel(n, layers, shapes, *refs):
    (x_hbm, dy_hbm, wg_hbm, wu_hbm, wd_hbm, md_hbm, vd_hbm) = refs[:7]
    (OG, OU, OD, ALL, PW, PM, PV) = refs[7:14]
    (A, AT, D, DT, H, ACT, DG, DU, DA, WG, WU, WD, G, RU, RD, SQ, *sems) = refs[14:]
    x_sem, dy_sem, w_sem, ahead_sem, send_sem, recv_sem, sq_send, sq_recv = sems
    tokens, dim, ff, blocks = shapes
    share = ff // n
    tiles = share // LANES
    tile = n * LANES
    tb = tokens // blocks
    half = n // 2
    hr = LANES // 2
    cols = tile // 2
    me = lax.axis_index("dp")
    up, down = lax.rem(me + 1, n), lax.rem(me + n - 1, n)
    ring = lambda d: lax.rem(me + d + n, n)

    def tok(i):
        return at(i, tb)

    def fetch(k):
        slot = lax.rem(k, 2)
        layer = lax.rem(k // tiles, 2)
        t = lax.rem(k, tiles)

        def one(b):
            place = pl.ds(pl.multiple_of(b * share + t * LANES, LANES), LANES)
            here = at(b, LANES)
            pltpu.make_async_copy(wg_hbm.at[layer, :, place], WG.at[slot, :, here], w_sem.at[slot, 0]).start()
            pltpu.make_async_copy(wu_hbm.at[layer, :, place], WU.at[slot, :, here], w_sem.at[slot, 1]).start()
            pltpu.make_async_copy(wd_hbm.at[layer, place, :], WD.at[slot, here, :], w_sem.at[slot, 2]).start()

        loop(n, one)

    def fetched(k):
        slot = lax.rem(k, 2)
        pltpu.make_async_copy(WG.at[slot], WG.at[slot], w_sem.at[slot, 0]).wait()
        pltpu.make_async_copy(WU.at[slot], WU.at[slot], w_sem.at[slot, 1]).wait()
        pltpu.make_async_copy(WD.at[slot], WD.at[slot], w_sem.at[slot, 2]).wait()

    def x_copy(i):
        return pltpu.make_async_copy(x_hbm.at[0, tok(i), :], H.at[tok(i), :], x_sem.at[i])

    def x_again(i):
        return pltpu.make_async_copy(x_hbm.at[0, tok(i), :], ACT.at[tok(i), pl.ds(0, dim)], x_sem.at[i])

    def dy_copy(i):
        return pltpu.make_async_copy(dy_hbm.at[0, tok(i), :], D.at[tok(i), :], dy_sem.at[i])

    barrier = pltpu.get_barrier_semaphore()
    for d in range(1, n):
        pl.semaphore_signal(barrier, inc=1, device_id={"dp": ring(d)}, device_id_type=MESH)

    loop(blocks, lambda i: x_copy(i).start())
    fetch(0)
    loop(blocks, lambda i: dy_copy(i).start())

    def first_norm(i):
        wide = H[tok(i), :].astype(F32)
        A[tok(i), :] = (wide * scale_of(wide)).astype(BF16)
        DA[tok(i), :] = jnp.zeros((tb, dim), F32)

    def forward(k, i):
        slot = lax.rem(k, 2)
        for j in range(2):
            here = pl.ds(j * cols, cols)
            g = dot(A[tok(i), :], WG[slot, :, here])
            u = dot(A[tok(i), :], WU[slot, :, here])
            s = 0.5 * jnp.tanh(0.5 * g) + 0.5
            ACT[tok(i), here] = (g * s * u).astype(BF16)
        DA[tok(i), :] += dot(ACT[tok(i), :], WD[slot])

    def second_norm(i):
        h = (H[tok(i), :].astype(F32) + DA[tok(i), :].astype(BF16).astype(F32)).astype(BF16)
        wide = h.astype(F32)
        return h, (wide * scale_of(wide)).astype(BF16)

    def second_norm_kept(i, h, a):
        H[tok(i), :] = h
        A[tok(i), :] = a
        AT[:, tok(i)] = a.T

    x_copy(0).wait()
    first_norm(0)
    fetched(0)
    fetch(1)

    def opening(i):
        x_copy(i + 1).wait()
        forward(0, i)
        first_norm(i + 1)

    loop(blocks - 1, opening)

    def middle(j):
        q = blocks - 1 + j
        k, i = q // blocks, lax.rem(q, blocks)

        @pl.when(i == 0)
        def _():
            fetched(k)
            fetch(k + 1)

        @pl.when(j < blocks)
        def _():
            dy_copy(j).wait()

        forward(k, i)
        seen = jnp.minimum(j, blocks - 1)
        DT[:, tok(seen)] = D[tok(seen), :].T

    loop((tiles - 2) * blocks + 2, middle)

    def closing(i):
        normed = second_norm(i)
        forward(tiles - 1, i + 1)
        second_norm_kept(i, *normed)

    loop(blocks - 1, closing)
    second_norm_kept(blocks - 1, *second_norm(blocks - 1))

    pl.semaphore_wait(barrier, n - 1)

    def remote(src, dst, slot, u, way, step):
        return pltpu.make_async_remote_copy(
            src_ref=src,
            dst_ref=dst,
            send_sem=send_sem.at[slot, way, step],
            recv_sem=recv_sem.at[u, way, step],
            device_id={"dp": (up, down)[way]},
            device_id_type=MESH,
        )

    low, high, whole = pl.ds(0, hr), pl.ds(hr, hr), pl.ds(0, 2 * hr)
    lands = (RU, RD)

    def rows(step):
        return pl.ds(pl.multiple_of(hr + (step - 1) * 2 * hr, hr), 2 * hr)

    def begin_low(u, slot):
        remote(G.at[slot, ring(half), low], RU.at[u, low], slot, u, 0, 0).start()
        remote(G.at[slot, ring(1 - half), low], RD.at[u, pl.ds(hr, hr)], slot, u, 1, 1).start()

    def begin_high(u, slot):
        remote(G.at[slot, ring(half), high], RD.at[u, low], slot, u, 1, 0).start()
        remote(G.at[slot, ring(half - 1), high], RU.at[u, pl.ds(2 * hr, hr)], slot, u, 0, 1).start()

    def received(u, way, step):
        dst = lands[way].at[u, low] if isinstance(step, int) and step == 0 else lands[way].at[u, rows(step)]
        pltpu.make_async_copy(dst, dst, recv_sem.at[u, way, step]).wait()

    def add(land, place, mine):
        land[place] = (land[place].astype(F32) + mine.astype(F32)).astype(BF16)

    def second_low(u, slot):
        received(u, 0, 0)
        add(RU, (u, low), G[slot, ring(half - 1), low])
        remote(RU.at[u, low], RU.at[u, pl.ds(hr, hr)], slot, u, 0, 1).start()

    def second_high(u, slot):
        received(u, 1, 0)
        add(RD, (u, low), G[slot, ring(1 - half), high])
        remote(RD.at[u, low], RD.at[u, pl.ds(2 * hr, hr)], slot, u, 1, 1).start()

    def later(u, slot, step):
        received(u, 0, step - 1)
        received(u, 1, step - 1)
        add(RU, (u, rows(step - 1)), G[slot, ring(half - step)])
        add(RD, (u, rows(step - 1)), G[slot, ring(step - half)])
        remote(RU.at[u, rows(step - 1)], RU.at[u, rows(step)], slot, u, 0, step).start()
        remote(RD.at[u, rows(step - 1)], RD.at[u, rows(step)], slot, u, 1, step).start()

    def finish(u, slot, which, layer, t):
        received(u, 0, half - 1)
        received(u, 1, half - 1)
        total = G[slot, me].astype(F32) + RU[u, rows(half - 1)].astype(F32) + RD[u, rows(half - 1)].astype(F32)
        total = total.astype(BF16)
        wide = total.astype(F32)
        SQ[...] += jnp.sum((wide * wide).reshape(-1, 8, dim), axis=0)
        if which == 0:
            OD[layer, at(t, LANES), :] = total
        else:
            out = (OG, OU)[which - 1]
            for b in range(n):
                piece = total[hr * (b // (n // 2)) : hr * (b // (n // 2)) + hr, LANES * (b % (n // 2)) : LANES * (b % (n // 2)) + LANES]
                out[layer, :, pl.ds(pl.multiple_of(b * share + t * LANES, LANES), LANES)] = piece
        for way in range(2):
            for step in range(half):
                src = G.at[slot, 0, whole] if step > 0 else G.at[slot, 0, low]
                pltpu.make_async_copy(src, src, send_sem.at[slot, way, step]).wait()

    SQ[...] = jnp.zeros_like(SQ)

    def tile_step(k):
        wk = k + tiles
        slot = lax.rem(wk, 2)
        base = lax.rem(k, 2) * 3
        prev = 3 - base
        u0 = 3 * k
        p0 = u0 - 3
        going = k >= 1
        old_t = lax.rem(k - 1 + tiles, tiles)
        old_layer = jnp.where(k - 1 < tiles, 1, 0)
        fetched(wk)

        @pl.when(k < 2 * tiles - 1)
        def _():
            fetch(wk + 1)

        def when(cond):
            return pl.when(going & cond)

        def hidden(j, i):
            for b, c in ((0, 0), (0, 1), (1, 0), (1, 1)):
                here = pl.ds(pl.multiple_of(j * cols + c * (cols // 2), cols // 2), cols // 2)
                place = tok(2 * i + b)
                g = dot(A[place, :], WG[slot, :, here])
                u = dot(A[place, :], WU[slot, :, here])
                back = dot_t(D[place, :], WD[slot, here, :]).astype(BF16).astype(F32)
                s = 0.5 * jnp.tanh(0.5 * g) + 0.5
                silu = g * s
                ACT[place, here] = (silu * u).astype(BF16)
                DU[place, here] = (back * silu).astype(BF16)
                DG[place, here] = (back * u * (s + silu * (1.0 - s))).astype(BF16)

        def wide_part(src, unit, j):
            part = dot(AT[...], src[:, at(j, cols)]).astype(BF16)
            G[base + unit, :, at(j, hr), :] = part.reshape(n, dim // n, cols)

        def halves(j):
            def some(i):
                hidden(j, i)

                @when((j == 0) & (i == 0))
                def _():
                    later(p0 + 1, prev + 1, 3)

            loop(blocks // 2, some)

            @when(j == 1)
            def _():
                finish(p0 + 1, prev + 1, 1, old_layer, old_t)

            wide_part(DG, 1, j)

            @pl.when(j == 0)
            def _():
                begin_low(u0 + 1, base + 1)

            @when(j == 0)
            def _():
                later(p0, prev, 2)

            @pl.when(j == 1)
            def _():
                begin_high(u0 + 1, base + 1)

            @when(j == 1)
            def _():
                later(p0, prev, 3)

            @pl.when(j == 1)
            def _():
                second_low(u0 + 1, base + 1)

            wide_part(DU, 2, j)

            @pl.when(j == 0)
            def _():
                begin_low(u0 + 2, base + 2)

            @when(j == 0)
            def _():
                later(p0 + 2, prev + 2, 3)

            @pl.when(j == 1)
            def _():
                begin_high(u0 + 2, base + 2)
                second_low(u0 + 2, base + 2)

        loop(2, halves)

        def down_part(j):
            part = dot(DT[...], ACT[:, at(j, cols)])
            flipped = part.T.astype(BF16)
            for b in range(cols // LANES):
                G[base, j * (cols // LANES) + b] = flipped[b * LANES : (b + 1) * LANES]

            @pl.when(j == 0)
            def _():
                second_high(u0 + 1, base + 1)

            @when(j == 0)
            def _():
                finish(p0 + 2, prev + 2, 2, old_layer, old_t)

        loop(2, down_part)
        begin_low(u0, base)
        begin_high(u0, base)

        @pl.when(k == tiles - 1)
        def _():
            loop(blocks, lambda i: x_again(i).start())

        def ring_part(i):
            @pl.when(i == 1)
            def _():
                second_high(u0 + 2, base + 2)

            @when(i == 1)
            def _():
                finish(p0, prev, 0, old_layer, old_t)

            @pl.when(i == 2)
            def _():
                later(u0 + 1, base + 1, 2)

        @pl.when(k < tiles)
        def _():
            def input_part(i):
                so_far = jnp.where(k == 0, 0.0, DA[tok(i), :])
                DA[tok(i), :] = so_far + (dot_t(DG[tok(i), :], WG[slot]) + dot_t(DU[tok(i), :], WU[slot]))
                ring_part(i)

            loop(blocks, input_part)

        @pl.when(k >= tiles)
        def _():
            loop(blocks, ring_part)

        @pl.when(k == tiles - 1)
        def _():
            def between(i):
                h = H[tok(i), :].astype(F32)
                da = DA[tok(i), :].astype(BF16).astype(F32)
                r = scale_of(h)
                dh = (r * da - h * (r * r * r * jnp.mean(h * da, -1, keepdims=True))).astype(BF16)
                d = (D[tok(i), :].astype(F32) + dh.astype(F32)).astype(BF16)
                D[tok(i), :] = d
                DT[:, tok(i)] = d.T
                x_again(i).wait()
                wide = ACT[tok(i), pl.ds(0, dim)].astype(F32)
                a = (wide * scale_of(wide)).astype(BF16)
                A[tok(i), :] = a
                AT[:, tok(i)] = a.T

                @pl.when(i == 1)
                def _():
                    second_low(u0, base)
                    second_high(u0, base)

            loop(blocks, between)

        @pl.when(k != tiles - 1)
        def _():
            second_low(u0, base)
            second_high(u0, base)

        later(u0 + 2, base + 2, 2)

    loop(2 * tiles, tile_step)

    ahead = (
        pltpu.make_async_copy(wd_hbm.at[layers - 1, at(me, share), :], PW, ahead_sem.at[0]),
        pltpu.make_async_copy(md_hbm.at[layers - 1], PM, ahead_sem.at[1]),
        pltpu.make_async_copy(vd_hbm.at[layers - 1], PV, ahead_sem.at[2]),
    )
    for copy in ahead:
        copy.start()

    end = 2 * tiles - 1
    u0, base = 3 * end, (end % 2) * 3
    later(u0 + 1, base + 1, 3)
    later(u0, base, 2)
    later(u0 + 2, base + 2, 3)
    later(u0, base, 3)
    for j in (1, 2, 0):
        finish(u0 + j, base + j, j, 0, tiles - 1)

    squares = SQ[:, :LANES]
    for j in range(1, dim // LANES):
        squares += SQ[:, j * LANES : (j + 1) * LANES]
    ALL[me] = squares

    def tell(d):
        return pltpu.make_async_remote_copy(
            src_ref=ALL.at[me],
            dst_ref=ALL.at[me],
            send_sem=sq_send.at[d],
            recv_sem=sq_recv.at[d],
            device_id={"dp": ring(d)},
            device_id_type=MESH,
        )

    for d in range(1, n):
        tell(d).start()
    for d in range(1, n):
        tell(d).wait()
    for copy in ahead:
        copy.wait()


def gradients(n, x, dy, w_gate, w_up, w_down, m_down, v_down):
    layers, dim, ff = w_gate.shape
    tokens = x.shape[1]
    blocks = 4
    share = ff // n
    tiles = share // LANES
    tile = n * LANES
    units = 3 * layers * tiles
    half = n // 2
    land = LANES // 2 + LANES * (half - 1)
    any_space = pl.BlockSpec(memory_space=pl.ANY)
    return pl.pallas_call(
        functools.partial(grad_kernel, n, layers, (tokens, dim, ff, blocks)),
        out_shape=tuple(
            kept(shape, dtype)
            for shape, dtype in (
                ((layers, dim // n, ff), BF16),
                ((layers, dim // n, ff), BF16),
                ((layers, share, dim), BF16),
                ((n, 8, LANES), F32),
                ((share, dim), BF16),
                ((share, dim), F32),
                ((share, dim), F32),
            )
        ),
        in_specs=[any_space] * 7,
        out_specs=(pl.BlockSpec(memory_space=pltpu.VMEM),) * 7,
        scratch_shapes=[
            pltpu.VMEM((tokens, dim), BF16),
            pltpu.VMEM((dim, tokens), BF16),
            pltpu.VMEM((tokens, dim), BF16),
            pltpu.VMEM((dim, tokens), BF16),
            pltpu.VMEM((tokens, dim), BF16),
            pltpu.VMEM((tokens, tile), BF16),
            pltpu.VMEM((tokens, tile), BF16),
            pltpu.VMEM((tokens, tile), BF16),
            pltpu.VMEM((tokens, dim), F32),
            pltpu.VMEM((2, dim, tile), BF16),
            pltpu.VMEM((2, dim, tile), BF16),
            pltpu.VMEM((2, tile, dim), BF16),
            pltpu.VMEM((6, n, LANES, dim), BF16),
            pltpu.VMEM((units, land, dim), BF16),
            pltpu.VMEM((units, land, dim), BF16),
            pltpu.VMEM((8, dim), F32),
            pltpu.SemaphoreType.DMA((blocks,)),
            pltpu.SemaphoreType.DMA((blocks,)),
            pltpu.SemaphoreType.DMA((2, 3)),
            pltpu.SemaphoreType.DMA((3,)),
            pltpu.SemaphoreType.DMA((6, 2, half)),
            pltpu.SemaphoreType.DMA((units, 2, half)),
            pltpu.SemaphoreType.DMA((n,)),
            pltpu.SemaphoreType.DMA((n,)),
        ],
        compiler_params=pltpu.CompilerParams(collective_id=0, has_side_effects=True, vmem_limit_bytes=59 * 2**20),
        name="grads",
    )(*(pinned(t, pltpu.HBM) for t in (x, dy, w_gate, w_up, w_down, m_down, v_down)))


def update_kernel(n, count, parts, *refs):
    G, w_hbm, m_hbm, v_hbm = (refs[i : i + 3] for i in (0, 4, 10, 13))
    SQ, PW, PM, PV = refs[3], *refs[7:10]
    N, M, V = (refs[i : i + 3] for i in (16, 19, 22))
    W = refs[25:28]
    in_sem, send_sem, recv_sem = refs[28:]
    me = lax.axis_index("dp")
    half = n // 2
    up, down = lax.rem(me + 1, n), lax.rem(me + n - 1, n)
    ring = lambda d: lax.rem(me + d + n, n)
    layers = G[0].shape[0]

    barrier = pltpu.get_barrier_semaphore()
    for peer in (up, down):
        pl.semaphore_signal(barrier, inc=1, device_id={"dp": peer}, device_id_type=MESH)

    order = [(a, l) for l in reversed(range(layers)) for a in (2, 0, 1)]
    loads = {}
    for a, l in order[1:]:
        rows = G[a].shape[1]
        own = pl.ds(pl.multiple_of(me * rows, rows), rows)
        loads[a, l] = (
            pltpu.make_async_copy(w_hbm[a].at[l, own, :], W[a].at[l], in_sem.at[0, a, l]),
            pltpu.make_async_copy(m_hbm[a].at[l], M[a].at[l], in_sem.at[1, a, l]),
            pltpu.make_async_copy(v_hbm[a].at[l], V[a].at[l], in_sem.at[2, a, l]),
        )
    total = jnp.sum(jnp.sum(SQ[...], axis=0), axis=(0, 1), keepdims=True)
    factor = jnp.minimum(1.0, 0.5 * lax.rsqrt(total / count + 1e-30))

    def shape(a):
        rows, cols = G[a].shape[1:]
        return (rows, cols // parts, 0) if a < 2 else (rows // parts, cols, 1)

    def place(a, l, p, owner, part):
        rows = G[a].shape[1]
        r, c, split = shape(a)
        hr = r // 2
        start = owner * rows + (p * r if split else 0)
        start, size = (start, r) if part == 2 else (start + part * hr, hr)
        return (l, pl.ds(pl.multiple_of(start, hr), size), pl.ds(0 if split else p * c, c))

    def send(i, a, l, p, way, step):
        owner = ring(-step) if way == 0 else ring(step)
        ref = N[a].at[place(a, l, p, owner, 2 if step < half - 1 else way)]
        return pltpu.make_async_remote_copy(
            src_ref=ref,
            dst_ref=ref,
            send_sem=send_sem.at[i, way, step],
            recv_sem=recv_sem.at[i, way, step],
            device_id={"dp": (up, down)[way]},
            device_id_type=MESH,
        )

    def came(i, a, l, p, way, step):
        owner = ring(-step - 1) if way == 0 else ring(step + 1)
        where = place(a, l, p, owner, 2 if step < half - 1 else way)
        ref = N[a].at[where]
        pltpu.make_async_copy(ref, ref, recv_sem.at[i, way, step]).wait()

    def adam(a, l, p):
        r, c, split = shape(a)
        rows = G[a].shape[1]
        step = 32
        lane = pl.ds(0 if split else p * c, c)

        def some(i):
            row = pl.ds(pl.multiple_of((p * r if split else 0) + i * step, step), step)
            old = (PW[row, lane], PM[row, lane], PV[row, lane]) if (a, l) == order[0] else (W[a][l, row, lane], M[a][l, row, lane], V[a][l, row, lane])
            g = G[a][l, row, lane].astype(F32) * factor
            m = 0.9 * old[1] + 0.1 * g
            v = 0.95 * old[2] + 0.05 * g * g
            M[a][l, row, lane] = m
            V[a][l, row, lane] = v
            w = old[0].astype(F32)
            new = (w - 0.02 * (m * lax.rsqrt(v + 1e-8) + 0.1 * w)).astype(BF16)
            there = pl.ds(pl.multiple_of(me * rows + (p * r if split else 0) + i * step, step), step)
            N[a][l, there, lane] = new

        loop(r // step, some)

    chunks = []
    for a, l in order:
        for p in range(parts):
            chunks.append((len(chunks), a, l, p))
    for i, a, l, p in chunks:
        if p == 0:
            for copy in loads.get((a, l), ()):
                copy.wait()
        adam(a, l, p)
        if i == 0:
            pl.semaphore_wait(barrier, 2)
        send(i, a, l, p, 0, 0).start()
        send(i, a, l, p, 1, 0).start()
        if i == 0:
            for copies in loads.values():
                for copy in copies:
                    copy.start()
    for step in range(half):
        for i, a, l, p in chunks:
            for way in range(2):
                came(i, a, l, p, way, step)
                if step < half - 1:
                    send(i, a, l, p, way, step + 1).start()
    for i, a, l, p in chunks:
        for way in range(2):
            for step in range(half):
                send(i, a, l, p, way, step).wait_send()


def store_kernel(count, *refs):
    src, dst, sem = refs[:count], refs[count : 2 * count], refs[-1]
    copies = [
        pltpu.make_async_copy(a.at[l], b.at[l], sem.at[i, l])
        for i, (a, b) in enumerate(zip(src, dst, strict=True))
        for l in range(a.shape[0])
    ]
    for copy in copies:
        copy.start()
    for copy in copies:
        copy.wait()


def store(arrays):
    count = len(arrays)
    return pl.pallas_call(
        functools.partial(store_kernel, count),
        out_shape=tuple(jax.ShapeDtypeStruct(t.shape, t.dtype) for t in arrays),
        in_specs=[pl.BlockSpec(memory_space=pltpu.VMEM)] * count,
        out_specs=(pl.BlockSpec(memory_space=pl.ANY),) * count,
        scratch_shapes=[pltpu.SemaphoreType.DMA((count, arrays[0].shape[0]))],
        compiler_params=pltpu.CompilerParams(vmem_limit_bytes=2**20),
        name="store",
    )(*(pinned(t, pltpu.VMEM) for t in arrays))


def update(n, made, w, m, v):
    layers = w[0].shape[0]
    parts = 2
    chunks = layers * 3 * parts
    count = sum(t.size for t in w)
    any_space = pl.BlockSpec(memory_space=pl.ANY)
    in_vmem = pl.BlockSpec(memory_space=pltpu.VMEM)
    half = n // 2
    g, squares, ahead = made[:3], made[3], made[4:]
    return pl.pallas_call(
        functools.partial(update_kernel, n, float(count), parts),
        out_shape=tuple(kept(t.shape, BF16) for t in w) + tuple(kept(t.shape, F32) for t in m + v),
        in_specs=[in_vmem] * 4 + [any_space] * 3 + [in_vmem] * 3 + [any_space] * 6,
        out_specs=(in_vmem,) * 9,
        scratch_shapes=[pltpu.VMEM(t.shape, BF16) for t in m]
        + [
            pltpu.SemaphoreType.DMA((3, 3, layers)),
            pltpu.SemaphoreType.DMA((chunks, 2, half)),
            pltpu.SemaphoreType.DMA((chunks, 2, half)),
        ],
        compiler_params=pltpu.CompilerParams(collective_id=1, has_side_effects=True, vmem_limit_bytes=12 * 2**20),
        name="update",
    )(
        *(pinned(t, pltpu.VMEM) for t in (*g, squares)),
        *(pinned(t, pltpu.HBM) for t in w),
        *(pinned(t, pltpu.VMEM) for t in ahead),
        *(pinned(t, pltpu.HBM) for t in (*m, *v)),
    )


def solution(mesh):
    n = mesh.shape["dp"]

    def step(x, dy, *arrays):
        w, m, v = (arrays[i : i + 3] for i in (0, 3, 6))
        return store(update(n, gradients(n, x, dy, *w, m[2], v[2]), w, m, v))

    shard = P(None, "dp", None)
    return jax.shard_map(
        step,
        mesh=mesh,
        in_specs=(P(("rep", "dp"), None, None),) * 2 + (P(),) * 3 + (shard,) * 6,
        out_specs=(P("rep", None, None),) * 3 + (P("rep", "dp", None),) * 6,
        check_vma=False,
    )
```

```python
import functools

import jax
import jax.numpy as jnp
from jax import lax
from jax.experimental import pallas as pl
from jax.experimental.pallas import tpu as pltpu
from jax.sharding import PartitionSpec as P

F32 = jnp.float32
BF16 = jnp.bfloat16
MESH = pl.DeviceIdType.MESH
LANES = 128
LATE = 2


def dot(a, b):
    return jnp.dot(a, b, preferred_element_type=F32)


def dot_t(a, b):
    return lax.dot_general(a, b, (((1,), (1,)), ((), ())), preferred_element_type=F32)


def scale_of(wide):
    return lax.rsqrt(jnp.mean(wide * wide, -1, keepdims=True) + 1e-6)


def pinned(t, space):
    return pltpu.with_memory_space_constraint(t, space)


def kept(shape, dtype):
    return pltpu.VMEM(shape, dtype)


def loop(count, body):
    lax.fori_loop(0, count, lambda i, c: (body(i), c)[1], 0)


def at(i, size):
    return pl.ds(pl.multiple_of(i * size, size), size)


def grad_kernel(n, layers, shapes, *refs):
    (x_hbm, dy_hbm, wg_hbm, wu_hbm, wd_hbm, md_hbm, vd_hbm) = refs[:7]
    (OG, OU, OD, ALL, PW, PM, PV) = refs[7:14]
    (A, AT, D, DT, H, ACT, DG, DU, DA, WG, WU, WD, G, RU, RD, SQ, *sems) = refs[14:]
    x_sem, dy_sem, w_sem, ahead_sem, send_sem, recv_sem, sq_send, sq_recv = sems
    tokens, dim, ff, blocks = shapes
    share = ff // n
    tiles = share // LANES
    tile = n * LANES
    tb = tokens // blocks
    half = n // 2
    hr = LANES // 2
    cols = tile // 2
    me = lax.axis_index("dp")
    up, down = lax.rem(me + 1, n), lax.rem(me + n - 1, n)
    ring = lambda d: lax.rem(me + d + n, n)

    def tok(i):
        return at(i, tb)

    def fetch(k):
        slot = lax.rem(k, 2)
        layer = lax.rem(k // tiles, 2)
        t = lax.rem(k, tiles)

        def one(b):
            place = pl.ds(pl.multiple_of(b * share + t * LANES, LANES), LANES)
            here = at(b, LANES)
            pltpu.make_async_copy(wg_hbm.at[layer, :, place], WG.at[slot, :, here], w_sem.at[slot, 0]).start()
            pltpu.make_async_copy(wu_hbm.at[layer, :, place], WU.at[slot, :, here], w_sem.at[slot, 1]).start()
            pltpu.make_async_copy(wd_hbm.at[layer, place, :], WD.at[slot, here, :], w_sem.at[slot, 2]).start()

        loop(n, one)

    def fetched(k):
        slot = lax.rem(k, 2)
        pltpu.make_async_copy(WG.at[slot], WG.at[slot], w_sem.at[slot, 0]).wait()
        pltpu.make_async_copy(WU.at[slot], WU.at[slot], w_sem.at[slot, 1]).wait()
        pltpu.make_async_copy(WD.at[slot], WD.at[slot], w_sem.at[slot, 2]).wait()

    def x_copy(i):
        return pltpu.make_async_copy(x_hbm.at[0, tok(i), :], H.at[tok(i), :], x_sem.at[i])

    def x_again(i):
        return pltpu.make_async_copy(x_hbm.at[0, tok(i), :], ACT.at[tok(i), pl.ds(0, dim)], x_sem.at[i])

    def dy_copy(i):
        return pltpu.make_async_copy(dy_hbm.at[0, tok(i), :], D.at[tok(i), :], dy_sem.at[i])

    barrier = pltpu.get_barrier_semaphore()
    for d in range(1, n):
        pl.semaphore_signal(barrier, inc=1, device_id={"dp": ring(d)}, device_id_type=MESH)

    loop(blocks, lambda i: x_copy(i).start())
    fetch(0)
    loop(blocks, lambda i: dy_copy(i).start())

    def first_norm(i):
        wide = H[tok(i), :].astype(F32)
        A[tok(i), :] = (wide * scale_of(wide)).astype(BF16)
        DA[tok(i), :] = jnp.zeros((tb, dim), F32)

    def forward(k, i):
        slot = lax.rem(k, 2)
        for j in range(2):
            here = pl.ds(j * cols, cols)
            g = dot(A[tok(i), :], WG[slot, :, here])
            u = dot(A[tok(i), :], WU[slot, :, here])
            s = 0.5 * jnp.tanh(0.5 * g) + 0.5
            ACT[tok(i), here] = (g * s * u).astype(BF16)
        DA[tok(i), :] += dot(ACT[tok(i), :], WD[slot])

    def second_norm(i):
        h = (H[tok(i), :].astype(F32) + DA[tok(i), :].astype(BF16).astype(F32)).astype(BF16)
        wide = h.astype(F32)
        return h, (wide * scale_of(wide)).astype(BF16)

    def second_norm_kept(i, h, a):
        H[tok(i), :] = h
        A[tok(i), :] = a
        AT[:, tok(i)] = a.T

    x_copy(0).wait()
    first_norm(0)
    fetched(0)
    fetch(1)

    def opening(i):
        x_copy(i + 1).wait()
        forward(0, i)
        first_norm(i + 1)

    loop(blocks - 1, opening)

    def middle(j):
        q = blocks - 1 + j
        k, i = q // blocks, lax.rem(q, blocks)

        @pl.when(i == 0)
        def _():
            fetched(k)
            fetch(k + 1)

        @pl.when(j < blocks)
        def _():
            dy_copy(j).wait()

        forward(k, i)
        seen = jnp.minimum(j, blocks - 1)
        DT[:, tok(seen)] = D[tok(seen), :].T

    loop((tiles - 2) * blocks + 2, middle)

    def closing(i):
        normed = second_norm(i)
        forward(tiles - 1, i + 1)
        second_norm_kept(i, *normed)

    loop(blocks - 1, closing)
    second_norm_kept(blocks - 1, *second_norm(blocks - 1))

    pl.semaphore_wait(barrier, n - 1)

    def remote(src, dst, slot, u, way, step):
        return pltpu.make_async_remote_copy(
            src_ref=src,
            dst_ref=dst,
            send_sem=send_sem.at[slot, way, step],
            recv_sem=recv_sem.at[u, way, step],
            device_id={"dp": (up, down)[way]},
            device_id_type=MESH,
        )

    low, high, whole = pl.ds(0, hr), pl.ds(hr, hr), pl.ds(0, 2 * hr)
    lands = (RU, RD)

    def rows(step):
        return pl.ds(pl.multiple_of(hr + (step - 1) * 2 * hr, hr), 2 * hr)

    def begin_low(u, slot):
        remote(G.at[slot, ring(half), low], RU.at[u, low], slot, u, 0, 0).start()
        remote(G.at[slot, ring(1 - half), low], RD.at[u, pl.ds(hr, hr)], slot, u, 1, 1).start()

    def begin_high(u, slot):
        remote(G.at[slot, ring(half), high], RD.at[u, low], slot, u, 1, 0).start()
        remote(G.at[slot, ring(half - 1), high], RU.at[u, pl.ds(2 * hr, hr)], slot, u, 0, 1).start()

    def received(u, way, step):
        dst = lands[way].at[u, low] if isinstance(step, int) and step == 0 else lands[way].at[u, rows(step)]
        pltpu.make_async_copy(dst, dst, recv_sem.at[u, way, step]).wait()

    def add(land, place, mine):
        land[place] = (land[place].astype(F32) + mine.astype(F32)).astype(BF16)

    def second_low(u, slot):
        received(u, 0, 0)
        add(RU, (u, low), G[slot, ring(half - 1), low])
        remote(RU.at[u, low], RU.at[u, pl.ds(hr, hr)], slot, u, 0, 1).start()

    def second_high(u, slot):
        received(u, 1, 0)
        add(RD, (u, low), G[slot, ring(1 - half), high])
        remote(RD.at[u, low], RD.at[u, pl.ds(2 * hr, hr)], slot, u, 1, 1).start()

    def later(u, slot, step):
        received(u, 0, step - 1)
        received(u, 1, step - 1)
        add(RU, (u, rows(step - 1)), G[slot, ring(half - step)])
        add(RD, (u, rows(step - 1)), G[slot, ring(step - half)])
        remote(RU.at[u, rows(step - 1)], RU.at[u, rows(step)], slot, u, 0, step).start()
        remote(RD.at[u, rows(step - 1)], RD.at[u, rows(step)], slot, u, 1, step).start()

    def finish(u, slot, which, layer, t):
        received(u, 0, half - 1)
        received(u, 1, half - 1)
        total = G[slot, me].astype(F32) + RU[u, rows(half - 1)].astype(F32) + RD[u, rows(half - 1)].astype(F32)
        total = total.astype(BF16)
        wide = total.astype(F32)
        SQ[...] += jnp.sum((wide * wide).reshape(-1, 8, dim), axis=0)
        if which == 0:
            OD[layer, at(t, LANES), :] = total
        else:
            out = (OG, OU)[which - 1]
            for b in range(n):
                piece = total[hr * (b // (n // 2)) : hr * (b // (n // 2)) + hr, LANES * (b % (n // 2)) : LANES * (b % (n // 2)) + LANES]
                out[layer, :, pl.ds(pl.multiple_of(b * share + t * LANES, LANES), LANES)] = piece
        for way in range(2):
            for step in range(half):
                src = G.at[slot, 0, whole] if step > 0 else G.at[slot, 0, low]
                pltpu.make_async_copy(src, src, send_sem.at[slot, way, step]).wait()

    SQ[...] = jnp.zeros_like(SQ)

    def tile_step(k):
        wk = k + tiles
        slot = lax.rem(wk, 2)
        base = lax.rem(k, 2) * 3
        prev = 3 - base
        u0 = 3 * k
        p0 = u0 - 3
        going = k >= 1
        old_t = lax.rem(k - 1 + tiles, tiles)
        old_layer = jnp.where(k - 1 < tiles, 1, 0)
        fetched(wk)

        @pl.when(k < 2 * tiles - 1)
        def _():
            fetch(wk + 1)

        def when(cond):
            return pl.when(going & cond)

        def hidden(j, i):
            for b, c in ((0, 0), (0, 1), (1, 0), (1, 1)):
                here = pl.ds(pl.multiple_of(j * cols + c * (cols // 2), cols // 2), cols // 2)
                place = tok(2 * i + b)
                g = dot(A[place, :], WG[slot, :, here])
                u = dot(A[place, :], WU[slot, :, here])
                back = dot_t(D[place, :], WD[slot, here, :]).astype(BF16).astype(F32)
                s = 0.5 * jnp.tanh(0.5 * g) + 0.5
                silu = g * s
                ACT[place, here] = (silu * u).astype(BF16)
                DU[place, here] = (back * silu).astype(BF16)
                DG[place, here] = (back * u * (s + silu * (1.0 - s))).astype(BF16)

        def wide_part(src, unit, j):
            part = dot(AT[...], src[:, at(j, cols)]).astype(BF16)
            G[base + unit, :, at(j, hr), :] = part.reshape(n, dim // n, cols)

        def halves(j):
            def some(i):
                hidden(j, i)

                @when((j == 0) & (i == 0))
                def _():
                    later(p0 + 1, prev + 1, 3)

            loop(blocks // 2, some)

            @when(j == 1)
            def _():
                finish(p0 + 1, prev + 1, 1, old_layer, old_t)

            wide_part(DG, 1, j)

            @pl.when(j == 0)
            def _():
                begin_low(u0 + 1, base + 1)

            @when(j == 0)
            def _():
                later(p0, prev, 2)

            @pl.when(j == 1)
            def _():
                begin_high(u0 + 1, base + 1)

            @when(j == 1)
            def _():
                later(p0, prev, 3)

            @pl.when(j == 1)
            def _():
                second_low(u0 + 1, base + 1)

            wide_part(DU, 2, j)

            @pl.when(j == 0)
            def _():
                begin_low(u0 + 2, base + 2)

            @when(j == 0)
            def _():
                later(p0 + 2, prev + 2, 3)

            @pl.when(j == 1)
            def _():
                begin_high(u0 + 2, base + 2)
                second_low(u0 + 2, base + 2)

        loop(2, halves)

        def down_part(j):
            part = dot(DT[...], ACT[:, at(j, cols)])
            flipped = part.T.astype(BF16)
            for b in range(cols // LANES):
                G[base, j * (cols // LANES) + b] = flipped[b * LANES : (b + 1) * LANES]

            @pl.when(j == 0)
            def _():
                second_high(u0 + 1, base + 1)

            @when(j == 0)
            def _():
                finish(p0 + 2, prev + 2, 2, old_layer, old_t)

        loop(2, down_part)
        begin_low(u0, base)
        begin_high(u0, base)

        @pl.when(k == tiles - 1)
        def _():
            loop(blocks, lambda i: x_again(i).start())

        def ring_part(i):
            @pl.when(i == 1)
            def _():
                second_high(u0 + 2, base + 2)

            @when(i == 1)
            def _():
                finish(p0, prev, 0, old_layer, old_t)

            @pl.when(i == 2)
            def _():
                later(u0 + 1, base + 1, 2)

        @pl.when(k < tiles)
        def _():
            def input_part(i):
                so_far = jnp.where(k == 0, 0.0, DA[tok(i), :])
                DA[tok(i), :] = so_far + (dot_t(DG[tok(i), :], WG[slot]) + dot_t(DU[tok(i), :], WU[slot]))
                ring_part(i)

            loop(blocks, input_part)

        @pl.when(k >= tiles)
        def _():
            loop(blocks, ring_part)

        @pl.when(k == tiles - 1)
        def _():
            def between(i):
                h = H[tok(i), :].astype(F32)
                da = DA[tok(i), :].astype(BF16).astype(F32)
                r = scale_of(h)
                dh = (r * da - h * (r * r * r * jnp.mean(h * da, -1, keepdims=True))).astype(BF16)
                d = (D[tok(i), :].astype(F32) + dh.astype(F32)).astype(BF16)
                D[tok(i), :] = d
                DT[:, tok(i)] = d.T
                x_again(i).wait()
                wide = ACT[tok(i), pl.ds(0, dim)].astype(F32)
                a = (wide * scale_of(wide)).astype(BF16)
                A[tok(i), :] = a
                AT[:, tok(i)] = a.T

                @pl.when(i == 1)
                def _():
                    second_low(u0, base)
                    second_high(u0, base)

            loop(blocks, between)

        @pl.when(k != tiles - 1)
        def _():
            second_low(u0, base)
            second_high(u0, base)

        later(u0 + 2, base + 2, 2)

    loop(2 * tiles, tile_step)

    ahead = (
        pltpu.make_async_copy(wd_hbm.at[layers - 1, at(me, share), :], PW, ahead_sem.at[0]),
        pltpu.make_async_copy(md_hbm.at[layers - 1], PM, ahead_sem.at[1]),
        pltpu.make_async_copy(vd_hbm.at[layers - 1], PV, ahead_sem.at[2]),
    )
    for copy in ahead:
        copy.start()

    end = 2 * tiles - 1
    u0, base = 3 * end, (end % 2) * 3
    later(u0 + 1, base + 1, 3)
    later(u0, base, 2)
    later(u0 + 2, base + 2, 3)
    later(u0, base, 3)
    for j in (1, 2, 0):
        finish(u0 + j, base + j, j, 0, tiles - 1)

    squares = SQ[:, :LANES]
    for j in range(1, dim // LANES):
        squares += SQ[:, j * LANES : (j + 1) * LANES]
    ALL[me] = squares

    def tell(d):
        return pltpu.make_async_remote_copy(
            src_ref=ALL.at[me],
            dst_ref=ALL.at[me],
            send_sem=sq_send.at[d],
            recv_sem=sq_recv.at[d],
            device_id={"dp": ring(d)},
            device_id_type=MESH,
        )

    for d in range(1, n):
        tell(d).start()
    for d in range(1, n):
        tell(d).wait()
    for copy in ahead:
        copy.wait()


def gradients(n, x, dy, w_gate, w_up, w_down, m_down, v_down):
    layers, dim, ff = w_gate.shape
    tokens = x.shape[1]
    blocks = 4
    share = ff // n
    tiles = share // LANES
    tile = n * LANES
    units = 3 * layers * tiles
    half = n // 2
    land = LANES // 2 + LANES * (half - 1)
    any_space = pl.BlockSpec(memory_space=pl.ANY)
    return pl.pallas_call(
        functools.partial(grad_kernel, n, layers, (tokens, dim, ff, blocks)),
        out_shape=tuple(
            kept(shape, dtype)
            for shape, dtype in (
                ((layers, dim // n, ff), BF16),
                ((layers, dim // n, ff), BF16),
                ((layers, share, dim), BF16),
                ((n, 8, LANES), F32),
                ((share, dim), BF16),
                ((share, dim), F32),
                ((share, dim), F32),
            )
        ),
        in_specs=[any_space] * 7,
        out_specs=(pl.BlockSpec(memory_space=pltpu.VMEM),) * 7,
        scratch_shapes=[
            pltpu.VMEM((tokens, dim), BF16),
            pltpu.VMEM((dim, tokens), BF16),
            pltpu.VMEM((tokens, dim), BF16),
            pltpu.VMEM((dim, tokens), BF16),
            pltpu.VMEM((tokens, dim), BF16),
            pltpu.VMEM((tokens, tile), BF16),
            pltpu.VMEM((tokens, tile), BF16),
            pltpu.VMEM((tokens, tile), BF16),
            pltpu.VMEM((tokens, dim), F32),
            pltpu.VMEM((2, dim, tile), BF16),
            pltpu.VMEM((2, dim, tile), BF16),
            pltpu.VMEM((2, tile, dim), BF16),
            pltpu.VMEM((6, n, LANES, dim), BF16),
            pltpu.VMEM((units, land, dim), BF16),
            pltpu.VMEM((units, land, dim), BF16),
            pltpu.VMEM((8, dim), F32),
            pltpu.SemaphoreType.DMA((blocks,)),
            pltpu.SemaphoreType.DMA((blocks,)),
            pltpu.SemaphoreType.DMA((2, 3)),
            pltpu.SemaphoreType.DMA((3,)),
            pltpu.SemaphoreType.DMA((6, 2, half)),
            pltpu.SemaphoreType.DMA((units, 2, half)),
            pltpu.SemaphoreType.DMA((n,)),
            pltpu.SemaphoreType.DMA((n,)),
        ],
        compiler_params=pltpu.CompilerParams(collective_id=0, has_side_effects=True, vmem_limit_bytes=59 * 2**20),
        name="grads",
    )(*(pinned(t, pltpu.HBM) for t in (x, dy, w_gate, w_up, w_down, m_down, v_down)))


def update_kernel(n, count, parts, *refs):
    G, w_hbm, m_hbm, v_hbm = (refs[i : i + 3] for i in (0, 4, 10, 13))
    SQ, PW, PM, PV = refs[3], *refs[7:10]
    N, M, V = (refs[i : i + 3] for i in (16, 19, 22))
    last = refs[25:27]
    W = refs[27:30]
    in_sem, last_sem, send_sem, recv_sem = refs[30:]
    me = lax.axis_index("dp")
    half = n // 2
    up, down = lax.rem(me + 1, n), lax.rem(me + n - 1, n)
    ring = lambda d: lax.rem(me + d + n, n)
    layers = G[0].shape[0]

    barrier = pltpu.get_barrier_semaphore()
    for peer in (up, down):
        pl.semaphore_signal(barrier, inc=1, device_id={"dp": peer}, device_id_type=MESH)

    order = [(a, l) for l in reversed(range(layers)) for a in (2, 0, 1)]
    loads = {}
    for a, l in order[1:]:
        rows = G[a].shape[1]
        own = pl.ds(pl.multiple_of(me * rows, rows), rows)
        loads[a, l] = (
            pltpu.make_async_copy(w_hbm[a].at[l, own, :], W[a].at[l], in_sem.at[0, a, l]),
            pltpu.make_async_copy(m_hbm[a].at[l], M[a].at[l], in_sem.at[1, a, l]),
            pltpu.make_async_copy(v_hbm[a].at[l], V[a].at[l], in_sem.at[2, a, l]),
        )
    total = jnp.sum(jnp.sum(SQ[...], axis=0), axis=(0, 1), keepdims=True)
    factor = jnp.minimum(1.0, 0.5 * lax.rsqrt(total / count + 1e-30))

    def shape(a):
        rows, cols = G[a].shape[1:]
        return (rows, cols // parts, 0) if a < 2 else (rows // parts, cols, 1)

    def place(a, l, p, owner, part):
        rows = G[a].shape[1]
        r, c, split = shape(a)
        hr = r // 2
        start = owner * rows + (p * r if split else 0)
        start, size = (start, r) if part == 2 else (start + part * hr, hr)
        return (l, pl.ds(pl.multiple_of(start, hr), size), pl.ds(0 if split else p * c, c))

    def send(i, a, l, p, way, step):
        owner = ring(-step) if way == 0 else ring(step)
        ref = N[a].at[place(a, l, p, owner, 2 if step < half - 1 else way)]
        return pltpu.make_async_remote_copy(
            src_ref=ref,
            dst_ref=ref,
            send_sem=send_sem.at[i, way, step],
            recv_sem=recv_sem.at[i, way, step],
            device_id={"dp": (up, down)[way]},
            device_id_type=MESH,
        )

    def came(i, a, l, p, way, step):
        owner = ring(-step - 1) if way == 0 else ring(step + 1)
        where = place(a, l, p, owner, 2 if step < half - 1 else way)
        ref = N[a].at[where]
        pltpu.make_async_copy(ref, ref, recv_sem.at[i, way, step]).wait()

    def adam(a, l, p):
        r, c, split = shape(a)
        rows = G[a].shape[1]
        step = 32
        lane = pl.ds(0 if split else p * c, c)

        def some(i):
            row = pl.ds(pl.multiple_of((p * r if split else 0) + i * step, step), step)
            old = (PW[row, lane], PM[row, lane], PV[row, lane]) if (a, l) == order[0] else (W[a][l, row, lane], M[a][l, row, lane], V[a][l, row, lane])
            g = G[a][l, row, lane].astype(F32) * factor
            m = 0.9 * old[1] + 0.1 * g
            v = 0.95 * old[2] + 0.05 * g * g
            M[a][l, row, lane] = m
            V[a][l, row, lane] = v
            w = old[0].astype(F32)
            new = (w - 0.02 * (m * lax.rsqrt(v + 1e-8) + 0.1 * w)).astype(BF16)
            there = pl.ds(pl.multiple_of(me * rows + (p * r if split else 0) + i * step, step), step)
            N[a][l, there, lane] = new

        loop(r // step, some)

    chunks = []
    for a, l in order:
        for p in range(parts):
            chunks.append((len(chunks), a, l, p))
    for i, a, l, p in chunks:
        if p == 0:
            for copy in loads.get((a, l), ()):
                copy.wait()
        adam(a, l, p)
        if i == 0:
            pl.semaphore_wait(barrier, 2)
        send(i, a, l, p, 0, 0).start()
        send(i, a, l, p, 1, 0).start()
        if i == 0:
            for copies in loads.values():
                for copy in copies:
                    copy.start()
    late = order[len(order) - LATE :]

    def hops(a, l):
        return half - 1 if (a, l) in late else half

    def to_permute(a, l, way):
        rows = G[a].shape[1]
        owner = ring(1 - half) if way == 0 else ring(half - 1)
        src = N[a].at[l, pl.ds(pl.multiple_of(owner * rows + way * (rows // 2), rows // 2), rows // 2), :]
        return pltpu.make_async_copy(src, last[way].at[late.index((a, l))], last_sem.at[way, late.index((a, l))])

    for step in range(half):
        for i, a, l, p in chunks:
            for way in range(2):
                if step < hops(a, l):
                    came(i, a, l, p, way, step)
                if step < hops(a, l) - 1:
                    send(i, a, l, p, way, step + 1).start()
                elif step == half - 2 and p == parts - 1:
                    to_permute(a, l, way).start()
    for i, a, l, p in chunks:
        for way in range(2):
            for step in range(hops(a, l)):
                send(i, a, l, p, way, step).wait_send()
    for a, l in late:
        for way in range(2):
            to_permute(a, l, way).wait()


def store_kernel(count, *refs):
    src, dst, sem = refs[:count], refs[count : 2 * count], refs[-1]
    copies = [
        pltpu.make_async_copy(a.at[l], b.at[l], sem.at[i, l])
        for i, (a, b) in enumerate(zip(src, dst, strict=True))
        for l in range(a.shape[0])
    ]
    for copy in copies:
        copy.start()
    for copy in copies:
        copy.wait()


def store(arrays):
    count = len(arrays)
    return pl.pallas_call(
        functools.partial(store_kernel, count),
        out_shape=tuple(jax.ShapeDtypeStruct(t.shape, t.dtype) for t in arrays),
        in_specs=[pl.BlockSpec(memory_space=pltpu.VMEM)] * count,
        out_specs=(pl.BlockSpec(memory_space=pl.ANY),) * count,
        scratch_shapes=[pltpu.SemaphoreType.DMA((count, arrays[0].shape[0]))],
        compiler_params=pltpu.CompilerParams(vmem_limit_bytes=2**20),
        cost_estimate=pl.CostEstimate(flops=10_000_000_000, bytes_accessed=0, transcendentals=0),
        name="store",
    )(*(pinned(t, pltpu.VMEM) for t in arrays))


def place_kernel(n, count, *refs):
    up_ref, down_ref = refs[count : count + 2]
    outs, sem = refs[count + 2 : -1], refs[-1]
    opposite = lax.rem(lax.axis_index("dp") + n // 2, n)
    hr = up_ref.shape[1]
    copies = []
    for i, out in enumerate(outs):
        for way, src in enumerate((up_ref, down_ref)):
            there = pl.ds(pl.multiple_of(opposite * 2 * hr + way * hr, hr), hr)
            copies.append(pltpu.make_async_copy(src.at[i], out.at[0, there, :], sem.at[i, way]))
    for copy in copies:
        copy.start()
    for copy in copies:
        copy.wait()


def place_last(n, arrays, came):
    count = len(arrays)
    any_space = pl.BlockSpec(memory_space=pl.ANY)
    in_vmem = pl.BlockSpec(memory_space=pltpu.VMEM)
    return pl.pallas_call(
        functools.partial(place_kernel, n, count),
        out_shape=tuple(jax.ShapeDtypeStruct(t.shape, t.dtype) for t in arrays),
        in_specs=[any_space] * count + [in_vmem] * 2,
        out_specs=(any_space,) * count,
        scratch_shapes=[pltpu.SemaphoreType.DMA((count, 2))],
        input_output_aliases={i: i for i in range(count)},
        compiler_params=pltpu.CompilerParams(vmem_limit_bytes=2**20),
        name="place",
    )(*(pinned(t, pltpu.HBM) for t in arrays), *came)


def update(n, made, w, m, v):
    layers = w[0].shape[0]
    parts = 2
    chunks = layers * 3 * parts
    count = sum(t.size for t in w)
    any_space = pl.BlockSpec(memory_space=pl.ANY)
    in_vmem = pl.BlockSpec(memory_space=pltpu.VMEM)
    half = n // 2
    g, squares, ahead = made[:3], made[3], made[4:]
    return pl.pallas_call(
        functools.partial(update_kernel, n, float(count), parts),
        out_shape=tuple(kept(t.shape, BF16) for t in w)
        + tuple(kept(t.shape, F32) for t in m + v)
        + (jax.ShapeDtypeStruct((LATE, m[0].shape[1] // 2, m[0].shape[2]), BF16),) * 2,
        in_specs=[in_vmem] * 4 + [any_space] * 3 + [in_vmem] * 3 + [any_space] * 6,
        out_specs=(in_vmem,) * 9 + (any_space,) * 2,
        scratch_shapes=[pltpu.VMEM(t.shape, BF16) for t in m]
        + [
            pltpu.SemaphoreType.DMA((3, 3, layers)),
            pltpu.SemaphoreType.DMA((2, LATE)),
            pltpu.SemaphoreType.DMA((chunks, 2, half)),
            pltpu.SemaphoreType.DMA((chunks, 2, half)),
        ],
        compiler_params=pltpu.CompilerParams(collective_id=1, has_side_effects=True, vmem_limit_bytes=12 * 2**20),
        name="update",
    )(
        *(pinned(t, pltpu.VMEM) for t in (*g, squares)),
        *(pinned(t, pltpu.HBM) for t in w),
        *(pinned(t, pltpu.VMEM) for t in ahead),
        *(pinned(t, pltpu.HBM) for t in (*m, *v)),
    )


def solution(mesh):
    n = mesh.shape["dp"]

    def step(x, dy, *arrays):
        w, m, v = (arrays[i : i + 3] for i in (0, 3, 6))
        *new, up, down = update(n, gradients(n, x, dy, *w, m[2], v[2]), w, m, v)
        came = tuple(lax.ppermute(t, "dp", [(i, (i + d) % n) for i in range(n)]) for t, d in ((up, 1), (down, -1)))
        out = store(new)
        return (*place_last(n, out[:LATE], came), *out[LATE:])

    shard = P(None, "dp", None)
    return jax.shard_map(
        step,
        mesh=mesh,
        in_specs=(P(("rep", "dp"), None, None),) * 2 + (P(),) * 3 + (shard,) * 6,
        out_specs=(P("rep", None, None),) * 3 + (P("rep", "dp", None),) * 6,
        check_vma=False,
    )
```

```python
import functools

import jax
import jax.numpy as jnp
from jax import lax
from jax.experimental import pallas as pl
from jax.experimental.pallas import tpu as pltpu
from jax.sharding import PartitionSpec as P

F32 = jnp.float32
BF16 = jnp.bfloat16
MESH = pl.DeviceIdType.MESH
LANES = 128
LATE = 2


def dot(a, b):
    return jnp.dot(a, b, preferred_element_type=F32)


def dot_t(a, b):
    return lax.dot_general(a, b, (((1,), (1,)), ((), ())), preferred_element_type=F32)


def scale_of(wide):
    return lax.rsqrt(jnp.mean(wide * wide, -1, keepdims=True) + 1e-6)


def pinned(t, space):
    return pltpu.with_memory_space_constraint(t, space)


def kept(shape, dtype):
    return pltpu.VMEM(shape, dtype)


def loop(count, body):
    lax.fori_loop(0, count, lambda i, c: (body(i), c)[1], 0)


def at(i, size):
    return pl.ds(pl.multiple_of(i * size, size), size)


def grad_kernel(n, layers, shapes, *refs):
    (x_hbm, dy_hbm, wg_hbm, wu_hbm, wd_hbm, md_hbm, vd_hbm) = refs[:7]
    (OG, OU, OD, ALL, PW, PM, PV) = refs[7:14]
    (A, AT, D, DT, H, ACT, DG, DU, DA, WG, WU, WD, G, RU, RD, SQ, *sems) = refs[14:]
    x_sem, dy_sem, w_sem, ahead_sem, send_sem, recv_sem, low_sem, sq_send, sq_recv = sems
    tokens, dim, ff, blocks = shapes
    share = ff // n
    tiles = share // LANES
    tile = n * LANES
    tb = tokens // blocks
    half = n // 2
    hr = LANES // 2
    cols = tile // 2
    me = lax.axis_index("dp")
    up, down = lax.rem(me + 1, n), lax.rem(me + n - 1, n)
    ring = lambda d: lax.rem(me + d + n, n)

    def tok(i):
        return at(i, tb)

    def fetch(k):
        slot = lax.rem(k, 2)
        layer = lax.rem(k // tiles, 2)
        t = lax.rem(k, tiles)

        def one(b):
            place = pl.ds(pl.multiple_of(b * share + t * LANES, LANES), LANES)
            here = at(b, LANES)
            pltpu.make_async_copy(wg_hbm.at[layer, :, place], WG.at[slot, :, here], w_sem.at[slot, 0]).start()
            pltpu.make_async_copy(wu_hbm.at[layer, :, place], WU.at[slot, :, here], w_sem.at[slot, 1]).start()
            pltpu.make_async_copy(wd_hbm.at[layer, place, :], WD.at[slot, here, :], w_sem.at[slot, 2]).start()

        loop(n, one)

    def fetched(k):
        slot = lax.rem(k, 2)
        pltpu.make_async_copy(WG.at[slot], WG.at[slot], w_sem.at[slot, 0]).wait()
        pltpu.make_async_copy(WU.at[slot], WU.at[slot], w_sem.at[slot, 1]).wait()
        pltpu.make_async_copy(WD.at[slot], WD.at[slot], w_sem.at[slot, 2]).wait()

    def x_copy(i):
        return pltpu.make_async_copy(x_hbm.at[0, tok(i), :], H.at[tok(i), :], x_sem.at[i])

    def x_again(i):
        return pltpu.make_async_copy(x_hbm.at[0, tok(i), :], ACT.at[tok(i), pl.ds(0, dim)], x_sem.at[i])

    def dy_copy(i):
        return pltpu.make_async_copy(dy_hbm.at[0, tok(i), :], D.at[tok(i), :], dy_sem.at[i])

    barrier = pltpu.get_barrier_semaphore()
    for d in range(1, n):
        pl.semaphore_signal(barrier, inc=1, device_id={"dp": ring(d)}, device_id_type=MESH)

    x_copy(0).start()
    fetch(0)
    loop(blocks - 1, lambda i: x_copy(i + 1).start())
    loop(blocks, lambda i: dy_copy(i).start())

    def first_norm(i):
        wide = H[tok(i), :].astype(F32)
        A[tok(i), :] = (wide * scale_of(wide)).astype(BF16)
        DA[tok(i), :] = jnp.zeros((tb, dim), F32)

    def forward(k, i):
        slot = lax.rem(k, 2)
        for j in range(2):
            here = pl.ds(j * cols, cols)
            g = dot(A[tok(i), :], WG[slot, :, here])
            u = dot(A[tok(i), :], WU[slot, :, here])
            s = 0.5 * jnp.tanh(0.5 * g) + 0.5
            ACT[tok(i), here] = (g * s * u).astype(BF16)
        DA[tok(i), :] += dot(ACT[tok(i), :], WD[slot])

    def second_norm(i):
        h = (H[tok(i), :].astype(F32) + DA[tok(i), :].astype(BF16).astype(F32)).astype(BF16)
        wide = h.astype(F32)
        return h, (wide * scale_of(wide)).astype(BF16)

    def second_norm_kept(i, h, a):
        H[tok(i), :] = h
        A[tok(i), :] = a
        AT[:, tok(i)] = a.T

    x_copy(0).wait()
    first_norm(0)
    fetched(0)
    fetch(1)

    def opening(i):
        x_copy(i + 1).wait()
        forward(0, i)
        first_norm(i + 1)

    loop(blocks - 1, opening)

    def middle(j):
        q = blocks - 1 + j
        k, i = q // blocks, lax.rem(q, blocks)

        @pl.when(i == 0)
        def _():
            fetched(k)
            fetch(k + 1)

        @pl.when(j < blocks)
        def _():
            dy_copy(j).wait()

        forward(k, i)
        seen = jnp.minimum(j, blocks - 1)
        DT[:, tok(seen)] = D[tok(seen), :].T

    loop((tiles - 2) * blocks + 2, middle)

    def closing(i):
        normed = second_norm(i)
        forward(tiles - 1, i + 1)
        second_norm_kept(i, *normed)

    loop(blocks - 1, closing)
    second_norm_kept(blocks - 1, *second_norm(blocks - 1))

    pl.semaphore_wait(barrier, n - 1)

    def remote(src, dst, slot, u, way, step, arrival=None):
        return pltpu.make_async_remote_copy(
            src_ref=src,
            dst_ref=dst,
            send_sem=send_sem.at[slot, way, step],
            recv_sem=recv_sem.at[u, way, step] if arrival is None else arrival,
            device_id={"dp": (up, down)[way]},
            device_id_type=MESH,
        )

    low, high, whole = pl.ds(0, hr), pl.ds(hr, hr), pl.ds(0, 2 * hr)
    lands = (RU, RD)

    def rows(step):
        return pl.ds(hr + (step - 1) * 2 * hr, 2 * hr)

    def begin_low(u, slot):
        remote(G.at[slot, ring(half), low], RU.at[u, low], slot, u, 0, 0).start()
        remote(G.at[slot, ring(1 - half), low], RD.at[u, pl.ds(hr, hr)], slot, u, 1, 1, low_sem.at[u]).start()

    def begin_high(u, slot):
        remote(G.at[slot, ring(half), high], RD.at[u, low], slot, u, 1, 0).start()
        remote(G.at[slot, ring(half - 1), high], RU.at[u, pl.ds(2 * hr, hr)], slot, u, 0, 1).start()

    def arrived(land, sem):
        pltpu.make_async_copy(land, land, sem).wait()

    def received(u, way, step):
        if (way, step) == (1, 1):
            arrived(RD.at[u, pl.ds(hr, hr)], low_sem.at[u])
            arrived(RD.at[u, pl.ds(2 * hr, hr)], recv_sem.at[u, 1, 1])
        else:
            arrived(lands[way].at[u, rows(step) if step else low], recv_sem.at[u, way, step])

    def add(land, place, mine):
        land[place] = (land[place].astype(F32) + mine.astype(F32)).astype(BF16)

    def second_low(u, slot):
        received(u, 0, 0)
        add(RU, (u, low), G[slot, ring(half - 1), low])
        remote(RU.at[u, low], RU.at[u, pl.ds(hr, hr)], slot, u, 0, 1).start()

    def second_high(u, slot):
        received(u, 1, 0)
        add(RD, (u, low), G[slot, ring(1 - half), high])
        remote(RD.at[u, low], RD.at[u, pl.ds(2 * hr, hr)], slot, u, 1, 1).start()

    def pass_on(u, slot, way, step):
        received(u, way, step - 1)
        add(lands[way], (u, rows(step - 1)), G[slot, ring(half - step if way == 0 else step - half)])
        remote(lands[way].at[u, rows(step - 1)], lands[way].at[u, rows(step)], slot, u, way, step).start()

    def later(u, slot, step):
        pass_on(u, slot, 0, step)
        pass_on(u, slot, 1, step)

    def half_on(u, slot, part, sem):
        here, there = pl.ds((1 + part) * hr, hr), pl.ds((3 + part) * hr, hr)
        arrived(RD.at[u, here], sem)
        add(RD, (u, here), G[slot, ring(2 - half), (low, high)[part]])
        remote(RD.at[u, here], RD.at[u, there], slot, u, 1, 2).start()

    def third_low(u, slot):
        half_on(u, slot, 0, low_sem.at[u])

    def third_rest(u, slot):
        pass_on(u, slot, 0, 2)
        half_on(u, slot, 1, recv_sem.at[u, 1, 1])

    def finish(u, slot, which, layer, t):
        received(u, 0, half - 1)
        received(u, 1, half - 1)
        total = G[slot, me].astype(F32) + RU[u, rows(half - 1)].astype(F32) + RD[u, rows(half - 1)].astype(F32)
        total = total.astype(BF16)
        wide = total.astype(F32)
        SQ[...] += jnp.sum((wide * wide).reshape(-1, 8, dim), axis=0)
        if which == 0:
            OD[layer, at(t, LANES), :] = total
        else:
            out = (OG, OU)[which - 1]
            for b in range(n):
                piece = total[hr * (b // (n // 2)) : hr * (b // (n // 2)) + hr, LANES * (b % (n // 2)) : LANES * (b % (n // 2)) + LANES]
                out[layer, :, pl.ds(pl.multiple_of(b * share + t * LANES, LANES), LANES)] = piece
        for way in range(2):
            for step in range(half):
                src = G.at[slot, 0, whole] if step > 0 else G.at[slot, 0, low]
                pltpu.make_async_copy(src, src, send_sem.at[slot, way, step]).wait()

    SQ[...] = jnp.zeros_like(SQ)

    def tile_step(k):
        wk = k + tiles
        slot = lax.rem(wk, 2)
        base = lax.rem(k, 2) * 3
        prev = 3 - base
        u0 = 3 * k
        p0 = u0 - 3
        going = k >= 1
        old_t = lax.rem(k - 1 + tiles, tiles)
        old_layer = jnp.where(k - 1 < tiles, 1, 0)
        fetched(wk)

        @pl.when(k < 2 * tiles - 1)
        def _():
            fetch(wk + 1)

        def when(cond):
            return pl.when(going & cond)

        def hidden(j, i):
            for b, c in ((0, 0), (0, 1), (1, 0), (1, 1)):
                here = pl.ds(pl.multiple_of(j * cols + c * (cols // 2), cols // 2), cols // 2)
                place = tok(2 * i + b)
                g = dot(A[place, :], WG[slot, :, here])
                u = dot(A[place, :], WU[slot, :, here])
                back = dot_t(D[place, :], WD[slot, here, :]).astype(BF16).astype(F32)
                s = 0.5 * jnp.tanh(0.5 * g) + 0.5
                silu = g * s
                ACT[place, here] = (silu * u).astype(BF16)
                DU[place, here] = (back * silu).astype(BF16)
                DG[place, here] = (back * u * (s + silu * (1.0 - s))).astype(BF16)

        def wide_part(src, unit, j):
            part = dot(AT[...], src[:, at(j, cols)]).astype(BF16)
            G[base + unit, :, at(j, hr), :] = part.reshape(n, dim // n, cols)

        gate, upper = (u0 + 1, base + 1), (u0 + 2, base + 2)
        old, old_gate, old_upper = (p0, prev), (p0 + 1, prev + 1), (p0 + 2, prev + 2)

        def halves(j):
            def some(i):
                hidden(j, i)

                @when((j == 0) & (i == 0))
                def _():
                    later(*old, 2)
                    later(*old_upper, 3)

                @pl.when((k == 0) & (j == 1) & (i == 0))
                def _():
                    third_low(*gate)

                @pl.when((k == 0) & (j == 1) & (i == 1))
                def _():
                    second_low(*upper)

            loop(blocks // 2, some)
            wide_part(DG, 1, j)

            @pl.when(j == 0)
            def _():
                begin_low(*gate)

            @pl.when(j == 1)
            def _():
                begin_high(*gate)

            @pl.when((j == 1) & (k == 0))
            def _():
                second_low(*gate)

            wide_part(DU, 2, j)

            @pl.when(j == 0)
            def _():
                begin_low(*upper)

            @pl.when(j == 1)
            def _():
                begin_high(*upper)

            @when(j == 1)
            def _():
                later(*old, 3)
                finish(*old_gate, 1, old_layer, old_t)
                finish(*old_upper, 2, old_layer, old_t)
                second_low(*gate)

            @pl.when((j == 1) & (k == 0))
            def _():
                third_low(*upper)

        loop(2, halves)

        def down_part(j):
            part = dot(DT[...], ACT[:, at(j, cols)])
            flipped = part.T.astype(BF16)
            for b in range(cols // LANES):
                G[base, j * (cols // LANES) + b] = flipped[b * LANES : (b + 1) * LANES]

            @pl.when(j == 0)
            def _():
                second_high(*gate)

        loop(2, down_part)
        begin_low(u0, base)
        begin_high(u0, base)

        @pl.when(going)
        def _():
            second_low(*upper)

        @pl.when(k == tiles - 1)
        def _():
            loop(blocks, lambda i: x_again(i).start())

        def ring_part(i):
            @pl.when(i == 0)
            def _():
                second_high(*upper)

            @pl.when((i == 0) & (k == 0))
            def _():
                second_low(u0, base)
                third_rest(*gate)

            @when(i == 2)
            def _():
                finish(*old, 0, old_layer, old_t)
                later(*gate, 2)

        @pl.when(k < tiles)
        def _():
            def input_part(i):
                so_far = jnp.where(k == 0, 0.0, DA[tok(i), :])
                DA[tok(i), :] = so_far + (dot_t(DG[tok(i), :], WG[slot]) + dot_t(DU[tok(i), :], WU[slot]))
                ring_part(i)

            loop(blocks, input_part)

        @pl.when(k >= tiles)
        def _():
            loop(blocks, ring_part)

        @pl.when(k == tiles - 1)
        def _():
            def between(i):
                h = H[tok(i), :].astype(F32)
                da = DA[tok(i), :].astype(BF16).astype(F32)
                r = scale_of(h)
                dh = (r * da - h * (r * r * r * jnp.mean(h * da, -1, keepdims=True))).astype(BF16)
                d = (D[tok(i), :].astype(F32) + dh.astype(F32)).astype(BF16)
                D[tok(i), :] = d
                DT[:, tok(i)] = d.T
                x_again(i).wait()
                wide = ACT[tok(i), pl.ds(0, dim)].astype(F32)
                a = (wide * scale_of(wide)).astype(BF16)
                A[tok(i), :] = a
                AT[:, tok(i)] = a.T

                @pl.when(i == 1)
                def _():
                    second_low(u0, base)
                    second_high(u0, base)

            loop(blocks, between)

        @pl.when(going & (k != tiles - 1))
        def _():
            second_low(u0, base)

        @pl.when(k != tiles - 1)
        def _():
            second_high(u0, base)

        @pl.when(k == 0)
        def _():
            third_rest(*upper)

        @pl.when(going)
        def _():
            later(*upper, 2)

        later(*gate, 3)

    loop(2 * tiles, tile_step)

    ahead = (
        pltpu.make_async_copy(wd_hbm.at[layers - 1, at(me, share), :], PW, ahead_sem.at[0]),
        pltpu.make_async_copy(md_hbm.at[layers - 1], PM, ahead_sem.at[1]),
        pltpu.make_async_copy(vd_hbm.at[layers - 1], PV, ahead_sem.at[2]),
    )
    for copy in ahead:
        copy.start()

    end = 2 * tiles - 1
    u0, base = 3 * end, (end % 2) * 3
    later(u0, base, 2)
    later(u0 + 2, base + 2, 3)
    later(u0, base, 3)
    for j in (1, 2, 0):
        finish(u0 + j, base + j, j, 0, tiles - 1)

    squares = SQ[:, :LANES]
    for j in range(1, dim // LANES):
        squares += SQ[:, j * LANES : (j + 1) * LANES]
    ALL[me] = squares

    def tell(d):
        return pltpu.make_async_remote_copy(
            src_ref=ALL.at[me],
            dst_ref=ALL.at[me],
            send_sem=sq_send.at[d],
            recv_sem=sq_recv.at[d],
            device_id={"dp": ring(d)},
            device_id_type=MESH,
        )

    for d in range(1, n):
        tell(d).start()
    for d in range(1, n):
        tell(d).wait()
    for copy in ahead:
        copy.wait()


def gradients(n, x, dy, w_gate, w_up, w_down, m_down, v_down):
    layers, dim, ff = w_gate.shape
    tokens = x.shape[1]
    blocks = 4
    share = ff // n
    tiles = share // LANES
    tile = n * LANES
    units = 3 * layers * tiles
    half = n // 2
    land = LANES // 2 + LANES * (half - 1)
    any_space = pl.BlockSpec(memory_space=pl.ANY)
    return pl.pallas_call(
        functools.partial(grad_kernel, n, layers, (tokens, dim, ff, blocks)),
        out_shape=tuple(
            kept(shape, dtype)
            for shape, dtype in (
                ((layers, dim // n, ff), BF16),
                ((layers, dim // n, ff), BF16),
                ((layers, share, dim), BF16),
                ((n, 8, LANES), F32),
                ((share, dim), BF16),
                ((share, dim), F32),
                ((share, dim), F32),
            )
        ),
        in_specs=[any_space] * 7,
        out_specs=(pl.BlockSpec(memory_space=pltpu.VMEM),) * 7,
        scratch_shapes=[
            pltpu.VMEM((tokens, dim), BF16),
            pltpu.VMEM((dim, tokens), BF16),
            pltpu.VMEM((tokens, dim), BF16),
            pltpu.VMEM((dim, tokens), BF16),
            pltpu.VMEM((tokens, dim), BF16),
            pltpu.VMEM((tokens, tile), BF16),
            pltpu.VMEM((tokens, tile), BF16),
            pltpu.VMEM((tokens, tile), BF16),
            pltpu.VMEM((tokens, dim), F32),
            pltpu.VMEM((2, dim, tile), BF16),
            pltpu.VMEM((2, dim, tile), BF16),
            pltpu.VMEM((2, tile, dim), BF16),
            pltpu.VMEM((6, n, LANES, dim), BF16),
            pltpu.VMEM((units, land, dim), BF16),
            pltpu.VMEM((units, land, dim), BF16),
            pltpu.VMEM((8, dim), F32),
            pltpu.SemaphoreType.DMA((blocks,)),
            pltpu.SemaphoreType.DMA((blocks,)),
            pltpu.SemaphoreType.DMA((2, 3)),
            pltpu.SemaphoreType.DMA((3,)),
            pltpu.SemaphoreType.DMA((6, 2, half)),
            pltpu.SemaphoreType.DMA((units, 2, half)),
            pltpu.SemaphoreType.DMA((units,)),
            pltpu.SemaphoreType.DMA((n,)),
            pltpu.SemaphoreType.DMA((n,)),
        ],
        compiler_params=pltpu.CompilerParams(collective_id=0, has_side_effects=True, vmem_limit_bytes=59 * 2**20),
        name="grads",
    )(*(pinned(t, pltpu.HBM) for t in (x, dy, w_gate, w_up, w_down, m_down, v_down)))


def update_kernel(n, count, parts, *refs):
    G, w_hbm, m_hbm, v_hbm = (refs[i : i + 3] for i in (0, 4, 10, 13))
    SQ, PW, PM, PV = refs[3], *refs[7:10]
    N, M, V = (refs[i : i + 3] for i in (16, 19, 22))
    last = refs[25:27]
    W = refs[27:30]
    in_sem, last_sem, send_sem, recv_sem = refs[30:]
    me = lax.axis_index("dp")
    half = n // 2
    up, down = lax.rem(me + 1, n), lax.rem(me + n - 1, n)
    ring = lambda d: lax.rem(me + d + n, n)
    layers = G[0].shape[0]

    barrier = pltpu.get_barrier_semaphore()
    for peer in (up, down):
        pl.semaphore_signal(barrier, inc=1, device_id={"dp": peer}, device_id_type=MESH)

    order = [(a, l) for l in reversed(range(layers)) for a in (2, 0, 1)]
    loads = {}
    for a, l in order[1:]:
        rows = G[a].shape[1]
        own = pl.ds(pl.multiple_of(me * rows, rows), rows)
        loads[a, l] = (
            pltpu.make_async_copy(w_hbm[a].at[l, own, :], W[a].at[l], in_sem.at[0, a, l]),
            pltpu.make_async_copy(m_hbm[a].at[l], M[a].at[l], in_sem.at[1, a, l]),
            pltpu.make_async_copy(v_hbm[a].at[l], V[a].at[l], in_sem.at[2, a, l]),
        )
    total = jnp.sum(jnp.sum(SQ[...], axis=0), axis=(0, 1), keepdims=True)
    factor = jnp.minimum(1.0, 0.5 * lax.rsqrt(total / count + 1e-30))

    def shape(a):
        rows, cols = G[a].shape[1:]
        return (rows, cols // parts, 0) if a < 2 else (rows // parts, cols, 1)

    def place(a, l, p, owner, part):
        rows = G[a].shape[1]
        r, c, split = shape(a)
        hr = r // 2
        start = owner * rows + (p * r if split else 0)
        start, size = (start, r) if part == 2 else (start + part * hr, hr)
        return (l, pl.ds(pl.multiple_of(start, hr), size), pl.ds(0 if split else p * c, c))

    def send(i, a, l, p, way, step):
        owner = ring(-step) if way == 0 else ring(step)
        ref = N[a].at[place(a, l, p, owner, 2 if step < half - 1 else way)]
        return pltpu.make_async_remote_copy(
            src_ref=ref,
            dst_ref=ref,
            send_sem=send_sem.at[i, way, step],
            recv_sem=recv_sem.at[i, way, step],
            device_id={"dp": (up, down)[way]},
            device_id_type=MESH,
        )

    def came(i, a, l, p, way, step):
        owner = ring(-step - 1) if way == 0 else ring(step + 1)
        where = place(a, l, p, owner, 2 if step < half - 1 else way)
        ref = N[a].at[where]
        pltpu.make_async_copy(ref, ref, recv_sem.at[i, way, step]).wait()

    def adam(a, l, p):
        r, c, split = shape(a)
        rows = G[a].shape[1]
        step = 32
        lane = pl.ds(0 if split else p * c, c)

        def some(i):
            row = pl.ds(pl.multiple_of((p * r if split else 0) + i * step, step), step)
            old = (PW[row, lane], PM[row, lane], PV[row, lane]) if (a, l) == order[0] else (W[a][l, row, lane], M[a][l, row, lane], V[a][l, row, lane])
            g = G[a][l, row, lane].astype(F32) * factor
            m = 0.9 * old[1] + 0.1 * g
            v = 0.95 * old[2] + 0.05 * g * g
            M[a][l, row, lane] = m
            V[a][l, row, lane] = v
            w = old[0].astype(F32)
            new = (w - 0.02 * (m * lax.rsqrt(v + 1e-8) + 0.1 * w)).astype(BF16)
            there = pl.ds(pl.multiple_of(me * rows + (p * r if split else 0) + i * step, step), step)
            N[a][l, there, lane] = new

        loop(r // step, some)

    chunks = []
    for a, l in order:
        for p in range(parts):
            chunks.append((len(chunks), a, l, p))
    for i, a, l, p in chunks:
        if p == 0:
            for copy in loads.get((a, l), ()):
                copy.wait()
        adam(a, l, p)
        if i == 0:
            pl.semaphore_wait(barrier, 2)
        send(i, a, l, p, 0, 0).start()
        send(i, a, l, p, 1, 0).start()
        if i == 0:
            for copies in loads.values():
                for copy in copies:
                    copy.start()
    late = order[len(order) - LATE :]

    def hops(a, l):
        return half - 1 if (a, l) in late else half

    def to_permute(a, l, way):
        rows = G[a].shape[1]
        owner = ring(1 - half) if way == 0 else ring(half - 1)
        src = N[a].at[l, pl.ds(pl.multiple_of(owner * rows + way * (rows // 2), rows // 2), rows // 2), :]
        return pltpu.make_async_copy(src, last[way].at[late.index((a, l))], last_sem.at[way, late.index((a, l))])

    for step in range(half):
        for i, a, l, p in chunks:
            for way in range(2):
                if step < hops(a, l):
                    came(i, a, l, p, way, step)
                if step < hops(a, l) - 1:
                    send(i, a, l, p, way, step + 1).start()
                elif step == half - 2 and p == parts - 1:
                    to_permute(a, l, way).start()
    for i, a, l, p in chunks:
        for way in range(2):
            for step in range(hops(a, l)):
                send(i, a, l, p, way, step).wait_send()
    for a, l in late:
        for way in range(2):
            to_permute(a, l, way).wait()


def store_kernel(count, *refs):
    src, dst, sem = refs[:count], refs[count : 2 * count], refs[-1]
    copies = [
        pltpu.make_async_copy(a.at[l], b.at[l], sem.at[i, l])
        for i, (a, b) in enumerate(zip(src, dst, strict=True))
        for l in range(a.shape[0])
    ]
    for copy in copies:
        copy.start()
    for copy in copies:
        copy.wait()


def store(arrays):
    count = len(arrays)
    return pl.pallas_call(
        functools.partial(store_kernel, count),
        out_shape=tuple(jax.ShapeDtypeStruct(t.shape, t.dtype) for t in arrays),
        in_specs=[pl.BlockSpec(memory_space=pltpu.VMEM)] * count,
        out_specs=(pl.BlockSpec(memory_space=pl.ANY),) * count,
        scratch_shapes=[pltpu.SemaphoreType.DMA((count, arrays[0].shape[0]))],
        compiler_params=pltpu.CompilerParams(vmem_limit_bytes=2**20),
        cost_estimate=pl.CostEstimate(flops=10_000_000_000, bytes_accessed=0, transcendentals=0),
        name="store",
    )(*(pinned(t, pltpu.VMEM) for t in arrays))


def place_kernel(n, count, *refs):
    up_ref, down_ref = refs[count : count + 2]
    outs, sem = refs[count + 2 : -1], refs[-1]
    opposite = lax.rem(lax.axis_index("dp") + n // 2, n)
    hr = up_ref.shape[1]
    copies = []
    for i, out in enumerate(outs):
        for way, src in enumerate((up_ref, down_ref)):
            there = pl.ds(pl.multiple_of(opposite * 2 * hr + way * hr, hr), hr)
            copies.append(pltpu.make_async_copy(src.at[i], out.at[0, there, :], sem.at[i, way]))
    for copy in copies:
        copy.start()
    for copy in copies:
        copy.wait()


def place_last(n, arrays, came):
    count = len(arrays)
    any_space = pl.BlockSpec(memory_space=pl.ANY)
    in_vmem = pl.BlockSpec(memory_space=pltpu.VMEM)
    return pl.pallas_call(
        functools.partial(place_kernel, n, count),
        out_shape=tuple(jax.ShapeDtypeStruct(t.shape, t.dtype) for t in arrays),
        in_specs=[any_space] * count + [in_vmem] * 2,
        out_specs=(any_space,) * count,
        scratch_shapes=[pltpu.SemaphoreType.DMA((count, 2))],
        input_output_aliases={i: i for i in range(count)},
        compiler_params=pltpu.CompilerParams(vmem_limit_bytes=2**20),
        name="place",
    )(*(pinned(t, pltpu.HBM) for t in arrays), *came)


def update(n, made, w, m, v):
    layers = w[0].shape[0]
    parts = 2
    chunks = layers * 3 * parts
    count = sum(t.size for t in w)
    any_space = pl.BlockSpec(memory_space=pl.ANY)
    in_vmem = pl.BlockSpec(memory_space=pltpu.VMEM)
    half = n // 2
    g, squares, ahead = made[:3], made[3], made[4:]
    return pl.pallas_call(
        functools.partial(update_kernel, n, float(count), parts),
        out_shape=tuple(kept(t.shape, BF16) for t in w)
        + tuple(kept(t.shape, F32) for t in m + v)
        + (jax.ShapeDtypeStruct((LATE, m[0].shape[1] // 2, m[0].shape[2]), BF16),) * 2,
        in_specs=[in_vmem] * 4 + [any_space] * 3 + [in_vmem] * 3 + [any_space] * 6,
        out_specs=(in_vmem,) * 9 + (any_space,) * 2,
        scratch_shapes=[pltpu.VMEM(t.shape, BF16) for t in m]
        + [
            pltpu.SemaphoreType.DMA((3, 3, layers)),
            pltpu.SemaphoreType.DMA((2, LATE)),
            pltpu.SemaphoreType.DMA((chunks, 2, half)),
            pltpu.SemaphoreType.DMA((chunks, 2, half)),
        ],
        compiler_params=pltpu.CompilerParams(collective_id=1, has_side_effects=True, vmem_limit_bytes=12 * 2**20),
        name="update",
    )(
        *(pinned(t, pltpu.VMEM) for t in (*g, squares)),
        *(pinned(t, pltpu.HBM) for t in w),
        *(pinned(t, pltpu.VMEM) for t in ahead),
        *(pinned(t, pltpu.HBM) for t in (*m, *v)),
    )


def solution(mesh):
    n = mesh.shape["dp"]

    def step(x, dy, *arrays):
        w, m, v = (arrays[i : i + 3] for i in (0, 3, 6))
        *new, up, down = update(n, gradients(n, x, dy, *w, m[2], v[2]), w, m, v)
        came = tuple(lax.ppermute(t, "dp", [(i, (i + d) % n) for i in range(n)]) for t, d in ((up, 1), (down, -1)))
        out = store(new)
        return (*place_last(n, out[:LATE], came), *out[LATE:])

    shard = P(None, "dp", None)
    return jax.shard_map(
        step,
        mesh=mesh,
        in_specs=(P(("rep", "dp"), None, None),) * 2 + (P(),) * 3 + (shard,) * 6,
        out_specs=(P("rep", None, None),) * 3 + (P("rep", "dp", None),) * 6,
        check_vma=False,
    )
```

```python
import functools

import jax
import jax.numpy as jnp
from jax import lax
from jax.experimental import pallas as pl
from jax.experimental.pallas import tpu as pltpu
from jax.sharding import PartitionSpec as P

F32 = jnp.float32
BF16 = jnp.bfloat16
MESH = pl.DeviceIdType.MESH
LANES = 128
LATE = 4


def dot(a, b):
    return jnp.dot(a, b, preferred_element_type=F32)


def dot_t(a, b):
    return lax.dot_general(a, b, (((1,), (1,)), ((), ())), preferred_element_type=F32)


def scale_of(wide):
    return lax.rsqrt(jnp.mean(wide * wide, -1, keepdims=True) + 1e-6)


def pinned(t, space):
    return pltpu.with_memory_space_constraint(t, space)


def kept(shape, dtype):
    return pltpu.VMEM(shape, dtype)


def loop(count, body):
    lax.fori_loop(0, count, lambda i, c: (body(i), c)[1], 0)


def at(i, size):
    return pl.ds(pl.multiple_of(i * size, size), size)


def grad_kernel(n, layers, shapes, *refs):
    (x_hbm, dy_hbm, wg_hbm, wu_hbm, wd_hbm, md_hbm, vd_hbm) = refs[:7]
    (OG, OU, OD, ALL, PW, PM, PV) = refs[7:14]
    (A, AT, D, DT, H, ACT, DG, DU, DA, WG, WU, WD, G, RU, RD, SQ, *sems) = refs[14:]
    x_sem, dy_sem, w_sem, ahead_sem, send_sem, recv_sem, low_sem, sq_send, sq_recv = sems
    tokens, dim, ff, blocks = shapes
    share = ff // n
    tiles = share // LANES
    tile = n * LANES
    tb = tokens // blocks
    half = n // 2
    hr = LANES // 2
    cols = tile // 2
    me = lax.axis_index("dp")
    up, down = lax.rem(me + 1, n), lax.rem(me + n - 1, n)
    ring = lambda d: lax.rem(me + d + n, n)

    def tok(i):
        return at(i, tb)

    def fetch(k):
        slot = lax.rem(k, 2)
        layer = lax.rem(k // tiles, 2)
        t = lax.rem(k, tiles)

        def one(b):
            place = pl.ds(pl.multiple_of(b * share + t * LANES, LANES), LANES)
            here = at(b, LANES)
            pltpu.make_async_copy(wg_hbm.at[layer, :, place], WG.at[slot, :, here], w_sem.at[slot, 0]).start()
            pltpu.make_async_copy(wu_hbm.at[layer, :, place], WU.at[slot, :, here], w_sem.at[slot, 1]).start()
            pltpu.make_async_copy(wd_hbm.at[layer, place, :], WD.at[slot, here, :], w_sem.at[slot, 2]).start()

        loop(n, one)

    def fetched(k):
        slot = lax.rem(k, 2)
        pltpu.make_async_copy(WG.at[slot], WG.at[slot], w_sem.at[slot, 0]).wait()
        pltpu.make_async_copy(WU.at[slot], WU.at[slot], w_sem.at[slot, 1]).wait()
        pltpu.make_async_copy(WD.at[slot], WD.at[slot], w_sem.at[slot, 2]).wait()

    def x_copy(i):
        return pltpu.make_async_copy(x_hbm.at[0, tok(i), :], H.at[tok(i), :], x_sem.at[i])

    def x_again(i):
        return pltpu.make_async_copy(x_hbm.at[0, tok(i), :], ACT.at[tok(i), pl.ds(0, dim)], x_sem.at[i])

    def dy_copy(i):
        return pltpu.make_async_copy(dy_hbm.at[0, tok(i), :], D.at[tok(i), :], dy_sem.at[i])

    barrier = pltpu.get_barrier_semaphore()
    for d in range(1, n):
        pl.semaphore_signal(barrier, inc=1, device_id={"dp": ring(d)}, device_id_type=MESH)

    x_copy(0).start()
    fetch(0)
    loop(blocks - 1, lambda i: x_copy(i + 1).start())
    loop(blocks, lambda i: dy_copy(i).start())

    def first_norm(i):
        wide = H[tok(i), :].astype(F32)
        A[tok(i), :] = (wide * scale_of(wide)).astype(BF16)
        DA[tok(i), :] = jnp.zeros((tb, dim), F32)

    def forward(k, i):
        slot = lax.rem(k, 2)
        for j in range(2):
            here = pl.ds(j * cols, cols)
            g = dot(A[tok(i), :], WG[slot, :, here])
            u = dot(A[tok(i), :], WU[slot, :, here])
            s = 0.5 * jnp.tanh(0.5 * g) + 0.5
            ACT[tok(i), here] = (g * s * u).astype(BF16)
        DA[tok(i), :] += dot(ACT[tok(i), :], WD[slot])

    def second_norm(i):
        h = (H[tok(i), :].astype(F32) + DA[tok(i), :].astype(BF16).astype(F32)).astype(BF16)
        wide = h.astype(F32)
        return h, (wide * scale_of(wide)).astype(BF16)

    def second_norm_kept(i, h, a):
        H[tok(i), :] = h
        A[tok(i), :] = a
        AT[:, tok(i)] = a.T

    x_copy(0).wait()
    first_norm(0)
    fetched(0)
    fetch(1)

    def opening(i):
        x_copy(i + 1).wait()
        forward(0, i)
        first_norm(i + 1)

    loop(blocks - 1, opening)

    def middle(j):
        q = blocks - 1 + j
        k, i = q // blocks, lax.rem(q, blocks)

        @pl.when(i == 0)
        def _():
            fetched(k)
            fetch(k + 1)

        @pl.when(j < blocks)
        def _():
            dy_copy(j).wait()

        forward(k, i)
        seen = jnp.minimum(j, blocks - 1)
        DT[:, tok(seen)] = D[tok(seen), :].T

    loop((tiles - 2) * blocks + 2, middle)

    def closing(i):
        normed = second_norm(i)
        forward(tiles - 1, i + 1)
        second_norm_kept(i, *normed)

    loop(blocks - 1, closing)
    second_norm_kept(blocks - 1, *second_norm(blocks - 1))

    pl.semaphore_wait(barrier, n - 1)

    def remote(src, dst, slot, u, way, step, arrival=None):
        return pltpu.make_async_remote_copy(
            src_ref=src,
            dst_ref=dst,
            send_sem=send_sem.at[slot, way, step],
            recv_sem=recv_sem.at[u, way, step] if arrival is None else arrival,
            device_id={"dp": (up, down)[way]},
            device_id_type=MESH,
        )

    low, high, whole = pl.ds(0, hr), pl.ds(hr, hr), pl.ds(0, 2 * hr)
    lands = (RU, RD)

    def rows(step):
        return pl.ds(hr + (step - 1) * 2 * hr, 2 * hr)

    def begin_low(u, slot):
        remote(G.at[slot, ring(half), low], RU.at[u, low], slot, u, 0, 0).start()
        remote(G.at[slot, ring(1 - half), low], RD.at[u, pl.ds(hr, hr)], slot, u, 1, 1, low_sem.at[u]).start()

    def begin_high(u, slot):
        remote(G.at[slot, ring(half), high], RD.at[u, low], slot, u, 1, 0).start()
        remote(G.at[slot, ring(half - 1), high], RU.at[u, pl.ds(2 * hr, hr)], slot, u, 0, 1).start()

    def arrived(land, sem):
        pltpu.make_async_copy(land, land, sem).wait()

    def received(u, way, step):
        if (way, step) == (1, 1):
            arrived(RD.at[u, pl.ds(hr, hr)], low_sem.at[u])
            arrived(RD.at[u, pl.ds(2 * hr, hr)], recv_sem.at[u, 1, 1])
        else:
            arrived(lands[way].at[u, rows(step) if step else low], recv_sem.at[u, way, step])

    def add(land, place, mine):
        land[place] = (land[place].astype(F32) + mine.astype(F32)).astype(BF16)

    def second_low(u, slot):
        received(u, 0, 0)
        add(RU, (u, low), G[slot, ring(half - 1), low])
        remote(RU.at[u, low], RU.at[u, pl.ds(hr, hr)], slot, u, 0, 1).start()

    def second_high(u, slot):
        received(u, 1, 0)
        add(RD, (u, low), G[slot, ring(1 - half), high])
        remote(RD.at[u, low], RD.at[u, pl.ds(2 * hr, hr)], slot, u, 1, 1).start()

    def pass_on(u, slot, way, step):
        received(u, way, step - 1)
        add(lands[way], (u, rows(step - 1)), G[slot, ring(half - step if way == 0 else step - half)])
        remote(lands[way].at[u, rows(step - 1)], lands[way].at[u, rows(step)], slot, u, way, step).start()

    def later(u, slot, step):
        pass_on(u, slot, 0, step)
        pass_on(u, slot, 1, step)

    def half_on(u, slot, part, sem):
        here, there = pl.ds((1 + part) * hr, hr), pl.ds((3 + part) * hr, hr)
        arrived(RD.at[u, here], sem)
        add(RD, (u, here), G[slot, ring(2 - half), (low, high)[part]])
        remote(RD.at[u, here], RD.at[u, there], slot, u, 1, 2).start()

    def third_low(u, slot):
        half_on(u, slot, 0, low_sem.at[u])

    def third_rest(u, slot):
        pass_on(u, slot, 0, 2)
        half_on(u, slot, 1, recv_sem.at[u, 1, 1])

    def finish(u, slot, which, layer, t):
        received(u, 0, half - 1)
        received(u, 1, half - 1)
        total = G[slot, me].astype(F32) + RU[u, rows(half - 1)].astype(F32) + RD[u, rows(half - 1)].astype(F32)
        total = total.astype(BF16)
        wide = total.astype(F32)
        SQ[...] += jnp.sum((wide * wide).reshape(-1, 8, dim), axis=0)
        if which == 0:
            OD[layer, at(t, LANES), :] = total
        else:
            out = (OG, OU)[which - 1]
            for b in range(n):
                piece = total[hr * (b // (n // 2)) : hr * (b // (n // 2)) + hr, LANES * (b % (n // 2)) : LANES * (b % (n // 2)) + LANES]
                out[layer, :, pl.ds(pl.multiple_of(b * share + t * LANES, LANES), LANES)] = piece
        for way in range(2):
            for step in range(half):
                src = G.at[slot, 0, whole] if step > 0 else G.at[slot, 0, low]
                pltpu.make_async_copy(src, src, send_sem.at[slot, way, step]).wait()

    SQ[...] = jnp.zeros_like(SQ)

    def tile_step(k):
        wk = k + tiles
        slot = lax.rem(wk, 2)
        base = lax.rem(k, 2) * 3
        prev = 3 - base
        u0 = 3 * k
        p0 = u0 - 3
        going = k >= 1
        old_t = lax.rem(k - 1 + tiles, tiles)
        old_layer = jnp.where(k - 1 < tiles, 1, 0)
        fetched(wk)

        @pl.when(k < 2 * tiles - 1)
        def _():
            fetch(wk + 1)

        def when(cond):
            return pl.when(going & cond)

        def hidden(j, i):
            for b, c in ((0, 0), (0, 1), (1, 0), (1, 1)):
                here = pl.ds(pl.multiple_of(j * cols + c * (cols // 2), cols // 2), cols // 2)
                place = tok(2 * i + b)
                g = dot(A[place, :], WG[slot, :, here])
                u = dot(A[place, :], WU[slot, :, here])
                back = dot_t(D[place, :], WD[slot, here, :]).astype(BF16).astype(F32)
                s = 0.5 * jnp.tanh(0.5 * g) + 0.5
                silu = g * s
                ACT[place, here] = (silu * u).astype(BF16)
                DU[place, here] = (back * silu).astype(BF16)
                DG[place, here] = (back * u * (s + silu * (1.0 - s))).astype(BF16)

        def wide_part(src, unit, j):
            part = dot(AT[...], src[:, at(j, cols)]).astype(BF16)
            G[base + unit, :, at(j, hr), :] = part.reshape(n, dim // n, cols)

        gate, upper = (u0 + 1, base + 1), (u0 + 2, base + 2)
        old, old_gate, old_upper = (p0, prev), (p0 + 1, prev + 1), (p0 + 2, prev + 2)

        def halves(j):
            def some(i):
                hidden(j, i)

                @when((j == 0) & (i == 0))
                def _():
                    later(*old, 2)
                    later(*old_upper, 3)

                @pl.when((k == 0) & (j == 1) & (i == 0))
                def _():
                    third_low(*gate)

                @pl.when((k == 0) & (j == 1) & (i == 1))
                def _():
                    second_low(*upper)

            loop(blocks // 2, some)
            wide_part(DG, 1, j)

            @pl.when(j == 0)
            def _():
                begin_low(*gate)

            @pl.when(j == 1)
            def _():
                begin_high(*gate)

            @pl.when((j == 1) & (k == 0))
            def _():
                second_low(*gate)

            wide_part(DU, 2, j)

            @pl.when(j == 0)
            def _():
                begin_low(*upper)

            @pl.when(j == 1)
            def _():
                begin_high(*upper)

            @when(j == 1)
            def _():
                later(*old, 3)
                finish(*old_gate, 1, old_layer, old_t)
                finish(*old_upper, 2, old_layer, old_t)
                second_low(*gate)

            @pl.when((j == 1) & (k == 0))
            def _():
                third_low(*upper)

        loop(2, halves)

        def down_part(j):
            part = dot(DT[...], ACT[:, at(j, cols)])
            flipped = part.T.astype(BF16)
            for b in range(cols // LANES):
                G[base, j * (cols // LANES) + b] = flipped[b * LANES : (b + 1) * LANES]

            @pl.when(j == 0)
            def _():
                second_high(*gate)

        loop(2, down_part)
        begin_low(u0, base)
        begin_high(u0, base)

        @pl.when(going)
        def _():
            second_low(*upper)

        @pl.when(k == tiles - 1)
        def _():
            loop(blocks, lambda i: x_again(i).start())

        def ring_part(i):
            @pl.when(i == 0)
            def _():
                second_high(*upper)

            @pl.when((i == 0) & (k == 0))
            def _():
                second_low(u0, base)
                third_rest(*gate)

            @when(i == 2)
            def _():
                finish(*old, 0, old_layer, old_t)
                later(*gate, 2)

        @pl.when(k < tiles)
        def _():
            def input_part(i):
                so_far = jnp.where(k == 0, 0.0, DA[tok(i), :])
                DA[tok(i), :] = so_far + (dot_t(DG[tok(i), :], WG[slot]) + dot_t(DU[tok(i), :], WU[slot]))
                ring_part(i)

            loop(blocks, input_part)

        @pl.when(k >= tiles)
        def _():
            loop(blocks, ring_part)

        @pl.when(k == tiles - 1)
        def _():
            def between(i):
                h = H[tok(i), :].astype(F32)
                da = DA[tok(i), :].astype(BF16).astype(F32)
                r = scale_of(h)
                dh = (r * da - h * (r * r * r * jnp.mean(h * da, -1, keepdims=True))).astype(BF16)
                d = (D[tok(i), :].astype(F32) + dh.astype(F32)).astype(BF16)
                D[tok(i), :] = d
                DT[:, tok(i)] = d.T
                x_again(i).wait()
                wide = ACT[tok(i), pl.ds(0, dim)].astype(F32)
                a = (wide * scale_of(wide)).astype(BF16)
                A[tok(i), :] = a
                AT[:, tok(i)] = a.T

                @pl.when(i == 1)
                def _():
                    second_low(u0, base)
                    second_high(u0, base)

            loop(blocks, between)

        @pl.when(going & (k != tiles - 1))
        def _():
            second_low(u0, base)

        @pl.when(k != tiles - 1)
        def _():
            second_high(u0, base)

        @pl.when(k == 0)
        def _():
            third_rest(*upper)

        @pl.when(going)
        def _():
            later(*upper, 2)

        later(*gate, 3)

    loop(2 * tiles, tile_step)

    ahead = (
        pltpu.make_async_copy(wd_hbm.at[layers - 1, at(me, share), :], PW, ahead_sem.at[0]),
        pltpu.make_async_copy(md_hbm.at[layers - 1], PM, ahead_sem.at[1]),
        pltpu.make_async_copy(vd_hbm.at[layers - 1], PV, ahead_sem.at[2]),
    )
    for copy in ahead:
        copy.start()

    end = 2 * tiles - 1
    u0, base = 3 * end, (end % 2) * 3
    later(u0, base, 2)
    later(u0 + 2, base + 2, 3)
    later(u0, base, 3)
    for j in (1, 2, 0):
        finish(u0 + j, base + j, j, 0, tiles - 1)

    squares = SQ[:, :LANES]
    for j in range(1, dim // LANES):
        squares += SQ[:, j * LANES : (j + 1) * LANES]
    ALL[me] = squares

    def tell(d):
        return pltpu.make_async_remote_copy(
            src_ref=ALL.at[me],
            dst_ref=ALL.at[me],
            send_sem=sq_send.at[d],
            recv_sem=sq_recv.at[d],
            device_id={"dp": ring(d)},
            device_id_type=MESH,
        )

    for d in range(1, n):
        tell(d).start()
    for d in range(1, n):
        tell(d).wait()
    for copy in ahead:
        copy.wait()


def gradients(n, x, dy, w_gate, w_up, w_down, m_down, v_down):
    layers, dim, ff = w_gate.shape
    tokens = x.shape[1]
    blocks = 4
    share = ff // n
    tiles = share // LANES
    tile = n * LANES
    units = 3 * layers * tiles
    half = n // 2
    land = LANES // 2 + LANES * (half - 1)
    any_space = pl.BlockSpec(memory_space=pl.ANY)
    return pl.pallas_call(
        functools.partial(grad_kernel, n, layers, (tokens, dim, ff, blocks)),
        out_shape=tuple(
            kept(shape, dtype)
            for shape, dtype in (
                ((layers, dim // n, ff), BF16),
                ((layers, dim // n, ff), BF16),
                ((layers, share, dim), BF16),
                ((n, 8, LANES), F32),
                ((share, dim), BF16),
                ((share, dim), F32),
                ((share, dim), F32),
            )
        ),
        in_specs=[any_space] * 7,
        out_specs=(pl.BlockSpec(memory_space=pltpu.VMEM),) * 7,
        scratch_shapes=[
            pltpu.VMEM((tokens, dim), BF16),
            pltpu.VMEM((dim, tokens), BF16),
            pltpu.VMEM((tokens, dim), BF16),
            pltpu.VMEM((dim, tokens), BF16),
            pltpu.VMEM((tokens, dim), BF16),
            pltpu.VMEM((tokens, tile), BF16),
            pltpu.VMEM((tokens, tile), BF16),
            pltpu.VMEM((tokens, tile), BF16),
            pltpu.VMEM((tokens, dim), F32),
            pltpu.VMEM((2, dim, tile), BF16),
            pltpu.VMEM((2, dim, tile), BF16),
            pltpu.VMEM((2, tile, dim), BF16),
            pltpu.VMEM((6, n, LANES, dim), BF16),
            pltpu.VMEM((units, land, dim), BF16),
            pltpu.VMEM((units, land, dim), BF16),
            pltpu.VMEM((8, dim), F32),
            pltpu.SemaphoreType.DMA((blocks,)),
            pltpu.SemaphoreType.DMA((blocks,)),
            pltpu.SemaphoreType.DMA((2, 3)),
            pltpu.SemaphoreType.DMA((3,)),
            pltpu.SemaphoreType.DMA((6, 2, half)),
            pltpu.SemaphoreType.DMA((units, 2, half)),
            pltpu.SemaphoreType.DMA((units,)),
            pltpu.SemaphoreType.DMA((n,)),
            pltpu.SemaphoreType.DMA((n,)),
        ],
        compiler_params=pltpu.CompilerParams(collective_id=0, has_side_effects=True, vmem_limit_bytes=59 * 2**20),
        name="grads",
    )(*(pinned(t, pltpu.HBM) for t in (x, dy, w_gate, w_up, w_down, m_down, v_down)))


def turns(layers):
    return [(2, l) for l in reversed(range(layers))] + [(a, l) for l in reversed(range(layers)) for a in (0, 1)]


def update_kernel(n, count, parts, *refs):
    G, w_hbm, m_hbm, v_hbm = (refs[i : i + 3] for i in (0, 4, 10, 13))
    SQ, PW, PM, PV = refs[3], *refs[7:10]
    N, M, V = (refs[i : i + 3] for i in (16, 19, 22))
    last = refs[25:27]
    W = refs[27:30]
    in_sem, last_sem, send_sem, recv_sem = refs[30:]
    me = lax.axis_index("dp")
    half = n // 2
    up, down = lax.rem(me + 1, n), lax.rem(me + n - 1, n)
    ring = lambda d: lax.rem(me + d + n, n)
    layers = G[0].shape[0]

    barrier = pltpu.get_barrier_semaphore()
    for peer in (up, down):
        pl.semaphore_signal(barrier, inc=1, device_id={"dp": peer}, device_id_type=MESH)

    order = turns(layers)
    loads = {}
    for a, l in order[1:]:
        rows = G[a].shape[1]
        own = pl.ds(pl.multiple_of(me * rows, rows), rows)
        loads[a, l] = (
            pltpu.make_async_copy(w_hbm[a].at[l, own, :], W[a].at[l], in_sem.at[0, a, l]),
            pltpu.make_async_copy(m_hbm[a].at[l], M[a].at[l], in_sem.at[1, a, l]),
            pltpu.make_async_copy(v_hbm[a].at[l], V[a].at[l], in_sem.at[2, a, l]),
        )
    total = jnp.sum(jnp.sum(SQ[...], axis=0), axis=(0, 1), keepdims=True)
    factor = jnp.minimum(1.0, 0.5 * lax.rsqrt(total / count + 1e-30))

    def shape(a):
        rows, cols = G[a].shape[1:]
        return (rows, cols // parts, 0) if a < 2 else (rows // parts, cols, 1)

    def place(a, l, p, owner, part):
        rows = G[a].shape[1]
        r, c, split = shape(a)
        hr = r // 2
        start = owner * rows + (p * r if split else 0)
        start, size = (start, r) if part == 2 else (start + part * hr, hr)
        return (l, pl.ds(pl.multiple_of(start, hr), size), pl.ds(0 if split else p * c, c))

    def send(i, a, l, p, way, step):
        owner = ring(-step) if way == 0 else ring(step)
        ref = N[a].at[place(a, l, p, owner, 2 if step < half - 1 else way)]
        return pltpu.make_async_remote_copy(
            src_ref=ref,
            dst_ref=ref,
            send_sem=send_sem.at[i, way, step],
            recv_sem=recv_sem.at[i, way, step],
            device_id={"dp": (up, down)[way]},
            device_id_type=MESH,
        )

    def came(i, a, l, p, way, step):
        owner = ring(-step - 1) if way == 0 else ring(step + 1)
        where = place(a, l, p, owner, 2 if step < half - 1 else way)
        ref = N[a].at[where]
        pltpu.make_async_copy(ref, ref, recv_sem.at[i, way, step]).wait()

    def adam(a, l, p):
        r, c, split = shape(a)
        rows = G[a].shape[1]
        step = 32
        lane = pl.ds(0 if split else p * c, c)

        def some(i):
            row = pl.ds(pl.multiple_of((p * r if split else 0) + i * step, step), step)
            old = (PW[row, lane], PM[row, lane], PV[row, lane]) if (a, l) == order[0] else (W[a][l, row, lane], M[a][l, row, lane], V[a][l, row, lane])
            g = G[a][l, row, lane].astype(F32) * factor
            m = 0.9 * old[1] + 0.1 * g
            v = 0.95 * old[2] + 0.05 * g * g
            M[a][l, row, lane] = m
            V[a][l, row, lane] = v
            w = old[0].astype(F32)
            new = (w - 0.02 * (m * lax.rsqrt(v + 1e-8) + 0.1 * w)).astype(BF16)
            there = pl.ds(pl.multiple_of(me * rows + (p * r if split else 0) + i * step, step), step)
            N[a][l, there, lane] = new

        loop(r // step, some)

    chunks = []
    for a, l in order:
        for p in range(parts):
            chunks.append((len(chunks), a, l, p))
    for i, a, l, p in chunks:
        if p == 0:
            for copy in loads.get((a, l), ()):
                copy.wait()
        adam(a, l, p)
        if i == 0:
            pl.semaphore_wait(barrier, 2)
        send(i, a, l, p, 0, 0).start()
        send(i, a, l, p, 1, 0).start()
        if i == 0:
            for copies in loads.values():
                for copy in copies:
                    copy.start()
    late = order[len(order) - LATE :]

    def hops(a, l):
        return half - 1 if (a, l) in late else half

    def to_permute(a, l, way):
        rows = G[a].shape[1]
        owner = ring(1 - half) if way == 0 else ring(half - 1)
        src = N[a].at[l, pl.ds(pl.multiple_of(owner * rows + way * (rows // 2), rows // 2), rows // 2), :]
        return pltpu.make_async_copy(src, last[way].at[late.index((a, l))], last_sem.at[way, late.index((a, l))])

    for step in range(half):
        for i, a, l, p in chunks:
            for way in range(2):
                if step < hops(a, l):
                    came(i, a, l, p, way, step)
                if step < hops(a, l) - 1:
                    send(i, a, l, p, way, step + 1).start()
                elif step == half - 2 and p == parts - 1:
                    to_permute(a, l, way).start()
    for i, a, l, p in chunks:
        for way in range(2):
            for step in range(hops(a, l)):
                send(i, a, l, p, way, step).wait_send()
    for a, l in late:
        for way in range(2):
            to_permute(a, l, way).wait()


def store_kernel(count, *refs):
    src, dst, sem = refs[:count], refs[count : 2 * count], refs[-1]
    copies = [
        pltpu.make_async_copy(a.at[l], b.at[l], sem.at[i, l])
        for i, (a, b) in enumerate(zip(src, dst, strict=True))
        for l in range(a.shape[0])
    ]
    for copy in copies:
        copy.start()
    for copy in copies:
        copy.wait()


def store(arrays):
    count = len(arrays)
    return pl.pallas_call(
        functools.partial(store_kernel, count),
        out_shape=tuple(jax.ShapeDtypeStruct(t.shape, t.dtype) for t in arrays),
        in_specs=[pl.BlockSpec(memory_space=pltpu.VMEM)] * count,
        out_specs=(pl.BlockSpec(memory_space=pl.ANY),) * count,
        scratch_shapes=[pltpu.SemaphoreType.DMA((count, arrays[0].shape[0]))],
        compiler_params=pltpu.CompilerParams(vmem_limit_bytes=2**20),
        cost_estimate=pl.CostEstimate(flops=10_000_000_000, bytes_accessed=0, transcendentals=0),
        name="store",
    )(*(pinned(t, pltpu.VMEM) for t in arrays))


def place_kernel(n, count, *refs):
    up_ref, down_ref = refs[count : count + 2]
    outs, sem = refs[count + 2 : -1], refs[-1]
    opposite = lax.rem(lax.axis_index("dp") + n // 2, n)
    hr = up_ref.shape[1]
    copies = []
    for i, (a, l) in enumerate(turns(outs[0].shape[0])[-LATE:]):
        for way, src in enumerate((up_ref, down_ref)):
            there = pl.ds(pl.multiple_of(opposite * 2 * hr + way * hr, hr), hr)
            copies.append(pltpu.make_async_copy(src.at[i], outs[a].at[l, there, :], sem.at[i, way]))
    for copy in copies:
        copy.start()
    for copy in copies:
        copy.wait()


def place_last(n, arrays, came):
    count = len(arrays)
    any_space = pl.BlockSpec(memory_space=pl.ANY)
    in_vmem = pl.BlockSpec(memory_space=pltpu.VMEM)
    return pl.pallas_call(
        functools.partial(place_kernel, n, count),
        out_shape=tuple(jax.ShapeDtypeStruct(t.shape, t.dtype) for t in arrays),
        in_specs=[any_space] * count + [in_vmem] * 2,
        out_specs=(any_space,) * count,
        scratch_shapes=[pltpu.SemaphoreType.DMA((LATE, 2))],
        input_output_aliases={i: i for i in range(count)},
        compiler_params=pltpu.CompilerParams(vmem_limit_bytes=2**20),
        name="place",
    )(*(pinned(t, pltpu.HBM) for t in arrays), *came)


def update(n, made, w, m, v):
    layers = w[0].shape[0]
    parts = 2
    chunks = layers * 3 * parts
    count = sum(t.size for t in w)
    any_space = pl.BlockSpec(memory_space=pl.ANY)
    in_vmem = pl.BlockSpec(memory_space=pltpu.VMEM)
    half = n // 2
    g, squares, ahead = made[:3], made[3], made[4:]
    return pl.pallas_call(
        functools.partial(update_kernel, n, float(count), parts),
        out_shape=tuple(kept(t.shape, BF16) for t in w)
        + tuple(kept(t.shape, F32) for t in m + v)
        + (jax.ShapeDtypeStruct((LATE, m[0].shape[1] // 2, m[0].shape[2]), BF16),) * 2,
        in_specs=[in_vmem] * 4 + [any_space] * 3 + [in_vmem] * 3 + [any_space] * 6,
        out_specs=(in_vmem,) * 9 + (any_space,) * 2,
        scratch_shapes=[pltpu.VMEM(t.shape, BF16) for t in m]
        + [
            pltpu.SemaphoreType.DMA((3, 3, layers)),
            pltpu.SemaphoreType.DMA((2, LATE)),
            pltpu.SemaphoreType.DMA((chunks, 2, half)),
            pltpu.SemaphoreType.DMA((chunks, 2, half)),
        ],
        compiler_params=pltpu.CompilerParams(collective_id=1, has_side_effects=True, vmem_limit_bytes=12 * 2**20),
        name="update",
    )(
        *(pinned(t, pltpu.VMEM) for t in (*g, squares)),
        *(pinned(t, pltpu.HBM) for t in w),
        *(pinned(t, pltpu.VMEM) for t in ahead),
        *(pinned(t, pltpu.HBM) for t in (*m, *v)),
    )


def solution(mesh):
    n = mesh.shape["dp"]

    def step(x, dy, *arrays):
        w, m, v = (arrays[i : i + 3] for i in (0, 3, 6))
        *new, up, down = update(n, gradients(n, x, dy, *w, m[2], v[2]), w, m, v)
        came = tuple(lax.ppermute(t, "dp", [(i, (i + d) % n) for i in range(n)]) for t, d in ((up, 1), (down, -1)))
        out = store(new)
        return (*place_last(n, out[:2], came), *out[2:])

    shard = P(None, "dp", None)
    return jax.shard_map(
        step,
        mesh=mesh,
        in_specs=(P(("rep", "dp"), None, None),) * 2 + (P(),) * 3 + (shard,) * 6,
        out_specs=(P("rep", None, None),) * 3 + (P("rep", "dp", None),) * 6,
        check_vma=False,
    )
```

```python
import functools

import jax
import jax.numpy as jnp
from jax import lax
from jax.experimental import pallas as pl
from jax.experimental.pallas import tpu as pltpu
from jax.sharding import PartitionSpec as P

F32 = jnp.float32
BF16 = jnp.bfloat16
MESH = pl.DeviceIdType.MESH
LANES = 128
LATE = 4


def dot(a, b):
    return jnp.dot(a, b, preferred_element_type=F32)


def dot_t(a, b):
    return lax.dot_general(a, b, (((1,), (1,)), ((), ())), preferred_element_type=F32)


def scale_of(wide):
    return lax.rsqrt(jnp.mean(wide * wide, -1, keepdims=True) + 1e-6)


def pinned(t, space):
    return pltpu.with_memory_space_constraint(t, space)


def kept(shape, dtype):
    return pltpu.VMEM(shape, dtype)


def loop(count, body):
    lax.fori_loop(0, count, lambda i, c: (body(i), c)[1], 0)


def at(i, size):
    return pl.ds(pl.multiple_of(i * size, size), size)


def grad_kernel(n, layers, shapes, *refs):
    (x_hbm, dy_hbm, wg_hbm, wu_hbm, wd_hbm, md_hbm, vd_hbm) = refs[:7]
    (OG, OU, OD, ALL, PW, PM, PV) = refs[7:14]
    (A, AT, D, DT, H, ACT, DG, DU, DA, WG, WU, WD, G, RU, RD, SQ, *sems) = refs[14:]
    x_sem, dy_sem, w_sem, ahead_sem, send_sem, recv_sem, low_sem, sq_send, sq_recv = sems
    tokens, dim, ff, blocks = shapes
    share = ff // n
    tiles = share // LANES
    tile = n * LANES
    tb = tokens // blocks
    half = n // 2
    hr = LANES // 2
    cols = tile // 2
    me = lax.axis_index("dp")
    up, down = lax.rem(me + 1, n), lax.rem(me + n - 1, n)
    ring = lambda d: lax.rem(me + d + n, n)

    def tok(i):
        return at(i, tb)

    def fetch(k):
        slot = lax.rem(k, 2)
        layer = lax.rem(k // tiles, 2)
        t = lax.rem(k, tiles)

        def one(b):
            place = pl.ds(pl.multiple_of(b * share + t * LANES, LANES), LANES)
            here = at(b, LANES)
            pltpu.make_async_copy(wg_hbm.at[layer, :, place], WG.at[slot, :, here], w_sem.at[slot, 0]).start()
            pltpu.make_async_copy(wu_hbm.at[layer, :, place], WU.at[slot, :, here], w_sem.at[slot, 1]).start()
            pltpu.make_async_copy(wd_hbm.at[layer, place, :], WD.at[slot, here, :], w_sem.at[slot, 2]).start()

        loop(n, one)

    def fetched(k):
        slot = lax.rem(k, 2)
        pltpu.make_async_copy(WG.at[slot], WG.at[slot], w_sem.at[slot, 0]).wait()
        pltpu.make_async_copy(WU.at[slot], WU.at[slot], w_sem.at[slot, 1]).wait()
        pltpu.make_async_copy(WD.at[slot], WD.at[slot], w_sem.at[slot, 2]).wait()

    def x_copy(i):
        return pltpu.make_async_copy(x_hbm.at[0, tok(i), :], H.at[tok(i), :], x_sem.at[i])

    def x_again(i):
        return pltpu.make_async_copy(x_hbm.at[0, tok(i), :], ACT.at[tok(i), pl.ds(0, dim)], x_sem.at[i])

    def dy_copy(i):
        return pltpu.make_async_copy(dy_hbm.at[0, tok(i), :], D.at[tok(i), :], dy_sem.at[i])

    barrier = pltpu.get_barrier_semaphore()
    for d in range(1, n):
        pl.semaphore_signal(barrier, inc=1, device_id={"dp": ring(d)}, device_id_type=MESH)

    x_copy(0).start()
    fetch(0)
    loop(blocks - 1, lambda i: x_copy(i + 1).start())
    loop(blocks, lambda i: dy_copy(i).start())

    def first_norm(i):
        wide = H[tok(i), :].astype(F32)
        A[tok(i), :] = (wide * scale_of(wide)).astype(BF16)
        DA[tok(i), :] = jnp.zeros((tb, dim), F32)

    def forward(k, i, act=ACT):
        slot = lax.rem(k, 2)
        for j in range(4):
            here = pl.ds(j * (tile // 4), tile // 4)
            g = dot(A[tok(i), :], WG[slot, :, here])
            u = dot(A[tok(i), :], WU[slot, :, here])
            s = 0.5 * jnp.tanh(0.5 * g) + 0.5
            act[tok(i), here] = (g * s * u).astype(BF16)
        DA[tok(i), :] += dot(act[tok(i), :], WD[slot])

    def second_norm(i):
        h = (H[tok(i), :].astype(F32) + DA[tok(i), :].astype(BF16).astype(F32)).astype(BF16)
        wide = h.astype(F32)
        return h, (wide * scale_of(wide)).astype(BF16)

    def second_norm_kept(i, h, a):
        H[tok(i), :] = h
        A[tok(i), :] = a
        AT[:, tok(i)] = a.T

    x_copy(0).wait()
    first_norm(0)
    fetched(0)
    fetch(1)

    def opening(i):
        x_copy(i + 1).wait()
        forward(0, i)
        first_norm(i + 1)

    loop(blocks - 1, opening)

    def middle(j):
        q = blocks - 1 + 2 * j

        @pl.when(lax.rem(q + 1, blocks) == 0)
        def _():
            fetched((q + 1) // blocks)

        @pl.when((lax.rem(q, blocks) == 1) & (q // blocks < tiles - 1))
        def _():
            fetch(q // blocks + 1)

        seen = [jnp.minimum(2 * j + d, blocks - 1) for d in range(2)]

        @pl.when(2 * j < blocks)
        def _():
            dy_copy(2 * j).wait()
            dy_copy(2 * j + 1).wait()

        forward(q // blocks, lax.rem(q, blocks))
        forward((q + 1) // blocks, lax.rem(q + 1, blocks), DG)
        for i in seen:
            DT[:, tok(i)] = D[tok(i), :].T

    loop((tiles - 2) * blocks // 2 + 1, middle)
    fetch(tiles)

    def closing(i):
        normed = second_norm(i)
        forward(tiles - 1, i + 1)
        second_norm_kept(i, *normed)

    loop(blocks - 1, closing)
    second_norm_kept(blocks - 1, *second_norm(blocks - 1))

    pl.semaphore_wait(barrier, n - 1)

    def remote(src, dst, slot, u, way, step, arrival=None):
        return pltpu.make_async_remote_copy(
            src_ref=src,
            dst_ref=dst,
            send_sem=send_sem.at[slot, way, step],
            recv_sem=recv_sem.at[u, way, step] if arrival is None else arrival,
            device_id={"dp": (up, down)[way]},
            device_id_type=MESH,
        )

    low, high, whole = pl.ds(0, hr), pl.ds(hr, hr), pl.ds(0, 2 * hr)
    lands = (RU, RD)

    def rows(step):
        return pl.ds(hr + (step - 1) * 2 * hr, 2 * hr)

    def begin_low(u, slot):
        remote(G.at[slot, ring(half), low], RU.at[u, low], slot, u, 0, 0).start()
        remote(G.at[slot, ring(1 - half), low], RD.at[u, pl.ds(hr, hr)], slot, u, 1, 1, low_sem.at[u]).start()

    def begin_high(u, slot):
        remote(G.at[slot, ring(half), high], RD.at[u, low], slot, u, 1, 0).start()
        remote(G.at[slot, ring(half - 1), high], RU.at[u, pl.ds(2 * hr, hr)], slot, u, 0, 1).start()

    def arrived(land, sem):
        pltpu.make_async_copy(land, land, sem).wait()

    def received(u, way, step):
        if (way, step) == (1, 1):
            arrived(RD.at[u, pl.ds(hr, hr)], low_sem.at[u])
            arrived(RD.at[u, pl.ds(2 * hr, hr)], recv_sem.at[u, 1, 1])
        else:
            arrived(lands[way].at[u, rows(step) if step else low], recv_sem.at[u, way, step])

    def add(land, place, mine):
        land[place] = (land[place].astype(F32) + mine.astype(F32)).astype(BF16)

    def second_low(u, slot):
        received(u, 0, 0)
        add(RU, (u, low), G[slot, ring(half - 1), low])
        remote(RU.at[u, low], RU.at[u, pl.ds(hr, hr)], slot, u, 0, 1).start()

    def second_high(u, slot):
        received(u, 1, 0)
        add(RD, (u, low), G[slot, ring(1 - half), high])
        remote(RD.at[u, low], RD.at[u, pl.ds(2 * hr, hr)], slot, u, 1, 1).start()

    def pass_on(u, slot, way, step):
        received(u, way, step - 1)
        add(lands[way], (u, rows(step - 1)), G[slot, ring(half - step if way == 0 else step - half)])
        remote(lands[way].at[u, rows(step - 1)], lands[way].at[u, rows(step)], slot, u, way, step).start()

    def later(u, slot, step):
        pass_on(u, slot, 0, step)
        pass_on(u, slot, 1, step)

    def half_on(u, slot, part, sem):
        here, there = pl.ds((1 + part) * hr, hr), pl.ds((3 + part) * hr, hr)
        arrived(RD.at[u, here], sem)
        add(RD, (u, here), G[slot, ring(2 - half), (low, high)[part]])
        remote(RD.at[u, here], RD.at[u, there], slot, u, 1, 2).start()

    def third_low(u, slot):
        half_on(u, slot, 0, low_sem.at[u])

    def third_rest(u, slot):
        pass_on(u, slot, 0, 2)
        half_on(u, slot, 1, recv_sem.at[u, 1, 1])

    def finish(u, slot, which, layer, t):
        received(u, 0, half - 1)
        received(u, 1, half - 1)
        total = G[slot, me].astype(F32) + RU[u, rows(half - 1)].astype(F32) + RD[u, rows(half - 1)].astype(F32)
        total = total.astype(BF16)
        wide = total.astype(F32)
        SQ[...] += jnp.sum((wide * wide).reshape(-1, 8, dim), axis=0)
        if which == 0:
            OD[layer, at(t, LANES), :] = total
        else:
            out = (OG, OU)[which - 1]
            for b in range(n):
                piece = total[hr * (b // (n // 2)) : hr * (b // (n // 2)) + hr, LANES * (b % (n // 2)) : LANES * (b % (n // 2)) + LANES]
                out[layer, :, pl.ds(pl.multiple_of(b * share + t * LANES, LANES), LANES)] = piece
        for way in range(2):
            for step in range(half):
                src = G.at[slot, 0, whole] if step > 0 else G.at[slot, 0, low]
                pltpu.make_async_copy(src, src, send_sem.at[slot, way, step]).wait()

    SQ[...] = jnp.zeros_like(SQ)

    def tile_step(k):
        wk = k + tiles
        slot = lax.rem(wk, 2)
        base = lax.rem(k, 2) * 3
        prev = 3 - base
        u0 = 3 * k
        p0 = u0 - 3
        going = k >= 1
        old_t = lax.rem(k - 1 + tiles, tiles)
        old_layer = jnp.where(k - 1 < tiles, 1, 0)
        fetched(wk)

        @pl.when(k < 2 * tiles - 1)
        def _():
            fetch(wk + 1)

        def when(cond):
            return pl.when(going & cond)

        def hidden(j, i):
            place = pl.ds(pl.multiple_of(i * 2 * tb, 2 * tb), 2 * tb)
            for c in range(2):
                here = pl.ds(pl.multiple_of(j * cols + c * (cols // 2), cols // 2), cols // 2)
                g = dot(A[place, :], WG[slot, :, here])
                u = dot(A[place, :], WU[slot, :, here])
                back = dot_t(D[place, :], WD[slot, here, :]).astype(BF16).astype(F32)
                s = 0.5 * jnp.tanh(0.5 * g) + 0.5
                silu = g * s
                ACT[place, here] = (silu * u).astype(BF16)
                DU[place, here] = (back * silu).astype(BF16)
                DG[place, here] = (back * u * (s + silu * (1.0 - s))).astype(BF16)

        def wide_part(src, unit, j):
            part = dot(AT[...], src[:, at(j, cols)]).astype(BF16)
            G[base + unit, :, at(j, hr), :] = part.reshape(n, dim // n, cols)

        gate, upper = (u0 + 1, base + 1), (u0 + 2, base + 2)
        old, old_gate, old_upper = (p0, prev), (p0 + 1, prev + 1), (p0 + 2, prev + 2)

        def halves(j):
            def some(i):
                hidden(j, i)

                @when((j == 0) & (i == 0))
                def _():
                    later(*old, 2)
                    later(*old_upper, 3)

                @pl.when((k == 0) & (j == 1) & (i == 0))
                def _():
                    third_low(*gate)

                @pl.when((k == 0) & (j == 1) & (i == 1))
                def _():
                    second_low(*upper)

            loop(blocks // 2, some)
            wide_part(DG, 1, j)

            @pl.when(j == 0)
            def _():
                begin_low(*gate)

            @pl.when(j == 1)
            def _():
                begin_high(*gate)

            @pl.when((j == 1) & (k == 0))
            def _():
                second_low(*gate)

            wide_part(DU, 2, j)

            @pl.when(j == 0)
            def _():
                begin_low(*upper)

            @pl.when(j == 1)
            def _():
                begin_high(*upper)

            @when(j == 1)
            def _():
                later(*old, 3)
                finish(*old_gate, 1, old_layer, old_t)
                finish(*old_upper, 2, old_layer, old_t)
                second_low(*gate)

            @pl.when((j == 1) & (k == 0))
            def _():
                third_low(*upper)

        loop(2, halves)

        def down_part(j):
            part = dot(DT[...], ACT[:, at(j, cols)])
            flipped = part.T.astype(BF16)
            for b in range(cols // LANES):
                G[base, j * (cols // LANES) + b] = flipped[b * LANES : (b + 1) * LANES]

            @pl.when(j == 0)
            def _():
                second_high(*gate)

        loop(2, down_part)
        begin_low(u0, base)
        begin_high(u0, base)

        @pl.when(going)
        def _():
            second_low(*upper)

        @pl.when(k == tiles - 1)
        def _():
            loop(blocks, lambda i: x_again(i).start())

        def ring_part(i):
            @pl.when(i == 0)
            def _():
                second_high(*upper)

            @pl.when((i == 0) & (k == 0))
            def _():
                second_low(u0, base)
                third_rest(*gate)

            @when(i == 2)
            def _():
                finish(*old, 0, old_layer, old_t)
                later(*gate, 2)

        @pl.when(k < tiles)
        def _():
            def input_part(i):
                so_far = jnp.where(k == 0, 0.0, DA[tok(i), :])
                DA[tok(i), :] = so_far + (dot_t(DG[tok(i), :], WG[slot]) + dot_t(DU[tok(i), :], WU[slot]))
                ring_part(i)

            loop(blocks, input_part)

        @pl.when(k >= tiles)
        def _():
            loop(blocks, ring_part)

        @pl.when(k == tiles - 1)
        def _():
            def between(i):
                h = H[tok(i), :].astype(F32)
                da = DA[tok(i), :].astype(BF16).astype(F32)
                r = scale_of(h)
                dh = (r * da - h * (r * r * r * jnp.mean(h * da, -1, keepdims=True))).astype(BF16)
                d = (D[tok(i), :].astype(F32) + dh.astype(F32)).astype(BF16)
                D[tok(i), :] = d
                DT[:, tok(i)] = d.T
                x_again(i).wait()
                wide = ACT[tok(i), pl.ds(0, dim)].astype(F32)
                a = (wide * scale_of(wide)).astype(BF16)
                A[tok(i), :] = a
                AT[:, tok(i)] = a.T

                @pl.when(i == 1)
                def _():
                    second_low(u0, base)
                    second_high(u0, base)

            loop(blocks, between)

        @pl.when(going & (k != tiles - 1))
        def _():
            second_low(u0, base)

        @pl.when(k != tiles - 1)
        def _():
            second_high(u0, base)

        @pl.when(k == 0)
        def _():
            third_rest(*upper)

        @pl.when(going)
        def _():
            later(*upper, 2)

        later(*gate, 3)

    loop(2 * tiles, tile_step)

    ahead = (
        pltpu.make_async_copy(wd_hbm.at[layers - 1, at(me, share), :], PW, ahead_sem.at[0]),
        pltpu.make_async_copy(md_hbm.at[layers - 1], PM, ahead_sem.at[1]),
        pltpu.make_async_copy(vd_hbm.at[layers - 1], PV, ahead_sem.at[2]),
    )
    for copy in ahead:
        copy.start()

    end = 2 * tiles - 1
    u0, base = 3 * end, (end % 2) * 3
    later(u0, base, 2)
    later(u0 + 2, base + 2, 3)
    later(u0, base, 3)
    for j in (1, 2, 0):
        finish(u0 + j, base + j, j, 0, tiles - 1)

    squares = SQ[:, :LANES]
    for j in range(1, dim // LANES):
        squares += SQ[:, j * LANES : (j + 1) * LANES]
    ALL[me] = squares

    def tell(d):
        return pltpu.make_async_remote_copy(
            src_ref=ALL.at[me],
            dst_ref=ALL.at[me],
            send_sem=sq_send.at[d],
            recv_sem=sq_recv.at[d],
            device_id={"dp": ring(d)},
            device_id_type=MESH,
        )

    for d in range(1, n):
        tell(d).start()
    for d in range(1, n):
        tell(d).wait()
    for copy in ahead:
        copy.wait()


def gradients(n, x, dy, w_gate, w_up, w_down, m_down, v_down):
    layers, dim, ff = w_gate.shape
    tokens = x.shape[1]
    blocks = 4
    share = ff // n
    tiles = share // LANES
    tile = n * LANES
    units = 3 * layers * tiles
    half = n // 2
    land = LANES // 2 + LANES * (half - 1)
    any_space = pl.BlockSpec(memory_space=pl.ANY)
    return pl.pallas_call(
        functools.partial(grad_kernel, n, layers, (tokens, dim, ff, blocks)),
        out_shape=tuple(
            kept(shape, dtype)
            for shape, dtype in (
                ((layers, dim // n, ff), BF16),
                ((layers, dim // n, ff), BF16),
                ((layers, share, dim), BF16),
                ((n, 8, LANES), F32),
                ((share, dim), BF16),
                ((share, dim), F32),
                ((share, dim), F32),
            )
        ),
        in_specs=[any_space] * 7,
        out_specs=(pl.BlockSpec(memory_space=pltpu.VMEM),) * 7,
        scratch_shapes=[
            pltpu.VMEM((tokens, dim), BF16),
            pltpu.VMEM((dim, tokens), BF16),
            pltpu.VMEM((tokens, dim), BF16),
            pltpu.VMEM((dim, tokens), BF16),
            pltpu.VMEM((tokens, dim), BF16),
            pltpu.VMEM((tokens, tile), BF16),
            pltpu.VMEM((tokens, tile), BF16),
            pltpu.VMEM((tokens, tile), BF16),
            pltpu.VMEM((tokens, dim), F32),
            pltpu.VMEM((2, dim, tile), BF16),
            pltpu.VMEM((2, dim, tile), BF16),
            pltpu.VMEM((2, tile, dim), BF16),
            pltpu.VMEM((6, n, LANES, dim), BF16),
            pltpu.VMEM((units, land, dim), BF16),
            pltpu.VMEM((units, land, dim), BF16),
            pltpu.VMEM((8, dim), F32),
            pltpu.SemaphoreType.DMA((blocks,)),
            pltpu.SemaphoreType.DMA((blocks,)),
            pltpu.SemaphoreType.DMA((2, 3)),
            pltpu.SemaphoreType.DMA((3,)),
            pltpu.SemaphoreType.DMA((6, 2, half)),
            pltpu.SemaphoreType.DMA((units, 2, half)),
            pltpu.SemaphoreType.DMA((units,)),
            pltpu.SemaphoreType.DMA((n,)),
            pltpu.SemaphoreType.DMA((n,)),
        ],
        compiler_params=pltpu.CompilerParams(collective_id=0, has_side_effects=True, vmem_limit_bytes=59 * 2**20),
        name="grads",
    )(*(pinned(t, pltpu.HBM) for t in (x, dy, w_gate, w_up, w_down, m_down, v_down)))


def turns(layers):
    return [(2, l) for l in reversed(range(layers))] + [(a, l) for l in reversed(range(layers)) for a in (0, 1)]


def update_kernel(n, count, parts, *refs):
    G, w_hbm, m_hbm, v_hbm = (refs[i : i + 3] for i in (0, 4, 10, 13))
    SQ, PW, PM, PV = refs[3], *refs[7:10]
    N, M, V = (refs[i : i + 3] for i in (16, 19, 22))
    last = refs[25:27]
    W = refs[27:30]
    in_sem, last_sem, send_sem, recv_sem = refs[30:]
    me = lax.axis_index("dp")
    half = n // 2
    up, down = lax.rem(me + 1, n), lax.rem(me + n - 1, n)
    ring = lambda d: lax.rem(me + d + n, n)
    layers = G[0].shape[0]

    barrier = pltpu.get_barrier_semaphore()
    for peer in (up, down):
        pl.semaphore_signal(barrier, inc=1, device_id={"dp": peer}, device_id_type=MESH)

    order = turns(layers)
    loads = {}
    for a, l in order[1:]:
        rows = G[a].shape[1]
        own = pl.ds(pl.multiple_of(me * rows, rows), rows)
        loads[a, l] = (
            pltpu.make_async_copy(w_hbm[a].at[l, own, :], W[a].at[l], in_sem.at[0, a, l]),
            pltpu.make_async_copy(m_hbm[a].at[l], M[a].at[l], in_sem.at[1, a, l]),
            pltpu.make_async_copy(v_hbm[a].at[l], V[a].at[l], in_sem.at[2, a, l]),
        )
    total = jnp.sum(jnp.sum(SQ[...], axis=0), axis=(0, 1), keepdims=True)
    factor = jnp.minimum(1.0, 0.5 * lax.rsqrt(total / count + 1e-30))

    def shape(a):
        rows, cols = G[a].shape[1:]
        return (rows, cols // parts, 0) if a < 2 else (rows // parts, cols, 1)

    def place(a, l, p, owner, part):
        rows = G[a].shape[1]
        r, c, split = shape(a)
        hr = r // 2
        start = owner * rows + (p * r if split else 0)
        start, size = (start, r) if part == 2 else (start + part * hr, hr)
        return (l, pl.ds(pl.multiple_of(start, hr), size), pl.ds(0 if split else p * c, c))

    def send(i, a, l, p, way, step):
        owner = ring(-step) if way == 0 else ring(step)
        ref = N[a].at[place(a, l, p, owner, 2 if step < half - 1 else way)]
        return pltpu.make_async_remote_copy(
            src_ref=ref,
            dst_ref=ref,
            send_sem=send_sem.at[i, way, step],
            recv_sem=recv_sem.at[i, way, step],
            device_id={"dp": (up, down)[way]},
            device_id_type=MESH,
        )

    def came(i, a, l, p, way, step):
        owner = ring(-step - 1) if way == 0 else ring(step + 1)
        where = place(a, l, p, owner, 2 if step < half - 1 else way)
        ref = N[a].at[where]
        pltpu.make_async_copy(ref, ref, recv_sem.at[i, way, step]).wait()

    def adam(a, l, p):
        r, c, split = shape(a)
        rows = G[a].shape[1]
        step = 32
        lane = pl.ds(0 if split else p * c, c)

        def some(i):
            row = pl.ds(pl.multiple_of((p * r if split else 0) + i * step, step), step)
            old = (PW[row, lane], PM[row, lane], PV[row, lane]) if (a, l) == order[0] else (W[a][l, row, lane], M[a][l, row, lane], V[a][l, row, lane])
            g = G[a][l, row, lane].astype(F32) * factor
            m = 0.9 * old[1] + 0.1 * g
            v = 0.95 * old[2] + 0.05 * g * g
            M[a][l, row, lane] = m
            V[a][l, row, lane] = v
            w = old[0].astype(F32)
            new = (w - 0.02 * (m * lax.rsqrt(v + 1e-8) + 0.1 * w)).astype(BF16)
            there = pl.ds(pl.multiple_of(me * rows + (p * r if split else 0) + i * step, step), step)
            N[a][l, there, lane] = new

        loop(r // step, some)

    chunks = []
    for a, l in order:
        for p in range(parts):
            chunks.append((len(chunks), a, l, p))
    for i, a, l, p in chunks:
        if p == 0:
            for copy in loads.get((a, l), ()):
                copy.wait()
        adam(a, l, p)
        if i == 0:
            pl.semaphore_wait(barrier, 2)
        send(i, a, l, p, 0, 0).start()
        send(i, a, l, p, 1, 0).start()
        if i == 0:
            for copies in loads.values():
                for copy in copies:
                    copy.start()
    late = order[len(order) - LATE :]

    def hops(a, l):
        return half - 1 if (a, l) in late else half

    def to_permute(a, l, way):
        rows = G[a].shape[1]
        owner = ring(1 - half) if way == 0 else ring(half - 1)
        src = N[a].at[l, pl.ds(pl.multiple_of(owner * rows + way * (rows // 2), rows // 2), rows // 2), :]
        return pltpu.make_async_copy(src, last[way].at[late.index((a, l))], last_sem.at[way, late.index((a, l))])

    for step in range(half):
        for i, a, l, p in chunks:
            for way in range(2):
                if step < hops(a, l):
                    came(i, a, l, p, way, step)
                if step < hops(a, l) - 1:
                    send(i, a, l, p, way, step + 1).start()
                elif step == half - 2 and p == parts - 1:
                    to_permute(a, l, way).start()
    for i, a, l, p in chunks:
        for way in range(2):
            for step in range(hops(a, l)):
                send(i, a, l, p, way, step).wait_send()
    for a, l in late:
        for way in range(2):
            to_permute(a, l, way).wait()


def store_kernel(count, *refs):
    src, dst, sem = refs[:count], refs[count : 2 * count], refs[-1]
    copies = [
        pltpu.make_async_copy(a.at[l], b.at[l], sem.at[i, l])
        for i, (a, b) in enumerate(zip(src, dst, strict=True))
        for l in range(a.shape[0])
    ]
    for copy in copies:
        copy.start()
    for copy in copies:
        copy.wait()


def store(arrays):
    count = len(arrays)
    return pl.pallas_call(
        functools.partial(store_kernel, count),
        out_shape=tuple(jax.ShapeDtypeStruct(t.shape, t.dtype) for t in arrays),
        in_specs=[pl.BlockSpec(memory_space=pltpu.VMEM)] * count,
        out_specs=(pl.BlockSpec(memory_space=pl.ANY),) * count,
        scratch_shapes=[pltpu.SemaphoreType.DMA((count, arrays[0].shape[0]))],
        compiler_params=pltpu.CompilerParams(vmem_limit_bytes=2**20),
        cost_estimate=pl.CostEstimate(flops=10_000_000_000, bytes_accessed=0, transcendentals=0),
        name="store",
    )(*(pinned(t, pltpu.VMEM) for t in arrays))


def place_kernel(n, count, *refs):
    up_ref, down_ref = refs[count : count + 2]
    outs, sem = refs[count + 2 : -1], refs[-1]
    opposite = lax.rem(lax.axis_index("dp") + n // 2, n)
    hr = up_ref.shape[1]
    copies = []
    for i, (a, l) in enumerate(turns(outs[0].shape[0])[-LATE:]):
        for way, src in enumerate((up_ref, down_ref)):
            there = pl.ds(pl.multiple_of(opposite * 2 * hr + way * hr, hr), hr)
            copies.append(pltpu.make_async_copy(src.at[i], outs[a].at[l, there, :], sem.at[i, way]))
    for copy in copies:
        copy.start()
    for copy in copies:
        copy.wait()


def place_last(n, arrays, came):
    count = len(arrays)
    any_space = pl.BlockSpec(memory_space=pl.ANY)
    in_vmem = pl.BlockSpec(memory_space=pltpu.VMEM)
    return pl.pallas_call(
        functools.partial(place_kernel, n, count),
        out_shape=tuple(jax.ShapeDtypeStruct(t.shape, t.dtype) for t in arrays),
        in_specs=[any_space] * count + [in_vmem] * 2,
        out_specs=(any_space,) * count,
        scratch_shapes=[pltpu.SemaphoreType.DMA((LATE, 2))],
        input_output_aliases={i: i for i in range(count)},
        compiler_params=pltpu.CompilerParams(vmem_limit_bytes=2**20),
        name="place",
    )(*(pinned(t, pltpu.HBM) for t in arrays), *came)


def update(n, made, w, m, v):
    layers = w[0].shape[0]
    parts = 2
    chunks = layers * 3 * parts
    count = sum(t.size for t in w)
    any_space = pl.BlockSpec(memory_space=pl.ANY)
    in_vmem = pl.BlockSpec(memory_space=pltpu.VMEM)
    half = n // 2
    g, squares, ahead = made[:3], made[3], made[4:]
    return pl.pallas_call(
        functools.partial(update_kernel, n, float(count), parts),
        out_shape=tuple(kept(t.shape, BF16) for t in w)
        + tuple(kept(t.shape, F32) for t in m + v)
        + (jax.ShapeDtypeStruct((LATE, m[0].shape[1] // 2, m[0].shape[2]), BF16),) * 2,
        in_specs=[in_vmem] * 4 + [any_space] * 3 + [in_vmem] * 3 + [any_space] * 6,
        out_specs=(in_vmem,) * 9 + (any_space,) * 2,
        scratch_shapes=[pltpu.VMEM(t.shape, BF16) for t in m]
        + [
            pltpu.SemaphoreType.DMA((3, 3, layers)),
            pltpu.SemaphoreType.DMA((2, LATE)),
            pltpu.SemaphoreType.DMA((chunks, 2, half)),
            pltpu.SemaphoreType.DMA((chunks, 2, half)),
        ],
        compiler_params=pltpu.CompilerParams(collective_id=1, has_side_effects=True, vmem_limit_bytes=12 * 2**20),
        name="update",
    )(
        *(pinned(t, pltpu.VMEM) for t in (*g, squares)),
        *(pinned(t, pltpu.HBM) for t in w),
        *(pinned(t, pltpu.VMEM) for t in ahead),
        *(pinned(t, pltpu.HBM) for t in (*m, *v)),
    )


def solution(mesh):
    n = mesh.shape["dp"]

    def step(x, dy, *arrays):
        w, m, v = (arrays[i : i + 3] for i in (0, 3, 6))
        *new, up, down = update(n, gradients(n, x, dy, *w, m[2], v[2]), w, m, v)
        came = tuple(lax.ppermute(t, "dp", [(i, (i + d) % n) for i in range(n)]) for t, d in ((up, 1), (down, -1)))
        out = store(new)
        return (*place_last(n, out[:2], came), *out[2:])

    shard = P(None, "dp", None)
    return jax.shard_map(
        step,
        mesh=mesh,
        in_specs=(P(("rep", "dp"), None, None),) * 2 + (P(),) * 3 + (shard,) * 6,
        out_specs=(P("rep", None, None),) * 3 + (P("rep", "dp", None),) * 6,
        check_vma=False,
    )
```

```python
import functools

import jax
import jax.numpy as jnp
from jax import lax
from jax.experimental import pallas as pl
from jax.experimental.pallas import tpu as pltpu
from jax.sharding import PartitionSpec as P

F32 = jnp.float32
BF16 = jnp.bfloat16
MESH = pl.DeviceIdType.MESH
LANES = 128
LATE = 4


def dot(a, b):
    return jnp.dot(a, b, preferred_element_type=F32)


def dot_t(a, b):
    return lax.dot_general(a, b, (((1,), (1,)), ((), ())), preferred_element_type=F32)


def scale_of(wide):
    return lax.rsqrt(jnp.mean(wide * wide, -1, keepdims=True) + 1e-6)


def pinned(t, space):
    return pltpu.with_memory_space_constraint(t, space)


def kept(shape, dtype):
    return pltpu.VMEM(shape, dtype)


def loop(count, body):
    lax.fori_loop(0, count, lambda i, c: (body(i), c)[1], 0)


def at(i, size):
    return pl.ds(pl.multiple_of(i * size, size), size)


def grad_kernel(n, layers, shapes, *refs):
    (x_hbm, dy_hbm, wg_hbm, wu_hbm, wd_hbm, md_hbm, vd_hbm) = refs[:7]
    (OG, OU, OD, ALL, PW, PM, PV) = refs[7:14]
    (A, AT, D, DT, H, ACT, DG, DU, DA, WG, WU, WD, G, RU, RD, SQ, *sems) = refs[14:]
    x_sem, dy_sem, w_sem, ahead_sem, send_sem, recv_sem, low_sem, sq_send, sq_recv = sems
    tokens, dim, ff, blocks = shapes
    share = ff // n
    tiles = share // LANES
    tile = n * LANES
    tb = tokens // blocks
    half = n // 2
    hr = LANES // 2
    cols = tile // 2
    me = lax.axis_index("dp")
    up, down = lax.rem(me + 1, n), lax.rem(me + n - 1, n)
    ring = lambda d: lax.rem(me + d + n, n)

    def tok(i):
        return at(i, tb)

    def fetch(k):
        slot = lax.rem(k, 2)
        layer = lax.rem(k // tiles, 2)
        t = lax.rem(k, tiles)

        def one(b):
            place = pl.ds(pl.multiple_of(b * share + t * LANES, LANES), LANES)
            here = at(b, LANES)
            pltpu.make_async_copy(wg_hbm.at[layer, :, place], WG.at[slot, :, here], w_sem.at[slot, 0]).start()
            pltpu.make_async_copy(wu_hbm.at[layer, :, place], WU.at[slot, :, here], w_sem.at[slot, 1]).start()
            pltpu.make_async_copy(wd_hbm.at[layer, place, :], WD.at[slot, here, :], w_sem.at[slot, 2]).start()

        loop(n, one)

    def fetched(k):
        slot = lax.rem(k, 2)
        pltpu.make_async_copy(WG.at[slot], WG.at[slot], w_sem.at[slot, 0]).wait()
        pltpu.make_async_copy(WU.at[slot], WU.at[slot], w_sem.at[slot, 1]).wait()
        pltpu.make_async_copy(WD.at[slot], WD.at[slot], w_sem.at[slot, 2]).wait()

    def x_copy(i):
        return pltpu.make_async_copy(x_hbm.at[0, tok(i), :], H.at[tok(i), :], x_sem.at[i])

    def x_again(i):
        return pltpu.make_async_copy(x_hbm.at[0, tok(i), :], ACT.at[tok(i), pl.ds(0, dim)], x_sem.at[i])

    def dy_copy(i):
        return pltpu.make_async_copy(dy_hbm.at[0, tok(i), :], D.at[tok(i), :], dy_sem.at[i])

    barrier = pltpu.get_barrier_semaphore()
    for d in range(1, n):
        pl.semaphore_signal(barrier, inc=1, device_id={"dp": ring(d)}, device_id_type=MESH)

    x_copy(0).start()
    fetch(0)
    loop(blocks - 1, lambda i: x_copy(i + 1).start())
    loop(blocks, lambda i: dy_copy(i).start())

    def first_norm(i):
        wide = H[tok(i), :].astype(F32)
        A[tok(i), :] = (wide * scale_of(wide)).astype(BF16)
        DA[tok(i), :] = jnp.zeros((tb, dim), F32)

    def forward(k, i, act=ACT):
        slot = lax.rem(k, 2)
        for j in range(4):
            here = pl.ds(j * (tile // 4), tile // 4)
            g = dot(A[tok(i), :], WG[slot, :, here])
            u = dot(A[tok(i), :], WU[slot, :, here])
            s = 0.5 * jnp.tanh(0.5 * g) + 0.5
            act[tok(i), here] = (g * s * u).astype(BF16)
        DA[tok(i), :] += dot(act[tok(i), :], WD[slot])

    def second_norm(i):
        h = (H[tok(i), :].astype(F32) + DA[tok(i), :].astype(BF16).astype(F32)).astype(BF16)
        wide = h.astype(F32)
        return h, (wide * scale_of(wide)).astype(BF16)

    def second_norm_kept(i, h, a):
        H[tok(i), :] = h
        A[tok(i), :] = a
        AT[:, tok(i)] = a.T

    x_copy(0).wait()
    first_norm(0)
    fetched(0)
    fetch(1)

    def opening(i):
        x_copy(i + 1).wait()
        forward(0, i)
        first_norm(i + 1)

    loop(blocks - 1, opening)

    def middle(j):
        q = blocks - 1 + 2 * j

        @pl.when(lax.rem(q + 1, blocks) == 0)
        def _():
            fetched((q + 1) // blocks)

        @pl.when((lax.rem(q, blocks) == 1) & (q // blocks < tiles - 1))
        def _():
            fetch(q // blocks + 1)

        seen = [jnp.minimum(2 * j + d, blocks - 1) for d in range(2)]

        @pl.when(2 * j < blocks)
        def _():
            dy_copy(2 * j).wait()
            dy_copy(2 * j + 1).wait()

        forward(q // blocks, lax.rem(q, blocks))
        forward((q + 1) // blocks, lax.rem(q + 1, blocks), DG)
        for i in seen:
            DT[:, tok(i)] = D[tok(i), :].T

    loop((tiles - 2) * blocks // 2 + 1, middle)
    fetch(tiles)

    def closing(i):
        normed = second_norm(i)
        forward(tiles - 1, i + 1)
        second_norm_kept(i, *normed)

    loop(blocks - 1, closing)
    second_norm_kept(blocks - 1, *second_norm(blocks - 1))

    pl.semaphore_wait(barrier, n - 1)

    def remote(src, dst, slot, u, way, step, arrival=None):
        return pltpu.make_async_remote_copy(
            src_ref=src,
            dst_ref=dst,
            send_sem=send_sem.at[slot, way, step],
            recv_sem=recv_sem.at[u, way, step] if arrival is None else arrival,
            device_id={"dp": (up, down)[way]},
            device_id_type=MESH,
        )

    low, high, whole = pl.ds(0, hr), pl.ds(hr, hr), pl.ds(0, 2 * hr)
    lands = (RU, RD)

    def rows(step):
        return pl.ds(hr + (step - 1) * 2 * hr, 2 * hr)

    def begin_low(u, slot):
        remote(G.at[slot, ring(half), low], RU.at[u, low], slot, u, 0, 0).start()
        remote(G.at[slot, ring(1 - half), low], RD.at[u, pl.ds(hr, hr)], slot, u, 1, 1, low_sem.at[u]).start()

    def begin_high(u, slot):
        remote(G.at[slot, ring(half), high], RD.at[u, low], slot, u, 1, 0).start()
        remote(G.at[slot, ring(half - 1), high], RU.at[u, pl.ds(2 * hr, hr)], slot, u, 0, 1).start()

    def arrived(land, sem):
        pltpu.make_async_copy(land, land, sem).wait()

    def received(u, way, step):
        if (way, step) == (1, 1):
            arrived(RD.at[u, pl.ds(hr, hr)], low_sem.at[u])
            arrived(RD.at[u, pl.ds(2 * hr, hr)], recv_sem.at[u, 1, 1])
        else:
            arrived(lands[way].at[u, rows(step) if step else low], recv_sem.at[u, way, step])

    def add(land, place, mine):
        land[place] = (land[place].astype(F32) + mine.astype(F32)).astype(BF16)

    def second_low(u, slot):
        received(u, 0, 0)
        add(RU, (u, low), G[slot, ring(half - 1), low])
        remote(RU.at[u, low], RU.at[u, pl.ds(hr, hr)], slot, u, 0, 1).start()

    def second_high(u, slot):
        received(u, 1, 0)
        add(RD, (u, low), G[slot, ring(1 - half), high])
        remote(RD.at[u, low], RD.at[u, pl.ds(2 * hr, hr)], slot, u, 1, 1).start()

    def pass_on(u, slot, way, step):
        received(u, way, step - 1)
        add(lands[way], (u, rows(step - 1)), G[slot, ring(half - step if way == 0 else step - half)])
        remote(lands[way].at[u, rows(step - 1)], lands[way].at[u, rows(step)], slot, u, way, step).start()

    def later(u, slot, step):
        pass_on(u, slot, 0, step)
        pass_on(u, slot, 1, step)

    def half_on(u, slot, part, sem):
        here, there = pl.ds((1 + part) * hr, hr), pl.ds((3 + part) * hr, hr)
        arrived(RD.at[u, here], sem)
        add(RD, (u, here), G[slot, ring(2 - half), (low, high)[part]])
        remote(RD.at[u, here], RD.at[u, there], slot, u, 1, 2).start()

    def third_low(u, slot):
        half_on(u, slot, 0, low_sem.at[u])

    def third_rest(u, slot):
        pass_on(u, slot, 0, 2)
        half_on(u, slot, 1, recv_sem.at[u, 1, 1])

    def finish(u, slot, which, layer, t):
        received(u, 0, half - 1)
        received(u, 1, half - 1)
        total = G[slot, me].astype(F32) + RU[u, rows(half - 1)].astype(F32) + RD[u, rows(half - 1)].astype(F32)
        total = total.astype(BF16)
        wide = total.astype(F32)
        SQ[...] += jnp.sum((wide * wide).reshape(-1, 8, dim), axis=0)
        if which == 0:
            OD[layer, at(t, LANES), :] = total
        else:
            out = (OG, OU)[which - 1]
            for b in range(n):
                piece = total[hr * (b // (n // 2)) : hr * (b // (n // 2)) + hr, LANES * (b % (n // 2)) : LANES * (b % (n // 2)) + LANES]
                out[layer, :, pl.ds(pl.multiple_of(b * share + t * LANES, LANES), LANES)] = piece
        for way in range(2):
            for step in range(half):
                src = G.at[slot, 0, whole] if step > 0 else G.at[slot, 0, low]
                pltpu.make_async_copy(src, src, send_sem.at[slot, way, step]).wait()

    SQ[...] = jnp.zeros_like(SQ)

    end = 2 * tiles - 1

    def tile_step(k):
        wk = k + tiles
        slot = lax.rem(wk, 2)
        base = lax.rem(k, 2) * 3
        prev = 3 - base
        u0 = 3 * k
        p0 = u0 - 3
        going = k >= 1
        old_t = lax.rem(k - 1 + tiles, tiles)
        old_layer = jnp.where(k - 1 < tiles, 1, 0)
        fetched(wk)

        @pl.when(k < 2 * tiles - 1)
        def _():
            fetch(wk + 1)

        def when(cond):
            return pl.when(going & cond)

        def hidden(j, i):
            place = pl.ds(pl.multiple_of(i * 2 * tb, 2 * tb), 2 * tb)
            for c in range(2):
                here = pl.ds(pl.multiple_of(j * cols + c * (cols // 2), cols // 2), cols // 2)
                g = dot(A[place, :], WG[slot, :, here])
                u = dot(A[place, :], WU[slot, :, here])
                back = dot_t(D[place, :], WD[slot, here, :]).astype(BF16).astype(F32)
                s = 0.5 * jnp.tanh(0.5 * g) + 0.5
                silu = g * s
                ACT[place, here] = (silu * u).astype(BF16)
                DU[place, here] = (back * silu).astype(BF16)
                DG[place, here] = (back * u * (s + silu * (1.0 - s))).astype(BF16)

        def wide_part(src, unit, j):
            part = dot(AT[...], src[:, at(j, cols)]).astype(BF16)
            G[base + unit, :, at(j, hr), :] = part.reshape(n, dim // n, cols)

        gate, upper = (u0 + 1, base + 1), (u0 + 2, base + 2)
        old, old_gate, old_upper = (p0, prev), (p0 + 1, prev + 1), (p0 + 2, prev + 2)

        def halves(j):
            def some(i):
                hidden(j, i)

                @when((j == 0) & (i == 0))
                def _():
                    later(*old, 2)
                    later(*old_upper, 3)

                @pl.when((k == 0) & (j == 1) & (i == 0))
                def _():
                    third_low(*gate)

                @pl.when((k == 0) & (j == 1) & (i == 1))
                def _():
                    second_low(*upper)

            loop(blocks // 2, some)
            wide_part(DG, 1, j)

            @pl.when(j == 0)
            def _():
                begin_low(*gate)

            @pl.when(j == 1)
            def _():
                begin_high(*gate)

            @pl.when((j == 1) & (k == 0))
            def _():
                second_low(*gate)

            wide_part(DU, 2, j)

            @pl.when(j == 0)
            def _():
                begin_low(*upper)

            @pl.when(j == 1)
            def _():
                begin_high(*upper)

            @when(j == 1)
            def _():
                later(*old, 3)
                finish(*old_gate, 1, old_layer, old_t)
                finish(*old_upper, 2, old_layer, old_t)
                second_low(*gate)

            @pl.when((j == 1) & (k == 0))
            def _():
                third_low(*upper)

        loop(2, halves)

        def down_part(j):
            part = dot(DT[...], ACT[:, at(j, cols)])
            flipped = part.T.astype(BF16)
            for b in range(cols // LANES):
                G[base, j * (cols // LANES) + b] = flipped[b * LANES : (b + 1) * LANES]

            @pl.when(j == 0)
            def _():
                second_high(*gate)

        loop(2, down_part)

        @pl.when(k < end)
        def _():
            begin_low(u0, base)
            begin_high(u0, base)

        @when(k < end)
        def _():
            second_low(*upper)

        @pl.when(k == tiles - 1)
        def _():
            loop(blocks, lambda i: x_again(i).start())

        def ring_part(i):
            @pl.when(i == 0)
            def _():
                second_high(*upper)

            @pl.when((i == 0) & (k == 0))
            def _():
                second_low(u0, base)
                third_rest(*gate)

            @when(i == 2)
            def _():
                finish(*old, 0, old_layer, old_t)
                later(*gate, 2)

        @pl.when(k < tiles)
        def _():
            def input_part(i):
                so_far = jnp.where(k == 0, 0.0, DA[tok(i), :])
                DA[tok(i), :] = so_far + (dot_t(DG[tok(i), :], WG[slot]) + dot_t(DU[tok(i), :], WU[slot]))
                ring_part(i)

            loop(blocks, input_part)

        @pl.when((k >= tiles) & (k < end))
        def _():
            loop(blocks, ring_part)

        @pl.when(k == tiles - 1)
        def _():
            def between(i):
                h = H[tok(i), :].astype(F32)
                da = DA[tok(i), :].astype(BF16).astype(F32)
                r = scale_of(h)
                dh = (r * da - h * (r * r * r * jnp.mean(h * da, -1, keepdims=True))).astype(BF16)
                d = (D[tok(i), :].astype(F32) + dh.astype(F32)).astype(BF16)
                D[tok(i), :] = d
                DT[:, tok(i)] = d.T
                x_again(i).wait()
                wide = ACT[tok(i), pl.ds(0, dim)].astype(F32)
                a = (wide * scale_of(wide)).astype(BF16)
                A[tok(i), :] = a
                AT[:, tok(i)] = a.T

                @pl.when(i == 1)
                def _():
                    second_low(u0, base)
                    second_high(u0, base)

            loop(blocks, between)

        @when((k != tiles - 1) & (k < end))
        def _():
            second_low(u0, base)

        @pl.when((k != tiles - 1) & (k < end))
        def _():
            second_high(u0, base)

        @pl.when(k == 0)
        def _():
            third_rest(*upper)

        @when(k < end)
        def _():
            later(*upper, 2)

        @pl.when(k < end)
        def _():
            later(*gate, 3)

    loop(2 * tiles, tile_step)

    ahead = (
        pltpu.make_async_copy(wd_hbm.at[layers - 1, at(me, share), :], PW, ahead_sem.at[0]),
        pltpu.make_async_copy(md_hbm.at[layers - 1], PM, ahead_sem.at[1]),
        pltpu.make_async_copy(vd_hbm.at[layers - 1], PV, ahead_sem.at[2]),
    )
    for copy in ahead:
        copy.start()

    base = (end % 2) * 3
    down_unit, gate, upper = ((3 * end + j, base + j) for j in range(3))
    begin_high(*down_unit)
    second_high(*upper)
    begin_low(*down_unit)
    second_low(*upper)
    second_high(*down_unit)
    second_low(*down_unit)
    for step in range(2, half):
        for unit in (gate, upper, down_unit):
            later(*unit, step)
    finish(*gate, 1, 0, tiles - 1)
    finish(3 * (end - 1), 3 - base, 0, 0, tiles - 2)
    finish(*upper, 2, 0, tiles - 1)
    finish(*down_unit, 0, 0, tiles - 1)

    squares = SQ[:, :LANES]
    for j in range(1, dim // LANES):
        squares += SQ[:, j * LANES : (j + 1) * LANES]
    ALL[me] = squares

    def tell(d):
        return pltpu.make_async_remote_copy(
            src_ref=ALL.at[me],
            dst_ref=ALL.at[me],
            send_sem=sq_send.at[d],
            recv_sem=sq_recv.at[d],
            device_id={"dp": ring(d)},
            device_id_type=MESH,
        )

    for d in range(1, n):
        tell(d).start()
    for d in range(1, n):
        tell(d).wait()
    for copy in ahead:
        copy.wait()


def gradients(n, x, dy, w_gate, w_up, w_down, m_down, v_down):
    layers, dim, ff = w_gate.shape
    tokens = x.shape[1]
    blocks = 4
    share = ff // n
    tiles = share // LANES
    tile = n * LANES
    units = 3 * layers * tiles
    half = n // 2
    land = LANES // 2 + LANES * (half - 1)
    any_space = pl.BlockSpec(memory_space=pl.ANY)
    return pl.pallas_call(
        functools.partial(grad_kernel, n, layers, (tokens, dim, ff, blocks)),
        out_shape=tuple(
            kept(shape, dtype)
            for shape, dtype in (
                ((layers, dim // n, ff), BF16),
                ((layers, dim // n, ff), BF16),
                ((layers, share, dim), BF16),
                ((n, 8, LANES), F32),
                ((share, dim), BF16),
                ((share, dim), F32),
                ((share, dim), F32),
            )
        ),
        in_specs=[any_space] * 7,
        out_specs=(pl.BlockSpec(memory_space=pltpu.VMEM),) * 7,
        scratch_shapes=[
            pltpu.VMEM((tokens, dim), BF16),
            pltpu.VMEM((dim, tokens), BF16),
            pltpu.VMEM((tokens, dim), BF16),
            pltpu.VMEM((dim, tokens), BF16),
            pltpu.VMEM((tokens, dim), BF16),
            pltpu.VMEM((tokens, tile), BF16),
            pltpu.VMEM((tokens, tile), BF16),
            pltpu.VMEM((tokens, tile), BF16),
            pltpu.VMEM((tokens, dim), F32),
            pltpu.VMEM((2, dim, tile), BF16),
            pltpu.VMEM((2, dim, tile), BF16),
            pltpu.VMEM((2, tile, dim), BF16),
            pltpu.VMEM((6, n, LANES, dim), BF16),
            pltpu.VMEM((units, land, dim), BF16),
            pltpu.VMEM((units, land, dim), BF16),
            pltpu.VMEM((8, dim), F32),
            pltpu.SemaphoreType.DMA((blocks,)),
            pltpu.SemaphoreType.DMA((blocks,)),
            pltpu.SemaphoreType.DMA((2, 3)),
            pltpu.SemaphoreType.DMA((3,)),
            pltpu.SemaphoreType.DMA((6, 2, half)),
            pltpu.SemaphoreType.DMA((units, 2, half)),
            pltpu.SemaphoreType.DMA((units,)),
            pltpu.SemaphoreType.DMA((n,)),
            pltpu.SemaphoreType.DMA((n,)),
        ],
        compiler_params=pltpu.CompilerParams(collective_id=0, has_side_effects=True, vmem_limit_bytes=59 * 2**20),
        name="grads",
    )(*(pinned(t, pltpu.HBM) for t in (x, dy, w_gate, w_up, w_down, m_down, v_down)))


def turns(layers):
    return [(2, l) for l in reversed(range(layers))] + [(a, l) for l in reversed(range(layers)) for a in (0, 1)]


def update_kernel(n, count, parts, *refs):
    G, w_hbm, m_hbm, v_hbm = (refs[i : i + 3] for i in (0, 4, 10, 13))
    SQ, PW, PM, PV = refs[3], *refs[7:10]
    N, M, V = (refs[i : i + 3] for i in (16, 19, 22))
    last = refs[25:27]
    W = refs[27:30]
    in_sem, last_sem, send_sem, recv_sem = refs[30:]
    me = lax.axis_index("dp")
    half = n // 2
    up, down = lax.rem(me + 1, n), lax.rem(me + n - 1, n)
    ring = lambda d: lax.rem(me + d + n, n)
    layers = G[0].shape[0]

    barrier = pltpu.get_barrier_semaphore()
    for peer in (up, down):
        pl.semaphore_signal(barrier, inc=1, device_id={"dp": peer}, device_id_type=MESH)

    order = turns(layers)
    loads = {}
    for a, l in order[1:]:
        rows = G[a].shape[1]
        own = pl.ds(pl.multiple_of(me * rows, rows), rows)
        loads[a, l] = (
            pltpu.make_async_copy(w_hbm[a].at[l, own, :], W[a].at[l], in_sem.at[0, a, l]),
            pltpu.make_async_copy(m_hbm[a].at[l], M[a].at[l], in_sem.at[1, a, l]),
            pltpu.make_async_copy(v_hbm[a].at[l], V[a].at[l], in_sem.at[2, a, l]),
        )
    total = jnp.sum(jnp.sum(SQ[...], axis=0), axis=(0, 1), keepdims=True)
    factor = jnp.minimum(1.0, 0.5 * lax.rsqrt(total / count + 1e-30))

    def shape(a):
        rows, cols = G[a].shape[1:]
        return (rows, cols // parts, 0) if a < 2 else (rows // parts, cols, 1)

    def place(a, l, p, owner, part):
        rows = G[a].shape[1]
        r, c, split = shape(a)
        hr = r // 2
        start = owner * rows + (p * r if split else 0)
        start, size = (start, r) if part == 2 else (start + part * hr, hr)
        return (l, pl.ds(pl.multiple_of(start, hr), size), pl.ds(0 if split else p * c, c))

    def send(i, a, l, p, way, step):
        owner = ring(-step) if way == 0 else ring(step)
        ref = N[a].at[place(a, l, p, owner, 2 if step < half - 1 else way)]
        return pltpu.make_async_remote_copy(
            src_ref=ref,
            dst_ref=ref,
            send_sem=send_sem.at[i, way, step],
            recv_sem=recv_sem.at[i, way, step],
            device_id={"dp": (up, down)[way]},
            device_id_type=MESH,
        )

    def came(i, a, l, p, way, step):
        owner = ring(-step - 1) if way == 0 else ring(step + 1)
        where = place(a, l, p, owner, 2 if step < half - 1 else way)
        ref = N[a].at[where]
        pltpu.make_async_copy(ref, ref, recv_sem.at[i, way, step]).wait()

    def adam(a, l, p):
        r, c, split = shape(a)
        rows = G[a].shape[1]
        step = 32
        lane = pl.ds(0 if split else p * c, c)

        def some(i):
            row = pl.ds(pl.multiple_of((p * r if split else 0) + i * step, step), step)
            old = (PW[row, lane], PM[row, lane], PV[row, lane]) if (a, l) == order[0] else (W[a][l, row, lane], M[a][l, row, lane], V[a][l, row, lane])
            g = G[a][l, row, lane].astype(F32) * factor
            m = 0.9 * old[1] + 0.1 * g
            v = 0.95 * old[2] + 0.05 * g * g
            M[a][l, row, lane] = m
            V[a][l, row, lane] = v
            w = old[0].astype(F32)
            new = (w - 0.02 * (m * lax.rsqrt(v + 1e-8) + 0.1 * w)).astype(BF16)
            there = pl.ds(pl.multiple_of(me * rows + (p * r if split else 0) + i * step, step), step)
            N[a][l, there, lane] = new

        loop(r // step, some)

    chunks = []
    for a, l in order:
        for p in range(parts):
            chunks.append((len(chunks), a, l, p))
    for i, a, l, p in chunks:
        if p == 0:
            for copy in loads.get((a, l), ()):
                copy.wait()
        adam(a, l, p)
        if i == 0:
            pl.semaphore_wait(barrier, 2)
        send(i, a, l, p, 0, 0).start()
        send(i, a, l, p, 1, 0).start()
        if i == 0:
            for copies in loads.values():
                for copy in copies:
                    copy.start()
    late = order[len(order) - LATE :]

    def hops(a, l):
        return half - 1 if (a, l) in late else half

    def to_permute(a, l, way):
        rows = G[a].shape[1]
        owner = ring(1 - half) if way == 0 else ring(half - 1)
        src = N[a].at[l, pl.ds(pl.multiple_of(owner * rows + way * (rows // 2), rows // 2), rows // 2), :]
        return pltpu.make_async_copy(src, last[way].at[late.index((a, l))], last_sem.at[way, late.index((a, l))])

    for step in range(half):
        for i, a, l, p in chunks:
            for way in range(2):
                if step < hops(a, l):
                    came(i, a, l, p, way, step)
                if step < hops(a, l) - 1:
                    send(i, a, l, p, way, step + 1).start()
                elif step == half - 2 and p == parts - 1:
                    to_permute(a, l, way).start()
    for i, a, l, p in chunks:
        for way in range(2):
            for step in range(hops(a, l)):
                send(i, a, l, p, way, step).wait_send()
    for a, l in late:
        for way in range(2):
            to_permute(a, l, way).wait()


def store_kernel(count, *refs):
    src, dst, sem = refs[:count], refs[count : 2 * count], refs[-1]
    copies = [
        pltpu.make_async_copy(a.at[l], b.at[l], sem.at[i, l])
        for i, (a, b) in enumerate(zip(src, dst, strict=True))
        for l in range(a.shape[0])
    ]
    for copy in copies:
        copy.start()
    for copy in copies:
        copy.wait()


def store(arrays):
    count = len(arrays)
    return pl.pallas_call(
        functools.partial(store_kernel, count),
        out_shape=tuple(jax.ShapeDtypeStruct(t.shape, t.dtype) for t in arrays),
        in_specs=[pl.BlockSpec(memory_space=pltpu.VMEM)] * count,
        out_specs=(pl.BlockSpec(memory_space=pl.ANY),) * count,
        scratch_shapes=[pltpu.SemaphoreType.DMA((count, arrays[0].shape[0]))],
        compiler_params=pltpu.CompilerParams(vmem_limit_bytes=2**20),
        cost_estimate=pl.CostEstimate(flops=10_000_000_000, bytes_accessed=0, transcendentals=0),
        name="store",
    )(*(pinned(t, pltpu.VMEM) for t in arrays))


def place_kernel(n, count, *refs):
    up_ref, down_ref = refs[count : count + 2]
    outs, sem = refs[count + 2 : -1], refs[-1]
    opposite = lax.rem(lax.axis_index("dp") + n // 2, n)
    hr = up_ref.shape[1]
    copies = []
    for i, (a, l) in enumerate(turns(outs[0].shape[0])[-LATE:]):
        for way, src in enumerate((up_ref, down_ref)):
            there = pl.ds(pl.multiple_of(opposite * 2 * hr + way * hr, hr), hr)
            copies.append(pltpu.make_async_copy(src.at[i], outs[a].at[l, there, :], sem.at[i, way]))
    for copy in copies:
        copy.start()
    for copy in copies:
        copy.wait()


def place_last(n, arrays, came):
    count = len(arrays)
    any_space = pl.BlockSpec(memory_space=pl.ANY)
    in_vmem = pl.BlockSpec(memory_space=pltpu.VMEM)
    return pl.pallas_call(
        functools.partial(place_kernel, n, count),
        out_shape=tuple(jax.ShapeDtypeStruct(t.shape, t.dtype) for t in arrays),
        in_specs=[any_space] * count + [in_vmem] * 2,
        out_specs=(any_space,) * count,
        scratch_shapes=[pltpu.SemaphoreType.DMA((LATE, 2))],
        input_output_aliases={i: i for i in range(count)},
        compiler_params=pltpu.CompilerParams(vmem_limit_bytes=2**20),
        name="place",
    )(*(pinned(t, pltpu.HBM) for t in arrays), *came)


def update(n, made, w, m, v):
    layers = w[0].shape[0]
    parts = 2
    chunks = layers * 3 * parts
    count = sum(t.size for t in w)
    any_space = pl.BlockSpec(memory_space=pl.ANY)
    in_vmem = pl.BlockSpec(memory_space=pltpu.VMEM)
    half = n // 2
    g, squares, ahead = made[:3], made[3], made[4:]
    return pl.pallas_call(
        functools.partial(update_kernel, n, float(count), parts),
        out_shape=tuple(kept(t.shape, BF16) for t in w)
        + tuple(kept(t.shape, F32) for t in m + v)
        + (jax.ShapeDtypeStruct((LATE, m[0].shape[1] // 2, m[0].shape[2]), BF16),) * 2,
        in_specs=[in_vmem] * 4 + [any_space] * 3 + [in_vmem] * 3 + [any_space] * 6,
        out_specs=(in_vmem,) * 9 + (any_space,) * 2,
        scratch_shapes=[pltpu.VMEM(t.shape, BF16) for t in m]
        + [
            pltpu.SemaphoreType.DMA((3, 3, layers)),
            pltpu.SemaphoreType.DMA((2, LATE)),
            pltpu.SemaphoreType.DMA((chunks, 2, half)),
            pltpu.SemaphoreType.DMA((chunks, 2, half)),
        ],
        compiler_params=pltpu.CompilerParams(collective_id=1, has_side_effects=True, vmem_limit_bytes=12 * 2**20),
        name="update",
    )(
        *(pinned(t, pltpu.VMEM) for t in (*g, squares)),
        *(pinned(t, pltpu.HBM) for t in w),
        *(pinned(t, pltpu.VMEM) for t in ahead),
        *(pinned(t, pltpu.HBM) for t in (*m, *v)),
    )


def solution(mesh):
    n = mesh.shape["dp"]

    def step(x, dy, *arrays):
        w, m, v = (arrays[i : i + 3] for i in (0, 3, 6))
        *new, up, down = update(n, gradients(n, x, dy, *w, m[2], v[2]), w, m, v)
        came = tuple(lax.ppermute(t, "dp", [(i, (i + d) % n) for i in range(n)]) for t, d in ((up, 1), (down, -1)))
        out = store(new)
        return (*place_last(n, out[:2], came), *out[2:])

    shard = P(None, "dp", None)
    return jax.shard_map(
        step,
        mesh=mesh,
        in_specs=(P(("rep", "dp"), None, None),) * 2 + (P(),) * 3 + (shard,) * 6,
        out_specs=(P("rep", None, None),) * 3 + (P("rep", "dp", None),) * 6,
        check_vma=False,
    )
```

```python
import functools

import jax
import jax.numpy as jnp
from jax import lax
from jax.experimental import pallas as pl
from jax.experimental.pallas import tpu as pltpu
from jax.sharding import PartitionSpec as P

F32 = jnp.float32
BF16 = jnp.bfloat16
MESH = pl.DeviceIdType.MESH
LANES = 128
LATE = 4


def dot(a, b):
    return jnp.dot(a, b, preferred_element_type=F32)


def dot_t(a, b):
    return lax.dot_general(a, b, (((1,), (1,)), ((), ())), preferred_element_type=F32)


def scale_of(wide):
    return lax.rsqrt(jnp.mean(wide * wide, -1, keepdims=True) + 1e-6)


def pinned(t, space):
    return pltpu.with_memory_space_constraint(t, space)


def kept(shape, dtype):
    return pltpu.VMEM(shape, dtype)


def loop(count, body):
    lax.fori_loop(0, count, lambda i, c: (body(i), c)[1], 0)


def at(i, size):
    return pl.ds(pl.multiple_of(i * size, size), size)


def grad_kernel(n, layers, shapes, *refs):
    (x_hbm, dy_hbm, wg_hbm, wu_hbm, wd_hbm, md_hbm, vd_hbm) = refs[:7]
    (OG, OU, OD, ALL, PW, PM, PV) = refs[7:14]
    (A, AT, D, DT, H, ACT, DG, DU, DA, WG, WU, WD, G, RU, RD, SQ, *sems) = refs[14:]
    x_sem, dy_sem, w_sem, ahead_sem, send_sem, recv_sem, low_sem, sq_send, sq_recv = sems
    tokens, dim, ff, blocks = shapes
    share = ff // n
    tiles = share // LANES
    tile = n * LANES
    tb = tokens // blocks
    half = n // 2
    hr = LANES // 2
    cols = tile // 2
    me = lax.axis_index("dp")
    up, down = lax.rem(me + 1, n), lax.rem(me + n - 1, n)
    ring = lambda d: lax.rem(me + d + n, n)

    def tok(i):
        return at(i, tb)

    def fetch(k):
        slot = lax.rem(k, 2)
        layer = lax.rem(k // tiles, 2)
        t = lax.rem(k, tiles)

        def one(b):
            place = pl.ds(pl.multiple_of(b * share + t * LANES, LANES), LANES)
            here = at(b, LANES)
            pltpu.make_async_copy(wg_hbm.at[layer, :, place], WG.at[slot, :, here], w_sem.at[slot, 0]).start()
            pltpu.make_async_copy(wu_hbm.at[layer, :, place], WU.at[slot, :, here], w_sem.at[slot, 1]).start()
            pltpu.make_async_copy(wd_hbm.at[layer, place, :], WD.at[slot, here, :], w_sem.at[slot, 2]).start()

        loop(n, one)

    def fetched(k):
        slot = lax.rem(k, 2)
        pltpu.make_async_copy(WG.at[slot], WG.at[slot], w_sem.at[slot, 0]).wait()
        pltpu.make_async_copy(WU.at[slot], WU.at[slot], w_sem.at[slot, 1]).wait()
        pltpu.make_async_copy(WD.at[slot], WD.at[slot], w_sem.at[slot, 2]).wait()

    def x_copy(i):
        return pltpu.make_async_copy(x_hbm.at[0, tok(i), :], H.at[tok(i), :], x_sem.at[i])

    def x_again(i):
        return pltpu.make_async_copy(x_hbm.at[0, tok(i), :], ACT.at[tok(i), pl.ds(0, dim)], x_sem.at[i])

    def dy_copy(i):
        return pltpu.make_async_copy(dy_hbm.at[0, tok(i), :], D.at[tok(i), :], dy_sem.at[i])

    x_copy(0).start()
    fetch(0)
    x_copy(1).start()
    barrier = pltpu.get_barrier_semaphore()
    for d in range(1, n):
        pl.semaphore_signal(barrier, inc=1, device_id={"dp": ring(d)}, device_id_type=MESH)

    def first_norm(i):
        wide = H[tok(i), :].astype(F32)
        A[tok(i), :] = (wide * scale_of(wide)).astype(BF16)
        DA[tok(i), :] = jnp.zeros((tb, dim), F32)

    def forward(k, i, act=ACT):
        slot = lax.rem(k, 2)
        for j in range(4):
            here = pl.ds(j * (tile // 4), tile // 4)
            g = dot(A[tok(i), :], WG[slot, :, here])
            u = dot(A[tok(i), :], WU[slot, :, here])
            s = 0.5 * jnp.tanh(0.5 * g) + 0.5
            act[tok(i), here] = (g * s * u).astype(BF16)
        DA[tok(i), :] += dot(act[tok(i), :], WD[slot])

    def second_norm(i):
        h = (H[tok(i), :].astype(F32) + DA[tok(i), :].astype(BF16).astype(F32)).astype(BF16)
        wide = h.astype(F32)
        return h, (wide * scale_of(wide)).astype(BF16)

    def second_norm_kept(i, h, a):
        H[tok(i), :] = h
        A[tok(i), :] = a
        AT[:, tok(i)] = a.T

    x_copy(0).wait()
    first_norm(0)
    fetched(0)
    loop(blocks - 2, lambda i: x_copy(i + 2).start())
    fetch(1)
    loop(blocks, lambda i: dy_copy(i).start())

    def opening(i):
        x_copy(i + 1).wait()
        forward(0, i)
        first_norm(i + 1)

    loop(blocks - 1, opening)

    def middle(j):
        q = blocks - 1 + 2 * j

        @pl.when(lax.rem(q + 1, blocks) == 0)
        def _():
            fetched((q + 1) // blocks)

        @pl.when((lax.rem(q, blocks) == 1) & (q // blocks < tiles - 1))
        def _():
            fetch(q // blocks + 1)

        seen = [jnp.minimum(2 * j + d, blocks - 1) for d in range(2)]

        @pl.when(2 * j < blocks)
        def _():
            dy_copy(2 * j).wait()
            dy_copy(2 * j + 1).wait()

        forward(q // blocks, lax.rem(q, blocks))
        forward((q + 1) // blocks, lax.rem(q + 1, blocks), DG)
        for i in seen:
            DT[:, tok(i)] = D[tok(i), :].T

    loop((tiles - 2) * blocks // 2 + 1, middle)
    fetch(tiles)

    def closing(i):
        normed = second_norm(i)
        forward(tiles - 1, i + 1)
        second_norm_kept(i, *normed)

    loop(blocks - 1, closing)

    def hidden(slot, j, i, pieces=1):
        size = 2 * tb // pieces
        for p, c in [(p, c) for p in range(pieces) for c in range(2)]:
            place = at(i * pieces + p, size)
            here = at(2 * j + c, cols // 2)
            g = dot(A[place, :], WG[slot, :, here])
            u = dot(A[place, :], WU[slot, :, here])
            back = dot_t(D[place, :], WD[slot, here, :]).astype(BF16).astype(F32)
            s = 0.5 * jnp.tanh(0.5 * g) + 0.5
            silu = g * s
            ACT[place, here] = (silu * u).astype(BF16)
            DU[place, here] = (back * silu).astype(BF16)
            DG[place, here] = (back * u * (s + silu * (1.0 - s))).astype(BF16)

    fetched(tiles)
    normed = second_norm(blocks - 1)
    hidden(tiles % 2, 0, 0, 2)
    second_norm_kept(blocks - 1, *normed)

    pl.semaphore_wait(barrier, n - 1)

    def remote(src, dst, slot, u, way, step, arrival=None):
        return pltpu.make_async_remote_copy(
            src_ref=src,
            dst_ref=dst,
            send_sem=send_sem.at[slot, way, step],
            recv_sem=recv_sem.at[u, way, step] if arrival is None else arrival,
            device_id={"dp": (up, down)[way]},
            device_id_type=MESH,
        )

    low, high, whole = pl.ds(0, hr), pl.ds(hr, hr), pl.ds(0, 2 * hr)
    lands = (RU, RD)

    def rows(step):
        return pl.ds(hr + (step - 1) * 2 * hr, 2 * hr)

    def begin_low(u, slot):
        remote(G.at[slot, ring(half), low], RU.at[u, low], slot, u, 0, 0).start()
        remote(G.at[slot, ring(1 - half), low], RD.at[u, pl.ds(hr, hr)], slot, u, 1, 1, low_sem.at[u]).start()

    def begin_high(u, slot):
        remote(G.at[slot, ring(half), high], RD.at[u, low], slot, u, 1, 0).start()
        remote(G.at[slot, ring(half - 1), high], RU.at[u, pl.ds(2 * hr, hr)], slot, u, 0, 1).start()

    def arrived(land, sem):
        pltpu.make_async_copy(land, land, sem).wait()

    def received(u, way, step):
        if (way, step) == (1, 1):
            arrived(RD.at[u, pl.ds(hr, hr)], low_sem.at[u])
            arrived(RD.at[u, pl.ds(2 * hr, hr)], recv_sem.at[u, 1, 1])
        else:
            arrived(lands[way].at[u, rows(step) if step else low], recv_sem.at[u, way, step])

    def add(land, place, mine):
        land[place] = (land[place].astype(F32) + mine.astype(F32)).astype(BF16)

    def second_low(u, slot):
        received(u, 0, 0)
        add(RU, (u, low), G[slot, ring(half - 1), low])
        remote(RU.at[u, low], RU.at[u, pl.ds(hr, hr)], slot, u, 0, 1).start()

    def second_high(u, slot):
        received(u, 1, 0)
        add(RD, (u, low), G[slot, ring(1 - half), high])
        remote(RD.at[u, low], RD.at[u, pl.ds(2 * hr, hr)], slot, u, 1, 1).start()

    def pass_on(u, slot, way, step):
        received(u, way, step - 1)
        add(lands[way], (u, rows(step - 1)), G[slot, ring(half - step if way == 0 else step - half)])
        remote(lands[way].at[u, rows(step - 1)], lands[way].at[u, rows(step)], slot, u, way, step).start()

    def later(u, slot, step):
        pass_on(u, slot, 0, step)
        pass_on(u, slot, 1, step)

    def half_on(u, slot, part, sem):
        here, there = pl.ds((1 + part) * hr, hr), pl.ds((3 + part) * hr, hr)
        arrived(RD.at[u, here], sem)
        add(RD, (u, here), G[slot, ring(2 - half), (low, high)[part]])
        remote(RD.at[u, here], RD.at[u, there], slot, u, 1, 2).start()

    def third_low(u, slot):
        half_on(u, slot, 0, low_sem.at[u])

    def third_rest(u, slot):
        pass_on(u, slot, 0, 2)
        half_on(u, slot, 1, recv_sem.at[u, 1, 1])

    def finish(u, slot, which, layer, t):
        received(u, 0, half - 1)
        received(u, 1, half - 1)
        total = G[slot, me].astype(F32) + RU[u, rows(half - 1)].astype(F32) + RD[u, rows(half - 1)].astype(F32)
        total = total.astype(BF16)
        wide = total.astype(F32)
        SQ[...] += jnp.sum((wide * wide).reshape(-1, 8, dim), axis=0)
        if which == 0:
            OD[layer, at(t, LANES), :] = total
        else:
            out = (OG, OU)[which - 1]
            for b in range(n):
                piece = total[hr * (b // (n // 2)) : hr * (b // (n // 2)) + hr, LANES * (b % (n // 2)) : LANES * (b % (n // 2)) + LANES]
                out[layer, :, pl.ds(pl.multiple_of(b * share + t * LANES, LANES), LANES)] = piece
        for way in range(2):
            for step in range(half):
                src = G.at[slot, 0, whole] if step > 0 else G.at[slot, 0, low]
                pltpu.make_async_copy(src, src, send_sem.at[slot, way, step]).wait()

    SQ[...] = jnp.zeros_like(SQ)

    end = 2 * tiles - 1

    def tile_step(k):
        wk = k + tiles
        slot = lax.rem(wk, 2)
        base = lax.rem(k, 2) * 3
        prev = 3 - base
        u0 = 3 * k
        p0 = u0 - 3
        going = k >= 1
        old_t = lax.rem(k - 1 + tiles, tiles)
        old_layer = jnp.where(k - 1 < tiles, 1, 0)

        @pl.when(k > 0)
        def _():
            fetched(wk)

        @pl.when(k < 2 * tiles - 1)
        def _():
            fetch(wk + 1)

        def when(cond):
            return pl.when(going & cond)

        def wide_part(src, unit, j):
            part = dot(AT[...], src[:, at(j, cols)]).astype(BF16)
            G[base + unit, :, at(j, hr), :] = part.reshape(n, dim // n, cols)

        gate, upper = (u0 + 1, base + 1), (u0 + 2, base + 2)
        old, old_gate, old_upper = (p0, prev), (p0 + 1, prev + 1), (p0 + 2, prev + 2)

        def halves(j):
            def some(i):
                @pl.when((k > 0) | (j > 0) | (i > 0))
                def _():
                    hidden(slot, j, i)

                @when((j == 0) & (i == 0))
                def _():
                    later(*old, 2)
                    later(*old_upper, 3)

                @pl.when((k == 0) & (j == 1) & (i == 0))
                def _():
                    third_low(*gate)

                @pl.when((k == 0) & (j == 1) & (i == 1))
                def _():
                    second_low(*upper)

            loop(blocks // 2, some)
            wide_part(DG, 1, j)

            @pl.when(j == 0)
            def _():
                begin_low(*gate)

            @pl.when(j == 1)
            def _():
                begin_high(*gate)

            @pl.when((j == 1) & (k == 0))
            def _():
                second_low(*gate)

            wide_part(DU, 2, j)

            @pl.when(j == 0)
            def _():
                begin_low(*upper)

            @pl.when(j == 1)
            def _():
                begin_high(*upper)

            @when(j == 1)
            def _():
                later(*old, 3)
                finish(*old_gate, 1, old_layer, old_t)
                finish(*old_upper, 2, old_layer, old_t)
                second_low(*gate)

            @pl.when((j == 1) & (k == 0))
            def _():
                third_low(*upper)

        loop(2, halves)

        def down_part(j):
            part = dot(DT[...], ACT[:, at(j, cols)])
            flipped = part.T.astype(BF16)
            for b in range(cols // LANES):
                G[base, j * (cols // LANES) + b] = flipped[b * LANES : (b + 1) * LANES]

            @pl.when(j == 0)
            def _():
                second_high(*gate)

        loop(2, down_part)

        @pl.when(k < end)
        def _():
            begin_low(u0, base)
            begin_high(u0, base)

        @when(k < end)
        def _():
            second_low(*upper)

        @pl.when(k == tiles - 1)
        def _():
            loop(blocks, lambda i: x_again(i).start())

        def ring_part(i):
            @pl.when(i == 0)
            def _():
                second_high(*upper)

            @pl.when((i == 0) & (k == 0))
            def _():
                second_low(u0, base)
                third_rest(*gate)

            @when(i == 2)
            def _():
                finish(*old, 0, old_layer, old_t)
                later(*gate, 2)

        @pl.when(k < tiles)
        def _():
            def input_part(i):
                so_far = jnp.where(k == 0, 0.0, DA[tok(i), :])
                DA[tok(i), :] = so_far + (dot_t(DG[tok(i), :], WG[slot]) + dot_t(DU[tok(i), :], WU[slot]))
                ring_part(i)

            loop(blocks, input_part)

        @pl.when((k >= tiles) & (k < end))
        def _():
            loop(blocks, ring_part)

        @pl.when(k == tiles - 1)
        def _():
            def between(i):
                h = H[tok(i), :].astype(F32)
                da = DA[tok(i), :].astype(BF16).astype(F32)
                r = scale_of(h)
                dh = (r * da - h * (r * r * r * jnp.mean(h * da, -1, keepdims=True))).astype(BF16)
                d = (D[tok(i), :].astype(F32) + dh.astype(F32)).astype(BF16)
                D[tok(i), :] = d
                DT[:, tok(i)] = d.T
                x_again(i).wait()
                wide = ACT[tok(i), pl.ds(0, dim)].astype(F32)
                a = (wide * scale_of(wide)).astype(BF16)
                A[tok(i), :] = a
                AT[:, tok(i)] = a.T

                @pl.when(i == 1)
                def _():
                    second_low(u0, base)
                    second_high(u0, base)

            loop(blocks, between)

        @when((k != tiles - 1) & (k < end))
        def _():
            second_low(u0, base)

        @pl.when((k != tiles - 1) & (k < end))
        def _():
            second_high(u0, base)

        @pl.when(k == 0)
        def _():
            third_rest(*upper)

        @when(k < end)
        def _():
            later(*upper, 2)

        @pl.when(k < end)
        def _():
            later(*gate, 3)

    loop(2 * tiles, tile_step)

    ahead = (
        pltpu.make_async_copy(wd_hbm.at[layers - 1, at(me, share), :], PW, ahead_sem.at[0]),
        pltpu.make_async_copy(md_hbm.at[layers - 1], PM, ahead_sem.at[1]),
        pltpu.make_async_copy(vd_hbm.at[layers - 1], PV, ahead_sem.at[2]),
    )
    for copy in ahead:
        copy.start()

    base = (end % 2) * 3
    down_unit, gate, upper = ((3 * end + j, base + j) for j in range(3))
    begin_high(*down_unit)
    second_high(*upper)
    begin_low(*down_unit)
    second_low(*upper)
    second_high(*down_unit)
    second_low(*down_unit)
    for step in range(2, half):
        for unit in (gate, upper, down_unit):
            later(*unit, step)
    finish(*gate, 1, 0, tiles - 1)
    finish(3 * (end - 1), 3 - base, 0, 0, tiles - 2)
    finish(*upper, 2, 0, tiles - 1)
    finish(*down_unit, 0, 0, tiles - 1)

    squares = SQ[:, :LANES]
    for j in range(1, dim // LANES):
        squares += SQ[:, j * LANES : (j + 1) * LANES]
    ALL[me] = squares

    def tell(d):
        return pltpu.make_async_remote_copy(
            src_ref=ALL.at[me],
            dst_ref=ALL.at[me],
            send_sem=sq_send.at[d],
            recv_sem=sq_recv.at[d],
            device_id={"dp": ring(d)},
            device_id_type=MESH,
        )

    for d in range(1, n):
        tell(d).start()
    for d in range(1, n):
        tell(d).wait()
    for copy in ahead:
        copy.wait()


def gradients(n, x, dy, w_gate, w_up, w_down, m_down, v_down):
    layers, dim, ff = w_gate.shape
    tokens = x.shape[1]
    blocks = 4
    share = ff // n
    tiles = share // LANES
    tile = n * LANES
    units = 3 * layers * tiles
    half = n // 2
    land = LANES // 2 + LANES * (half - 1)
    any_space = pl.BlockSpec(memory_space=pl.ANY)
    return pl.pallas_call(
        functools.partial(grad_kernel, n, layers, (tokens, dim, ff, blocks)),
        out_shape=tuple(
            kept(shape, dtype)
            for shape, dtype in (
                ((layers, dim // n, ff), BF16),
                ((layers, dim // n, ff), BF16),
                ((layers, share, dim), BF16),
                ((n, 8, LANES), F32),
                ((share, dim), BF16),
                ((share, dim), F32),
                ((share, dim), F32),
            )
        ),
        in_specs=[any_space] * 7,
        out_specs=(pl.BlockSpec(memory_space=pltpu.VMEM),) * 7,
        scratch_shapes=[
            pltpu.VMEM((tokens, dim), BF16),
            pltpu.VMEM((dim, tokens), BF16),
            pltpu.VMEM((tokens, dim), BF16),
            pltpu.VMEM((dim, tokens), BF16),
            pltpu.VMEM((tokens, dim), BF16),
            pltpu.VMEM((tokens, tile), BF16),
            pltpu.VMEM((tokens, tile), BF16),
            pltpu.VMEM((tokens, tile), BF16),
            pltpu.VMEM((tokens, dim), F32),
            pltpu.VMEM((2, dim, tile), BF16),
            pltpu.VMEM((2, dim, tile), BF16),
            pltpu.VMEM((2, tile, dim), BF16),
            pltpu.VMEM((6, n, LANES, dim), BF16),
            pltpu.VMEM((units, land, dim), BF16),
            pltpu.VMEM((units, land, dim), BF16),
            pltpu.VMEM((8, dim), F32),
            pltpu.SemaphoreType.DMA((blocks,)),
            pltpu.SemaphoreType.DMA((blocks,)),
            pltpu.SemaphoreType.DMA((2, 3)),
            pltpu.SemaphoreType.DMA((3,)),
            pltpu.SemaphoreType.DMA((6, 2, half)),
            pltpu.SemaphoreType.DMA((units, 2, half)),
            pltpu.SemaphoreType.DMA((units,)),
            pltpu.SemaphoreType.DMA((n,)),
            pltpu.SemaphoreType.DMA((n,)),
        ],
        compiler_params=pltpu.CompilerParams(collective_id=0, has_side_effects=True, vmem_limit_bytes=62_500_000),
        name="grads",
    )(*(pinned(t, pltpu.HBM) for t in (x, dy, w_gate, w_up, w_down, m_down, v_down)))


def turns(layers):
    return [(2, l) for l in reversed(range(layers))] + [(a, l) for l in reversed(range(layers)) for a in (0, 1)]


def update_kernel(n, count, parts, *refs):
    G, w_hbm, m_hbm, v_hbm = (refs[i : i + 3] for i in (0, 4, 10, 13))
    SQ, PW, PM, PV = refs[3], *refs[7:10]
    N, M, V = (refs[i : i + 3] for i in (16, 19, 22))
    last = refs[25:27]
    W = refs[27:30]
    in_sem, last_sem, send_sem, recv_sem = refs[30:]
    me = lax.axis_index("dp")
    half = n // 2
    up, down = lax.rem(me + 1, n), lax.rem(me + n - 1, n)
    ring = lambda d: lax.rem(me + d + n, n)
    layers = G[0].shape[0]

    barrier = pltpu.get_barrier_semaphore()
    for peer in (up, down):
        pl.semaphore_signal(barrier, inc=1, device_id={"dp": peer}, device_id_type=MESH)

    order = turns(layers)
    loads = {}
    for a, l in order[1:]:
        rows = G[a].shape[1]
        own = pl.ds(pl.multiple_of(me * rows, rows), rows)
        loads[a, l] = (
            pltpu.make_async_copy(w_hbm[a].at[l, own, :], W[a].at[l], in_sem.at[0, a, l]),
            pltpu.make_async_copy(m_hbm[a].at[l], M[a].at[l], in_sem.at[1, a, l]),
            pltpu.make_async_copy(v_hbm[a].at[l], V[a].at[l], in_sem.at[2, a, l]),
        )
    total = jnp.sum(jnp.sum(SQ[...], axis=0), axis=(0, 1), keepdims=True)
    factor = jnp.minimum(1.0, 0.5 * lax.rsqrt(total / count + 1e-30))

    def shape(a):
        rows, cols = G[a].shape[1:]
        return (rows, cols // parts, 0) if a < 2 else (rows // parts, cols, 1)

    def place(a, l, p, owner, part):
        rows = G[a].shape[1]
        r, c, split = shape(a)
        hr = r // 2
        start = owner * rows + (p * r if split else 0)
        start, size = (start, r) if part == 2 else (start + part * hr, hr)
        return (l, pl.ds(pl.multiple_of(start, hr), size), pl.ds(0 if split else p * c, c))

    def send(i, a, l, p, way, step):
        owner = ring(-step) if way == 0 else ring(step)
        ref = N[a].at[place(a, l, p, owner, 2 if step < half - 1 else way)]
        return pltpu.make_async_remote_copy(
            src_ref=ref,
            dst_ref=ref,
            send_sem=send_sem.at[i, way, step],
            recv_sem=recv_sem.at[i, way, step],
            device_id={"dp": (up, down)[way]},
            device_id_type=MESH,
        )

    def came(i, a, l, p, way, step):
        owner = ring(-step - 1) if way == 0 else ring(step + 1)
        where = place(a, l, p, owner, 2 if step < half - 1 else way)
        ref = N[a].at[where]
        pltpu.make_async_copy(ref, ref, recv_sem.at[i, way, step]).wait()

    def adam(a, l, p):
        r, c, split = shape(a)
        rows = G[a].shape[1]
        step = 32
        lane = pl.ds(0 if split else p * c, c)

        def some(i):
            row = pl.ds(pl.multiple_of((p * r if split else 0) + i * step, step), step)
            old = (PW[row, lane], PM[row, lane], PV[row, lane]) if (a, l) == order[0] else (W[a][l, row, lane], M[a][l, row, lane], V[a][l, row, lane])
            g = G[a][l, row, lane].astype(F32) * factor
            m = 0.9 * old[1] + 0.1 * g
            v = 0.95 * old[2] + 0.05 * g * g
            M[a][l, row, lane] = m
            V[a][l, row, lane] = v
            w = old[0].astype(F32)
            new = (w - 0.02 * (m * lax.rsqrt(v + 1e-8) + 0.1 * w)).astype(BF16)
            there = pl.ds(pl.multiple_of(me * rows + (p * r if split else 0) + i * step, step), step)
            N[a][l, there, lane] = new

        loop(r // step, some)

    chunks = []
    for a, l in order:
        for p in range(parts):
            chunks.append((len(chunks), a, l, p))
    for i, a, l, p in chunks:
        if p == 0:
            for copy in loads.get((a, l), ()):
                copy.wait()
        adam(a, l, p)
        if i == 0:
            pl.semaphore_wait(barrier, 2)
        send(i, a, l, p, 0, 0).start()
        send(i, a, l, p, 1, 0).start()
        if i == 0:
            for copies in loads.values():
                for copy in copies:
                    copy.start()
    late = order[len(order) - LATE :]

    def hops(a, l):
        return half - 1 if (a, l) in late else half

    def to_permute(a, l, way):
        rows = G[a].shape[1]
        owner = ring(1 - half) if way == 0 else ring(half - 1)
        src = N[a].at[l, pl.ds(pl.multiple_of(owner * rows + way * (rows // 2), rows // 2), rows // 2), :]
        return pltpu.make_async_copy(src, last[way].at[late.index((a, l))], last_sem.at[way, late.index((a, l))])

    for step in range(half):
        for i, a, l, p in chunks:
            for way in range(2):
                if step < hops(a, l):
                    came(i, a, l, p, way, step)
                if step < hops(a, l) - 1:
                    send(i, a, l, p, way, step + 1).start()
                elif step == half - 2 and p == parts - 1:
                    to_permute(a, l, way).start()
    for i, a, l, p in chunks:
        for way in range(2):
            for step in range(hops(a, l)):
                send(i, a, l, p, way, step).wait_send()
    for a, l in late:
        for way in range(2):
            to_permute(a, l, way).wait()


def store_kernel(count, *refs):
    src, dst, sem = refs[:count], refs[count : 2 * count], refs[-1]
    copies = [
        pltpu.make_async_copy(a.at[l], b.at[l], sem.at[i, l])
        for i, (a, b) in enumerate(zip(src, dst, strict=True))
        for l in range(a.shape[0])
    ]
    for copy in copies:
        copy.start()
    for copy in copies:
        copy.wait()


def store(arrays):
    count = len(arrays)
    return pl.pallas_call(
        functools.partial(store_kernel, count),
        out_shape=tuple(jax.ShapeDtypeStruct(t.shape, t.dtype) for t in arrays),
        in_specs=[pl.BlockSpec(memory_space=pltpu.VMEM)] * count,
        out_specs=(pl.BlockSpec(memory_space=pl.ANY),) * count,
        scratch_shapes=[pltpu.SemaphoreType.DMA((count, arrays[0].shape[0]))],
        compiler_params=pltpu.CompilerParams(vmem_limit_bytes=2**20),
        cost_estimate=pl.CostEstimate(flops=10_000_000_000, bytes_accessed=0, transcendentals=0),
        name="store",
    )(*(pinned(t, pltpu.VMEM) for t in arrays))


def place_kernel(n, count, *refs):
    up_ref, down_ref = refs[count : count + 2]
    outs, sem = refs[count + 2 : -1], refs[-1]
    opposite = lax.rem(lax.axis_index("dp") + n // 2, n)
    hr = up_ref.shape[1]
    copies = []
    for i, (a, l) in enumerate(turns(outs[0].shape[0])[-LATE:]):
        for way, src in enumerate((up_ref, down_ref)):
            there = pl.ds(pl.multiple_of(opposite * 2 * hr + way * hr, hr), hr)
            copies.append(pltpu.make_async_copy(src.at[i], outs[a].at[l, there, :], sem.at[i, way]))
    for copy in copies:
        copy.start()
    for copy in copies:
        copy.wait()


def place_last(n, arrays, came):
    count = len(arrays)
    any_space = pl.BlockSpec(memory_space=pl.ANY)
    in_vmem = pl.BlockSpec(memory_space=pltpu.VMEM)
    return pl.pallas_call(
        functools.partial(place_kernel, n, count),
        out_shape=tuple(jax.ShapeDtypeStruct(t.shape, t.dtype) for t in arrays),
        in_specs=[any_space] * count + [in_vmem] * 2,
        out_specs=(any_space,) * count,
        scratch_shapes=[pltpu.SemaphoreType.DMA((LATE, 2))],
        input_output_aliases={i: i for i in range(count)},
        compiler_params=pltpu.CompilerParams(vmem_limit_bytes=2**20),
        name="place",
    )(*(pinned(t, pltpu.HBM) for t in arrays), *came)


def update(n, made, w, m, v):
    layers = w[0].shape[0]
    parts = 2
    chunks = layers * 3 * parts
    count = sum(t.size for t in w)
    any_space = pl.BlockSpec(memory_space=pl.ANY)
    in_vmem = pl.BlockSpec(memory_space=pltpu.VMEM)
    half = n // 2
    g, squares, ahead = made[:3], made[3], made[4:]
    return pl.pallas_call(
        functools.partial(update_kernel, n, float(count), parts),
        out_shape=tuple(kept(t.shape, BF16) for t in w)
        + tuple(kept(t.shape, F32) for t in m + v)
        + (jax.ShapeDtypeStruct((LATE, m[0].shape[1] // 2, m[0].shape[2]), BF16),) * 2,
        in_specs=[in_vmem] * 4 + [any_space] * 3 + [in_vmem] * 3 + [any_space] * 6,
        out_specs=(in_vmem,) * 9 + (any_space,) * 2,
        scratch_shapes=[pltpu.VMEM(t.shape, BF16) for t in m]
        + [
            pltpu.SemaphoreType.DMA((3, 3, layers)),
            pltpu.SemaphoreType.DMA((2, LATE)),
            pltpu.SemaphoreType.DMA((chunks, 2, half)),
            pltpu.SemaphoreType.DMA((chunks, 2, half)),
        ],
        compiler_params=pltpu.CompilerParams(collective_id=1, has_side_effects=True, vmem_limit_bytes=12 * 2**20),
        name="update",
    )(
        *(pinned(t, pltpu.VMEM) for t in (*g, squares)),
        *(pinned(t, pltpu.HBM) for t in w),
        *(pinned(t, pltpu.VMEM) for t in ahead),
        *(pinned(t, pltpu.HBM) for t in (*m, *v)),
    )


def solution(mesh):
    n = mesh.shape["dp"]

    def step(x, dy, *arrays):
        w, m, v = (arrays[i : i + 3] for i in (0, 3, 6))
        *new, up, down = update(n, gradients(n, x, dy, *w, m[2], v[2]), w, m, v)
        came = tuple(lax.ppermute(t, "dp", [(i, (i + d) % n) for i in range(n)]) for t, d in ((up, 1), (down, -1)))
        out = store(new)
        return (*place_last(n, out[:2], came), *out[2:])

    shard = P(None, "dp", None)
    return jax.shard_map(
        step,
        mesh=mesh,
        in_specs=(P(("rep", "dp"), None, None),) * 2 + (P(),) * 3 + (shard,) * 6,
        out_specs=(P("rep", None, None),) * 3 + (P("rep", "dp", None),) * 6,
        check_vma=False,
    )
```

```python
import functools

import jax
import jax.numpy as jnp
from jax import lax
from jax.experimental import pallas as pl
from jax.experimental.pallas import tpu as pltpu
from jax.sharding import PartitionSpec as P

F32 = jnp.float32
BF16 = jnp.bfloat16
MESH = pl.DeviceIdType.MESH
LANES = 128
LATE = 4
TAIL = (
    ("H0d", "H1u", "L0d", "S2g0h", "L1u", "S2g1l", "F0d", "S2g0l", "S2g1h", "H1d", "L1d", "S2u0h", "S2d0h", "S2u1l", "S2d1l", "S2u1h", "S2u0l")
    + ("S3g0h", "S3g1l", "S2d1h", "S2d0l", "S3g1h", "S3g0l", "S3d1l", "S3d0h", "S3u0l", "S3u1h", "S3u0h", "S3u1l", "S3d1h", "S3d0l")
    + ("F1u", "F1g", "F1d")
)


def dot(a, b):
    return jnp.dot(a, b, preferred_element_type=F32)


def dot_t(a, b):
    return lax.dot_general(a, b, (((1,), (1,)), ((), ())), preferred_element_type=F32)


def scale_of(wide):
    return lax.rsqrt(jnp.mean(wide * wide, -1, keepdims=True) + 1e-6)


def pinned(t, space):
    return pltpu.with_memory_space_constraint(t, space)


def kept(shape, dtype):
    return pltpu.VMEM(shape, dtype)


def loop(count, body):
    lax.fori_loop(0, count, lambda i, c: (body(i), c)[1], 0)


def at(i, size):
    return pl.ds(pl.multiple_of(i * size, size), size)


def grad_kernel(n, layers, shapes, *refs):
    (x_hbm, dy_hbm, wg_hbm, wu_hbm, wd_hbm, md_hbm, vd_hbm) = refs[:7]
    (OG, OU, OD, ALL, PW, PM, PV) = refs[7:14]
    (A, AT, D, DT, H, ACT, DG, DU, DA, WG, WU, WD, G, RU, RD, SQ, *sems) = refs[14:]
    x_sem, dy_sem, w_sem, ahead_sem, send_sem, recv_sem, low_sem, high_sem, tail_sem, sq_send, sq_recv = sems
    tokens, dim, ff, blocks = shapes
    share = ff // n
    tiles = share // LANES
    tile = n * LANES
    tb = tokens // blocks
    half = n // 2
    hr = LANES // 2
    cols = tile // 2
    me = lax.axis_index("dp")
    up, down = lax.rem(me + 1, n), lax.rem(me + n - 1, n)
    ring = lambda d: lax.rem(me + d + n, n)

    def tok(i):
        return at(i, tb)

    def fetch(k):
        slot = lax.rem(k, 2)
        layer = lax.rem(k // tiles, 2)
        t = lax.rem(k, tiles)

        def one(b):
            place = pl.ds(pl.multiple_of(b * share + t * LANES, LANES), LANES)
            here = at(b, LANES)
            pltpu.make_async_copy(wg_hbm.at[layer, :, place], WG.at[slot, :, here], w_sem.at[slot, 0]).start()
            pltpu.make_async_copy(wu_hbm.at[layer, :, place], WU.at[slot, :, here], w_sem.at[slot, 1]).start()
            pltpu.make_async_copy(wd_hbm.at[layer, place, :], WD.at[slot, here, :], w_sem.at[slot, 2]).start()

        loop(n, one)

    def fetched(k):
        slot = lax.rem(k, 2)
        pltpu.make_async_copy(WG.at[slot], WG.at[slot], w_sem.at[slot, 0]).wait()
        pltpu.make_async_copy(WU.at[slot], WU.at[slot], w_sem.at[slot, 1]).wait()
        pltpu.make_async_copy(WD.at[slot], WD.at[slot], w_sem.at[slot, 2]).wait()

    def x_copy(i):
        return pltpu.make_async_copy(x_hbm.at[0, tok(i), :], H.at[tok(i), :], x_sem.at[i])

    def x_again(i):
        return pltpu.make_async_copy(x_hbm.at[0, tok(i), :], ACT.at[tok(i), pl.ds(0, dim)], x_sem.at[i])

    def dy_copy(i):
        return pltpu.make_async_copy(dy_hbm.at[0, tok(i), :], D.at[tok(i), :], dy_sem.at[i])

    x_copy(0).start()
    fetch(0)
    x_copy(1).start()
    barrier = pltpu.get_barrier_semaphore()
    for d in range(1, n):
        pl.semaphore_signal(barrier, inc=1, device_id={"dp": ring(d)}, device_id_type=MESH)

    def first_norm(i):
        wide = H[tok(i), :].astype(F32)
        A[tok(i), :] = (wide * scale_of(wide)).astype(BF16)
        DA[tok(i), :] = jnp.zeros((tb, dim), F32)

    def forward(k, i, act=ACT):
        slot = lax.rem(k, 2)
        for j in range(4):
            here = pl.ds(j * (tile // 4), tile // 4)
            g = dot(A[tok(i), :], WG[slot, :, here])
            u = dot(A[tok(i), :], WU[slot, :, here])
            s = 0.5 * jnp.tanh(0.5 * g) + 0.5
            act[tok(i), here] = (g * s * u).astype(BF16)
        DA[tok(i), :] += dot(act[tok(i), :], WD[slot])

    def second_norm(i):
        h = (H[tok(i), :].astype(F32) + DA[tok(i), :].astype(BF16).astype(F32)).astype(BF16)
        wide = h.astype(F32)
        return h, (wide * scale_of(wide)).astype(BF16)

    def second_norm_kept(i, h, a):
        H[tok(i), :] = h
        A[tok(i), :] = a
        AT[:, tok(i)] = a.T

    x_copy(0).wait()
    first_norm(0)
    fetched(0)
    loop(blocks - 2, lambda i: x_copy(i + 2).start())
    fetch(1)
    loop(blocks, lambda i: dy_copy(i).start())

    def opening(i):
        x_copy(i + 1).wait()
        forward(0, i)
        first_norm(i + 1)

    loop(blocks - 1, opening)

    def middle(j):
        q = blocks - 1 + 2 * j

        @pl.when(lax.rem(q + 1, blocks) == 0)
        def _():
            fetched((q + 1) // blocks)

        @pl.when((lax.rem(q, blocks) == 1) & (q // blocks < tiles - 1))
        def _():
            fetch(q // blocks + 1)

        seen = [jnp.minimum(2 * j + d, blocks - 1) for d in range(2)]

        @pl.when(2 * j < blocks)
        def _():
            dy_copy(2 * j).wait()
            dy_copy(2 * j + 1).wait()

        forward(q // blocks, lax.rem(q, blocks))
        forward((q + 1) // blocks, lax.rem(q + 1, blocks), DG)
        for i in seen:
            DT[:, tok(i)] = D[tok(i), :].T

    loop((tiles - 2) * blocks // 2 + 1, middle)
    fetch(tiles)

    def closing(i):
        normed = second_norm(i)
        forward(tiles - 1, i + 1)
        second_norm_kept(i, *normed)

    loop(blocks - 1, closing)

    def hidden(slot, j, i, pieces=1):
        size = 2 * tb // pieces
        for p, c in [(p, c) for p in range(pieces) for c in range(2)]:
            place = at(i * pieces + p, size)
            here = at(2 * j + c, cols // 2)
            g = dot(A[place, :], WG[slot, :, here])
            u = dot(A[place, :], WU[slot, :, here])
            back = dot_t(D[place, :], WD[slot, here, :]).astype(BF16).astype(F32)
            s = 0.5 * jnp.tanh(0.5 * g) + 0.5
            silu = g * s
            ACT[place, here] = (silu * u).astype(BF16)
            DU[place, here] = (back * silu).astype(BF16)
            DG[place, here] = (back * u * (s + silu * (1.0 - s))).astype(BF16)

    fetched(tiles)
    normed = second_norm(blocks - 1)
    hidden(tiles % 2, 0, 0, 2)
    second_norm_kept(blocks - 1, *normed)

    pl.semaphore_wait(barrier, n - 1)

    def remote(src, dst, slot, u, way, step, arrival=None):
        return pltpu.make_async_remote_copy(
            src_ref=src,
            dst_ref=dst,
            send_sem=send_sem.at[slot, way, step],
            recv_sem=recv_sem.at[u, way, step] if arrival is None else arrival,
            device_id={"dp": (up, down)[way]},
            device_id_type=MESH,
        )

    low, high, whole = pl.ds(0, hr), pl.ds(hr, hr), pl.ds(0, 2 * hr)
    lands = (RU, RD)

    def rows(step):
        return pl.ds(hr + (step - 1) * 2 * hr, 2 * hr)

    def begin_low(u, slot):
        remote(G.at[slot, ring(half), low], RU.at[u, low], slot, u, 0, 0).start()
        remote(G.at[slot, ring(1 - half), low], RD.at[u, pl.ds(hr, hr)], slot, u, 1, 1, low_sem.at[u]).start()

    def begin_high(u, slot):
        remote(G.at[slot, ring(half), high], RD.at[u, low], slot, u, 1, 0).start()
        remote(G.at[slot, ring(half - 1), high], RU.at[u, pl.ds(2 * hr, hr)], slot, u, 0, 1, high_sem.at[u]).start()

    def arrived(land, sem):
        pltpu.make_async_copy(land, land, sem).wait()

    def first_arrival(u, way, part):
        return (low_sem, high_sem)[part].at[u] if part != way else recv_sem.at[u, way, 1]

    def received(u, way, step):
        if step == 1:
            for part in range(2):
                arrived(lands[way].at[u, pl.ds((1 + part) * hr, hr)], first_arrival(u, way, part))
        else:
            arrived(lands[way].at[u, rows(step) if step else low], recv_sem.at[u, way, step])

    def add(land, place, mine):
        land[place] = (land[place].astype(F32) + mine.astype(F32)).astype(BF16)

    def second_low(u, slot):
        received(u, 0, 0)
        add(RU, (u, low), G[slot, ring(half - 1), low])
        remote(RU.at[u, low], RU.at[u, pl.ds(hr, hr)], slot, u, 0, 1).start()

    def second_high(u, slot):
        received(u, 1, 0)
        add(RD, (u, low), G[slot, ring(1 - half), high])
        remote(RD.at[u, low], RD.at[u, pl.ds(2 * hr, hr)], slot, u, 1, 1).start()

    def pass_on(u, slot, way, step):
        received(u, way, step - 1)
        add(lands[way], (u, rows(step - 1)), G[slot, ring(half - step if way == 0 else step - half)])
        remote(lands[way].at[u, rows(step - 1)], lands[way].at[u, rows(step)], slot, u, way, step).start()

    def later(u, slot, step):
        pass_on(u, slot, 0, step)
        pass_on(u, slot, 1, step)

    def half_on(u, slot, way, step, part, sem, arrival=None):
        here, there = (pl.ds((2 * step - d + part) * hr, hr) for d in (3, 1))
        arrived(lands[way].at[u, here], sem)
        add(lands[way], (u, here), G[slot, ring(half - step if way == 0 else step - half), (low, high)[part]])
        remote(lands[way].at[u, here], lands[way].at[u, there], slot, u, way, step, arrival).start()

    def third_low(u, slot):
        half_on(u, slot, 1, 2, 0, first_arrival(u, 1, 0))

    def third_rest(u, slot):
        pass_on(u, slot, 0, 2)
        half_on(u, slot, 1, 2, 1, first_arrival(u, 1, 1))

    def finish(u, slot, which, layer, t, halves=None):
        for way in range(2):
            if halves is None:
                received(u, way, half - 1)
            else:
                for part in range(2):
                    arrived(lands[way].at[u, pl.ds((2 * half - 3 + part) * hr, hr)], halves.at[way, half - 1, part])
        total = G[slot, me].astype(F32) + RU[u, rows(half - 1)].astype(F32) + RD[u, rows(half - 1)].astype(F32)
        total = total.astype(BF16)
        wide = total.astype(F32)
        SQ[...] += jnp.sum((wide * wide).reshape(-1, 8, dim), axis=0)
        if which == 0:
            OD[layer, at(t, LANES), :] = total
        else:
            out = (OG, OU)[which - 1]
            for b in range(n):
                piece = total[hr * (b // (n // 2)) : hr * (b // (n // 2)) + hr, LANES * (b % (n // 2)) : LANES * (b % (n // 2)) + LANES]
                out[layer, :, pl.ds(pl.multiple_of(b * share + t * LANES, LANES), LANES)] = piece
        for way in range(2):
            for step in range(half):
                src = G.at[slot, 0, whole] if step > 0 else G.at[slot, 0, low]
                pltpu.make_async_copy(src, src, send_sem.at[slot, way, step]).wait()

    SQ[...] = jnp.zeros_like(SQ)

    end = 2 * tiles - 1

    def tile_step(k):
        wk = k + tiles
        slot = lax.rem(wk, 2)
        base = lax.rem(k, 2) * 3
        prev = 3 - base
        u0 = 3 * k
        p0 = u0 - 3
        going = k >= 1
        old_t = lax.rem(k - 1 + tiles, tiles)
        old_layer = jnp.where(k - 1 < tiles, 1, 0)

        @pl.when(k > 0)
        def _():
            fetched(wk)

        @pl.when(k < 2 * tiles - 1)
        def _():
            fetch(wk + 1)

        def when(cond):
            return pl.when(going & cond)

        def wide_part(src, unit, j):
            part = dot(AT[...], src[:, at(j, cols)]).astype(BF16)
            G[base + unit, :, at(j, hr), :] = part.reshape(n, dim // n, cols)

        gate, upper = (u0 + 1, base + 1), (u0 + 2, base + 2)
        old, old_gate, old_upper = (p0, prev), (p0 + 1, prev + 1), (p0 + 2, prev + 2)

        def halves(j):
            def some(i):
                @pl.when((k > 0) | (j > 0) | (i > 0))
                def _():
                    hidden(slot, j, i)

                @when((j == 0) & (i == 0))
                def _():
                    later(*old, 2)
                    later(*old_upper, 3)

                @pl.when((k == 0) & (j == 1) & (i == 0))
                def _():
                    third_low(*gate)

                @pl.when((k == 0) & (j == 1) & (i == 1))
                def _():
                    second_low(*upper)

            loop(blocks // 2, some)
            wide_part(DG, 1, j)

            @pl.when(j == 0)
            def _():
                begin_low(*gate)

            @pl.when(j == 1)
            def _():
                begin_high(*gate)

            @pl.when((j == 1) & (k == 0))
            def _():
                second_low(*gate)

            wide_part(DU, 2, j)

            @pl.when(j == 0)
            def _():
                begin_low(*upper)

            @pl.when(j == 1)
            def _():
                begin_high(*upper)

            @when(j == 1)
            def _():
                later(*old, 3)
                finish(*old_gate, 1, old_layer, old_t)
                finish(*old_upper, 2, old_layer, old_t)
                second_low(*gate)

            @pl.when((j == 1) & (k == 0))
            def _():
                third_low(*upper)

        loop(2, halves)

        def down_part(j):
            part = dot(DT[...], ACT[:, at(j, cols)])
            flipped = part.T.astype(BF16)
            for b in range(cols // LANES):
                G[base, j * (cols // LANES) + b] = flipped[b * LANES : (b + 1) * LANES]

            @pl.when(j == 0)
            def _():
                second_high(*gate)

        loop(2, down_part)

        @pl.when(k < end)
        def _():
            begin_low(u0, base)
            begin_high(u0, base)

        @when(k < end)
        def _():
            second_low(*upper)

        @pl.when(k == tiles - 1)
        def _():
            loop(blocks, lambda i: x_again(i).start())

        def ring_part(i):
            @pl.when(i == 0)
            def _():
                second_high(*upper)

            @pl.when((i == 0) & (k == 0))
            def _():
                second_low(u0, base)
                third_rest(*gate)

            @when(i == 2)
            def _():
                finish(*old, 0, old_layer, old_t)
                later(*gate, 2)

        @pl.when(k < tiles)
        def _():
            def input_part(i):
                so_far = jnp.where(k == 0, 0.0, DA[tok(i), :])
                DA[tok(i), :] = so_far + (dot_t(DG[tok(i), :], WG[slot]) + dot_t(DU[tok(i), :], WU[slot]))
                ring_part(i)

            loop(blocks, input_part)

        @pl.when((k >= tiles) & (k < end))
        def _():
            loop(blocks, ring_part)

        @pl.when(k == tiles - 1)
        def _():
            def between(i):
                h = H[tok(i), :].astype(F32)
                da = DA[tok(i), :].astype(BF16).astype(F32)
                r = scale_of(h)
                dh = (r * da - h * (r * r * r * jnp.mean(h * da, -1, keepdims=True))).astype(BF16)
                d = (D[tok(i), :].astype(F32) + dh.astype(F32)).astype(BF16)
                D[tok(i), :] = d
                DT[:, tok(i)] = d.T
                x_again(i).wait()
                wide = ACT[tok(i), pl.ds(0, dim)].astype(F32)
                a = (wide * scale_of(wide)).astype(BF16)
                A[tok(i), :] = a
                AT[:, tok(i)] = a.T

                @pl.when(i == 1)
                def _():
                    second_low(u0, base)
                    second_high(u0, base)

            loop(blocks, between)

        @when((k != tiles - 1) & (k < end))
        def _():
            second_low(u0, base)

        @pl.when((k != tiles - 1) & (k < end))
        def _():
            second_high(u0, base)

        @pl.when(k == 0)
        def _():
            third_rest(*upper)

        @when(k < end)
        def _():
            later(*upper, 2)

        @pl.when(k < end)
        def _():
            later(*gate, 3)

    loop(2 * tiles, tile_step)

    ahead = (
        pltpu.make_async_copy(wd_hbm.at[layers - 1, at(me, share), :], PW, ahead_sem.at[0]),
        pltpu.make_async_copy(md_hbm.at[layers - 1], PM, ahead_sem.at[1]),
        pltpu.make_async_copy(vd_hbm.at[layers - 1], PV, ahead_sem.at[2]),
    )
    for copy in ahead:
        copy.start()

    base = (end % 2) * 3
    last = {x: (3 * end + j, base + j) for j, x in enumerate("dgu")}
    for name in TAIL:
        kind, x = name[:2], name[2]
        j = "dgu".index(x)
        sems = tail_sem.at[j]
        if kind == "L0":
            begin_low(*last[x])
        elif kind == "H0":
            begin_high(*last[x])
        elif kind == "L1":
            second_low(*last[x])
        elif kind == "H1":
            second_high(*last[x])
        elif kind == "F0":
            finish(3 * (end - 1) + j, 3 - base + j, j, 0, tiles - 2)
        elif kind == "F1":
            finish(*last[x], j, 0, tiles - 1, sems)
        else:
            step, way, part = int(kind[1]), int(name[3]), "lh".index(name[4])
            sem = first_arrival(last[x][0], way, part) if step == 2 else sems.at[way, step - 1, part]
            half_on(*last[x], way, step, part, sem, sems.at[way, step, part])

    squares = SQ[:, :LANES]
    for j in range(1, dim // LANES):
        squares += SQ[:, j * LANES : (j + 1) * LANES]
    ALL[me] = squares

    def tell(d):
        return pltpu.make_async_remote_copy(
            src_ref=ALL.at[me],
            dst_ref=ALL.at[me],
            send_sem=sq_send.at[d],
            recv_sem=sq_recv.at[d],
            device_id={"dp": ring(d)},
            device_id_type=MESH,
        )

    for d in range(1, n):
        tell(d).start()
    for d in range(1, n):
        tell(d).wait()
    for copy in ahead:
        copy.wait()


def gradients(n, x, dy, w_gate, w_up, w_down, m_down, v_down):
    layers, dim, ff = w_gate.shape
    tokens = x.shape[1]
    blocks = 4
    share = ff // n
    tiles = share // LANES
    tile = n * LANES
    units = 3 * layers * tiles
    half = n // 2
    land = LANES // 2 + LANES * (half - 1)
    any_space = pl.BlockSpec(memory_space=pl.ANY)
    return pl.pallas_call(
        functools.partial(grad_kernel, n, layers, (tokens, dim, ff, blocks)),
        out_shape=tuple(
            kept(shape, dtype)
            for shape, dtype in (
                ((layers, dim // n, ff), BF16),
                ((layers, dim // n, ff), BF16),
                ((layers, share, dim), BF16),
                ((n, 8, LANES), F32),
                ((share, dim), BF16),
                ((share, dim), F32),
                ((share, dim), F32),
            )
        ),
        in_specs=[any_space] * 7,
        out_specs=(pl.BlockSpec(memory_space=pltpu.VMEM),) * 7,
        scratch_shapes=[
            pltpu.VMEM((tokens, dim), BF16),
            pltpu.VMEM((dim, tokens), BF16),
            pltpu.VMEM((tokens, dim), BF16),
            pltpu.VMEM((dim, tokens), BF16),
            pltpu.VMEM((tokens, dim), BF16),
            pltpu.VMEM((tokens, tile), BF16),
            pltpu.VMEM((tokens, tile), BF16),
            pltpu.VMEM((tokens, tile), BF16),
            pltpu.VMEM((tokens, dim), F32),
            pltpu.VMEM((2, dim, tile), BF16),
            pltpu.VMEM((2, dim, tile), BF16),
            pltpu.VMEM((2, tile, dim), BF16),
            pltpu.VMEM((6, n, LANES, dim), BF16),
            pltpu.VMEM((units, land, dim), BF16),
            pltpu.VMEM((units, land, dim), BF16),
            pltpu.VMEM((8, dim), F32),
            pltpu.SemaphoreType.DMA((blocks,)),
            pltpu.SemaphoreType.DMA((blocks,)),
            pltpu.SemaphoreType.DMA((2, 3)),
            pltpu.SemaphoreType.DMA((3,)),
            pltpu.SemaphoreType.DMA((6, 2, half)),
            pltpu.SemaphoreType.DMA((units, 2, half)),
            pltpu.SemaphoreType.DMA((units,)),
            pltpu.SemaphoreType.DMA((units,)),
            pltpu.SemaphoreType.DMA((3, 2, half, 2)),
            pltpu.SemaphoreType.DMA((n,)),
            pltpu.SemaphoreType.DMA((n,)),
        ],
        compiler_params=pltpu.CompilerParams(collective_id=0, has_side_effects=True, vmem_limit_bytes=62_500_000),
        name="grads",
    )(*(pinned(t, pltpu.HBM) for t in (x, dy, w_gate, w_up, w_down, m_down, v_down)))


def turns(layers):
    return [(2, l) for l in reversed(range(layers))] + [(a, l) for l in reversed(range(layers)) for a in (0, 1)]


def update_kernel(n, count, parts, *refs):
    G, w_hbm, m_hbm, v_hbm = (refs[i : i + 3] for i in (0, 4, 10, 13))
    SQ, PW, PM, PV = refs[3], *refs[7:10]
    N, M, V = (refs[i : i + 3] for i in (16, 19, 22))
    last = refs[25:27]
    W = refs[27:30]
    in_sem, last_sem, send_sem, recv_sem = refs[30:]
    me = lax.axis_index("dp")
    half = n // 2
    up, down = lax.rem(me + 1, n), lax.rem(me + n - 1, n)
    ring = lambda d: lax.rem(me + d + n, n)
    layers = G[0].shape[0]

    barrier = pltpu.get_barrier_semaphore()
    for peer in (up, down):
        pl.semaphore_signal(barrier, inc=1, device_id={"dp": peer}, device_id_type=MESH)

    order = turns(layers)
    loads = {}
    for a, l in order[1:]:
        rows = G[a].shape[1]
        own = pl.ds(pl.multiple_of(me * rows, rows), rows)
        loads[a, l] = (
            pltpu.make_async_copy(w_hbm[a].at[l, own, :], W[a].at[l], in_sem.at[0, a, l]),
            pltpu.make_async_copy(m_hbm[a].at[l], M[a].at[l], in_sem.at[1, a, l]),
            pltpu.make_async_copy(v_hbm[a].at[l], V[a].at[l], in_sem.at[2, a, l]),
        )
    total = jnp.sum(jnp.sum(SQ[...], axis=0), axis=(0, 1), keepdims=True)
    factor = jnp.minimum(1.0, 0.5 * lax.rsqrt(total / count + 1e-30))

    def shape(a):
        rows, cols = G[a].shape[1:]
        return (rows, cols // parts, 0) if a < 2 else (rows // parts, cols, 1)

    def place(a, l, p, owner, part):
        rows = G[a].shape[1]
        r, c, split = shape(a)
        hr = r // 2
        start = owner * rows + (p * r if split else 0)
        start, size = (start, r) if part == 2 else (start + part * hr, hr)
        return (l, pl.ds(pl.multiple_of(start, hr), size), pl.ds(0 if split else p * c, c))

    def send(i, a, l, p, way, step):
        owner = ring(-step) if way == 0 else ring(step)
        ref = N[a].at[place(a, l, p, owner, 2 if step < half - 1 else way)]
        return pltpu.make_async_remote_copy(
            src_ref=ref,
            dst_ref=ref,
            send_sem=send_sem.at[i, way, step],
            recv_sem=recv_sem.at[i, way, step],
            device_id={"dp": (up, down)[way]},
            device_id_type=MESH,
        )

    def came(i, a, l, p, way, step):
        owner = ring(-step - 1) if way == 0 else ring(step + 1)
        where = place(a, l, p, owner, 2 if step < half - 1 else way)
        ref = N[a].at[where]
        pltpu.make_async_copy(ref, ref, recv_sem.at[i, way, step]).wait()

    def adam(a, l, p):
        r, c, split = shape(a)
        rows = G[a].shape[1]
        step = 32
        lane = pl.ds(0 if split else p * c, c)

        def some(i):
            row = pl.ds(pl.multiple_of((p * r if split else 0) + i * step, step), step)
            old = (PW[row, lane], PM[row, lane], PV[row, lane]) if (a, l) == order[0] else (W[a][l, row, lane], M[a][l, row, lane], V[a][l, row, lane])
            g = G[a][l, row, lane].astype(F32) * factor
            m = 0.9 * old[1] + 0.1 * g
            v = 0.95 * old[2] + 0.05 * g * g
            M[a][l, row, lane] = m
            V[a][l, row, lane] = v
            w = old[0].astype(F32)
            new = (w - 0.02 * (m * lax.rsqrt(v + 1e-8) + 0.1 * w)).astype(BF16)
            there = pl.ds(pl.multiple_of(me * rows + (p * r if split else 0) + i * step, step), step)
            N[a][l, there, lane] = new

        loop(r // step, some)

    chunks = []
    for a, l in order:
        for p in range(parts):
            chunks.append((len(chunks), a, l, p))
    for i, a, l, p in chunks:
        if p == 0:
            for copy in loads.get((a, l), ()):
                copy.wait()
        adam(a, l, p)
        if i == 0:
            pl.semaphore_wait(barrier, 2)
        send(i, a, l, p, 0, 0).start()
        send(i, a, l, p, 1, 0).start()
        if i == 0:
            for copies in loads.values():
                for copy in copies:
                    copy.start()
    late = order[len(order) - LATE :]

    def hops(a, l):
        return half - 1 if (a, l) in late else half

    def to_permute(a, l, way):
        rows = G[a].shape[1]
        owner = ring(1 - half) if way == 0 else ring(half - 1)
        src = N[a].at[l, pl.ds(pl.multiple_of(owner * rows + way * (rows // 2), rows // 2), rows // 2), :]
        return pltpu.make_async_copy(src, last[way].at[late.index((a, l))], last_sem.at[way, late.index((a, l))])

    for step in range(half):
        for i, a, l, p in chunks:
            for way in range(2):
                if step < hops(a, l):
                    came(i, a, l, p, way, step)
                if step < hops(a, l) - 1:
                    send(i, a, l, p, way, step + 1).start()
                elif step == half - 2 and p == parts - 1:
                    to_permute(a, l, way).start()
    for i, a, l, p in chunks:
        for way in range(2):
            for step in range(hops(a, l)):
                send(i, a, l, p, way, step).wait_send()
    for a, l in late:
        for way in range(2):
            to_permute(a, l, way).wait()


def store_kernel(count, *refs):
    src, dst, sem = refs[:count], refs[count : 2 * count], refs[-1]
    copies = [
        pltpu.make_async_copy(a.at[l], b.at[l], sem.at[i, l])
        for i, (a, b) in enumerate(zip(src, dst, strict=True))
        for l in range(a.shape[0])
    ]
    for copy in copies:
        copy.start()
    for copy in copies:
        copy.wait()


def store(arrays):
    count = len(arrays)
    return pl.pallas_call(
        functools.partial(store_kernel, count),
        out_shape=tuple(jax.ShapeDtypeStruct(t.shape, t.dtype) for t in arrays),
        in_specs=[pl.BlockSpec(memory_space=pltpu.VMEM)] * count,
        out_specs=(pl.BlockSpec(memory_space=pl.ANY),) * count,
        scratch_shapes=[pltpu.SemaphoreType.DMA((count, arrays[0].shape[0]))],
        compiler_params=pltpu.CompilerParams(vmem_limit_bytes=2**20),
        cost_estimate=pl.CostEstimate(flops=10_000_000_000, bytes_accessed=0, transcendentals=0),
        name="store",
    )(*(pinned(t, pltpu.VMEM) for t in arrays))


def place_kernel(n, count, *refs):
    up_ref, down_ref = refs[count : count + 2]
    outs, sem = refs[count + 2 : -1], refs[-1]
    opposite = lax.rem(lax.axis_index("dp") + n // 2, n)
    hr = up_ref.shape[1]
    copies = []
    for i, (a, l) in enumerate(turns(outs[0].shape[0])[-LATE:]):
        for way, src in enumerate((up_ref, down_ref)):
            there = pl.ds(pl.multiple_of(opposite * 2 * hr + way * hr, hr), hr)
            copies.append(pltpu.make_async_copy(src.at[i], outs[a].at[l, there, :], sem.at[i, way]))
    for copy in copies:
        copy.start()
    for copy in copies:
        copy.wait()


def place_last(n, arrays, came):
    count = len(arrays)
    any_space = pl.BlockSpec(memory_space=pl.ANY)
    in_vmem = pl.BlockSpec(memory_space=pltpu.VMEM)
    return pl.pallas_call(
        functools.partial(place_kernel, n, count),
        out_shape=tuple(jax.ShapeDtypeStruct(t.shape, t.dtype) for t in arrays),
        in_specs=[any_space] * count + [in_vmem] * 2,
        out_specs=(any_space,) * count,
        scratch_shapes=[pltpu.SemaphoreType.DMA((LATE, 2))],
        input_output_aliases={i: i for i in range(count)},
        compiler_params=pltpu.CompilerParams(vmem_limit_bytes=2**20),
        name="place",
    )(*(pinned(t, pltpu.HBM) for t in arrays), *came)


def update(n, made, w, m, v):
    layers = w[0].shape[0]
    parts = 2
    chunks = layers * 3 * parts
    count = sum(t.size for t in w)
    any_space = pl.BlockSpec(memory_space=pl.ANY)
    in_vmem = pl.BlockSpec(memory_space=pltpu.VMEM)
    half = n // 2
    g, squares, ahead = made[:3], made[3], made[4:]
    return pl.pallas_call(
        functools.partial(update_kernel, n, float(count), parts),
        out_shape=tuple(kept(t.shape, BF16) for t in w)
        + tuple(kept(t.shape, F32) for t in m + v)
        + (jax.ShapeDtypeStruct((LATE, m[0].shape[1] // 2, m[0].shape[2]), BF16),) * 2,
        in_specs=[in_vmem] * 4 + [any_space] * 3 + [in_vmem] * 3 + [any_space] * 6,
        out_specs=(in_vmem,) * 9 + (any_space,) * 2,
        scratch_shapes=[pltpu.VMEM(t.shape, BF16) for t in m]
        + [
            pltpu.SemaphoreType.DMA((3, 3, layers)),
            pltpu.SemaphoreType.DMA((2, LATE)),
            pltpu.SemaphoreType.DMA((chunks, 2, half)),
            pltpu.SemaphoreType.DMA((chunks, 2, half)),
        ],
        compiler_params=pltpu.CompilerParams(collective_id=1, has_side_effects=True, vmem_limit_bytes=12 * 2**20),
        name="update",
    )(
        *(pinned(t, pltpu.VMEM) for t in (*g, squares)),
        *(pinned(t, pltpu.HBM) for t in w),
        *(pinned(t, pltpu.VMEM) for t in ahead),
        *(pinned(t, pltpu.HBM) for t in (*m, *v)),
    )


def solution(mesh):
    n = mesh.shape["dp"]

    def step(x, dy, *arrays):
        w, m, v = (arrays[i : i + 3] for i in (0, 3, 6))
        *new, up, down = update(n, gradients(n, x, dy, *w, m[2], v[2]), w, m, v)
        came = tuple(lax.ppermute(t, "dp", [(i, (i + d) % n) for i in range(n)]) for t, d in ((up, 1), (down, -1)))
        out = store(new)
        return (*place_last(n, out[:2], came), *out[2:])

    shard = P(None, "dp", None)
    return jax.shard_map(
        step,
        mesh=mesh,
        in_specs=(P(("rep", "dp"), None, None),) * 2 + (P(),) * 3 + (shard,) * 6,
        out_specs=(P("rep", None, None),) * 3 + (P("rep", "dp", None),) * 6,
        check_vma=False,
    )
```

```python
import functools

import jax
import jax.numpy as jnp
from jax import lax
from jax.experimental import pallas as pl
from jax.experimental.pallas import tpu as pltpu
from jax.sharding import PartitionSpec as P

F32 = jnp.float32
BF16 = jnp.bfloat16
MESH = pl.DeviceIdType.MESH
LANES = 128
LATE = 4


def dot(a, b):
    return jnp.dot(a, b, preferred_element_type=F32)


def dot_t(a, b):
    return lax.dot_general(a, b, (((1,), (1,)), ((), ())), preferred_element_type=F32)


def scale_of(wide):
    return lax.rsqrt(jnp.mean(wide * wide, -1, keepdims=True) + 1e-6)


def pinned(t, space):
    return pltpu.with_memory_space_constraint(t, space)


def kept(shape, dtype):
    return pltpu.VMEM(shape, dtype)


def loop(count, body):
    lax.fori_loop(0, count, lambda i, c: (body(i), c)[1], 0)


def at(i, size):
    return pl.ds(pl.multiple_of(i * size, size), size)


def grad_kernel(n, layers, shapes, *refs):
    (x_hbm, dy_hbm, wg_hbm, wu_hbm, wd_hbm, md_hbm, vd_hbm) = refs[:7]
    (OG, OU, OD, ALL, PW, PM, PV) = refs[7:14]
    (A, AT, D, DT, H, ACT, DG, DU, DA, WG, WU, WD, G, RU, RD, SQ, *sems) = refs[14:]
    x_sem, dy_sem, w_sem, ahead_sem, send_sem, recv_sem, low_sem, sq_send, sq_recv = sems
    tokens, dim, ff, blocks = shapes
    share = ff // n
    tiles = share // LANES
    tile = n * LANES
    tb = tokens // blocks
    half = n // 2
    hr = LANES // 2
    cols = tile // 2
    me = lax.axis_index("dp")
    up, down = lax.rem(me + 1, n), lax.rem(me + n - 1, n)
    ring = lambda d: lax.rem(me + d + n, n)

    def tok(i):
        return at(i, tb)

    def fetch(k):
        slot = lax.rem(k, 2)
        layer = lax.rem(k // tiles, 2)
        t = lax.rem(k, tiles)

        def one(b):
            place = pl.ds(pl.multiple_of(b * share + t * LANES, LANES), LANES)
            here = at(b, LANES)
            pltpu.make_async_copy(wg_hbm.at[layer, :, place], WG.at[slot, :, here], w_sem.at[slot, 0]).start()
            pltpu.make_async_copy(wu_hbm.at[layer, :, place], WU.at[slot, :, here], w_sem.at[slot, 1]).start()
            pltpu.make_async_copy(wd_hbm.at[layer, place, :], WD.at[slot, here, :], w_sem.at[slot, 2]).start()

        loop(n, one)

    def fetched(k):
        slot = lax.rem(k, 2)
        pltpu.make_async_copy(WG.at[slot], WG.at[slot], w_sem.at[slot, 0]).wait()
        pltpu.make_async_copy(WU.at[slot], WU.at[slot], w_sem.at[slot, 1]).wait()
        pltpu.make_async_copy(WD.at[slot], WD.at[slot], w_sem.at[slot, 2]).wait()

    def x_copy(i):
        return pltpu.make_async_copy(x_hbm.at[0, tok(i), :], H.at[tok(i), :], x_sem.at[i])

    def x_again(i):
        return pltpu.make_async_copy(x_hbm.at[0, tok(i), :], ACT.at[tok(i), pl.ds(0, dim)], x_sem.at[i])

    def dy_copy(i):
        return pltpu.make_async_copy(dy_hbm.at[0, tok(i), :], D.at[tok(i), :], dy_sem.at[i])

    x_copy(0).start()
    fetch(0)
    x_copy(1).start()
    barrier = pltpu.get_barrier_semaphore()
    for d in range(1, n):
        pl.semaphore_signal(barrier, inc=1, device_id={"dp": ring(d)}, device_id_type=MESH)

    def first_norm(i):
        wide = H[tok(i), :].astype(F32)
        A[tok(i), :] = (wide * scale_of(wide)).astype(BF16)
        DA[tok(i), :] = jnp.zeros((tb, dim), F32)

    def forward(k, i, act=ACT):
        slot = lax.rem(k, 2)
        for j in range(4):
            here = pl.ds(j * (tile // 4), tile // 4)
            g = dot(A[tok(i), :], WG[slot, :, here])
            u = dot(A[tok(i), :], WU[slot, :, here])
            s = 0.5 * jnp.tanh(0.5 * g) + 0.5
            act[tok(i), here] = (g * s * u).astype(BF16)
        DA[tok(i), :] += dot(act[tok(i), :], WD[slot])

    def second_norm(i):
        h = (H[tok(i), :].astype(F32) + DA[tok(i), :].astype(BF16).astype(F32)).astype(BF16)
        wide = h.astype(F32)
        return h, (wide * scale_of(wide)).astype(BF16)

    def second_norm_kept(i, h, a):
        H[tok(i), :] = h
        A[tok(i), :] = a
        AT[:, tok(i)] = a.T

    x_copy(0).wait()
    first_norm(0)
    fetched(0)
    loop(blocks - 2, lambda i: x_copy(i + 2).start())
    fetch(1)
    loop(blocks, lambda i: dy_copy(i).start())

    def opening(i):
        x_copy(i + 1).wait()
        forward(0, i)
        first_norm(i + 1)

    loop(blocks - 1, opening)

    def middle(j):
        q = blocks - 1 + 2 * j

        @pl.when(lax.rem(q + 1, blocks) == 0)
        def _():
            fetched((q + 1) // blocks)

        @pl.when((lax.rem(q, blocks) == 1) & (q // blocks < tiles - 1))
        def _():
            fetch(q // blocks + 1)

        seen = [jnp.minimum(2 * j + d, blocks - 1) for d in range(2)]

        @pl.when(2 * j < blocks)
        def _():
            dy_copy(2 * j).wait()
            dy_copy(2 * j + 1).wait()

        forward(q // blocks, lax.rem(q, blocks))
        forward((q + 1) // blocks, lax.rem(q + 1, blocks), DG)
        for i in seen:
            DT[:, tok(i)] = D[tok(i), :].T

    loop((tiles - 2) * blocks // 2 + 1, middle)
    fetch(tiles)

    def closing(i):
        normed = second_norm(i)
        forward(tiles - 1, i + 1)
        second_norm_kept(i, *normed)

    loop(blocks - 1, closing)

    def hidden(slot, j, i, pieces=1):
        size = 2 * tb // pieces
        for p, c in [(p, c) for p in range(pieces) for c in range(2)]:
            place = at(i * pieces + p, size)
            here = at(2 * j + c, cols // 2)
            g = dot(A[place, :], WG[slot, :, here])
            u = dot(A[place, :], WU[slot, :, here])
            back = dot_t(D[place, :], WD[slot, here, :]).astype(BF16).astype(F32)
            s = 0.5 * jnp.tanh(0.5 * g) + 0.5
            silu = g * s
            ACT[place, here] = (silu * u).astype(BF16)
            DU[place, here] = (back * silu).astype(BF16)
            DG[place, here] = (back * u * (s + silu * (1.0 - s))).astype(BF16)

    fetched(tiles)
    normed = second_norm(blocks - 1)
    hidden(tiles % 2, 0, 0, 2)
    second_norm_kept(blocks - 1, *normed)

    pl.semaphore_wait(barrier, n - 1)

    def remote(src, dst, slot, u, way, step, arrival=None):
        return pltpu.make_async_remote_copy(
            src_ref=src,
            dst_ref=dst,
            send_sem=send_sem.at[slot, way, step],
            recv_sem=recv_sem.at[u, way, step] if arrival is None else arrival,
            device_id={"dp": (up, down)[way]},
            device_id_type=MESH,
        )

    low, high, whole = pl.ds(0, hr), pl.ds(hr, hr), pl.ds(0, 2 * hr)
    lands = (RU, RD)

    def rows(step):
        return pl.ds(hr + (step - 1) * 2 * hr, 2 * hr)

    def begin_low(u, slot):
        remote(G.at[slot, ring(half), low], RU.at[u, low], slot, u, 0, 0).start()
        remote(G.at[slot, ring(1 - half), low], RD.at[u, pl.ds(hr, hr)], slot, u, 1, 1, low_sem.at[u]).start()

    def begin_high(u, slot):
        remote(G.at[slot, ring(half), high], RD.at[u, low], slot, u, 1, 0).start()
        remote(G.at[slot, ring(half - 1), high], RU.at[u, pl.ds(2 * hr, hr)], slot, u, 0, 1).start()

    def arrived(land, sem):
        pltpu.make_async_copy(land, land, sem).wait()

    def received(u, way, step):
        if (way, step) == (1, 1):
            arrived(RD.at[u, pl.ds(hr, hr)], low_sem.at[u])
            arrived(RD.at[u, pl.ds(2 * hr, hr)], recv_sem.at[u, 1, 1])
        else:
            arrived(lands[way].at[u, rows(step) if step else low], recv_sem.at[u, way, step])

    def add(land, place, mine):
        land[place] = (land[place].astype(F32) + mine.astype(F32)).astype(BF16)

    def second_low(u, slot):
        received(u, 0, 0)
        add(RU, (u, low), G[slot, ring(half - 1), low])
        remote(RU.at[u, low], RU.at[u, pl.ds(hr, hr)], slot, u, 0, 1).start()

    def second_high(u, slot):
        received(u, 1, 0)
        add(RD, (u, low), G[slot, ring(1 - half), high])
        remote(RD.at[u, low], RD.at[u, pl.ds(2 * hr, hr)], slot, u, 1, 1).start()

    def pass_on(u, slot, way, step):
        received(u, way, step - 1)
        add(lands[way], (u, rows(step - 1)), G[slot, ring(half - step if way == 0 else step - half)])
        remote(lands[way].at[u, rows(step - 1)], lands[way].at[u, rows(step)], slot, u, way, step).start()

    def later(u, slot, step):
        pass_on(u, slot, 0, step)
        pass_on(u, slot, 1, step)

    def half_on(u, slot, part, sem):
        here, there = pl.ds((1 + part) * hr, hr), pl.ds((3 + part) * hr, hr)
        arrived(RD.at[u, here], sem)
        add(RD, (u, here), G[slot, ring(2 - half), (low, high)[part]])
        remote(RD.at[u, here], RD.at[u, there], slot, u, 1, 2).start()

    def third_low(u, slot):
        half_on(u, slot, 0, low_sem.at[u])

    def third_rest(u, slot):
        pass_on(u, slot, 0, 2)
        half_on(u, slot, 1, recv_sem.at[u, 1, 1])

    def finish(u, slot, which, layer, t):
        received(u, 0, half - 1)
        received(u, 1, half - 1)
        total = G[slot, me].astype(F32) + RU[u, rows(half - 1)].astype(F32) + RD[u, rows(half - 1)].astype(F32)
        total = total.astype(BF16)
        wide = total.astype(F32)
        SQ[...] += jnp.sum((wide * wide).reshape(-1, 8, dim), axis=0)
        if which == 0:
            OD[layer, at(t, LANES), :] = total
        else:
            out = (OG, OU)[which - 1]
            for b in range(n):
                piece = total[hr * (b // (n // 2)) : hr * (b // (n // 2)) + hr, LANES * (b % (n // 2)) : LANES * (b % (n // 2)) + LANES]
                out[layer, :, pl.ds(pl.multiple_of(b * share + t * LANES, LANES), LANES)] = piece
        for way in range(2):
            for step in range(half):
                src = G.at[slot, 0, whole] if step > 0 else G.at[slot, 0, low]
                pltpu.make_async_copy(src, src, send_sem.at[slot, way, step]).wait()

    SQ[...] = jnp.zeros_like(SQ)

    end = 2 * tiles - 1

    def tile_step(k):
        wk = k + tiles
        slot = lax.rem(wk, 2)
        base = lax.rem(k, 2) * 3
        prev = 3 - base
        u0 = 3 * k
        p0 = u0 - 3
        going = k >= 1
        old_t = lax.rem(k - 1 + tiles, tiles)
        old_layer = jnp.where(k - 1 < tiles, 1, 0)

        @pl.when(k > 0)
        def _():
            fetched(wk)

        @pl.when(k < 2 * tiles - 1)
        def _():
            fetch(wk + 1)

        def when(cond):
            return pl.when(going & cond)

        def wide_part(src, unit, j):
            part = dot(AT[...], src[:, at(j, cols)]).astype(BF16)
            G[base + unit, :, at(j, hr), :] = part.reshape(n, dim // n, cols)

        gate, upper = (u0 + 1, base + 1), (u0 + 2, base + 2)
        old, old_gate, old_upper = (p0, prev), (p0 + 1, prev + 1), (p0 + 2, prev + 2)

        held = (k == 0) & (lax.rem(lax.axis_index("rep"), 2) == 0)

        def halves(j):
            def some(i):
                @pl.when((k > 0) | (j > 0) | (i > 0))
                def _():
                    hidden(slot, j, i)

                @when((j == 0) & (i == 0))
                def _():
                    later(*old, 2)
                    later(*old_upper, 3)

                @pl.when((k == 0) & (j == 1) & (i == 0))
                def _():
                    third_low(*gate)

                @pl.when((k == 0) & (j == 1) & (i == 1))
                def _():
                    second_low(*upper)

            loop(blocks // 2, some)
            wide_part(DG, 1, j)

            @pl.when((j == 0) & jnp.logical_not(held))
            def _():
                begin_low(*gate)

            @pl.when(j == 1)
            def _():
                begin_high(*gate)

            @pl.when((j == 1) & (k == 0))
            def _():
                second_low(*gate)

            wide_part(DU, 2, j)

            @pl.when((j == 0) & held)
            def _():
                begin_low(*gate)

            @pl.when(j == 0)
            def _():
                begin_low(*upper)

            @pl.when(j == 1)
            def _():
                begin_high(*upper)

            @when(j == 1)
            def _():
                later(*old, 3)
                finish(*old_gate, 1, old_layer, old_t)
                finish(*old_upper, 2, old_layer, old_t)
                second_low(*gate)

            @pl.when((j == 1) & (k == 0))
            def _():
                third_low(*upper)

        loop(2, halves)

        def down_part(j):
            part = dot(DT[...], ACT[:, at(j, cols)])
            flipped = part.T.astype(BF16)
            for b in range(cols // LANES):
                G[base, j * (cols // LANES) + b] = flipped[b * LANES : (b + 1) * LANES]

            @pl.when(j == 0)
            def _():
                second_high(*gate)

        loop(2, down_part)

        @pl.when(k < end)
        def _():
            begin_low(u0, base)
            begin_high(u0, base)

        @when(k < end)
        def _():
            second_low(*upper)

        @pl.when(k == tiles - 1)
        def _():
            loop(blocks, lambda i: x_again(i).start())

        def ring_part(i):
            @pl.when(i == 0)
            def _():
                second_high(*upper)

            @pl.when((i == 0) & (k == 0))
            def _():
                second_low(u0, base)
                third_rest(*gate)

            @when(i == 2)
            def _():
                finish(*old, 0, old_layer, old_t)
                later(*gate, 2)

        @pl.when(k < tiles)
        def _():
            def input_part(i):
                so_far = jnp.where(k == 0, 0.0, DA[tok(i), :])
                DA[tok(i), :] = so_far + (dot_t(DG[tok(i), :], WG[slot]) + dot_t(DU[tok(i), :], WU[slot]))
                ring_part(i)

            loop(blocks, input_part)

        @pl.when((k >= tiles) & (k < end))
        def _():
            loop(blocks, ring_part)

        @pl.when(k == tiles - 1)
        def _():
            def between(i):
                h = H[tok(i), :].astype(F32)
                da = DA[tok(i), :].astype(BF16).astype(F32)
                r = scale_of(h)
                dh = (r * da - h * (r * r * r * jnp.mean(h * da, -1, keepdims=True))).astype(BF16)
                d = (D[tok(i), :].astype(F32) + dh.astype(F32)).astype(BF16)
                D[tok(i), :] = d
                DT[:, tok(i)] = d.T
                x_again(i).wait()
                wide = ACT[tok(i), pl.ds(0, dim)].astype(F32)
                a = (wide * scale_of(wide)).astype(BF16)
                A[tok(i), :] = a
                AT[:, tok(i)] = a.T

                @pl.when(i == 1)
                def _():
                    second_low(u0, base)
                    second_high(u0, base)

            loop(blocks, between)

        @when((k != tiles - 1) & (k < end))
        def _():
            second_low(u0, base)

        @pl.when((k != tiles - 1) & (k < end))
        def _():
            second_high(u0, base)

        @pl.when(k == 0)
        def _():
            third_rest(*upper)

        @when(k < end)
        def _():
            later(*upper, 2)

        @pl.when(k < end)
        def _():
            later(*gate, 3)

    loop(2 * tiles, tile_step)

    ahead = (
        pltpu.make_async_copy(wd_hbm.at[layers - 1, at(me, share), :], PW, ahead_sem.at[0]),
        pltpu.make_async_copy(md_hbm.at[layers - 1], PM, ahead_sem.at[1]),
        pltpu.make_async_copy(vd_hbm.at[layers - 1], PV, ahead_sem.at[2]),
    )
    for copy in ahead:
        copy.start()

    base = (end % 2) * 3
    down_unit, gate, upper = ((3 * end + j, base + j) for j in range(3))
    begin_high(*down_unit)
    second_high(*upper)
    begin_low(*down_unit)
    second_low(*upper)
    second_high(*down_unit)
    second_low(*down_unit)
    for step in range(2, half):
        for unit in (gate, upper, down_unit):
            later(*unit, step)
    finish(*gate, 1, 0, tiles - 1)
    finish(3 * (end - 1), 3 - base, 0, 0, tiles - 2)
    finish(*upper, 2, 0, tiles - 1)
    finish(*down_unit, 0, 0, tiles - 1)

    squares = SQ[:, :LANES]
    for j in range(1, dim // LANES):
        squares += SQ[:, j * LANES : (j + 1) * LANES]
    ALL[me] = squares

    def tell(d):
        return pltpu.make_async_remote_copy(
            src_ref=ALL.at[me],
            dst_ref=ALL.at[me],
            send_sem=sq_send.at[d],
            recv_sem=sq_recv.at[d],
            device_id={"dp": ring(d)},
            device_id_type=MESH,
        )

    for d in range(1, n):
        tell(d).start()
    for d in range(1, n):
        tell(d).wait()
    for copy in ahead:
        copy.wait()


def gradients(n, x, dy, w_gate, w_up, w_down, m_down, v_down):
    layers, dim, ff = w_gate.shape
    tokens = x.shape[1]
    blocks = 4
    share = ff // n
    tiles = share // LANES
    tile = n * LANES
    units = 3 * layers * tiles
    half = n // 2
    land = LANES // 2 + LANES * (half - 1)
    any_space = pl.BlockSpec(memory_space=pl.ANY)
    return pl.pallas_call(
        functools.partial(grad_kernel, n, layers, (tokens, dim, ff, blocks)),
        out_shape=tuple(
            kept(shape, dtype)
            for shape, dtype in (
                ((layers, dim // n, ff), BF16),
                ((layers, dim // n, ff), BF16),
                ((layers, share, dim), BF16),
                ((n, 8, LANES), F32),
                ((share, dim), BF16),
                ((share, dim), F32),
                ((share, dim), F32),
            )
        ),
        in_specs=[any_space] * 7,
        out_specs=(pl.BlockSpec(memory_space=pltpu.VMEM),) * 7,
        scratch_shapes=[
            pltpu.VMEM((tokens, dim), BF16),
            pltpu.VMEM((dim, tokens), BF16),
            pltpu.VMEM((tokens, dim), BF16),
            pltpu.VMEM((dim, tokens), BF16),
            pltpu.VMEM((tokens, dim), BF16),
            pltpu.VMEM((tokens, tile), BF16),
            pltpu.VMEM((tokens, tile), BF16),
            pltpu.VMEM((tokens, tile), BF16),
            pltpu.VMEM((tokens, dim), F32),
            pltpu.VMEM((2, dim, tile), BF16),
            pltpu.VMEM((2, dim, tile), BF16),
            pltpu.VMEM((2, tile, dim), BF16),
            pltpu.VMEM((6, n, LANES, dim), BF16),
            pltpu.VMEM((units, land, dim), BF16),
            pltpu.VMEM((units, land, dim), BF16),
            pltpu.VMEM((8, dim), F32),
            pltpu.SemaphoreType.DMA((blocks,)),
            pltpu.SemaphoreType.DMA((blocks,)),
            pltpu.SemaphoreType.DMA((2, 3)),
            pltpu.SemaphoreType.DMA((3,)),
            pltpu.SemaphoreType.DMA((6, 2, half)),
            pltpu.SemaphoreType.DMA((units, 2, half)),
            pltpu.SemaphoreType.DMA((units,)),
            pltpu.SemaphoreType.DMA((n,)),
            pltpu.SemaphoreType.DMA((n,)),
        ],
        compiler_params=pltpu.CompilerParams(collective_id=0, has_side_effects=True, vmem_limit_bytes=62_500_000),
        name="grads",
    )(*(pinned(t, pltpu.HBM) for t in (x, dy, w_gate, w_up, w_down, m_down, v_down)))


def turns(layers):
    return [(2, l) for l in reversed(range(layers))] + [(a, l) for l in reversed(range(layers)) for a in (0, 1)]


def update_kernel(n, count, parts, *refs):
    G, w_hbm, m_hbm, v_hbm = (refs[i : i + 3] for i in (0, 4, 10, 13))
    SQ, PW, PM, PV = refs[3], *refs[7:10]
    N, M, V = (refs[i : i + 3] for i in (16, 19, 22))
    last = refs[25:27]
    W = refs[27:30]
    in_sem, last_sem, send_sem, recv_sem = refs[30:]
    me = lax.axis_index("dp")
    half = n // 2
    up, down = lax.rem(me + 1, n), lax.rem(me + n - 1, n)
    ring = lambda d: lax.rem(me + d + n, n)
    layers = G[0].shape[0]

    barrier = pltpu.get_barrier_semaphore()
    for peer in (up, down):
        pl.semaphore_signal(barrier, inc=1, device_id={"dp": peer}, device_id_type=MESH)

    order = turns(layers)
    loads = {}
    for a, l in order[1:]:
        rows = G[a].shape[1]
        own = pl.ds(pl.multiple_of(me * rows, rows), rows)
        loads[a, l] = (
            pltpu.make_async_copy(w_hbm[a].at[l, own, :], W[a].at[l], in_sem.at[0, a, l]),
            pltpu.make_async_copy(m_hbm[a].at[l], M[a].at[l], in_sem.at[1, a, l]),
            pltpu.make_async_copy(v_hbm[a].at[l], V[a].at[l], in_sem.at[2, a, l]),
        )
    total = jnp.sum(jnp.sum(SQ[...], axis=0), axis=(0, 1), keepdims=True)
    factor = jnp.minimum(1.0, 0.5 * lax.rsqrt(total / count + 1e-30))

    def shape(a):
        rows, cols = G[a].shape[1:]
        return (rows, cols // parts, 0) if a < 2 else (rows // parts, cols, 1)

    def place(a, l, p, owner, part):
        rows = G[a].shape[1]
        r, c, split = shape(a)
        hr = r // 2
        start = owner * rows + (p * r if split else 0)
        start, size = (start, r) if part == 2 else (start + part * hr, hr)
        return (l, pl.ds(pl.multiple_of(start, hr), size), pl.ds(0 if split else p * c, c))

    def send(i, a, l, p, way, step):
        owner = ring(-step) if way == 0 else ring(step)
        ref = N[a].at[place(a, l, p, owner, 2 if step < half - 1 else way)]
        return pltpu.make_async_remote_copy(
            src_ref=ref,
            dst_ref=ref,
            send_sem=send_sem.at[i, way, step],
            recv_sem=recv_sem.at[i, way, step],
            device_id={"dp": (up, down)[way]},
            device_id_type=MESH,
        )

    def came(i, a, l, p, way, step):
        owner = ring(-step - 1) if way == 0 else ring(step + 1)
        where = place(a, l, p, owner, 2 if step < half - 1 else way)
        ref = N[a].at[where]
        pltpu.make_async_copy(ref, ref, recv_sem.at[i, way, step]).wait()

    def adam(a, l, p):
        r, c, split = shape(a)
        rows = G[a].shape[1]
        step = 32
        lane = pl.ds(0 if split else p * c, c)

        def some(i):
            row = pl.ds(pl.multiple_of((p * r if split else 0) + i * step, step), step)
            old = (PW[row, lane], PM[row, lane], PV[row, lane]) if (a, l) == order[0] else (W[a][l, row, lane], M[a][l, row, lane], V[a][l, row, lane])
            g = G[a][l, row, lane].astype(F32) * factor
            m = 0.9 * old[1] + 0.1 * g
            v = 0.95 * old[2] + 0.05 * g * g
            M[a][l, row, lane] = m
            V[a][l, row, lane] = v
            w = old[0].astype(F32)
            new = (w - 0.02 * (m * lax.rsqrt(v + 1e-8) + 0.1 * w)).astype(BF16)
            there = pl.ds(pl.multiple_of(me * rows + (p * r if split else 0) + i * step, step), step)
            N[a][l, there, lane] = new

        loop(r // step, some)

    chunks = []
    for a, l in order:
        for p in range(parts):
            chunks.append((len(chunks), a, l, p))
    for i, a, l, p in chunks:
        if p == 0:
            for copy in loads.get((a, l), ()):
                copy.wait()
        adam(a, l, p)
        if i == 0:
            pl.semaphore_wait(barrier, 2)
        send(i, a, l, p, 0, 0).start()
        send(i, a, l, p, 1, 0).start()
        if i == 0:
            for copies in loads.values():
                for copy in copies:
                    copy.start()
    late = order[len(order) - LATE :]

    def hops(a, l):
        return half - 1 if (a, l) in late else half

    def to_permute(a, l, way):
        rows = G[a].shape[1]
        owner = ring(1 - half) if way == 0 else ring(half - 1)
        src = N[a].at[l, pl.ds(pl.multiple_of(owner * rows + way * (rows // 2), rows // 2), rows // 2), :]
        return pltpu.make_async_copy(src, last[way].at[late.index((a, l))], last_sem.at[way, late.index((a, l))])

    for step in range(half):
        for i, a, l, p in chunks:
            for way in range(2):
                if step < hops(a, l):
                    came(i, a, l, p, way, step)
                if step < hops(a, l) - 1:
                    send(i, a, l, p, way, step + 1).start()
                elif step == half - 2 and p == parts - 1:
                    to_permute(a, l, way).start()
    for i, a, l, p in chunks:
        for way in range(2):
            for step in range(hops(a, l)):
                send(i, a, l, p, way, step).wait_send()
    for a, l in late:
        for way in range(2):
            to_permute(a, l, way).wait()


def store_kernel(n, count, *refs):
    src, dst, sem = refs[:count], refs[count : 2 * count], refs[-1]
    layers = src[0].shape[0]
    late = turns(layers)[-LATE:]
    opposite = lax.axis_index("dp") + n // 2
    copies = []
    for i, (a, b) in enumerate(zip(src, dst, strict=True)):
        rows = a.shape[1] // n
        for l in range(layers):
            if (i, l) in late:
                for d in range(1, n):
                    here = at(lax.rem(opposite + d, n), rows)
                    copies.append(pltpu.make_async_copy(a.at[l, here], b.at[l, here], sem.at[i, l, d]))
            else:
                copies.append(pltpu.make_async_copy(a.at[l], b.at[l], sem.at[i, l, 0]))
    for copy in copies:
        copy.start()
    for copy in copies:
        copy.wait()


def store(n, arrays):
    count = len(arrays)
    return pl.pallas_call(
        functools.partial(store_kernel, n, count),
        out_shape=tuple(jax.ShapeDtypeStruct(t.shape, t.dtype) for t in arrays),
        in_specs=[pl.BlockSpec(memory_space=pltpu.VMEM)] * count,
        out_specs=(pl.BlockSpec(memory_space=pl.ANY),) * count,
        scratch_shapes=[pltpu.SemaphoreType.DMA((count, arrays[0].shape[0], n))],
        compiler_params=pltpu.CompilerParams(vmem_limit_bytes=2**20),
        cost_estimate=pl.CostEstimate(flops=10_000_000_000, bytes_accessed=0, transcendentals=0),
        name="store",
    )(*(pinned(t, pltpu.VMEM) for t in arrays))


def place_kernel(n, count, *refs):
    up_ref, down_ref = refs[count : count + 2]
    outs, sem = refs[count + 2 : -1], refs[-1]
    opposite = lax.rem(lax.axis_index("dp") + n // 2, n)
    hr = up_ref.shape[1]
    copies = []
    for i, (a, l) in enumerate(turns(outs[0].shape[0])[-LATE:]):
        for way, src in enumerate((up_ref, down_ref)):
            there = pl.ds(pl.multiple_of(opposite * 2 * hr + way * hr, hr), hr)
            copies.append(pltpu.make_async_copy(src.at[i], outs[a].at[l, there, :], sem.at[i, way]))
    for copy in copies:
        copy.start()
    for copy in copies:
        copy.wait()


def place_last(n, arrays, came):
    count = len(arrays)
    any_space = pl.BlockSpec(memory_space=pl.ANY)
    in_vmem = pl.BlockSpec(memory_space=pltpu.VMEM)
    return pl.pallas_call(
        functools.partial(place_kernel, n, count),
        out_shape=tuple(jax.ShapeDtypeStruct(t.shape, t.dtype) for t in arrays),
        in_specs=[any_space] * count + [in_vmem] * 2,
        out_specs=(any_space,) * count,
        scratch_shapes=[pltpu.SemaphoreType.DMA((LATE, 2))],
        input_output_aliases={i: i for i in range(count)},
        compiler_params=pltpu.CompilerParams(vmem_limit_bytes=2**20),
        name="place",
    )(*(pinned(t, pltpu.HBM) for t in arrays), *came)


def update(n, made, w, m, v):
    layers = w[0].shape[0]
    parts = 2
    chunks = layers * 3 * parts
    count = sum(t.size for t in w)
    any_space = pl.BlockSpec(memory_space=pl.ANY)
    in_vmem = pl.BlockSpec(memory_space=pltpu.VMEM)
    half = n // 2
    g, squares, ahead = made[:3], made[3], made[4:]
    return pl.pallas_call(
        functools.partial(update_kernel, n, float(count), parts),
        out_shape=tuple(kept(t.shape, BF16) for t in w)
        + tuple(kept(t.shape, F32) for t in m + v)
        + (jax.ShapeDtypeStruct((LATE, m[0].shape[1] // 2, m[0].shape[2]), BF16),) * 2,
        in_specs=[in_vmem] * 4 + [any_space] * 3 + [in_vmem] * 3 + [any_space] * 6,
        out_specs=(in_vmem,) * 9 + (any_space,) * 2,
        scratch_shapes=[pltpu.VMEM(t.shape, BF16) for t in m]
        + [
            pltpu.SemaphoreType.DMA((3, 3, layers)),
            pltpu.SemaphoreType.DMA((2, LATE)),
            pltpu.SemaphoreType.DMA((chunks, 2, half)),
            pltpu.SemaphoreType.DMA((chunks, 2, half)),
        ],
        compiler_params=pltpu.CompilerParams(collective_id=1, has_side_effects=True, vmem_limit_bytes=12 * 2**20),
        name="update",
    )(
        *(pinned(t, pltpu.VMEM) for t in (*g, squares)),
        *(pinned(t, pltpu.HBM) for t in w),
        *(pinned(t, pltpu.VMEM) for t in ahead),
        *(pinned(t, pltpu.HBM) for t in (*m, *v)),
    )


def solution(mesh):
    n = mesh.shape["dp"]

    def step(x, dy, *arrays):
        w, m, v = (arrays[i : i + 3] for i in (0, 3, 6))
        *new, up, down = update(n, gradients(n, x, dy, *w, m[2], v[2]), w, m, v)
        came = tuple(lax.ppermute(t, "dp", [(i, (i + d) % n) for i in range(n)]) for t, d in ((up, 1), (down, -1)))
        out = store(n, new)
        return (*place_last(n, out[:2], came), *out[2:])

    shard = P(None, "dp", None)
    return jax.shard_map(
        step,
        mesh=mesh,
        in_specs=(P(("rep", "dp"), None, None),) * 2 + (P(),) * 3 + (shard,) * 6,
        out_specs=(P("rep", None, None),) * 3 + (P("rep", "dp", None),) * 6,
        check_vma=False,
    )
```

```python
import functools

import jax
import jax.numpy as jnp
from jax import lax
from jax.experimental import pallas as pl
from jax.experimental.pallas import tpu as pltpu
from jax.sharding import PartitionSpec as P

F32 = jnp.float32
BF16 = jnp.bfloat16
MESH = pl.DeviceIdType.MESH
LANES = 128
LATE = 4


def dot(a, b):
    return jnp.dot(a, b, preferred_element_type=F32)


def dot_t(a, b):
    return lax.dot_general(a, b, (((1,), (1,)), ((), ())), preferred_element_type=F32)


def scale_of(wide):
    return lax.rsqrt(jnp.mean(wide * wide, -1, keepdims=True) + 1e-6)


def pinned(t, space):
    return pltpu.with_memory_space_constraint(t, space)


def kept(shape, dtype):
    return pltpu.VMEM(shape, dtype)


def loop(count, body):
    lax.fori_loop(0, count, lambda i, c: (body(i), c)[1], 0)


def at(i, size):
    return pl.ds(pl.multiple_of(i * size, size), size)


def grad_kernel(n, layers, shapes, *refs):
    (x_hbm, dy_hbm, wg_hbm, wu_hbm, wd_hbm, md_hbm, vd_hbm) = refs[:7]
    (OG, OU, OD, ALL, PW, PM, PV) = refs[7:14]
    (A, AT, D, DT, H, ACT, DG, DU, DA, WG, WU, WD, G, RU, RD, SQ, *sems) = refs[14:]
    x_sem, dy_sem, w_sem, ahead_sem, send_sem, recv_sem, low_sem, sq_send, sq_recv = sems
    tokens, dim, ff, blocks = shapes
    share = ff // n
    tiles = share // LANES
    tile = n * LANES
    tb = tokens // blocks
    half = n // 2
    hr = LANES // 2
    cols = tile // 2
    me = lax.axis_index("dp")
    up, down = lax.rem(me + 1, n), lax.rem(me + n - 1, n)
    ring = lambda d: lax.rem(me + d + n, n)

    def tok(i):
        return at(i, tb)

    def fetch(k):
        slot = lax.rem(k, 2)
        layer = lax.rem(k // tiles, 2)
        t = lax.rem(k, tiles)

        def one(b):
            place = pl.ds(pl.multiple_of(b * share + t * LANES, LANES), LANES)
            here = at(b, LANES)
            pltpu.make_async_copy(wg_hbm.at[layer, :, place], WG.at[slot, :, here], w_sem.at[slot, 0]).start()
            pltpu.make_async_copy(wu_hbm.at[layer, :, place], WU.at[slot, :, here], w_sem.at[slot, 1]).start()
            pltpu.make_async_copy(wd_hbm.at[layer, place, :], WD.at[slot, here, :], w_sem.at[slot, 2]).start()

        loop(n, one)

    def fetched(k):
        slot = lax.rem(k, 2)
        pltpu.make_async_copy(WG.at[slot], WG.at[slot], w_sem.at[slot, 0]).wait()
        pltpu.make_async_copy(WU.at[slot], WU.at[slot], w_sem.at[slot, 1]).wait()
        pltpu.make_async_copy(WD.at[slot], WD.at[slot], w_sem.at[slot, 2]).wait()

    def x_copy(i):
        return pltpu.make_async_copy(x_hbm.at[0, tok(i), :], H.at[tok(i), :], x_sem.at[i])

    def x_again(i):
        return pltpu.make_async_copy(x_hbm.at[0, tok(i), :], ACT.at[tok(i), pl.ds(0, dim)], x_sem.at[i])

    def dy_copy(i):
        return pltpu.make_async_copy(dy_hbm.at[0, tok(i), :], D.at[tok(i), :], dy_sem.at[i])

    x_copy(0).start()
    fetch(0)
    x_copy(1).start()
    barrier = pltpu.get_barrier_semaphore()
    for d in range(1, n):
        pl.semaphore_signal(barrier, inc=1, device_id={"dp": ring(d)}, device_id_type=MESH)

    def first_norm(i):
        wide = H[tok(i), :].astype(F32)
        A[tok(i), :] = (wide * scale_of(wide)).astype(BF16)

    def forward(k, i, act=ACT, fresh=False):
        slot = k % 2 if isinstance(k, int) else lax.rem(k, 2)
        for j in range(4):
            here = pl.ds(j * (tile // 4), tile // 4)
            g = dot(A[tok(i), :], WG[slot, :, here])
            u = dot(A[tok(i), :], WU[slot, :, here])
            s = 0.5 * jnp.tanh(0.5 * g) + 0.5
            act[tok(i), here] = (g * s * u).astype(BF16)
        part = dot(act[tok(i), :], WD[slot])
        DA[tok(i), :] = part if fresh else DA[tok(i), :] + part

    def second_norm(i):
        h = (H[tok(i), :].astype(F32) + DA[tok(i), :].astype(BF16).astype(F32)).astype(BF16)
        wide = h.astype(F32)
        return h, (wide * scale_of(wide)).astype(BF16)

    def second_norm_kept(i, h, a):
        H[tok(i), :] = h
        A[tok(i), :] = a
        AT[:, tok(i)] = a.T

    x_copy(0).wait()
    first_norm(0)
    fetched(0)
    loop(blocks - 2, lambda i: x_copy(i + 2).start())
    fetch(1)
    loop(blocks, lambda i: dy_copy(i).start())

    def opening(j):
        i = 2 * j
        x_copy(i + 1).wait()

        @pl.when(i + 2 < blocks)
        def _():
            x_copy(i + 2).wait()

        forward(0, i, fresh=True)
        first_norm(i + 1)
        forward(0, i + 1, DG, True)
        first_norm(jnp.minimum(i + 2, blocks - 1))

    loop(blocks // 2, opening)

    def middle(j):
        k, i = 1 + 2 * j // blocks, lax.rem(2 * j, blocks)

        @pl.when(i == 0)
        def _():
            fetched(k)
            fetch(k + 1)

        @pl.when(2 * j < blocks)
        def _():
            dy_copy(i).wait()
            dy_copy(i + 1).wait()

        forward(k, i)
        forward(k, i + 1, DG)
        for d in range(2):
            DT[:, tok(i + d)] = D[tok(i + d), :].T

    loop((tiles - 2) * blocks // 2, middle)
    fetched(tiles - 1)
    fetch(tiles)

    @pl.when(me >= 0)
    def _():
        forward(tiles - 1, 0)
        normed = second_norm(0)
        forward(tiles - 1, 1, DG)
        second_norm_kept(0, *normed)

    for i in range(2, blocks, 2):

        @pl.when(me >= 0)
        def _(i=i):
            normed = second_norm(i - 1)
            forward(tiles - 1, i)
            second_norm_kept(i - 1, *normed)
            normed = second_norm(i)
            forward(tiles - 1, i + 1, DG)
            second_norm_kept(i, *normed)

    def hidden(slot, j, i, pieces=1):
        size = 2 * tb // pieces
        for p, c in [(p, c) for p in range(pieces) for c in range(2)]:
            place = at(i * pieces + p, size)
            here = at(2 * j + c, cols // 2)
            g = dot(A[place, :], WG[slot, :, here])
            u = dot(A[place, :], WU[slot, :, here])
            back = dot_t(D[place, :], WD[slot, here, :]).astype(BF16).astype(F32)
            s = 0.5 * jnp.tanh(0.5 * g) + 0.5
            silu = g * s
            ACT[place, here] = (silu * u).astype(BF16)
            DU[place, here] = (back * silu).astype(BF16)
            DG[place, here] = (back * u * (s + silu * (1.0 - s))).astype(BF16)

    fetched(tiles)
    normed = second_norm(blocks - 1)
    hidden(tiles % 2, 0, 0, 2)
    second_norm_kept(blocks - 1, *normed)

    pl.semaphore_wait(barrier, n - 1)

    def remote(src, dst, slot, u, way, step, arrival=None):
        return pltpu.make_async_remote_copy(
            src_ref=src,
            dst_ref=dst,
            send_sem=send_sem.at[slot, way, step],
            recv_sem=recv_sem.at[u, way, step] if arrival is None else arrival,
            device_id={"dp": (up, down)[way]},
            device_id_type=MESH,
        )

    low, high, whole = pl.ds(0, hr), pl.ds(hr, hr), pl.ds(0, 2 * hr)
    lands = (RU, RD)

    def rows(step):
        return pl.ds(hr + (step - 1) * 2 * hr, 2 * hr)

    def begin_low(u, slot):
        remote(G.at[slot, ring(half), low], RU.at[u, low], slot, u, 0, 0).start()
        remote(G.at[slot, ring(1 - half), low], RD.at[u, pl.ds(hr, hr)], slot, u, 1, 1, low_sem.at[u]).start()

    def begin_high(u, slot):
        remote(G.at[slot, ring(half), high], RD.at[u, low], slot, u, 1, 0).start()
        remote(G.at[slot, ring(half - 1), high], RU.at[u, pl.ds(2 * hr, hr)], slot, u, 0, 1).start()

    def arrived(land, sem):
        pltpu.make_async_copy(land, land, sem).wait()

    def received(u, way, step):
        if (way, step) == (1, 1):
            arrived(RD.at[u, pl.ds(hr, hr)], low_sem.at[u])
            arrived(RD.at[u, pl.ds(2 * hr, hr)], recv_sem.at[u, 1, 1])
        else:
            arrived(lands[way].at[u, rows(step) if step else low], recv_sem.at[u, way, step])

    def add(land, place, mine):
        land[place] = (land[place].astype(F32) + mine.astype(F32)).astype(BF16)

    def second_low(u, slot):
        received(u, 0, 0)
        add(RU, (u, low), G[slot, ring(half - 1), low])
        remote(RU.at[u, low], RU.at[u, pl.ds(hr, hr)], slot, u, 0, 1).start()

    def second_high(u, slot):
        received(u, 1, 0)
        add(RD, (u, low), G[slot, ring(1 - half), high])
        remote(RD.at[u, low], RD.at[u, pl.ds(2 * hr, hr)], slot, u, 1, 1).start()

    def pass_on(u, slot, way, step):
        received(u, way, step - 1)
        add(lands[way], (u, rows(step - 1)), G[slot, ring(half - step if way == 0 else step - half)])
        remote(lands[way].at[u, rows(step - 1)], lands[way].at[u, rows(step)], slot, u, way, step).start()

    def later(u, slot, step):
        pass_on(u, slot, 0, step)
        pass_on(u, slot, 1, step)

    def half_on(u, slot, part, sem):
        here, there = pl.ds((1 + part) * hr, hr), pl.ds((3 + part) * hr, hr)
        arrived(RD.at[u, here], sem)
        add(RD, (u, here), G[slot, ring(2 - half), (low, high)[part]])
        remote(RD.at[u, here], RD.at[u, there], slot, u, 1, 2).start()

    def third_low(u, slot):
        half_on(u, slot, 0, low_sem.at[u])

    def third_rest(u, slot):
        pass_on(u, slot, 0, 2)
        half_on(u, slot, 1, recv_sem.at[u, 1, 1])

    def finish(u, slot, which, layer, t):
        received(u, 0, half - 1)
        received(u, 1, half - 1)
        total = G[slot, me].astype(F32) + RU[u, rows(half - 1)].astype(F32) + RD[u, rows(half - 1)].astype(F32)
        total = total.astype(BF16)
        wide = total.astype(F32)
        SQ[...] += jnp.sum((wide * wide).reshape(-1, 8, dim), axis=0)
        if which == 0:
            OD[layer, at(t, LANES), :] = total
        else:
            out = (OG, OU)[which - 1]
            for b in range(n):
                piece = total[hr * (b // (n // 2)) : hr * (b // (n // 2)) + hr, LANES * (b % (n // 2)) : LANES * (b % (n // 2)) + LANES]
                out[layer, :, pl.ds(pl.multiple_of(b * share + t * LANES, LANES), LANES)] = piece
        for way in range(2):
            for step in range(half):
                src = G.at[slot, 0, whole] if step > 0 else G.at[slot, 0, low]
                pltpu.make_async_copy(src, src, send_sem.at[slot, way, step]).wait()

    SQ[...] = jnp.zeros_like(SQ)

    end = 2 * tiles - 1

    def tile_step(k):
        wk = k + tiles
        slot = lax.rem(wk, 2)
        base = lax.rem(k, 2) * 3
        prev = 3 - base
        u0 = 3 * k
        p0 = u0 - 3
        going = k >= 1
        old_t = lax.rem(k - 1 + tiles, tiles)
        old_layer = jnp.where(k - 1 < tiles, 1, 0)

        @pl.when(k > 0)
        def _():
            fetched(wk)

        @pl.when(k < 2 * tiles - 1)
        def _():
            fetch(wk + 1)

        def when(cond):
            return pl.when(going & cond)

        def wide_part(src, unit, j):
            part = dot(AT[...], src[:, at(j, cols)]).astype(BF16)
            G[base + unit, :, at(j, hr), :] = part.reshape(n, dim // n, cols)

        gate, upper = (u0 + 1, base + 1), (u0 + 2, base + 2)
        old, old_gate, old_upper = (p0, prev), (p0 + 1, prev + 1), (p0 + 2, prev + 2)

        def halves(j):
            def some(i):
                @pl.when((k > 0) | (j > 0) | (i > 0))
                def _():
                    hidden(slot, j, i)

                @when((j == 0) & (i == 0))
                def _():
                    later(*old, 2)
                    later(*old_upper, 3)

                @pl.when((k == 0) & (j == 1) & (i == 0))
                def _():
                    third_low(*gate)

                @pl.when((k == 0) & (j == 1) & (i == 1))
                def _():
                    second_low(*upper)

            loop(blocks // 2, some)
            wide_part(DG, 1, j)

            @pl.when(j == 0)
            def _():
                begin_low(*gate)

            @pl.when(j == 1)
            def _():
                begin_high(*gate)

            @pl.when((j == 1) & (k == 0))
            def _():
                second_low(*gate)

            wide_part(DU, 2, j)

            @pl.when(j == 0)
            def _():
                begin_low(*upper)

            @pl.when(j == 1)
            def _():
                begin_high(*upper)

            @when(j == 1)
            def _():
                later(*old, 3)
                finish(*old_gate, 1, old_layer, old_t)
                finish(*old_upper, 2, old_layer, old_t)
                second_low(*gate)

            @pl.when((j == 1) & (k == 0))
            def _():
                third_low(*upper)

        loop(2, halves)

        def down_part(j):
            part = dot(DT[...], ACT[:, at(j, cols)])
            flipped = part.T.astype(BF16)
            for b in range(cols // LANES):
                G[base, j * (cols // LANES) + b] = flipped[b * LANES : (b + 1) * LANES]

            @pl.when(j == 0)
            def _():
                second_high(*gate)

        loop(2, down_part)

        @pl.when(k < end)
        def _():
            begin_low(u0, base)
            begin_high(u0, base)

        @when(k < end)
        def _():
            second_low(*upper)

        @pl.when(k == tiles - 1)
        def _():
            loop(blocks, lambda i: x_again(i).start())

        def ring_part(i):
            @pl.when(i == 0)
            def _():
                second_high(*upper)

            @pl.when((i == 0) & (k == 0))
            def _():
                second_low(u0, base)
                third_rest(*gate)

            @when(i == 2)
            def _():
                finish(*old, 0, old_layer, old_t)
                later(*gate, 2)

        @pl.when(k < tiles)
        def _():
            def input_part(i):
                so_far = jnp.where(k == 0, 0.0, DA[tok(i), :])
                DA[tok(i), :] = so_far + (dot_t(DG[tok(i), :], WG[slot]) + dot_t(DU[tok(i), :], WU[slot]))
                ring_part(i)

            loop(blocks, input_part)

        @pl.when((k >= tiles) & (k < end))
        def _():
            loop(blocks, ring_part)

        @pl.when(k == tiles - 1)
        def _():
            def between(i):
                h = H[tok(i), :].astype(F32)
                da = DA[tok(i), :].astype(BF16).astype(F32)
                r = scale_of(h)
                dh = (r * da - h * (r * r * r * jnp.mean(h * da, -1, keepdims=True))).astype(BF16)
                d = (D[tok(i), :].astype(F32) + dh.astype(F32)).astype(BF16)
                D[tok(i), :] = d
                DT[:, tok(i)] = d.T
                x_again(i).wait()
                wide = ACT[tok(i), pl.ds(0, dim)].astype(F32)
                a = (wide * scale_of(wide)).astype(BF16)
                A[tok(i), :] = a
                AT[:, tok(i)] = a.T

                @pl.when(i == 1)
                def _():
                    second_low(u0, base)
                    second_high(u0, base)

            loop(blocks, between)

        @when((k != tiles - 1) & (k < end))
        def _():
            second_low(u0, base)

        @pl.when((k != tiles - 1) & (k < end))
        def _():
            second_high(u0, base)

        @pl.when(k == 0)
        def _():
            third_rest(*upper)

        @when(k < end)
        def _():
            later(*upper, 2)

        @pl.when(k < end)
        def _():
            later(*gate, 3)

    loop(2 * tiles, tile_step)

    ahead = (
        pltpu.make_async_copy(wd_hbm.at[layers - 1, at(me, share), :], PW, ahead_sem.at[0]),
        pltpu.make_async_copy(md_hbm.at[layers - 1], PM, ahead_sem.at[1]),
        pltpu.make_async_copy(vd_hbm.at[layers - 1], PV, ahead_sem.at[2]),
    )
    for copy in ahead:
        copy.start()

    base = (end % 2) * 3
    down_unit, gate, upper = ((3 * end + j, base + j) for j in range(3))
    begin_high(*down_unit)
    second_high(*upper)
    begin_low(*down_unit)
    second_low(*upper)
    second_high(*down_unit)
    second_low(*down_unit)
    for step in range(2, half):
        for unit in (gate, upper, down_unit):
            later(*unit, step)
    finish(*gate, 1, 0, tiles - 1)
    finish(3 * (end - 1), 3 - base, 0, 0, tiles - 2)
    finish(*upper, 2, 0, tiles - 1)
    finish(*down_unit, 0, 0, tiles - 1)

    squares = SQ[:, :LANES]
    for j in range(1, dim // LANES):
        squares += SQ[:, j * LANES : (j + 1) * LANES]
    ALL[me] = squares

    def tell(d):
        return pltpu.make_async_remote_copy(
            src_ref=ALL.at[me],
            dst_ref=ALL.at[me],
            send_sem=sq_send.at[d],
            recv_sem=sq_recv.at[d],
            device_id={"dp": ring(d)},
            device_id_type=MESH,
        )

    for d in range(1, n):
        tell(d).start()
    for d in range(1, n):
        tell(d).wait()
    for copy in ahead:
        copy.wait()


def gradients(n, x, dy, w_gate, w_up, w_down, m_down, v_down):
    layers, dim, ff = w_gate.shape
    tokens = x.shape[1]
    blocks = 4
    share = ff // n
    tiles = share // LANES
    tile = n * LANES
    units = 3 * layers * tiles
    half = n // 2
    land = LANES // 2 + LANES * (half - 1)
    any_space = pl.BlockSpec(memory_space=pl.ANY)
    return pl.pallas_call(
        functools.partial(grad_kernel, n, layers, (tokens, dim, ff, blocks)),
        out_shape=tuple(
            kept(shape, dtype)
            for shape, dtype in (
                ((layers, dim // n, ff), BF16),
                ((layers, dim // n, ff), BF16),
                ((layers, share, dim), BF16),
                ((n, 8, LANES), F32),
                ((share, dim), BF16),
                ((share, dim), F32),
                ((share, dim), F32),
            )
        ),
        in_specs=[any_space] * 7,
        out_specs=(pl.BlockSpec(memory_space=pltpu.VMEM),) * 7,
        scratch_shapes=[
            pltpu.VMEM((tokens, dim), BF16),
            pltpu.VMEM((dim, tokens), BF16),
            pltpu.VMEM((tokens, dim), BF16),
            pltpu.VMEM((dim, tokens), BF16),
            pltpu.VMEM((tokens, dim), BF16),
            pltpu.VMEM((tokens, tile), BF16),
            pltpu.VMEM((tokens, tile), BF16),
            pltpu.VMEM((tokens, tile), BF16),
            pltpu.VMEM((tokens, dim), F32),
            pltpu.VMEM((2, dim, tile), BF16),
            pltpu.VMEM((2, dim, tile), BF16),
            pltpu.VMEM((2, tile, dim), BF16),
            pltpu.VMEM((6, n, LANES, dim), BF16),
            pltpu.VMEM((units, land, dim), BF16),
            pltpu.VMEM((units, land, dim), BF16),
            pltpu.VMEM((8, dim), F32),
            pltpu.SemaphoreType.DMA((blocks,)),
            pltpu.SemaphoreType.DMA((blocks,)),
            pltpu.SemaphoreType.DMA((2, 3)),
            pltpu.SemaphoreType.DMA((3,)),
            pltpu.SemaphoreType.DMA((6, 2, half)),
            pltpu.SemaphoreType.DMA((units, 2, half)),
            pltpu.SemaphoreType.DMA((units,)),
            pltpu.SemaphoreType.DMA((n,)),
            pltpu.SemaphoreType.DMA((n,)),
        ],
        compiler_params=pltpu.CompilerParams(collective_id=0, has_side_effects=True, vmem_limit_bytes=62_500_000),
        name="grads",
    )(*(pinned(t, pltpu.HBM) for t in (x, dy, w_gate, w_up, w_down, m_down, v_down)))


def turns(layers):
    return [(2, l) for l in reversed(range(layers))] + [(a, l) for l in reversed(range(layers)) for a in (0, 1)]


def update_kernel(n, count, parts, *refs):
    G, w_hbm, m_hbm, v_hbm = (refs[i : i + 3] for i in (0, 4, 10, 13))
    SQ, PW, PM, PV = refs[3], *refs[7:10]
    N, M, V = (refs[i : i + 3] for i in (16, 19, 22))
    last = refs[25:27]
    W = refs[27:30]
    in_sem, last_sem, send_sem, recv_sem = refs[30:]
    me = lax.axis_index("dp")
    half = n // 2
    up, down = lax.rem(me + 1, n), lax.rem(me + n - 1, n)
    ring = lambda d: lax.rem(me + d + n, n)
    layers = G[0].shape[0]

    barrier = pltpu.get_barrier_semaphore()
    for peer in (up, down):
        pl.semaphore_signal(barrier, inc=1, device_id={"dp": peer}, device_id_type=MESH)

    order = turns(layers)
    loads = {}
    for a, l in order[1:]:
        rows = G[a].shape[1]
        own = pl.ds(pl.multiple_of(me * rows, rows), rows)
        loads[a, l] = (
            pltpu.make_async_copy(w_hbm[a].at[l, own, :], W[a].at[l], in_sem.at[0, a, l]),
            pltpu.make_async_copy(m_hbm[a].at[l], M[a].at[l], in_sem.at[1, a, l]),
            pltpu.make_async_copy(v_hbm[a].at[l], V[a].at[l], in_sem.at[2, a, l]),
        )
    total = jnp.sum(jnp.sum(SQ[...], axis=0), axis=(0, 1), keepdims=True)
    factor = jnp.minimum(1.0, 0.5 * lax.rsqrt(total / count + 1e-30))

    def shape(a):
        rows, cols = G[a].shape[1:]
        return (rows, cols // parts, 0) if a < 2 else (rows // parts, cols, 1)

    def place(a, l, p, owner, part):
        rows = G[a].shape[1]
        r, c, split = shape(a)
        hr = r // 2
        start = owner * rows + (p * r if split else 0)
        start, size = (start, r) if part == 2 else (start + part * hr, hr)
        return (l, pl.ds(pl.multiple_of(start, hr), size), pl.ds(0 if split else p * c, c))

    def send(i, a, l, p, way, step):
        owner = ring(-step) if way == 0 else ring(step)
        ref = N[a].at[place(a, l, p, owner, 2 if step < half - 1 else way)]
        return pltpu.make_async_remote_copy(
            src_ref=ref,
            dst_ref=ref,
            send_sem=send_sem.at[i, way, step],
            recv_sem=recv_sem.at[i, way, step],
            device_id={"dp": (up, down)[way]},
            device_id_type=MESH,
        )

    def came(i, a, l, p, way, step):
        owner = ring(-step - 1) if way == 0 else ring(step + 1)
        where = place(a, l, p, owner, 2 if step < half - 1 else way)
        ref = N[a].at[where]
        pltpu.make_async_copy(ref, ref, recv_sem.at[i, way, step]).wait()

    def adam(a, l, p):
        r, c, split = shape(a)
        rows = G[a].shape[1]
        step = 32
        lane = pl.ds(0 if split else p * c, c)

        def some(i):
            row = pl.ds(pl.multiple_of((p * r if split else 0) + i * step, step), step)
            old = (PW[row, lane], PM[row, lane], PV[row, lane]) if (a, l) == order[0] else (W[a][l, row, lane], M[a][l, row, lane], V[a][l, row, lane])
            g = G[a][l, row, lane].astype(F32) * factor
            m = 0.9 * old[1] + 0.1 * g
            v = 0.95 * old[2] + 0.05 * g * g
            M[a][l, row, lane] = m
            V[a][l, row, lane] = v
            w = old[0].astype(F32)
            new = (w - 0.02 * (m * lax.rsqrt(v + 1e-8) + 0.1 * w)).astype(BF16)
            there = pl.ds(pl.multiple_of(me * rows + (p * r if split else 0) + i * step, step), step)
            N[a][l, there, lane] = new

        loop(r // step, some)

    chunks = []
    for a, l in order:
        for p in range(parts):
            chunks.append((len(chunks), a, l, p))
    for i, a, l, p in chunks:
        if p == 0:
            for copy in loads.get((a, l), ()):
                copy.wait()
        adam(a, l, p)
        if i == 0:
            pl.semaphore_wait(barrier, 2)
        send(i, a, l, p, 0, 0).start()
        send(i, a, l, p, 1, 0).start()
        if i == 0:
            for copies in loads.values():
                for copy in copies:
                    copy.start()
    late = order[len(order) - LATE :]

    def hops(a, l):
        return half - 1 if (a, l) in late else half

    def to_permute(a, l, way):
        rows = G[a].shape[1]
        owner = ring(1 - half) if way == 0 else ring(half - 1)
        src = N[a].at[l, pl.ds(pl.multiple_of(owner * rows + way * (rows // 2), rows // 2), rows // 2), :]
        return pltpu.make_async_copy(src, last[way].at[late.index((a, l))], last_sem.at[way, late.index((a, l))])

    for step in range(half):
        for i, a, l, p in chunks:
            for way in range(2):
                if step < hops(a, l):
                    came(i, a, l, p, way, step)
                if step < hops(a, l) - 1:
                    send(i, a, l, p, way, step + 1).start()
                elif step == half - 2 and p == parts - 1:
                    to_permute(a, l, way).start()
    for i, a, l, p in chunks:
        for way in range(2):
            for step in range(hops(a, l)):
                send(i, a, l, p, way, step).wait_send()
    for a, l in late:
        for way in range(2):
            to_permute(a, l, way).wait()


def store_kernel(count, *refs):
    src, dst, sem = refs[:count], refs[count : 2 * count], refs[-1]
    copies = [
        pltpu.make_async_copy(a.at[l], b.at[l], sem.at[i, l])
        for i, (a, b) in enumerate(zip(src, dst, strict=True))
        for l in range(a.shape[0])
    ]
    for copy in copies:
        copy.start()
    for copy in copies:
        copy.wait()


def store(arrays):
    count = len(arrays)
    return pl.pallas_call(
        functools.partial(store_kernel, count),
        out_shape=tuple(jax.ShapeDtypeStruct(t.shape, t.dtype) for t in arrays),
        in_specs=[pl.BlockSpec(memory_space=pltpu.VMEM)] * count,
        out_specs=(pl.BlockSpec(memory_space=pl.ANY),) * count,
        scratch_shapes=[pltpu.SemaphoreType.DMA((count, arrays[0].shape[0]))],
        compiler_params=pltpu.CompilerParams(vmem_limit_bytes=2**20),
        cost_estimate=pl.CostEstimate(flops=10_000_000_000, bytes_accessed=0, transcendentals=0),
        name="store",
    )(*(pinned(t, pltpu.VMEM) for t in arrays))


def place_kernel(n, count, *refs):
    up_ref, down_ref = refs[count : count + 2]
    outs, sem = refs[count + 2 : -1], refs[-1]
    opposite = lax.rem(lax.axis_index("dp") + n // 2, n)
    hr = up_ref.shape[1]
    copies = []
    for i, (a, l) in enumerate(turns(outs[0].shape[0])[-LATE:]):
        for way, src in enumerate((up_ref, down_ref)):
            there = pl.ds(pl.multiple_of(opposite * 2 * hr + way * hr, hr), hr)
            copies.append(pltpu.make_async_copy(src.at[i], outs[a].at[l, there, :], sem.at[i, way]))
    for copy in copies:
        copy.start()
    for copy in copies:
        copy.wait()


def place_last(n, arrays, came):
    count = len(arrays)
    any_space = pl.BlockSpec(memory_space=pl.ANY)
    in_vmem = pl.BlockSpec(memory_space=pltpu.VMEM)
    return pl.pallas_call(
        functools.partial(place_kernel, n, count),
        out_shape=tuple(jax.ShapeDtypeStruct(t.shape, t.dtype) for t in arrays),
        in_specs=[any_space] * count + [in_vmem] * 2,
        out_specs=(any_space,) * count,
        scratch_shapes=[pltpu.SemaphoreType.DMA((LATE, 2))],
        input_output_aliases={i: i for i in range(count)},
        compiler_params=pltpu.CompilerParams(vmem_limit_bytes=2**20),
        name="place",
    )(*(pinned(t, pltpu.HBM) for t in arrays), *came)


def update(n, made, w, m, v):
    layers = w[0].shape[0]
    parts = 2
    chunks = layers * 3 * parts
    count = sum(t.size for t in w)
    any_space = pl.BlockSpec(memory_space=pl.ANY)
    in_vmem = pl.BlockSpec(memory_space=pltpu.VMEM)
    half = n // 2
    g, squares, ahead = made[:3], made[3], made[4:]
    return pl.pallas_call(
        functools.partial(update_kernel, n, float(count), parts),
        out_shape=tuple(kept(t.shape, BF16) for t in w)
        + tuple(kept(t.shape, F32) for t in m + v)
        + (jax.ShapeDtypeStruct((LATE, m[0].shape[1] // 2, m[0].shape[2]), BF16),) * 2,
        in_specs=[in_vmem] * 4 + [any_space] * 3 + [in_vmem] * 3 + [any_space] * 6,
        out_specs=(in_vmem,) * 9 + (any_space,) * 2,
        scratch_shapes=[pltpu.VMEM(t.shape, BF16) for t in m]
        + [
            pltpu.SemaphoreType.DMA((3, 3, layers)),
            pltpu.SemaphoreType.DMA((2, LATE)),
            pltpu.SemaphoreType.DMA((chunks, 2, half)),
            pltpu.SemaphoreType.DMA((chunks, 2, half)),
        ],
        compiler_params=pltpu.CompilerParams(collective_id=1, has_side_effects=True, vmem_limit_bytes=12 * 2**20),
        name="update",
    )(
        *(pinned(t, pltpu.VMEM) for t in (*g, squares)),
        *(pinned(t, pltpu.HBM) for t in w),
        *(pinned(t, pltpu.VMEM) for t in ahead),
        *(pinned(t, pltpu.HBM) for t in (*m, *v)),
    )


def solution(mesh):
    n = mesh.shape["dp"]

    def step(x, dy, *arrays):
        w, m, v = (arrays[i : i + 3] for i in (0, 3, 6))
        *new, up, down = update(n, gradients(n, x, dy, *w, m[2], v[2]), w, m, v)
        came = tuple(lax.ppermute(t, "dp", [(i, (i + d) % n) for i in range(n)]) for t, d in ((up, 1), (down, -1)))
        out = store(new)
        return (*place_last(n, out[:2], came), *out[2:])

    shard = P(None, "dp", None)
    return jax.shard_map(
        step,
        mesh=mesh,
        in_specs=(P(("rep", "dp"), None, None),) * 2 + (P(),) * 3 + (shard,) * 6,
        out_specs=(P("rep", None, None),) * 3 + (P("rep", "dp", None),) * 6,
        check_vma=False,
    )
```

```python
import functools

import jax
import jax.numpy as jnp
from jax import lax
from jax.experimental import pallas as pl
from jax.experimental.pallas import tpu as pltpu
from jax.sharding import PartitionSpec as P

F32 = jnp.float32
BF16 = jnp.bfloat16
MESH = pl.DeviceIdType.MESH
LANES = 128
LATE = 4


def dot(a, b):
    return jnp.dot(a, b, preferred_element_type=F32)


def dot_t(a, b):
    return lax.dot_general(a, b, (((1,), (1,)), ((), ())), preferred_element_type=F32)


def scale_of(wide):
    return lax.rsqrt(jnp.mean(wide * wide, -1, keepdims=True) + 1e-6)


def pinned(t, space):
    return pltpu.with_memory_space_constraint(t, space)


def kept(shape, dtype):
    return pltpu.VMEM(shape, dtype)


def loop(count, body):
    lax.fori_loop(0, count, lambda i, c: (body(i), c)[1], 0)


def at(i, size):
    return pl.ds(pl.multiple_of(i * size, size), size)


def grad_kernel(n, layers, shapes, *refs):
    (x_hbm, dy_hbm, wg_hbm, wu_hbm, wd_hbm, md_hbm, vd_hbm) = refs[:7]
    (OG, OU, OD, ALL, PW, PM, PV) = refs[7:14]
    (A, AT, D, DT, H, ACT, DGU, DA, WG, WU, WD, G, RU, RD, SQ, *sems) = refs[14:]
    x_sem, dy_sem, w_sem, ahead_sem, send_sem, recv_sem, low_sem, sq_send, sq_recv = sems
    tokens, dim, ff, blocks = shapes
    share = ff // n
    tiles = share // LANES
    tile = n * LANES
    tb = tokens // blocks
    half = n // 2
    hr = LANES // 2
    cols = tile // 2
    me = lax.axis_index("dp")
    up, down = lax.rem(me + 1, n), lax.rem(me + n - 1, n)
    ring = lambda d: lax.rem(me + d + n, n)

    def tok(i):
        return at(i, tb)

    def fetch(k):
        slot = lax.rem(k, 2)
        layer = lax.rem(k // tiles, 2)
        t = lax.rem(k, tiles)

        def one(b):
            place = pl.ds(pl.multiple_of(b * share + t * LANES, LANES), LANES)
            here = at(b, LANES)
            pltpu.make_async_copy(wg_hbm.at[layer, :, place], WG.at[slot, :, here], w_sem.at[slot, 0]).start()
            pltpu.make_async_copy(wu_hbm.at[layer, :, place], WU.at[slot, :, here], w_sem.at[slot, 1]).start()
            pltpu.make_async_copy(wd_hbm.at[layer, place, :], WD.at[slot, here, :], w_sem.at[slot, 2]).start()

        loop(n, one)

    def fetched(k):
        slot = lax.rem(k, 2)
        pltpu.make_async_copy(WG.at[slot], WG.at[slot], w_sem.at[slot, 0]).wait()
        pltpu.make_async_copy(WU.at[slot], WU.at[slot], w_sem.at[slot, 1]).wait()
        pltpu.make_async_copy(WD.at[slot], WD.at[slot], w_sem.at[slot, 2]).wait()

    def x_copy(i):
        return pltpu.make_async_copy(x_hbm.at[0, tok(i), :], H.at[tok(i), :], x_sem.at[i])

    def x_again(i):
        return pltpu.make_async_copy(x_hbm.at[0, tok(i), :], ACT.at[tok(i), pl.ds(0, dim)], x_sem.at[i])

    def dy_copy(i):
        return pltpu.make_async_copy(dy_hbm.at[0, tok(i), :], D.at[tok(i), :], dy_sem.at[i])

    x_copy(0).start()
    fetch(0)
    x_copy(1).start()
    barrier = pltpu.get_barrier_semaphore()
    for d in range(1, n):
        pl.semaphore_signal(barrier, inc=1, device_id={"dp": ring(d)}, device_id_type=MESH)

    def first_norm(i):
        wide = H[tok(i), :].astype(F32)
        A[tok(i), :] = (wide * scale_of(wide)).astype(BF16)
        DA[tok(i), :] = jnp.zeros((tb, dim), F32)

    def forward(k, i, act=ACT):
        slot = lax.rem(k, 2)
        for j in range(4):
            here = pl.ds(j * (tile // 4), tile // 4)
            g = dot(A[tok(i), :], WG[slot, :, here])
            u = dot(A[tok(i), :], WU[slot, :, here])
            s = 0.5 * jnp.tanh(0.5 * g) + 0.5
            act[tok(i), here] = (g * s * u).astype(BF16)
        DA[tok(i), :] += dot(act[tok(i), :], WD[slot])

    def second_norm(i):
        h = (H[tok(i), :].astype(F32) + DA[tok(i), :].astype(BF16).astype(F32)).astype(BF16)
        wide = h.astype(F32)
        return h, (wide * scale_of(wide)).astype(BF16)

    def second_norm_kept(i, h, a):
        H[tok(i), :] = h
        A[tok(i), :] = a
        AT[:, tok(i)] = a.T

    x_copy(0).wait()
    first_norm(0)
    fetched(0)
    loop(blocks - 2, lambda i: x_copy(i + 2).start())
    fetch(1)
    loop(blocks, lambda i: dy_copy(i).start())

    def opening(i):
        x_copy(i + 1).wait()
        forward(0, i)
        first_norm(i + 1)

    loop(blocks - 1, opening)

    def middle(j):
        q = blocks - 1 + 2 * j

        @pl.when(lax.rem(q + 1, blocks) == 0)
        def _():
            fetched((q + 1) // blocks)

        @pl.when((lax.rem(q, blocks) == 1) & (q // blocks < tiles - 1))
        def _():
            fetch(q // blocks + 1)

        seen = [jnp.minimum(2 * j + d, blocks - 1) for d in range(2)]

        @pl.when(2 * j < blocks)
        def _():
            dy_copy(2 * j).wait()
            dy_copy(2 * j + 1).wait()

        forward(q // blocks, lax.rem(q, blocks))
        forward((q + 1) // blocks, lax.rem(q + 1, blocks), DGU.at[0])
        for i in seen:
            DT[:, tok(i)] = D[tok(i), :].T

    loop((tiles - 2) * blocks // 2 + 1, middle)
    fetch(tiles)

    def closing(i):
        normed = second_norm(i)
        forward(tiles - 1, i + 1)
        second_norm_kept(i, *normed)

    loop(blocks - 1, closing)

    def hidden(slot, j, i):
        place = at(i, 2 * tb)
        for c in range(2):
            here = at(2 * j + c, cols // 2)
            g = dot(A[place, :], WG[slot, :, here])
            u = dot(A[place, :], WU[slot, :, here])
            back = dot_t(D[place, :], WD[slot, here, :]).astype(BF16).astype(F32)
            s = 0.5 * jnp.tanh(0.5 * g) + 0.5
            silu = g * s
            ACT[place, here] = (silu * u).astype(BF16)
            DGU[1, place, here] = (back * silu).astype(BF16)
            DGU[0, place, here] = (back * u * (s + silu * (1.0 - s))).astype(BF16)

    second_norm_kept(blocks - 1, *second_norm(blocks - 1))

    pl.semaphore_wait(barrier, n - 1)

    def remote(src, dst, slot, u, way, step, arrival=None):
        return pltpu.make_async_remote_copy(
            src_ref=src,
            dst_ref=dst,
            send_sem=send_sem.at[slot, way, step],
            recv_sem=recv_sem.at[u, way, step] if arrival is None else arrival,
            device_id={"dp": (up, down)[way]},
            device_id_type=MESH,
        )

    low, high, whole = pl.ds(0, hr), pl.ds(hr, hr), pl.ds(0, 2 * hr)
    lands = (RU, RD)

    def rows(step):
        return pl.ds(hr + (step - 1) * 2 * hr, 2 * hr)

    def begin_low(u, slot):
        remote(G.at[slot, ring(half), low], RU.at[u, low], slot, u, 0, 0).start()
        remote(G.at[slot, ring(1 - half), low], RD.at[u, pl.ds(hr, hr)], slot, u, 1, 1, low_sem.at[u]).start()

    def begin_high(u, slot):
        remote(G.at[slot, ring(half), high], RD.at[u, low], slot, u, 1, 0).start()
        remote(G.at[slot, ring(half - 1), high], RU.at[u, pl.ds(2 * hr, hr)], slot, u, 0, 1).start()

    def arrived(land, sem):
        pltpu.make_async_copy(land, land, sem).wait()

    def received(u, way, step):
        if (way, step) == (1, 1):
            arrived(RD.at[u, pl.ds(hr, hr)], low_sem.at[u])
            arrived(RD.at[u, pl.ds(2 * hr, hr)], recv_sem.at[u, 1, 1])
        else:
            arrived(lands[way].at[u, rows(step) if step else low], recv_sem.at[u, way, step])

    def add(land, place, mine):
        land[place] = (land[place].astype(F32) + mine.astype(F32)).astype(BF16)

    def second_low(u, slot):
        received(u, 0, 0)
        add(RU, (u, low), G[slot, ring(half - 1), low])
        remote(RU.at[u, low], RU.at[u, pl.ds(hr, hr)], slot, u, 0, 1).start()

    def second_high(u, slot):
        received(u, 1, 0)
        add(RD, (u, low), G[slot, ring(1 - half), high])
        remote(RD.at[u, low], RD.at[u, pl.ds(2 * hr, hr)], slot, u, 1, 1).start()

    def pass_on(u, slot, way, step):
        received(u, way, step - 1)
        add(lands[way], (u, rows(step - 1)), G[slot, ring(half - step if way == 0 else step - half)])
        remote(lands[way].at[u, rows(step - 1)], lands[way].at[u, rows(step)], slot, u, way, step).start()

    def later(u, slot, step):
        pass_on(u, slot, 0, step)
        pass_on(u, slot, 1, step)

    def half_on(u, slot, part, sem):
        here, there = pl.ds((1 + part) * hr, hr), pl.ds((3 + part) * hr, hr)
        arrived(RD.at[u, here], sem)
        add(RD, (u, here), G[slot, ring(2 - half), (low, high)[part]])
        remote(RD.at[u, here], RD.at[u, there], slot, u, 1, 2).start()

    def third_low(u, slot):
        half_on(u, slot, 0, low_sem.at[u])

    def third_rest(u, slot):
        pass_on(u, slot, 0, 2)
        half_on(u, slot, 1, recv_sem.at[u, 1, 1])

    def finish(u, slot, which, layer, t):
        received(u, 0, half - 1)
        received(u, 1, half - 1)
        total = G[slot, me].astype(F32) + RU[u, rows(half - 1)].astype(F32) + RD[u, rows(half - 1)].astype(F32)
        total = total.astype(BF16)
        wide = total.astype(F32)
        SQ[...] += jnp.sum((wide * wide).reshape(-1, 8, dim), axis=0)
        if which == 0:
            OD[layer, at(t, LANES), :] = total
        else:
            out = (OG, OU)[which - 1]
            for b in range(n):
                piece = total[hr * (b // (n // 2)) : hr * (b // (n // 2)) + hr, LANES * (b % (n // 2)) : LANES * (b % (n // 2)) + LANES]
                out[layer, :, pl.ds(pl.multiple_of(b * share + t * LANES, LANES), LANES)] = piece
        for way in range(2):
            for step in range(half):
                src = G.at[slot, 0, whole] if step > 0 else G.at[slot, 0, low]
                pltpu.make_async_copy(src, src, send_sem.at[slot, way, step]).wait()

    SQ[...] = jnp.zeros_like(SQ)

    end = 2 * tiles - 1

    def tile_step(k):
        wk = k + tiles
        slot = lax.rem(wk, 2)
        base = lax.rem(k, 2) * 3
        prev = 3 - base
        u0 = 3 * k
        p0 = u0 - 3
        going = k >= 1
        old_t = lax.rem(k - 1 + tiles, tiles)
        old_layer = jnp.where(k - 1 < tiles, 1, 0)
        fetched(wk)

        @pl.when(k < 2 * tiles - 1)
        def _():
            fetch(wk + 1)

        def when(cond):
            return pl.when(going & cond)

        gate, upper = (u0 + 1, base + 1), (u0 + 2, base + 2)
        old, old_gate, old_upper = (p0, prev), (p0 + 1, prev + 1), (p0 + 2, prev + 2)

        def halves(j):
            def some(i):
                hidden(slot, j, i)

                @when((j == 0) & (i == 0))
                def _():
                    later(*old, 2)
                    later(*old_upper, 3)

                @pl.when((k == 0) & (j == 1) & (i == 0))
                def _():
                    third_low(*gate)

                @pl.when((k == 0) & (j == 1) & (i == 1))
                def _():
                    second_low(*upper)

            loop(blocks // 2, some)

            def wide_part(c):
                unit = (u0 + 1 + c, base + 1 + c)
                part = dot(AT[...], DGU[c, :, at(j, cols)]).astype(BF16)
                G[unit[1], :, at(j, hr), :] = part.reshape(n, dim // n, cols)

                @pl.when(j == 0)
                def _():
                    begin_low(*unit)

                @pl.when(j == 1)
                def _():
                    begin_high(*unit)

                @pl.when((j == 1) & (k == 0) & (c == 0))
                def _():
                    second_low(*gate)

                @when((j == 1) & (c == 1))
                def _():
                    later(*old, 3)
                    finish(*old_gate, 1, old_layer, old_t)
                    finish(*old_upper, 2, old_layer, old_t)
                    second_low(*gate)

                @pl.when((j == 1) & (k == 0) & (c == 1))
                def _():
                    third_low(*upper)

            loop(2, wide_part)

        loop(2, halves)

        def down_part(j):
            part = dot(DT[...], ACT[:, at(j, cols)])
            flipped = part.T.astype(BF16)
            for b in range(cols // LANES):
                G[base, j * (cols // LANES) + b] = flipped[b * LANES : (b + 1) * LANES]

            @pl.when(j == 0)
            def _():
                second_high(*gate)

        loop(2, down_part)

        @pl.when(k < end)
        def _():
            begin_low(u0, base)
            begin_high(u0, base)

        @when(k < end)
        def _():
            second_low(*upper)

        @pl.when(k == tiles - 1)
        def _():
            loop(blocks, lambda i: x_again(i).start())

        def ring_part(i):
            @pl.when(i == 0)
            def _():
                second_high(*upper)

            @pl.when((i == 0) & (k == 0))
            def _():
                second_low(u0, base)
                third_rest(*gate)

            @when(i == 2)
            def _():
                finish(*old, 0, old_layer, old_t)
                later(*gate, 2)

        @pl.when(k < tiles)
        def _():
            def input_part(i):
                so_far = jnp.where(k == 0, 0.0, DA[tok(i), :])
                DA[tok(i), :] = so_far + (dot_t(DGU[0, tok(i), :], WG[slot]) + dot_t(DGU[1, tok(i), :], WU[slot]))
                ring_part(i)

            loop(blocks, input_part)

        @pl.when((k >= tiles) & (k < end))
        def _():
            loop(blocks, ring_part)

        @pl.when(k == tiles - 1)
        def _():
            def between(i):
                h = H[tok(i), :].astype(F32)
                da = DA[tok(i), :].astype(BF16).astype(F32)
                r = scale_of(h)
                dh = (r * da - h * (r * r * r * jnp.mean(h * da, -1, keepdims=True))).astype(BF16)
                d = (D[tok(i), :].astype(F32) + dh.astype(F32)).astype(BF16)
                D[tok(i), :] = d
                DT[:, tok(i)] = d.T
                x_again(i).wait()
                wide = ACT[tok(i), pl.ds(0, dim)].astype(F32)
                a = (wide * scale_of(wide)).astype(BF16)
                A[tok(i), :] = a
                AT[:, tok(i)] = a.T

                @pl.when(i == 1)
                def _():
                    second_low(u0, base)
                    second_high(u0, base)

            loop(blocks, between)

        @when((k != tiles - 1) & (k < end))
        def _():
            second_low(u0, base)

        @pl.when((k != tiles - 1) & (k < end))
        def _():
            second_high(u0, base)

        @pl.when(k == 0)
        def _():
            third_rest(*upper)

        @when(k < end)
        def _():
            later(*upper, 2)

        @pl.when(k < end)
        def _():
            later(*gate, 3)

    loop(2 * tiles, tile_step)

    ahead = (
        pltpu.make_async_copy(wd_hbm.at[layers - 1, at(me, share), :], PW, ahead_sem.at[0]),
        pltpu.make_async_copy(md_hbm.at[layers - 1], PM, ahead_sem.at[1]),
        pltpu.make_async_copy(vd_hbm.at[layers - 1], PV, ahead_sem.at[2]),
    )
    for copy in ahead:
        copy.start()

    base = (end % 2) * 3
    down_unit, gate, upper = ((3 * end + j, base + j) for j in range(3))
    begin_high(*down_unit)
    second_high(*upper)
    begin_low(*down_unit)
    second_low(*upper)
    second_high(*down_unit)
    second_low(*down_unit)
    for step in range(2, half):
        for unit in (gate, upper, down_unit):
            later(*unit, step)
    finish(*gate, 1, 0, tiles - 1)
    finish(3 * (end - 1), 3 - base, 0, 0, tiles - 2)
    finish(*upper, 2, 0, tiles - 1)
    finish(*down_unit, 0, 0, tiles - 1)

    squares = SQ[:, :LANES]
    for j in range(1, dim // LANES):
        squares += SQ[:, j * LANES : (j + 1) * LANES]
    ALL[me] = squares

    def tell(d):
        return pltpu.make_async_remote_copy(
            src_ref=ALL.at[me],
            dst_ref=ALL.at[me],
            send_sem=sq_send.at[d],
            recv_sem=sq_recv.at[d],
            device_id={"dp": ring(d)},
            device_id_type=MESH,
        )

    for d in range(1, n):
        tell(d).start()
    for d in range(1, n):
        tell(d).wait()
    for copy in ahead:
        copy.wait()


def gradients(n, x, dy, w_gate, w_up, w_down, m_down, v_down):
    layers, dim, ff = w_gate.shape
    tokens = x.shape[1]
    blocks = 4
    share = ff // n
    tiles = share // LANES
    tile = n * LANES
    units = 3 * layers * tiles
    half = n // 2
    land = LANES // 2 + LANES * (half - 1)
    any_space = pl.BlockSpec(memory_space=pl.ANY)
    return pl.pallas_call(
        functools.partial(grad_kernel, n, layers, (tokens, dim, ff, blocks)),
        out_shape=tuple(
            kept(shape, dtype)
            for shape, dtype in (
                ((layers, dim // n, ff), BF16),
                ((layers, dim // n, ff), BF16),
                ((layers, share, dim), BF16),
                ((n, 8, LANES), F32),
                ((share, dim), BF16),
                ((share, dim), F32),
                ((share, dim), F32),
            )
        ),
        in_specs=[any_space] * 7,
        out_specs=(pl.BlockSpec(memory_space=pltpu.VMEM),) * 7,
        scratch_shapes=[
            pltpu.VMEM((tokens, dim), BF16),
            pltpu.VMEM((dim, tokens), BF16),
            pltpu.VMEM((tokens, dim), BF16),
            pltpu.VMEM((dim, tokens), BF16),
            pltpu.VMEM((tokens, dim), BF16),
            pltpu.VMEM((tokens, tile), BF16),
            pltpu.VMEM((2, tokens, tile), BF16),
            pltpu.VMEM((tokens, dim), F32),
            pltpu.VMEM((2, dim, tile), BF16),
            pltpu.VMEM((2, dim, tile), BF16),
            pltpu.VMEM((2, tile, dim), BF16),
            pltpu.VMEM((6, n, LANES, dim), BF16),
            pltpu.VMEM((units, land, dim), BF16),
            pltpu.VMEM((units, land, dim), BF16),
            pltpu.VMEM((8, dim), F32),
            pltpu.SemaphoreType.DMA((blocks,)),
            pltpu.SemaphoreType.DMA((blocks,)),
            pltpu.SemaphoreType.DMA((2, 3)),
            pltpu.SemaphoreType.DMA((3,)),
            pltpu.SemaphoreType.DMA((6, 2, half)),
            pltpu.SemaphoreType.DMA((units, 2, half)),
            pltpu.SemaphoreType.DMA((units,)),
            pltpu.SemaphoreType.DMA((n,)),
            pltpu.SemaphoreType.DMA((n,)),
        ],
        compiler_params=pltpu.CompilerParams(collective_id=0, has_side_effects=True, vmem_limit_bytes=62_500_000),
        name="grads",
    )(*(pinned(t, pltpu.HBM) for t in (x, dy, w_gate, w_up, w_down, m_down, v_down)))


def turns(layers):
    return [(2, l) for l in reversed(range(layers))] + [(a, l) for l in reversed(range(layers)) for a in (0, 1)]


def update_kernel(n, count, parts, *refs):
    G, w_hbm, m_hbm, v_hbm = (refs[i : i + 3] for i in (0, 4, 10, 13))
    SQ, PW, PM, PV = refs[3], *refs[7:10]
    N, M, V = (refs[i : i + 3] for i in (16, 19, 22))
    last = refs[25:27]
    W = refs[27:30]
    in_sem, last_sem, send_sem, recv_sem = refs[30:]
    me = lax.axis_index("dp")
    half = n // 2
    up, down = lax.rem(me + 1, n), lax.rem(me + n - 1, n)
    ring = lambda d: lax.rem(me + d + n, n)
    layers = G[0].shape[0]

    barrier = pltpu.get_barrier_semaphore()
    for peer in (up, down):
        pl.semaphore_signal(barrier, inc=1, device_id={"dp": peer}, device_id_type=MESH)

    order = turns(layers)
    loads = {}
    for a, l in order[1:]:
        rows = G[a].shape[1]
        own = pl.ds(pl.multiple_of(me * rows, rows), rows)
        loads[a, l] = (
            pltpu.make_async_copy(w_hbm[a].at[l, own, :], W[a].at[l], in_sem.at[0, a, l]),
            pltpu.make_async_copy(m_hbm[a].at[l], M[a].at[l], in_sem.at[1, a, l]),
            pltpu.make_async_copy(v_hbm[a].at[l], V[a].at[l], in_sem.at[2, a, l]),
        )
    total = jnp.sum(jnp.sum(SQ[...], axis=0), axis=(0, 1), keepdims=True)
    factor = jnp.minimum(1.0, 0.5 * lax.rsqrt(total / count + 1e-30))

    def shape(a):
        rows, cols = G[a].shape[1:]
        return (rows, cols // parts, 0) if a < 2 else (rows // parts, cols, 1)

    def place(a, l, p, owner, part):
        rows = G[a].shape[1]
        r, c, split = shape(a)
        hr = r // 2
        start = owner * rows + (p * r if split else 0)
        start, size = (start, r) if part == 2 else (start + part * hr, hr)
        return (l, pl.ds(pl.multiple_of(start, hr), size), pl.ds(0 if split else p * c, c))

    def send(i, a, l, p, way, step):
        owner = ring(-step) if way == 0 else ring(step)
        ref = N[a].at[place(a, l, p, owner, 2 if step < half - 1 else way)]
        return pltpu.make_async_remote_copy(
            src_ref=ref,
            dst_ref=ref,
            send_sem=send_sem.at[i, way, step],
            recv_sem=recv_sem.at[i, way, step],
            device_id={"dp": (up, down)[way]},
            device_id_type=MESH,
        )

    def came(i, a, l, p, way, step):
        owner = ring(-step - 1) if way == 0 else ring(step + 1)
        where = place(a, l, p, owner, 2 if step < half - 1 else way)
        ref = N[a].at[where]
        pltpu.make_async_copy(ref, ref, recv_sem.at[i, way, step]).wait()

    def adam(a, l, p):
        r, c, split = shape(a)
        rows = G[a].shape[1]
        step = 32
        lane = pl.ds(0 if split else p * c, c)

        def some(i):
            row = pl.ds(pl.multiple_of((p * r if split else 0) + i * step, step), step)
            old = (PW[row, lane], PM[row, lane], PV[row, lane]) if (a, l) == order[0] else (W[a][l, row, lane], M[a][l, row, lane], V[a][l, row, lane])
            g = G[a][l, row, lane].astype(F32) * factor
            m = 0.9 * old[1] + 0.1 * g
            v = 0.95 * old[2] + 0.05 * g * g
            M[a][l, row, lane] = m
            V[a][l, row, lane] = v
            w = old[0].astype(F32)
            new = (w - 0.02 * (m * lax.rsqrt(v + 1e-8) + 0.1 * w)).astype(BF16)
            there = pl.ds(pl.multiple_of(me * rows + (p * r if split else 0) + i * step, step), step)
            N[a][l, there, lane] = new

        loop(r // step, some)

    chunks = []
    for a, l in order:
        for p in range(parts):
            chunks.append((len(chunks), a, l, p))
    for i, a, l, p in chunks:
        if p == 0:
            for copy in loads.get((a, l), ()):
                copy.wait()
        adam(a, l, p)
        if i == 0:
            pl.semaphore_wait(barrier, 2)
        send(i, a, l, p, 0, 0).start()
        send(i, a, l, p, 1, 0).start()
        if i == 0:
            for copies in loads.values():
                for copy in copies:
                    copy.start()
    late = order[len(order) - LATE :]

    def hops(a, l):
        return half - 1 if (a, l) in late else half

    def to_permute(a, l, way):
        rows = G[a].shape[1]
        owner = ring(1 - half) if way == 0 else ring(half - 1)
        src = N[a].at[l, pl.ds(pl.multiple_of(owner * rows + way * (rows // 2), rows // 2), rows // 2), :]
        return pltpu.make_async_copy(src, last[way].at[late.index((a, l))], last_sem.at[way, late.index((a, l))])

    for step in range(half):
        for i, a, l, p in chunks:
            for way in range(2):
                if step < hops(a, l):
                    came(i, a, l, p, way, step)
                if step < hops(a, l) - 1:
                    send(i, a, l, p, way, step + 1).start()
                elif step == half - 2 and p == parts - 1:
                    to_permute(a, l, way).start()
    for i, a, l, p in chunks:
        for way in range(2):
            for step in range(hops(a, l)):
                send(i, a, l, p, way, step).wait_send()
    for a, l in late:
        for way in range(2):
            to_permute(a, l, way).wait()


def store_kernel(count, *refs):
    src, dst, sem = refs[:count], refs[count : 2 * count], refs[-1]
    copies = [
        pltpu.make_async_copy(a.at[l], b.at[l], sem.at[i, l])
        for i, (a, b) in enumerate(zip(src, dst, strict=True))
        for l in range(a.shape[0])
    ]
    for copy in copies:
        copy.start()
    for copy in copies:
        copy.wait()


def store(arrays):
    count = len(arrays)
    return pl.pallas_call(
        functools.partial(store_kernel, count),
        out_shape=tuple(jax.ShapeDtypeStruct(t.shape, t.dtype) for t in arrays),
        in_specs=[pl.BlockSpec(memory_space=pltpu.VMEM)] * count,
        out_specs=(pl.BlockSpec(memory_space=pl.ANY),) * count,
        scratch_shapes=[pltpu.SemaphoreType.DMA((count, arrays[0].shape[0]))],
        compiler_params=pltpu.CompilerParams(vmem_limit_bytes=2**20),
        cost_estimate=pl.CostEstimate(flops=10_000_000_000, bytes_accessed=0, transcendentals=0),
        name="store",
    )(*(pinned(t, pltpu.VMEM) for t in arrays))


def place_kernel(n, count, *refs):
    up_ref, down_ref = refs[count : count + 2]
    outs, sem = refs[count + 2 : -1], refs[-1]
    opposite = lax.rem(lax.axis_index("dp") + n // 2, n)
    hr = up_ref.shape[1]
    copies = []
    for i, (a, l) in enumerate(turns(outs[0].shape[0])[-LATE:]):
        for way, src in enumerate((up_ref, down_ref)):
            there = pl.ds(pl.multiple_of(opposite * 2 * hr + way * hr, hr), hr)
            copies.append(pltpu.make_async_copy(src.at[i], outs[a].at[l, there, :], sem.at[i, way]))
    for copy in copies:
        copy.start()
    for copy in copies:
        copy.wait()


def place_last(n, arrays, came):
    count = len(arrays)
    any_space = pl.BlockSpec(memory_space=pl.ANY)
    in_vmem = pl.BlockSpec(memory_space=pltpu.VMEM)
    return pl.pallas_call(
        functools.partial(place_kernel, n, count),
        out_shape=tuple(jax.ShapeDtypeStruct(t.shape, t.dtype) for t in arrays),
        in_specs=[any_space] * count + [in_vmem] * 2,
        out_specs=(any_space,) * count,
        scratch_shapes=[pltpu.SemaphoreType.DMA((LATE, 2))],
        input_output_aliases={i: i for i in range(count)},
        compiler_params=pltpu.CompilerParams(vmem_limit_bytes=2**20),
        name="place",
    )(*(pinned(t, pltpu.HBM) for t in arrays), *came)


def update(n, made, w, m, v):
    layers = w[0].shape[0]
    parts = 2
    chunks = layers * 3 * parts
    count = sum(t.size for t in w)
    any_space = pl.BlockSpec(memory_space=pl.ANY)
    in_vmem = pl.BlockSpec(memory_space=pltpu.VMEM)
    half = n // 2
    g, squares, ahead = made[:3], made[3], made[4:]
    return pl.pallas_call(
        functools.partial(update_kernel, n, float(count), parts),
        out_shape=tuple(kept(t.shape, BF16) for t in w)
        + tuple(kept(t.shape, F32) for t in m + v)
        + (jax.ShapeDtypeStruct((LATE, m[0].shape[1] // 2, m[0].shape[2]), BF16),) * 2,
        in_specs=[in_vmem] * 4 + [any_space] * 3 + [in_vmem] * 3 + [any_space] * 6,
        out_specs=(in_vmem,) * 9 + (any_space,) * 2,
        scratch_shapes=[pltpu.VMEM(t.shape, BF16) for t in m]
        + [
            pltpu.SemaphoreType.DMA((3, 3, layers)),
            pltpu.SemaphoreType.DMA((2, LATE)),
            pltpu.SemaphoreType.DMA((chunks, 2, half)),
            pltpu.SemaphoreType.DMA((chunks, 2, half)),
        ],
        compiler_params=pltpu.CompilerParams(collective_id=1, has_side_effects=True, vmem_limit_bytes=12 * 2**20),
        name="update",
    )(
        *(pinned(t, pltpu.VMEM) for t in (*g, squares)),
        *(pinned(t, pltpu.HBM) for t in w),
        *(pinned(t, pltpu.VMEM) for t in ahead),
        *(pinned(t, pltpu.HBM) for t in (*m, *v)),
    )


def solution(mesh):
    n = mesh.shape["dp"]

    def step(x, dy, *arrays):
        w, m, v = (arrays[i : i + 3] for i in (0, 3, 6))
        *new, up, down = update(n, gradients(n, x, dy, *w, m[2], v[2]), w, m, v)
        came = tuple(lax.ppermute(t, "dp", [(i, (i + d) % n) for i in range(n)]) for t, d in ((up, 1), (down, -1)))
        out = store(new)
        return (*place_last(n, out[:2], came), *out[2:])

    shard = P(None, "dp", None)
    return jax.shard_map(
        step,
        mesh=mesh,
        in_specs=(P(("rep", "dp"), None, None),) * 2 + (P(),) * 3 + (shard,) * 6,
        out_specs=(P("rep", None, None),) * 3 + (P("rep", "dp", None),) * 6,
        check_vma=False,
    )
```

```python
import functools

import jax
import jax.numpy as jnp
from jax import lax
from jax.experimental import pallas as pl
from jax.experimental.pallas import tpu as pltpu
from jax.sharding import PartitionSpec as P

F32 = jnp.float32
BF16 = jnp.bfloat16
MESH = pl.DeviceIdType.MESH
LANES = 128
LATE = 4


def dot(a, b):
    return jnp.dot(a, b, preferred_element_type=F32)


def dot_t(a, b):
    return lax.dot_general(a, b, (((1,), (1,)), ((), ())), preferred_element_type=F32)


def scale_of(wide):
    return lax.rsqrt(jnp.mean(wide * wide, -1, keepdims=True) + 1e-6)


def pinned(t, space):
    return pltpu.with_memory_space_constraint(t, space)


def kept(shape, dtype):
    return pltpu.VMEM(shape, dtype)


def loop(count, body):
    lax.fori_loop(0, count, lambda i, c: (body(i), c)[1], 0)


def at(i, size):
    return pl.ds(pl.multiple_of(i * size, size), size)


def grad_kernel(n, layers, shapes, *refs):
    (x_hbm, dy_hbm, wg_hbm, wu_hbm, wd_hbm, md_hbm, vd_hbm) = refs[:7]
    (OG, OU, OD, ALL, PW, PM, PV) = refs[7:14]
    (A, AT, D, DT, H, ACT, DGU, DA, WG, WU, WD, G, RU, RD, SQ, *sems) = refs[14:]
    x_sem, dy_sem, w_sem, ahead_sem, send_sem, recv_sem, low_sem, sq_send, sq_recv = sems
    tokens, dim, ff, blocks = shapes
    share = ff // n
    tiles = share // LANES
    tile = n * LANES
    tb = tokens // blocks
    half = n // 2
    hr = LANES // 2
    cols = tile // 2
    me = lax.axis_index("dp")
    up, down = lax.rem(me + 1, n), lax.rem(me + n - 1, n)
    ring = lambda d: lax.rem(me + d + n, n)

    def tok(i):
        return at(i, tb)

    def fetch(k):
        slot = lax.rem(k, 2)
        layer = lax.rem(k // tiles, 2)
        t = lax.rem(k, tiles)

        def one(b):
            place = pl.ds(pl.multiple_of(b * share + t * LANES, LANES), LANES)
            here = at(b, LANES)
            pltpu.make_async_copy(wg_hbm.at[layer, :, place], WG.at[slot, :, here], w_sem.at[slot, 0]).start()
            pltpu.make_async_copy(wu_hbm.at[layer, :, place], WU.at[slot, :, here], w_sem.at[slot, 1]).start()
            pltpu.make_async_copy(wd_hbm.at[layer, place, :], WD.at[slot, here, :], w_sem.at[slot, 2]).start()

        loop(n, one)

    def fetched(k):
        slot = lax.rem(k, 2)
        pltpu.make_async_copy(WG.at[slot], WG.at[slot], w_sem.at[slot, 0]).wait()
        pltpu.make_async_copy(WU.at[slot], WU.at[slot], w_sem.at[slot, 1]).wait()
        pltpu.make_async_copy(WD.at[slot], WD.at[slot], w_sem.at[slot, 2]).wait()

    def x_copy(i):
        return pltpu.make_async_copy(x_hbm.at[0, tok(i), :], H.at[tok(i), :], x_sem.at[i])

    def x_again(i):
        return pltpu.make_async_copy(x_hbm.at[0, tok(i), :], ACT.at[tok(i), pl.ds(0, dim)], x_sem.at[i])

    def dy_copy(i):
        return pltpu.make_async_copy(dy_hbm.at[0, tok(i), :], D.at[tok(i), :], dy_sem.at[i])

    x_copy(0).start()
    fetch(0)
    x_copy(1).start()
    barrier = pltpu.get_barrier_semaphore()
    for d in range(1, n):
        pl.semaphore_signal(barrier, inc=1, device_id={"dp": ring(d)}, device_id_type=MESH)

    def first_norm(i):
        wide = H[tok(i), :].astype(F32)
        A[tok(i), :] = (wide * scale_of(wide)).astype(BF16)
        DA[tok(i), :] = jnp.zeros((tb, dim), F32)

    def forward(k, i, act=ACT):
        slot = lax.rem(k, 2)
        for j in range(4):
            here = pl.ds(j * (tile // 4), tile // 4)
            g = dot(A[tok(i), :], WG[slot, :, here])
            u = dot(A[tok(i), :], WU[slot, :, here])
            s = 0.5 * jnp.tanh(0.5 * g) + 0.5
            act[tok(i), here] = (g * s * u).astype(BF16)
        DA[tok(i), :] += dot(act[tok(i), :], WD[slot])

    def second_norm(i):
        h = (H[tok(i), :].astype(F32) + DA[tok(i), :].astype(BF16).astype(F32)).astype(BF16)
        wide = h.astype(F32)
        return h, (wide * scale_of(wide)).astype(BF16)

    def second_norm_kept(i, h, a):
        H[tok(i), :] = h
        A[tok(i), :] = a
        AT[:, tok(i)] = a.T

    x_copy(0).wait()
    first_norm(0)
    fetched(0)
    loop(blocks - 2, lambda i: x_copy(i + 2).start())
    fetch(1)
    loop(blocks, lambda i: dy_copy(i).start())

    def opening(i):
        x_copy(i + 1).wait()
        forward(0, i)
        first_norm(i + 1)

    loop(blocks - 1, opening)

    def middle(j):
        q = blocks - 1 + 2 * j

        @pl.when(lax.rem(q + 1, blocks) == 0)
        def _():
            fetched((q + 1) // blocks)

        @pl.when((lax.rem(q, blocks) == 1) & (q // blocks < tiles - 1))
        def _():
            fetch(q // blocks + 1)

        seen = [jnp.minimum(2 * j + d, blocks - 1) for d in range(2)]

        @pl.when(2 * j < blocks)
        def _():
            dy_copy(2 * j).wait()
            dy_copy(2 * j + 1).wait()

        forward(q // blocks, lax.rem(q, blocks))
        forward((q + 1) // blocks, lax.rem(q + 1, blocks), DGU.at[0])
        for i in seen:
            DT[:, tok(i)] = D[tok(i), :].T

    loop((tiles - 2) * blocks // 2 + 1, middle)
    fetch(tiles)

    def closing(i):
        normed = second_norm(i)
        forward(tiles - 1, i + 1)
        second_norm_kept(i, *normed)

    loop(blocks - 1, closing)

    def hidden(slot, j, i):
        place = at(i, 2 * tb)
        for c in range(2):
            here = at(2 * j + c, cols // 2)
            g = dot(A[place, :], WG[slot, :, here])
            u = dot(A[place, :], WU[slot, :, here])
            back = dot_t(D[place, :], WD[slot, here, :]).astype(BF16).astype(F32)
            s = 0.5 * jnp.tanh(0.5 * g) + 0.5
            silu = g * s
            ACT[place, here] = (silu * u).astype(BF16)
            DGU[1, place, here] = (back * silu).astype(BF16)
            DGU[0, place, here] = (back * u * (s + silu * (1.0 - s))).astype(BF16)

    second_norm_kept(blocks - 1, *second_norm(blocks - 1))

    pl.semaphore_wait(barrier, n - 1)

    def remote(src, dst, slot, u, way, step, arrival=None):
        return pltpu.make_async_remote_copy(
            src_ref=src,
            dst_ref=dst,
            send_sem=send_sem.at[slot, way, step],
            recv_sem=recv_sem.at[u, way, step] if arrival is None else arrival,
            device_id={"dp": (up, down)[way]},
            device_id_type=MESH,
        )

    low, high, whole = pl.ds(0, hr), pl.ds(hr, hr), pl.ds(0, 2 * hr)
    lands = (RU, RD)

    def rows(step):
        return pl.ds(hr + (step - 1) * 2 * hr, 2 * hr)

    def begin_low(u, slot):
        remote(G.at[slot, ring(half), low], RU.at[u, low], slot, u, 0, 0).start()
        remote(G.at[slot, ring(1 - half), low], RD.at[u, pl.ds(hr, hr)], slot, u, 1, 1, low_sem.at[u]).start()

    def begin_high(u, slot):
        remote(G.at[slot, ring(half), high], RD.at[u, low], slot, u, 1, 0).start()
        remote(G.at[slot, ring(half - 1), high], RU.at[u, pl.ds(2 * hr, hr)], slot, u, 0, 1).start()

    def arrived(land, sem):
        pltpu.make_async_copy(land, land, sem).wait()

    def received(u, way, step):
        if (way, step) == (1, 1):
            arrived(RD.at[u, pl.ds(hr, hr)], low_sem.at[u])
            arrived(RD.at[u, pl.ds(2 * hr, hr)], recv_sem.at[u, 1, 1])
        else:
            arrived(lands[way].at[u, rows(step) if step else low], recv_sem.at[u, way, step])

    def add(land, place, mine):
        land[place] = (land[place].astype(F32) + mine.astype(F32)).astype(BF16)

    def second_low(u, slot):
        received(u, 0, 0)
        add(RU, (u, low), G[slot, ring(half - 1), low])
        remote(RU.at[u, low], RU.at[u, pl.ds(hr, hr)], slot, u, 0, 1).start()

    def second_high(u, slot):
        received(u, 1, 0)
        add(RD, (u, low), G[slot, ring(1 - half), high])
        remote(RD.at[u, low], RD.at[u, pl.ds(2 * hr, hr)], slot, u, 1, 1).start()

    def pass_on(u, slot, way, step):
        received(u, way, step - 1)
        add(lands[way], (u, rows(step - 1)), G[slot, ring(half - step if way == 0 else step - half)])
        remote(lands[way].at[u, rows(step - 1)], lands[way].at[u, rows(step)], slot, u, way, step).start()

    def later(u, slot, step):
        pass_on(u, slot, 0, step)
        pass_on(u, slot, 1, step)

    def half_on(u, slot, part, sem):
        here, there = pl.ds((1 + part) * hr, hr), pl.ds((3 + part) * hr, hr)
        arrived(RD.at[u, here], sem)
        add(RD, (u, here), G[slot, ring(2 - half), (low, high)[part]])
        remote(RD.at[u, here], RD.at[u, there], slot, u, 1, 2).start()

    def third_low(u, slot):
        half_on(u, slot, 0, low_sem.at[u])

    def third_rest(u, slot):
        pass_on(u, slot, 0, 2)
        half_on(u, slot, 1, recv_sem.at[u, 1, 1])

    def finish(u, slot, which, layer, t):
        received(u, 0, half - 1)
        received(u, 1, half - 1)
        total = G[slot, me].astype(F32) + RU[u, rows(half - 1)].astype(F32) + RD[u, rows(half - 1)].astype(F32)
        total = total.astype(BF16)
        wide = total.astype(F32)
        SQ[...] += jnp.sum((wide * wide).reshape(-1, 8, dim), axis=0)
        if which == 0:
            OD[layer, at(t, LANES), :] = total
        else:
            out = (OG, OU)[which - 1]
            for b in range(n):
                piece = total[hr * (b // (n // 2)) : hr * (b // (n // 2)) + hr, LANES * (b % (n // 2)) : LANES * (b % (n // 2)) + LANES]
                out[layer, :, pl.ds(pl.multiple_of(b * share + t * LANES, LANES), LANES)] = piece
        for way in range(2):
            for step in range(half):
                src = G.at[slot, 0, whole] if step > 0 else G.at[slot, 0, low]
                pltpu.make_async_copy(src, src, send_sem.at[slot, way, step]).wait()

    SQ[...] = jnp.zeros_like(SQ)

    end = 2 * tiles - 1

    def tile_step(k):
        wk = k + tiles
        slot = lax.rem(wk, 2)
        base = lax.rem(k, 2) * 3
        prev = 3 - base
        u0 = 3 * k
        p0 = u0 - 3
        going = k >= 1
        old_t = lax.rem(k - 1 + tiles, tiles)
        old_layer = jnp.where(k - 1 < tiles, 1, 0)
        fetched(wk)

        @pl.when(k < 2 * tiles - 1)
        def _():
            fetch(wk + 1)

        def when(cond):
            return pl.when(going & cond)

        gate, upper = (u0 + 1, base + 1), (u0 + 2, base + 2)
        old, old_gate, old_upper = (p0, prev), (p0 + 1, prev + 1), (p0 + 2, prev + 2)

        def halves(j):
            def some(i):
                hidden(slot, j, i)

                @when((j == 0) & (i == 0))
                def _():
                    later(*old, 2)
                    later(*old_upper, 3)

                @pl.when((k == 0) & (j == 1) & (i == 0))
                def _():
                    third_low(*gate)

                @pl.when((k == 0) & (j == 1) & (i == 1))
                def _():
                    second_low(*upper)

            loop(blocks // 2, some)

            def wide_part(c):
                unit = (u0 + 1 + c, base + 1 + c)
                part = dot(AT[...], DGU[c, :, at(j, cols)]).astype(BF16)
                G[unit[1], :, at(j, hr), :] = part.reshape(n, dim // n, cols)

                @pl.when(j == 0)
                def _():
                    begin_low(*unit)

                @pl.when(j == 1)
                def _():
                    begin_high(*unit)

                @pl.when((j == 1) & (k == 0) & (c == 0))
                def _():
                    second_low(*gate)

                @when((j == 1) & (c == 1))
                def _():
                    later(*old, 3)
                    finish(*old_gate, 1, old_layer, old_t)
                    finish(*old_upper, 2, old_layer, old_t)
                    second_low(*gate)

                @pl.when((j == 1) & (k == 0) & (c == 1))
                def _():
                    third_low(*upper)

            loop(2, wide_part)

        loop(2, halves)

        def down_part(j):
            part = dot(DT[...], ACT[:, at(j, cols)])
            flipped = part.T.astype(BF16)
            for b in range(cols // LANES):
                G[base, j * (cols // LANES) + b] = flipped[b * LANES : (b + 1) * LANES]

            @pl.when(j == 0)
            def _():
                second_high(*gate)

        loop(2, down_part)

        @pl.when(k < end)
        def _():
            begin_low(u0, base)
            begin_high(u0, base)

        @when(k < end)
        def _():
            second_low(*upper)

        @pl.when(k == tiles - 1)
        def _():
            loop(blocks, lambda i: x_again(i).start())

        def ring_part(i):
            @pl.when(i == 0)
            def _():
                second_high(*upper)

            @pl.when((i == 0) & (k == 0))
            def _():
                second_low(u0, base)
                third_rest(*gate)

            @when(i == 2)
            def _():
                finish(*old, 0, old_layer, old_t)
                later(*gate, 2)

        @pl.when(k < tiles)
        def _():
            def input_part(i):
                so_far = jnp.where(k == 0, 0.0, DA[tok(i), :])
                DA[tok(i), :] = so_far + (dot_t(DGU[0, tok(i), :], WG[slot]) + dot_t(DGU[1, tok(i), :], WU[slot]))
                ring_part(i)

            loop(blocks, input_part)

        @pl.when((k >= tiles) & (k < end))
        def _():
            loop(blocks, ring_part)

        @pl.when(k == tiles - 1)
        def _():
            def between(i):
                h = H[tok(i), :].astype(F32)
                da = DA[tok(i), :].astype(BF16).astype(F32)
                r = scale_of(h)
                dh = (r * da - h * (r * r * r * jnp.mean(h * da, -1, keepdims=True))).astype(BF16)
                d = (D[tok(i), :].astype(F32) + dh.astype(F32)).astype(BF16)
                D[tok(i), :] = d
                DT[:, tok(i)] = d.T
                x_again(i).wait()
                wide = ACT[tok(i), pl.ds(0, dim)].astype(F32)
                a = (wide * scale_of(wide)).astype(BF16)
                A[tok(i), :] = a
                AT[:, tok(i)] = a.T

                @pl.when(i == 1)
                def _():
                    second_low(u0, base)
                    second_high(u0, base)

            loop(blocks, between)

        @when((k != tiles - 1) & (k < end))
        def _():
            second_low(u0, base)

        @pl.when((k != tiles - 1) & (k < end))
        def _():
            second_high(u0, base)

        @pl.when(k == 0)
        def _():
            third_rest(*upper)

        @when(k < end)
        def _():
            later(*upper, 2)

        @pl.when(k < end)
        def _():
            later(*gate, 3)

    loop(2 * tiles, tile_step)

    ahead = (
        pltpu.make_async_copy(wd_hbm.at[layers - 1, at(me, share), :], PW, ahead_sem.at[0]),
        pltpu.make_async_copy(md_hbm.at[layers - 1], PM, ahead_sem.at[1]),
        pltpu.make_async_copy(vd_hbm.at[layers - 1], PV, ahead_sem.at[2]),
    )
    for copy in ahead:
        copy.start()

    base = (end % 2) * 3
    down_unit, gate, upper = ((3 * end + j, base + j) for j in range(3))
    begin_high(*down_unit)
    second_high(*upper)
    begin_low(*down_unit)
    second_low(*upper)
    second_high(*down_unit)
    second_low(*down_unit)
    for step in range(2, half):
        for unit in (gate, upper, down_unit):
            later(*unit, step)
    finish(*gate, 1, 0, tiles - 1)
    finish(3 * (end - 1), 3 - base, 0, 0, tiles - 2)
    finish(*upper, 2, 0, tiles - 1)
    finish(*down_unit, 0, 0, tiles - 1)

    squares = SQ[:, :LANES]
    for j in range(1, dim // LANES):
        squares += SQ[:, j * LANES : (j + 1) * LANES]
    ALL[me] = squares

    def tell(d):
        return pltpu.make_async_remote_copy(
            src_ref=ALL.at[me],
            dst_ref=ALL.at[me],
            send_sem=sq_send.at[d],
            recv_sem=sq_recv.at[d],
            device_id={"dp": ring(d)},
            device_id_type=MESH,
        )

    for d in range(1, n):
        tell(d).start()
    for d in range(1, n):
        tell(d).wait()
    for copy in ahead:
        copy.wait()


def gradients(n, x, dy, w_gate, w_up, w_down, m_down, v_down):
    layers, dim, ff = w_gate.shape
    tokens = x.shape[1]
    blocks = 4
    share = ff // n
    tiles = share // LANES
    tile = n * LANES
    units = 3 * layers * tiles
    half = n // 2
    land = LANES // 2 + LANES * (half - 1)
    any_space = pl.BlockSpec(memory_space=pl.ANY)
    return pl.pallas_call(
        functools.partial(grad_kernel, n, layers, (tokens, dim, ff, blocks)),
        out_shape=tuple(
            kept(shape, dtype)
            for shape, dtype in (
                ((layers, dim // n, ff), BF16),
                ((layers, dim // n, ff), BF16),
                ((layers, share, dim), BF16),
                ((n, 8, LANES), F32),
                ((share, dim), BF16),
                ((share, dim), F32),
                ((share, dim), F32),
            )
        ),
        in_specs=[any_space] * 7,
        out_specs=(pl.BlockSpec(memory_space=pltpu.VMEM),) * 7,
        scratch_shapes=[
            pltpu.VMEM((tokens, dim), BF16),
            pltpu.VMEM((dim, tokens), BF16),
            pltpu.VMEM((tokens, dim), BF16),
            pltpu.VMEM((dim, tokens), BF16),
            pltpu.VMEM((tokens, dim), BF16),
            pltpu.VMEM((tokens, tile), BF16),
            pltpu.VMEM((2, tokens, tile), BF16),
            pltpu.VMEM((tokens, dim), F32),
            pltpu.VMEM((2, dim, tile), BF16),
            pltpu.VMEM((2, dim, tile), BF16),
            pltpu.VMEM((2, tile, dim), BF16),
            pltpu.VMEM((6, n, LANES, dim), BF16),
            pltpu.VMEM((units, land, dim), BF16),
            pltpu.VMEM((units, land, dim), BF16),
            pltpu.VMEM((8, dim), F32),
            pltpu.SemaphoreType.DMA((blocks,)),
            pltpu.SemaphoreType.DMA((blocks,)),
            pltpu.SemaphoreType.DMA((2, 3)),
            pltpu.SemaphoreType.DMA((3,)),
            pltpu.SemaphoreType.DMA((6, 2, half)),
            pltpu.SemaphoreType.DMA((units, 2, half)),
            pltpu.SemaphoreType.DMA((units,)),
            pltpu.SemaphoreType.DMA((n,)),
            pltpu.SemaphoreType.DMA((n,)),
        ],
        compiler_params=pltpu.CompilerParams(collective_id=0, has_side_effects=True, vmem_limit_bytes=62_500_000),
        name="grads",
    )(*(pinned(t, pltpu.HBM) for t in (x, dy, w_gate, w_up, w_down, m_down, v_down)))


def turns(layers):
    return [(2, l) for l in reversed(range(layers))] + [(a, l) for l in reversed(range(layers)) for a in (0, 1)]


def update_kernel(n, count, parts, *refs):
    G, w_hbm, m_hbm, v_hbm = (refs[i : i + 3] for i in (0, 4, 10, 13))
    SQ, PW, PM, PV = refs[3], *refs[7:10]
    N, M, V = (refs[i : i + 3] for i in (16, 19, 22))
    last = refs[25:27]
    W = refs[27:30]
    in_sem, last_sem, send_sem, recv_sem = refs[30:]
    me = lax.axis_index("dp")
    half = n // 2
    up, down = lax.rem(me + 1, n), lax.rem(me + n - 1, n)
    ring = lambda d: lax.rem(me + d + n, n)
    layers = G[0].shape[0]

    barrier = pltpu.get_barrier_semaphore()
    for peer in (up, down):
        pl.semaphore_signal(barrier, inc=1, device_id={"dp": peer}, device_id_type=MESH)

    order = turns(layers)
    loads = {}
    for a, l in order[1:]:
        rows = G[a].shape[1]
        own = pl.ds(pl.multiple_of(me * rows, rows), rows)
        loads[a, l] = (
            pltpu.make_async_copy(w_hbm[a].at[l, own, :], W[a].at[l], in_sem.at[0, a, l]),
            pltpu.make_async_copy(m_hbm[a].at[l], M[a].at[l], in_sem.at[1, a, l]),
            pltpu.make_async_copy(v_hbm[a].at[l], V[a].at[l], in_sem.at[2, a, l]),
        )
    total = jnp.sum(jnp.sum(SQ[...], axis=0), axis=(0, 1), keepdims=True)
    factor = jnp.minimum(1.0, 0.5 * lax.rsqrt(total / count + 1e-30))

    def shape(a):
        rows, cols = G[a].shape[1:]
        return (rows, cols // parts[a], 0) if a < 2 else (rows // parts[a], cols, 1)

    def place(a, l, p, owner, part):
        rows = G[a].shape[1]
        r, c, split = shape(a)
        hr = r // 2
        start = owner * rows + (p * r if split else 0)
        start, size = (start, r) if part == 2 else (start + part * hr, hr)
        return (l, pl.ds(pl.multiple_of(start, hr), size), pl.ds(0 if split else p * c, c))

    def send(i, a, l, p, way, step):
        owner = ring(-step) if way == 0 else ring(step)
        ref = N[a].at[place(a, l, p, owner, 2 if step < half - 1 else way)]
        return pltpu.make_async_remote_copy(
            src_ref=ref,
            dst_ref=ref,
            send_sem=send_sem.at[i, way, step],
            recv_sem=recv_sem.at[i, way, step],
            device_id={"dp": (up, down)[way]},
            device_id_type=MESH,
        )

    def came(i, a, l, p, way, step):
        owner = ring(-step - 1) if way == 0 else ring(step + 1)
        where = place(a, l, p, owner, 2 if step < half - 1 else way)
        ref = N[a].at[where]
        pltpu.make_async_copy(ref, ref, recv_sem.at[i, way, step]).wait()

    def adam(a, l, p):
        r, c, split = shape(a)
        rows = G[a].shape[1]
        step = 32
        lane = pl.ds(0 if split else p * c, c)

        def some(i):
            row = pl.ds(pl.multiple_of((p * r if split else 0) + i * step, step), step)
            old = (PW[row, lane], PM[row, lane], PV[row, lane]) if (a, l) == order[0] else (W[a][l, row, lane], M[a][l, row, lane], V[a][l, row, lane])
            g = G[a][l, row, lane].astype(F32) * factor
            m = 0.9 * old[1] + 0.1 * g
            v = 0.95 * old[2] + 0.05 * g * g
            M[a][l, row, lane] = m
            V[a][l, row, lane] = v
            w = old[0].astype(F32)
            new = (w - 0.02 * (m * lax.rsqrt(v + 1e-8) + 0.1 * w)).astype(BF16)
            there = pl.ds(pl.multiple_of(me * rows + (p * r if split else 0) + i * step, step), step)
            N[a][l, there, lane] = new

        loop(r // step, some)

    chunks = []
    for a, l in order:
        for p in range(parts[a]):
            chunks.append((len(chunks), a, l, p))
    for i, a, l, p in chunks:
        if p == 0:
            for copy in loads.get((a, l), ()):
                copy.wait()
        adam(a, l, p)
        if i == 0:
            pl.semaphore_wait(barrier, 2)
        send(i, a, l, p, 0, 0).start()
        send(i, a, l, p, 1, 0).start()
        if i == 0:
            for copies in loads.values():
                for copy in copies:
                    copy.start()
    late = order[len(order) - LATE :]

    def hops(a, l):
        return half - 1 if (a, l) in late else half

    def to_permute(a, l, way):
        rows = G[a].shape[1]
        owner = ring(1 - half) if way == 0 else ring(half - 1)
        src = N[a].at[l, pl.ds(pl.multiple_of(owner * rows + way * (rows // 2), rows // 2), rows // 2), :]
        return pltpu.make_async_copy(src, last[way].at[late.index((a, l))], last_sem.at[way, late.index((a, l))])

    for step in range(half):
        for i, a, l, p in chunks:
            for way in range(2):
                if step < hops(a, l):
                    came(i, a, l, p, way, step)
                if step < hops(a, l) - 1:
                    send(i, a, l, p, way, step + 1).start()
                elif step == half - 2 and p == parts[a] - 1:
                    to_permute(a, l, way).start()
    for i, a, l, p in chunks:
        for way in range(2):
            for step in range(hops(a, l)):
                send(i, a, l, p, way, step).wait_send()
    for a, l in late:
        for way in range(2):
            to_permute(a, l, way).wait()


def store_kernel(count, *refs):
    src, dst, sem = refs[:count], refs[count : 2 * count], refs[-1]
    copies = [pltpu.make_async_copy(a, b, sem.at[i]) for i, (a, b) in enumerate(zip(src, dst, strict=True))]
    for copy in copies:
        copy.start()
    for copy in copies:
        copy.wait()


def store(arrays):
    count = len(arrays)
    return pl.pallas_call(
        functools.partial(store_kernel, count),
        out_shape=tuple(jax.ShapeDtypeStruct(t.shape, t.dtype) for t in arrays),
        in_specs=[pl.BlockSpec(memory_space=pltpu.VMEM)] * count,
        out_specs=(pl.BlockSpec(memory_space=pl.ANY),) * count,
        scratch_shapes=[pltpu.SemaphoreType.DMA((count,))],
        compiler_params=pltpu.CompilerParams(vmem_limit_bytes=2**20),
        cost_estimate=pl.CostEstimate(flops=10_000_000_000, bytes_accessed=0, transcendentals=0),
        name="store",
    )(*(pinned(t, pltpu.VMEM) for t in arrays))


def place_kernel(n, count, *refs):
    up_ref, down_ref = refs[count : count + 2]
    outs, sem = refs[count + 2 : -1], refs[-1]
    opposite = lax.rem(lax.axis_index("dp") + n // 2, n)
    hr = up_ref.shape[1]
    copies = []
    for i, (a, l) in enumerate(turns(outs[0].shape[0])[-LATE:]):
        for way, src in enumerate((up_ref, down_ref)):
            there = pl.ds(pl.multiple_of(opposite * 2 * hr + way * hr, hr), hr)
            copies.append(pltpu.make_async_copy(src.at[i], outs[a].at[l, there, :], sem.at[i, way]))
    for copy in copies:
        copy.start()
    for copy in copies:
        copy.wait()


def place_last(n, arrays, came):
    count = len(arrays)
    any_space = pl.BlockSpec(memory_space=pl.ANY)
    in_vmem = pl.BlockSpec(memory_space=pltpu.VMEM)
    return pl.pallas_call(
        functools.partial(place_kernel, n, count),
        out_shape=tuple(jax.ShapeDtypeStruct(t.shape, t.dtype) for t in arrays),
        in_specs=[any_space] * count + [in_vmem] * 2,
        out_specs=(any_space,) * count,
        scratch_shapes=[pltpu.SemaphoreType.DMA((LATE, 2))],
        input_output_aliases={i: i for i in range(count)},
        compiler_params=pltpu.CompilerParams(vmem_limit_bytes=2**20),
        name="place",
    )(*(pinned(t, pltpu.HBM) for t in arrays), *came)


def update(n, made, w, m, v):
    layers = w[0].shape[0]
    parts = (2, 2, 4)
    chunks = layers * sum(parts)
    count = sum(t.size for t in w)
    any_space = pl.BlockSpec(memory_space=pl.ANY)
    in_vmem = pl.BlockSpec(memory_space=pltpu.VMEM)
    half = n // 2
    g, squares, ahead = made[:3], made[3], made[4:]
    return pl.pallas_call(
        functools.partial(update_kernel, n, float(count), parts),
        out_shape=tuple(kept(t.shape, BF16) for t in w)
        + tuple(kept(t.shape, F32) for t in m + v)
        + (jax.ShapeDtypeStruct((LATE, m[0].shape[1] // 2, m[0].shape[2]), BF16),) * 2,
        in_specs=[in_vmem] * 4 + [any_space] * 3 + [in_vmem] * 3 + [any_space] * 6,
        out_specs=(in_vmem,) * 9 + (any_space,) * 2,
        scratch_shapes=[pltpu.VMEM(t.shape, BF16) for t in m]
        + [
            pltpu.SemaphoreType.DMA((3, 3, layers)),
            pltpu.SemaphoreType.DMA((2, LATE)),
            pltpu.SemaphoreType.DMA((chunks, 2, half)),
            pltpu.SemaphoreType.DMA((chunks, 2, half)),
        ],
        compiler_params=pltpu.CompilerParams(collective_id=1, has_side_effects=True, vmem_limit_bytes=12 * 2**20),
        name="update",
    )(
        *(pinned(t, pltpu.VMEM) for t in (*g, squares)),
        *(pinned(t, pltpu.HBM) for t in w),
        *(pinned(t, pltpu.VMEM) for t in ahead),
        *(pinned(t, pltpu.HBM) for t in (*m, *v)),
    )


def solution(mesh):
    n = mesh.shape["dp"]

    def step(x, dy, *arrays):
        w, m, v = (arrays[i : i + 3] for i in (0, 3, 6))
        *new, up, down = update(n, gradients(n, x, dy, *w, m[2], v[2]), w, m, v)
        came = tuple(lax.ppermute(t, "dp", [(i, (i + d) % n) for i in range(n)]) for t, d in ((up, 1), (down, -1)))
        out = store(new)
        return (*place_last(n, out[:2], came), *out[2:])

    shard = P(None, "dp", None)
    return jax.shard_map(
        step,
        mesh=mesh,
        in_specs=(P(("rep", "dp"), None, None),) * 2 + (P(),) * 3 + (shard,) * 6,
        out_specs=(P("rep", None, None),) * 3 + (P("rep", "dp", None),) * 6,
        check_vma=False,
    )
```

```python
import functools

import jax
import jax.numpy as jnp
from jax import lax
from jax.experimental import pallas as pl
from jax.experimental.pallas import tpu as pltpu
from jax.sharding import PartitionSpec as P

F32 = jnp.float32
BF16 = jnp.bfloat16
MESH = pl.DeviceIdType.MESH
LANES = 128
LATE = 4


def dot(a, b):
    return jnp.dot(a, b, preferred_element_type=F32)


def dot_t(a, b):
    return lax.dot_general(a, b, (((1,), (1,)), ((), ())), preferred_element_type=F32)


def scale_of(wide):
    return lax.rsqrt(jnp.mean(wide * wide, -1, keepdims=True) + 1e-6)


def pinned(t, space):
    return pltpu.with_memory_space_constraint(t, space)


def kept(shape, dtype):
    return pltpu.VMEM(shape, dtype)


def loop(count, body):
    lax.fori_loop(0, count, lambda i, c: (body(i), c)[1], 0)


def at(i, size):
    return pl.ds(pl.multiple_of(i * size, size), size)


def grad_kernel(n, layers, shapes, *refs):
    (x_hbm, dy_hbm, wg_hbm, wu_hbm, wd_hbm, md_hbm, vd_hbm) = refs[:7]
    (OG, OU, OD, ALL, PW, PM, PV) = refs[7:14]
    (A, AT, D, DT, H, ACT, DG, DU, DA, WG, WU, WD, G, RU, RD, SQ, *sems) = refs[14:]
    x_sem, dy_sem, w_sem, ahead_sem, send_sem, recv_sem, low_sem, sq_send, sq_recv = sems
    tokens, dim, ff, blocks = shapes
    share = ff // n
    tiles = share // LANES
    tile = n * LANES
    tb = tokens // blocks
    half = n // 2
    hr = LANES // 2
    cols = tile // 2
    me = lax.axis_index("dp")
    up, down = lax.rem(me + 1, n), lax.rem(me + n - 1, n)
    ring = lambda d: lax.rem(me + d + n, n)

    def tok(i):
        return at(i, tb)

    def fetch(k):
        slot = lax.rem(k, 2)
        layer = lax.rem(k // tiles, 2)
        t = lax.rem(k, tiles)

        def one(b):
            place = pl.ds(pl.multiple_of(b * share + t * LANES, LANES), LANES)
            here = at(b, LANES)
            pltpu.make_async_copy(wg_hbm.at[layer, :, place], WG.at[slot, :, here], w_sem.at[slot, 0]).start()
            pltpu.make_async_copy(wu_hbm.at[layer, :, place], WU.at[slot, :, here], w_sem.at[slot, 1]).start()
            pltpu.make_async_copy(wd_hbm.at[layer, place, :], WD.at[slot, here, :], w_sem.at[slot, 2]).start()

        loop(n, one)

    def fetched(k):
        slot = lax.rem(k, 2)
        pltpu.make_async_copy(WG.at[slot], WG.at[slot], w_sem.at[slot, 0]).wait()
        pltpu.make_async_copy(WU.at[slot], WU.at[slot], w_sem.at[slot, 1]).wait()
        pltpu.make_async_copy(WD.at[slot], WD.at[slot], w_sem.at[slot, 2]).wait()

    def x_copy(i):
        return pltpu.make_async_copy(x_hbm.at[0, tok(i), :], H.at[tok(i), :], x_sem.at[i])

    def x_again(i):
        return pltpu.make_async_copy(x_hbm.at[0, tok(i), :], ACT.at[tok(i), pl.ds(0, dim)], x_sem.at[i])

    def dy_copy(i):
        return pltpu.make_async_copy(dy_hbm.at[0, tok(i), :], D.at[tok(i), :], dy_sem.at[i])

    x_copy(0).start()
    fetch(0)
    x_copy(1).start()
    barrier = pltpu.get_barrier_semaphore()
    for d in range(1, n):
        pl.semaphore_signal(barrier, inc=1, device_id={"dp": ring(d)}, device_id_type=MESH)

    def first_norm(i):
        wide = H[tok(i), :].astype(F32)
        A[tok(i), :] = (wide * scale_of(wide)).astype(BF16)
        DA[tok(i), :] = jnp.zeros((tb, dim), F32)

    def forward(k, i, act=ACT):
        slot = lax.rem(k, 2)
        for j in range(4):
            here = pl.ds(j * (tile // 4), tile // 4)
            g = dot(A[tok(i), :], WG[slot, :, here])
            u = dot(A[tok(i), :], WU[slot, :, here])
            s = 0.5 * jnp.tanh(0.5 * g) + 0.5
            act[tok(i), here] = (g * s * u).astype(BF16)
        DA[tok(i), :] += dot(act[tok(i), :], WD[slot])

    def second_norm(i):
        h = (H[tok(i), :].astype(F32) + DA[tok(i), :].astype(BF16).astype(F32)).astype(BF16)
        wide = h.astype(F32)
        return h, (wide * scale_of(wide)).astype(BF16)

    def second_norm_kept(i, h, a):
        H[tok(i), :] = h
        A[tok(i), :] = a
        AT[:, tok(i)] = a.T

    x_copy(0).wait()
    first_norm(0)
    fetched(0)
    loop(blocks - 2, lambda i: x_copy(i + 2).start())
    fetch(1)
    loop(blocks, lambda i: dy_copy(i).start())

    def opening(i):
        x_copy(i + 1).wait()
        forward(0, i)
        first_norm(i + 1)

    loop(blocks - 1, opening)

    def middle(j):
        q = blocks - 1 + 2 * j

        @pl.when(lax.rem(q + 1, blocks) == 0)
        def _():
            fetched((q + 1) // blocks)

        @pl.when((lax.rem(q, blocks) == 1) & (q // blocks < tiles - 1))
        def _():
            fetch(q // blocks + 1)

        seen = [jnp.minimum(2 * j + d, blocks - 1) for d in range(2)]

        @pl.when(2 * j < blocks)
        def _():
            dy_copy(2 * j).wait()
            dy_copy(2 * j + 1).wait()

        forward(q // blocks, lax.rem(q, blocks))
        forward((q + 1) // blocks, lax.rem(q + 1, blocks), DG)
        for i in seen:
            DT[:, tok(i)] = D[tok(i), :].T

    loop((tiles - 2) * blocks // 2 + 1, middle)
    fetch(tiles)

    def closing(i):
        normed = second_norm(i)
        forward(tiles - 1, i + 1)
        second_norm_kept(i, *normed)

    loop(blocks - 1, closing)

    def hidden(slot, j, i, pieces=1):
        size = 2 * tb // pieces
        for p, c in [(p, c) for p in range(pieces) for c in range(2)]:
            place = at(i * pieces + p, size)
            here = at(2 * j + c, cols // 2)
            g = dot(A[place, :], WG[slot, :, here])
            u = dot(A[place, :], WU[slot, :, here])
            back = dot_t(D[place, :], WD[slot, here, :]).astype(BF16).astype(F32)
            s = 0.5 * jnp.tanh(0.5 * g) + 0.5
            silu = g * s
            ACT[place, here] = (silu * u).astype(BF16)
            DU[place, here] = (back * silu).astype(BF16)
            DG[place, here] = (back * u * (s + silu * (1.0 - s))).astype(BF16)

    fetched(tiles)
    normed = second_norm(blocks - 1)
    hidden(tiles % 2, 0, 0, 2)
    second_norm_kept(blocks - 1, *normed)

    pl.semaphore_wait(barrier, n - 1)

    def remote(src, dst, slot, u, way, step, arrival=None):
        return pltpu.make_async_remote_copy(
            src_ref=src,
            dst_ref=dst,
            send_sem=send_sem.at[slot, way, step],
            recv_sem=recv_sem.at[u, way, step] if arrival is None else arrival,
            device_id={"dp": (up, down)[way]},
            device_id_type=MESH,
        )

    low, high, whole = pl.ds(0, hr), pl.ds(hr, hr), pl.ds(0, 2 * hr)
    lands = (RU, RD)

    def rows(step):
        return pl.ds(hr + (step - 1) * 2 * hr, 2 * hr)

    def begin_low(u, slot):
        remote(G.at[slot, ring(half), low], RU.at[u, low], slot, u, 0, 0).start()
        remote(G.at[slot, ring(1 - half), low], RD.at[u, pl.ds(hr, hr)], slot, u, 1, 1, low_sem.at[u]).start()

    def begin_high(u, slot):
        remote(G.at[slot, ring(half), high], RD.at[u, low], slot, u, 1, 0).start()
        remote(G.at[slot, ring(half - 1), high], RU.at[u, pl.ds(2 * hr, hr)], slot, u, 0, 1).start()

    def arrived(land, sem):
        pltpu.make_async_copy(land, land, sem).wait()

    def received(u, way, step):
        if (way, step) == (1, 1):
            arrived(RD.at[u, pl.ds(hr, hr)], low_sem.at[u])
            arrived(RD.at[u, pl.ds(2 * hr, hr)], recv_sem.at[u, 1, 1])
        else:
            arrived(lands[way].at[u, rows(step) if step else low], recv_sem.at[u, way, step])

    def add(land, place, mine):
        land[place] = (land[place].astype(F32) + mine.astype(F32)).astype(BF16)

    def second_low(u, slot):
        received(u, 0, 0)
        add(RU, (u, low), G[slot, ring(half - 1), low])
        remote(RU.at[u, low], RU.at[u, pl.ds(hr, hr)], slot, u, 0, 1).start()

    def second_high(u, slot):
        received(u, 1, 0)
        add(RD, (u, low), G[slot, ring(1 - half), high])
        remote(RD.at[u, low], RD.at[u, pl.ds(2 * hr, hr)], slot, u, 1, 1).start()

    def pass_on(u, slot, way, step):
        received(u, way, step - 1)
        add(lands[way], (u, rows(step - 1)), G[slot, ring(half - step if way == 0 else step - half)])
        remote(lands[way].at[u, rows(step - 1)], lands[way].at[u, rows(step)], slot, u, way, step).start()

    def later(u, slot, step):
        pass_on(u, slot, 0, step)
        pass_on(u, slot, 1, step)

    def half_on(u, slot, part, sem):
        here, there = pl.ds((1 + part) * hr, hr), pl.ds((3 + part) * hr, hr)
        arrived(RD.at[u, here], sem)
        add(RD, (u, here), G[slot, ring(2 - half), (low, high)[part]])
        remote(RD.at[u, here], RD.at[u, there], slot, u, 1, 2).start()

    def third_low(u, slot):
        half_on(u, slot, 0, low_sem.at[u])

    def third_rest(u, slot):
        pass_on(u, slot, 0, 2)
        half_on(u, slot, 1, recv_sem.at[u, 1, 1])

    def finish(u, slot, which, layer, t):
        received(u, 0, half - 1)
        received(u, 1, half - 1)
        total = G[slot, me].astype(F32) + RU[u, rows(half - 1)].astype(F32) + RD[u, rows(half - 1)].astype(F32)
        total = total.astype(BF16)
        wide = total.astype(F32)
        SQ[...] += jnp.sum((wide * wide).reshape(-1, 8, dim), axis=0)
        if which == 0:
            OD[layer, at(t, LANES), :] = total
        else:
            out = (OG, OU)[which - 1]
            for b in range(n):
                piece = total[hr * (b // (n // 2)) : hr * (b // (n // 2)) + hr, LANES * (b % (n // 2)) : LANES * (b % (n // 2)) + LANES]
                out[layer, :, pl.ds(pl.multiple_of(b * share + t * LANES, LANES), LANES)] = piece
        for way in range(2):
            for step in range(half):
                src = G.at[slot, 0, whole] if step > 0 else G.at[slot, 0, low]
                pltpu.make_async_copy(src, src, send_sem.at[slot, way, step]).wait()

    SQ[...] = jnp.zeros_like(SQ)

    end = 2 * tiles - 1

    def tile_step(k):
        wk = k + tiles
        slot = lax.rem(wk, 2)
        base = lax.rem(k, 2) * 3
        prev = 3 - base
        u0 = 3 * k
        p0 = u0 - 3
        going = k >= 1
        old_t = lax.rem(k - 1 + tiles, tiles)
        old_layer = jnp.where(k - 1 < tiles, 1, 0)

        @pl.when(k > 0)
        def _():
            fetched(wk)

        @pl.when(k < 2 * tiles - 1)
        def _():
            fetch(wk + 1)

        def when(cond):
            return pl.when(going & cond)

        def wide_part(src, unit, j):
            part = dot(AT[...], src[:, at(j, cols)]).astype(BF16)
            G[base + unit, :, at(j, hr), :] = part.reshape(n, dim // n, cols)

        gate, upper = (u0 + 1, base + 1), (u0 + 2, base + 2)
        old, old_gate, old_upper = (p0, prev), (p0 + 1, prev + 1), (p0 + 2, prev + 2)

        def halves(j):
            def some(i):
                @pl.when((k > 0) | (j > 0) | (i > 0))
                def _():
                    hidden(slot, j, i)

                @when((j == 0) & (i == 0))
                def _():
                    later(*old, 2)
                    later(*old_upper, 3)

                @pl.when((k == 0) & (j == 1) & (i == 0))
                def _():
                    third_low(*gate)

                @pl.when((k == 0) & (j == 1) & (i == 1))
                def _():
                    second_low(*upper)

            loop(blocks // 2, some)
            wide_part(DG, 1, j)

            @pl.when(j == 0)
            def _():
                begin_low(*gate)

            @pl.when(j == 1)
            def _():
                begin_high(*gate)

            @pl.when((j == 1) & (k == 0))
            def _():
                second_low(*gate)

            wide_part(DU, 2, j)

            @pl.when(j == 0)
            def _():
                begin_low(*upper)

            @pl.when(j == 1)
            def _():
                begin_high(*upper)

            @when(j == 1)
            def _():
                later(*old, 3)
                finish(*old_gate, 1, old_layer, old_t)
                finish(*old_upper, 2, old_layer, old_t)
                second_low(*gate)

            @pl.when((j == 1) & (k == 0))
            def _():
                third_low(*upper)

        loop(2, halves)

        def down_part(j):
            part = dot(DT[...], ACT[:, at(j, cols)])
            flipped = part.T.astype(BF16)
            for b in range(cols // LANES):
                G[base, j * (cols // LANES) + b] = flipped[b * LANES : (b + 1) * LANES]

            @pl.when(j == 0)
            def _():
                second_high(*gate)

        loop(2, down_part)

        @pl.when(k < end)
        def _():
            begin_low(u0, base)
            begin_high(u0, base)

        @when(k < end)
        def _():
            second_low(*upper)

        @pl.when(k == tiles - 1)
        def _():
            loop(blocks, lambda i: x_again(i).start())

        def ring_part(i):
            @pl.when(i == 0)
            def _():
                second_high(*upper)

            @pl.when((i == 0) & (k == 0))
            def _():
                second_low(u0, base)
                third_rest(*gate)

            @when(i == 2)
            def _():
                finish(*old, 0, old_layer, old_t)
                later(*gate, 2)

        @pl.when(k < tiles)
        def _():
            def input_part(i):
                so_far = jnp.where(k == 0, 0.0, DA[tok(i), :])
                DA[tok(i), :] = so_far + (dot_t(DG[tok(i), :], WG[slot]) + dot_t(DU[tok(i), :], WU[slot]))
                ring_part(i)

            loop(blocks, input_part)

        @pl.when((k >= tiles) & (k < end))
        def _():
            loop(blocks, ring_part)

        @pl.when(k == tiles - 1)
        def _():
            def between(i):
                h = H[tok(i), :].astype(F32)
                da = DA[tok(i), :].astype(BF16).astype(F32)
                r = scale_of(h)
                dh = (r * da - h * (r * r * r * jnp.mean(h * da, -1, keepdims=True))).astype(BF16)
                d = (D[tok(i), :].astype(F32) + dh.astype(F32)).astype(BF16)
                D[tok(i), :] = d
                DT[:, tok(i)] = d.T
                x_again(i).wait()
                wide = ACT[tok(i), pl.ds(0, dim)].astype(F32)
                a = (wide * scale_of(wide)).astype(BF16)
                A[tok(i), :] = a
                AT[:, tok(i)] = a.T

                @pl.when(i == 1)
                def _():
                    second_low(u0, base)
                    second_high(u0, base)

            loop(blocks, between)

        @when((k != tiles - 1) & (k < end))
        def _():
            second_low(u0, base)

        @pl.when((k != tiles - 1) & (k < end))
        def _():
            second_high(u0, base)

        @pl.when(k == 0)
        def _():
            third_rest(*upper)

        @when(k < end)
        def _():
            later(*upper, 2)

        @pl.when(k < end)
        def _():
            later(*gate, 3)

    loop(2 * tiles, tile_step)

    ahead = (
        pltpu.make_async_copy(wd_hbm.at[layers - 1, at(me, share), :], PW, ahead_sem.at[0]),
        pltpu.make_async_copy(md_hbm.at[layers - 1], PM, ahead_sem.at[1]),
        pltpu.make_async_copy(vd_hbm.at[layers - 1], PV, ahead_sem.at[2]),
    )
    for copy in ahead:
        copy.start()

    base = (end % 2) * 3
    down_unit, gate, upper = ((3 * end + j, base + j) for j in range(3))
    begin_high(*down_unit)
    second_high(*upper)
    begin_low(*down_unit)
    second_low(*upper)
    second_high(*down_unit)
    second_low(*down_unit)
    for step in range(2, half):
        for unit in (gate, upper, down_unit):
            later(*unit, step)
    finish(*gate, 1, 0, tiles - 1)
    finish(3 * (end - 1), 3 - base, 0, 0, tiles - 2)
    finish(*upper, 2, 0, tiles - 1)
    finish(*down_unit, 0, 0, tiles - 1)

    squares = SQ[:, :LANES]
    for j in range(1, dim // LANES):
        squares += SQ[:, j * LANES : (j + 1) * LANES]
    ALL[me] = squares

    def tell(d):
        return pltpu.make_async_remote_copy(
            src_ref=ALL.at[me],
            dst_ref=ALL.at[me],
            send_sem=sq_send.at[d],
            recv_sem=sq_recv.at[d],
            device_id={"dp": ring(d)},
            device_id_type=MESH,
        )

    order = sorted(range(1, n), key=lambda d: -min(d, n - d))
    for d in order:
        tell(d).start()
    for d in reversed(order):
        tell(d).wait()
    for copy in ahead:
        copy.wait()


def gradients(n, x, dy, w_gate, w_up, w_down, m_down, v_down):
    layers, dim, ff = w_gate.shape
    tokens = x.shape[1]
    blocks = 4
    share = ff // n
    tiles = share // LANES
    tile = n * LANES
    units = 3 * layers * tiles
    half = n // 2
    land = LANES // 2 + LANES * (half - 1)
    any_space = pl.BlockSpec(memory_space=pl.ANY)
    return pl.pallas_call(
        functools.partial(grad_kernel, n, layers, (tokens, dim, ff, blocks)),
        out_shape=tuple(
            kept(shape, dtype)
            for shape, dtype in (
                ((layers, dim // n, ff), BF16),
                ((layers, dim // n, ff), BF16),
                ((layers, share, dim), BF16),
                ((n, 8, LANES), F32),
                ((share, dim), BF16),
                ((share, dim), F32),
                ((share, dim), F32),
            )
        ),
        in_specs=[any_space] * 7,
        out_specs=(pl.BlockSpec(memory_space=pltpu.VMEM),) * 7,
        scratch_shapes=[
            pltpu.VMEM((tokens, dim), BF16),
            pltpu.VMEM((dim, tokens), BF16),
            pltpu.VMEM((tokens, dim), BF16),
            pltpu.VMEM((dim, tokens), BF16),
            pltpu.VMEM((tokens, dim), BF16),
            pltpu.VMEM((tokens, tile), BF16),
            pltpu.VMEM((tokens, tile), BF16),
            pltpu.VMEM((tokens, tile), BF16),
            pltpu.VMEM((tokens, dim), F32),
            pltpu.VMEM((2, dim, tile), BF16),
            pltpu.VMEM((2, dim, tile), BF16),
            pltpu.VMEM((2, tile, dim), BF16),
            pltpu.VMEM((6, n, LANES, dim), BF16),
            pltpu.VMEM((units, land, dim), BF16),
            pltpu.VMEM((units, land, dim), BF16),
            pltpu.VMEM((8, dim), F32),
            pltpu.SemaphoreType.DMA((blocks,)),
            pltpu.SemaphoreType.DMA((blocks,)),
            pltpu.SemaphoreType.DMA((2, 3)),
            pltpu.SemaphoreType.DMA((3,)),
            pltpu.SemaphoreType.DMA((6, 2, half)),
            pltpu.SemaphoreType.DMA((units, 2, half)),
            pltpu.SemaphoreType.DMA((units,)),
            pltpu.SemaphoreType.DMA((n,)),
            pltpu.SemaphoreType.DMA((n,)),
        ],
        compiler_params=pltpu.CompilerParams(collective_id=0, has_side_effects=True, vmem_limit_bytes=62_500_000),
        name="grads",
    )(*(pinned(t, pltpu.HBM) for t in (x, dy, w_gate, w_up, w_down, m_down, v_down)))


def turns(layers):
    return [(2, l) for l in reversed(range(layers))] + [(a, l) for l in reversed(range(layers)) for a in (0, 1)]


def update_kernel(n, count, parts, *refs):
    G, w_hbm, m_hbm, v_hbm = (refs[i : i + 3] for i in (0, 4, 10, 13))
    SQ, PW, PM, PV = refs[3], *refs[7:10]
    N, M, V = (refs[i : i + 3] for i in (16, 19, 22))
    last = refs[25:27]
    W = refs[27:30]
    in_sem, last_sem, send_sem, recv_sem = refs[30:]
    me = lax.axis_index("dp")
    half = n // 2
    up, down = lax.rem(me + 1, n), lax.rem(me + n - 1, n)
    ring = lambda d: lax.rem(me + d + n, n)
    layers = G[0].shape[0]

    barrier = pltpu.get_barrier_semaphore()
    for peer in (up, down):
        pl.semaphore_signal(barrier, inc=1, device_id={"dp": peer}, device_id_type=MESH)

    order = turns(layers)
    loads = {}
    for a, l in order[1:]:
        rows = G[a].shape[1]
        own = pl.ds(pl.multiple_of(me * rows, rows), rows)
        loads[a, l] = (
            pltpu.make_async_copy(w_hbm[a].at[l, own, :], W[a].at[l], in_sem.at[0, a, l]),
            pltpu.make_async_copy(m_hbm[a].at[l], M[a].at[l], in_sem.at[1, a, l]),
            pltpu.make_async_copy(v_hbm[a].at[l], V[a].at[l], in_sem.at[2, a, l]),
        )
    total = jnp.sum(jnp.sum(SQ[...], axis=0), axis=(0, 1), keepdims=True)
    factor = jnp.minimum(1.0, 0.5 * lax.rsqrt(total / count + 1e-30))

    def shape(a):
        rows, cols = G[a].shape[1:]
        return (rows, cols // parts, 0) if a < 2 else (rows // parts, cols, 1)

    def place(a, l, p, owner, part):
        rows = G[a].shape[1]
        r, c, split = shape(a)
        hr = r // 2
        start = owner * rows + (p * r if split else 0)
        start, size = (start, r) if part == 2 else (start + part * hr, hr)
        return (l, pl.ds(pl.multiple_of(start, hr), size), pl.ds(0 if split else p * c, c))

    def send(i, a, l, p, way, step):
        owner = ring(-step) if way == 0 else ring(step)
        ref = N[a].at[place(a, l, p, owner, 2 if step < half - 1 else way)]
        return pltpu.make_async_remote_copy(
            src_ref=ref,
            dst_ref=ref,
            send_sem=send_sem.at[i, way, step],
            recv_sem=recv_sem.at[i, way, step],
            device_id={"dp": (up, down)[way]},
            device_id_type=MESH,
        )

    def came(i, a, l, p, way, step):
        owner = ring(-step - 1) if way == 0 else ring(step + 1)
        where = place(a, l, p, owner, 2 if step < half - 1 else way)
        ref = N[a].at[where]
        pltpu.make_async_copy(ref, ref, recv_sem.at[i, way, step]).wait()

    def adam(a, l, p):
        r, c, split = shape(a)
        rows = G[a].shape[1]
        step = 32
        lane = pl.ds(0 if split else p * c, c)

        def some(i):
            row = pl.ds(pl.multiple_of((p * r if split else 0) + i * step, step), step)
            old = (PW[row, lane], PM[row, lane], PV[row, lane]) if (a, l) == order[0] else (W[a][l, row, lane], M[a][l, row, lane], V[a][l, row, lane])
            g = G[a][l, row, lane].astype(F32) * factor
            m = 0.9 * old[1] + 0.1 * g
            v = 0.95 * old[2] + 0.05 * g * g
            M[a][l, row, lane] = m
            V[a][l, row, lane] = v
            w = old[0].astype(F32)
            new = (w - 0.02 * (m * lax.rsqrt(v + 1e-8) + 0.1 * w)).astype(BF16)
            there = pl.ds(pl.multiple_of(me * rows + (p * r if split else 0) + i * step, step), step)
            N[a][l, there, lane] = new

        loop(r // step, some)

    chunks = []
    for a, l in order:
        for p in range(parts):
            chunks.append((len(chunks), a, l, p))
    for i, a, l, p in chunks:
        if p == 0:
            for copy in loads.get((a, l), ()):
                copy.wait()
        adam(a, l, p)
        if i == 0:
            pl.semaphore_wait(barrier, 2)
        send(i, a, l, p, 0, 0).start()
        send(i, a, l, p, 1, 0).start()
        if i == 0:
            for copies in loads.values():
                for copy in copies:
                    copy.start()
    late = order[len(order) - LATE :]

    def hops(a, l):
        return half - 1 if (a, l) in late else half

    def to_permute(a, l, way):
        rows = G[a].shape[1]
        owner = ring(1 - half) if way == 0 else ring(half - 1)
        src = N[a].at[l, pl.ds(pl.multiple_of(owner * rows + way * (rows // 2), rows // 2), rows // 2), :]
        return pltpu.make_async_copy(src, last[way].at[late.index((a, l))], last_sem.at[way, late.index((a, l))])

    for step in range(half):
        for i, a, l, p in chunks:
            for way in range(2):
                if step < hops(a, l):
                    came(i, a, l, p, way, step)
                if step < hops(a, l) - 1:
                    send(i, a, l, p, way, step + 1).start()
                elif step == half - 2 and p == parts - 1:
                    to_permute(a, l, way).start()
    for i, a, l, p in chunks:
        for way in range(2):
            for step in range(hops(a, l)):
                send(i, a, l, p, way, step).wait_send()
    for a, l in late:
        for way in range(2):
            to_permute(a, l, way).wait()


def store_kernel(count, *refs):
    src, dst, sem = refs[:count], refs[count : 2 * count], refs[-1]
    copies = [
        pltpu.make_async_copy(a.at[l], b.at[l], sem.at[i, l])
        for i, (a, b) in enumerate(zip(src, dst, strict=True))
        for l in range(a.shape[0])
    ]
    for copy in copies:
        copy.start()
    for copy in copies:
        copy.wait()


def store(arrays):
    count = len(arrays)
    return pl.pallas_call(
        functools.partial(store_kernel, count),
        out_shape=tuple(jax.ShapeDtypeStruct(t.shape, t.dtype) for t in arrays),
        in_specs=[pl.BlockSpec(memory_space=pltpu.VMEM)] * count,
        out_specs=(pl.BlockSpec(memory_space=pl.ANY),) * count,
        scratch_shapes=[pltpu.SemaphoreType.DMA((count, arrays[0].shape[0]))],
        compiler_params=pltpu.CompilerParams(vmem_limit_bytes=2**20),
        cost_estimate=pl.CostEstimate(flops=10_000_000_000, bytes_accessed=0, transcendentals=0),
        name="store",
    )(*(pinned(t, pltpu.VMEM) for t in arrays))


def place_kernel(n, count, *refs):
    up_ref, down_ref = refs[count : count + 2]
    outs, sem = refs[count + 2 : -1], refs[-1]
    opposite = lax.rem(lax.axis_index("dp") + n // 2, n)
    hr = up_ref.shape[1]
    copies = []
    for i, (a, l) in enumerate(turns(outs[0].shape[0])[-LATE:]):
        for way, src in enumerate((up_ref, down_ref)):
            there = pl.ds(pl.multiple_of(opposite * 2 * hr + way * hr, hr), hr)
            copies.append(pltpu.make_async_copy(src.at[i], outs[a].at[l, there, :], sem.at[i, way]))
    for copy in copies:
        copy.start()
    for copy in copies:
        copy.wait()


def place_last(n, arrays, came):
    count = len(arrays)
    any_space = pl.BlockSpec(memory_space=pl.ANY)
    in_vmem = pl.BlockSpec(memory_space=pltpu.VMEM)
    return pl.pallas_call(
        functools.partial(place_kernel, n, count),
        out_shape=tuple(jax.ShapeDtypeStruct(t.shape, t.dtype) for t in arrays),
        in_specs=[any_space] * count + [in_vmem] * 2,
        out_specs=(any_space,) * count,
        scratch_shapes=[pltpu.SemaphoreType.DMA((LATE, 2))],
        input_output_aliases={i: i for i in range(count)},
        compiler_params=pltpu.CompilerParams(vmem_limit_bytes=2**20),
        name="place",
    )(*(pinned(t, pltpu.HBM) for t in arrays), *came)


def update(n, made, w, m, v):
    layers = w[0].shape[0]
    parts = 2
    chunks = layers * 3 * parts
    count = sum(t.size for t in w)
    any_space = pl.BlockSpec(memory_space=pl.ANY)
    in_vmem = pl.BlockSpec(memory_space=pltpu.VMEM)
    half = n // 2
    g, squares, ahead = made[:3], made[3], made[4:]
    return pl.pallas_call(
        functools.partial(update_kernel, n, float(count), parts),
        out_shape=tuple(kept(t.shape, BF16) for t in w)
        + tuple(kept(t.shape, F32) for t in m + v)
        + (jax.ShapeDtypeStruct((LATE, m[0].shape[1] // 2, m[0].shape[2]), BF16),) * 2,
        in_specs=[in_vmem] * 4 + [any_space] * 3 + [in_vmem] * 3 + [any_space] * 6,
        out_specs=(in_vmem,) * 9 + (any_space,) * 2,
        scratch_shapes=[pltpu.VMEM(t.shape, BF16) for t in m]
        + [
            pltpu.SemaphoreType.DMA((3, 3, layers)),
            pltpu.SemaphoreType.DMA((2, LATE)),
            pltpu.SemaphoreType.DMA((chunks, 2, half)),
            pltpu.SemaphoreType.DMA((chunks, 2, half)),
        ],
        compiler_params=pltpu.CompilerParams(collective_id=1, has_side_effects=True, vmem_limit_bytes=12 * 2**20),
        name="update",
    )(
        *(pinned(t, pltpu.VMEM) for t in (*g, squares)),
        *(pinned(t, pltpu.HBM) for t in w),
        *(pinned(t, pltpu.VMEM) for t in ahead),
        *(pinned(t, pltpu.HBM) for t in (*m, *v)),
    )


def solution(mesh):
    n = mesh.shape["dp"]

    def step(x, dy, *arrays):
        w, m, v = (arrays[i : i + 3] for i in (0, 3, 6))
        *new, up, down = update(n, gradients(n, x, dy, *w, m[2], v[2]), w, m, v)
        came = tuple(lax.ppermute(t, "dp", [(i, (i + d) % n) for i in range(n)]) for t, d in ((up, 1), (down, -1)))
        out = store(new)
        return (*place_last(n, out[:2], came), *out[2:])

    shard = P(None, "dp", None)
    return jax.shard_map(
        step,
        mesh=mesh,
        in_specs=(P(("rep", "dp"), None, None),) * 2 + (P(),) * 3 + (shard,) * 6,
        out_specs=(P("rep", None, None),) * 3 + (P("rep", "dp", None),) * 6,
        check_vma=False,
    )
```
